32 devices in a mesh: dp: 4 (over z), ctx: 2 (over x), tp: 4 (over y, core).
Axes of the slice: x: 2, y: 2, z: 4, core: 2. Of those that a mesh axis runs over, the one named last changes fastest.
Arguments:
- tokens: bfloat16 [2, 4, 2048, 768], P(None, 'dp', ('ctx', 'tp')), may hold values from -6 to 6
- cotangent: bfloat16 [2, 4, 2048, 768], P(None, 'dp', ('ctx', 'tp')), may hold values from -6 to 6
- ln1_gain: bfloat16 [768], P(('dp', 'ctx')), may hold values from 0.5 to 1.5
- ln1_bias: bfloat16 [768], P(('dp', 'ctx')), may hold values from -1.25 to 1.25
- qkv_weight: bfloat16 [3, 768, 768], P(None, ('dp', 'ctx'), 'tp'), may hold values from -0.3125 to 0.3125
- qkv_bias: bfloat16 [3, 12, 64], P(None, 'tp', ('dp', 'ctx')), may hold values from -1.25 to 1.25
- out_weight: bfloat16 [768, 768], P('tp', ('dp', 'ctx')), may hold values from -1.5 to 1.5
- out_bias: bfloat16 [768], P(('dp', 'ctx')), may hold values from -1.25 to 1.25
- ln2_gain: bfloat16 [768], P(('dp', 'ctx')), may hold values from 0.5 to 1.5
- ln2_bias: bfloat16 [768], P(('dp', 'ctx')), may hold values from -1.25 to 1.25
- fc_weight: bfloat16 [768, 3072], P(('dp', 'ctx'), 'tp'), may hold values from -0.21875 to 0.21875
- fc_bias: bfloat16 [24, 128], P('tp', ('dp', 'ctx')), may hold values from -1.25 to 1.25
- proj_weight: bfloat16 [3072, 768], P('tp', ('dp', 'ctx')), may hold values from -0.21875 to 0.21875
- proj_bias: bfloat16 [768], P(('dp', 'ctx')), may hold values from -1.25 to 1.25
Outputs:
- activations: bfloat16 [2, 4, 2048, 768], P(None, 'dp', ('ctx', 'tp'))
- grad_tokens: float32 [2, 4, 2048, 768], P(None, 'dp', ('ctx', 'tp'))
- grad_ln1_gain: float32 [768], P(('dp', 'ctx'))
- grad_ln1_bias: float32 [768], P(('dp', 'ctx'))
- grad_qkv_weight: float32 [3, 768, 768], P(None, ('dp', 'ctx'), 'tp')
- grad_qkv_bias: float32 [3, 12, 64], P(None, 'tp', ('dp', 'ctx'))
- grad_out_weight: float32 [768, 768], P('tp', ('dp', 'ctx'))
- grad_out_bias: float32 [768], P(('dp', 'ctx'))
- grad_ln2_gain: float32 [768], P(('dp', 'ctx'))
- grad_ln2_bias: float32 [768], P(('dp', 'ctx'))
- grad_fc_weight: float32 [768, 3072], P(('dp', 'ctx'), 'tp')
- grad_fc_bias: float32 [24, 128], P('tp', ('dp', 'ctx'))
- grad_proj_weight: float32 [3072, 768], P('tp', ('dp', 'ctx'))
- grad_proj_bias: float32 [768], P(('dp', 'ctx'))
The draws below stay inside these ranges and needn't reach their ends.
All inputs are finite; a program needn't handle non-finite values.
Results may differ from the reference program's by a relative error of at most 0.013.
The reference program's roundings to bfloat16 on the way count: a program that leaves them out, or rounds other values in their place, can miss the bound.
Values may be sent and summed in bfloat16 or wider, within the bound.
No kernel may reach another device: no remote copies, remote signals or barrier semaphores. Data moves between devices by JAX's collectives and lax.ppermute only.
A program may use at most 128 MiB of HBM per device.

```python
import jax
import jax.numpy as jnp
from jax import lax

D = 768
HEADS = 12
HD = 64
FF = 3072
SEQ = 2048
MICRO = 2
SEQS = 4


def spiked(drawn, stream_key, source, target, shards_of, factor):
    owner, partner = [(jnp.arange(drawn.shape[axis_at]) // (drawn.shape[axis_at] // shards_of)).reshape([-1 if axis == axis_at else 1 for axis in range(drawn.ndim)]) for axis_at in (source, target)]
    chosen = jax.random.permutation(stream_key, shards_of)[partner]
    strong = (owner == chosen) | (owner == (partner + shards_of // 2) % shards_of)
    return jnp.where(strong, factor * drawn, drawn)


def shard_levels(own_key, extent, cuts, least, top_value):
    factor_of, own = 1.0, jax.random.fold_in(own_key, 6)
    for axis_at, parts in cuts:
        heights = jnp.exp(jax.random.uniform(jax.random.fold_in(own, axis_at), (parts,), jnp.float32, least / len(cuts), top_value / len(cuts)))
        factor_of = factor_of * jnp.repeat(heights, extent[axis_at] // parts).reshape([-1 if axis == axis_at else 1 for axis in range(len(extent))])
    return factor_of


def centred(own_key, dims, width, most, cuts=(), kind=jnp.bfloat16):
    entries = jax.random.normal(own_key, dims, jnp.float32) * width
    if len(cuts) > 0:
        entries = shard_levels(own_key, dims, cuts, -0.22, 0.18) * entries
    return jnp.clip(entries, min=-most, max=most).astype(kind)


def bell_draw_with(stream_key, shape, width, limit, cuts, heavy, kind=jnp.bfloat16):
    values = width * jax.random.normal(stream_key, shape, jnp.float32)
    if cuts:
        values = values * shard_levels(stream_key, shape, cuts, -0.22, 0.18)
    return jnp.clip(spiked(values, jax.random.fold_in(stream_key, 3), *heavy), -limit, limit).astype(kind)


def setup_inputs(seed: int = 0) -> dict:
    key_list = jax.random.split(jax.random.key(seed), 15)
    return {
        "tokens": bell_draw_with(key_list[0], (MICRO, SEQS, SEQ, D), 1.0, 6.0, ((1, 4), (2, 8)), (1, 3, 4, 2.0)),
        "cotangent": bell_draw_with(key_list[1], (MICRO, SEQS, SEQ, D), 1.0, 6.0, ((1, 4), (2, 8)), (1, 3, 4, 2.0)),
        "ln1_gain": jnp.clip(1.0 + 0.1 * jax.random.normal(key_list[2], (D,), jnp.float32), 0.5, 1.5).astype(jnp.bfloat16),
        "ln1_bias": centred(key_list[3], (D,), 0.2, 1.25, ((0, 8),)),
        "qkv_weight": centred(key_list[4], (3, D, D), (D // 2) ** -0.5, 0.3125, ((1, 8), (2, 4))),
        "qkv_bias": centred(key_list[5], (3, HEADS, HD), 0.2, 1.25, ((1, 4), (2, 8))),
        "out_weight": centred(key_list[6], (D, D), 16 ** -0.5, 1.5, ((0, 4), (1, 8))),
        "out_bias": centred(key_list[7], (D,), 0.2, 1.25, ((0, 8),)),
        "ln2_gain": jnp.clip(1.0 + 0.1 * jax.random.normal(key_list[8], (D,), jnp.float32), 0.5, 1.5).astype(jnp.bfloat16),
        "ln2_bias": centred(key_list[9], (D,), 0.2, 1.25, ((0, 8),)),
        "fc_weight": centred(key_list[10], (D, FF), D ** -0.5, 0.21875, ((0, 8), (1, 4))),
        "fc_bias": centred(key_list[11], (FF // 128, 128), 0.2, 1.25, ((0, 4), (1, 8))),
        "proj_weight": centred(key_list[12], (FF, D), (FF // 4) ** -0.5, 0.21875, ((0, 4), (1, 8))),
        "proj_bias": centred(key_list[13], (D,), 0.2, 1.25, ((0, 8),)),
    }


epsilon = 1e-05
highest = lax.Precision.HIGHEST

@jax.custom_vjp
def low(v):
    return lax.optimization_barrier(v.astype(jnp.bfloat16)).astype(jnp.float32)

@jax.custom_vjp
def low_back(v):
    return v

def low_keep(v):
    return (low(v), None)

def low_pass(kept, grad):
    return (grad,)

def back_keep(v):
    return (v, None)

def back_low(kept, grad):
    return (low(grad),)
low.defvjp(low_keep, low_pass)
low_back.defvjp(back_keep, back_low)

def layer_norm(rows, gain, shift):
    mean = lax.optimization_barrier(jnp.mean(rows, axis=-1, keepdims=True))
    centered = rows - mean
    spread = lax.optimization_barrier(jnp.mean(centered * centered, axis=-1, keepdims=True))
    return centered * lax.rsqrt(spread + epsilon) * gain + shift

def signed_block(query, keys, values, start, scale):
    scores = low_back(jnp.einsum('hqd,hkd->hqk', query, keys, precision=highest) * scale)
    row_pos = start + lax.broadcasted_iota(jnp.int32, (1, query.shape[1], 1), 1)
    key_pos = lax.broadcasted_iota(jnp.int32, (1, 1, keys.shape[1]), 2)
    allowed = key_pos <= row_pos
    masked = jnp.where(allowed, scores, 0.0)
    peak = lax.optimization_barrier(jnp.max(jnp.abs(masked), axis=2, keepdims=True))
    upper = jnp.where(allowed, jnp.exp(masked - peak), 0.0)
    lower = jnp.where(allowed, jnp.exp(-masked - peak), 0.0)
    total = 0.5 * lax.optimization_barrier(jnp.sum(upper + lower, axis=2, keepdims=True))
    weights = low(0.5 * (upper - lower) / total)
    return jnp.einsum('hqk,hkd->hqd', weights, values, precision=highest)

def forward(rows, parameters):
    gain_one, shift_one, joint_weight, joint_bias, out_weight, out_bias, gain_two, shift_two, fc_weight, fc_bias, proj_weight, proj_bias = parameters
    length = rows.shape[0]
    normed = low(layer_norm(rows, gain_one, shift_one))
    projected = jnp.einsum('rd,idc->irc', normed, joint_weight, precision=highest) + joint_bias[:, None, :]
    triple = low_back(low(projected))
    split = triple.reshape(3, length, HEADS, HD).transpose(0, 2, 1, 3)
    block = min(512, length)
    count = length // block
    query_blocks = split[0].reshape(HEADS, count, block, HD).transpose(1, 0, 2, 3)
    keys = split[1]
    values = split[2]

    def one(index):
        return signed_block(query_blocks[index], keys, values, index * block, HD ** (-0.5))
    mixed = lax.map(jax.checkpoint(one), jnp.arange(count, dtype=jnp.int32))
    mixed = low_back(low(mixed.transpose(0, 2, 1, 3).reshape(length, HEADS * HD)))
    branch = low_back(jnp.dot(mixed, out_weight, precision=highest) + out_bias)
    hidden = rows + branch
    normed_two = low(layer_norm(hidden, gain_two, shift_two))
    lifted = low_back(jnp.dot(normed_two, fc_weight, precision=highest) + fc_bias)
    activated = low(jax.nn.gelu(lifted, approximate=True))
    return hidden + jnp.dot(activated, proj_weight, precision=highest) + proj_bias

def reference(tokens, cotangent, ln1_gain, ln1_bias, qkv_weight, qkv_bias, out_weight, out_bias, ln2_gain, ln2_bias, fc_weight, fc_bias, proj_weight, proj_bias):
    wide = jnp.float32
    parameters = (ln1_gain.astype(wide), ln1_bias.astype(wide), qkv_weight.astype(wide), qkv_bias.astype(wide).reshape(3, D), out_weight.astype(wide), out_bias.astype(wide), ln2_gain.astype(wide), ln2_bias.astype(wide), fc_weight.astype(wide), fc_bias.astype(wide).reshape(FF), proj_weight.astype(wide), proj_bias.astype(wide))
    sequences = tokens.astype(wide).reshape(MICRO * SEQS, SEQ, D)
    returning = cotangent.astype(wide).reshape(MICRO * SEQS, SEQ, D)

    def one(totals, pair):
        rows, incoming = pair
        result, pull = jax.vjp(forward, rows, parameters)
        grad_rows, grad_parameters = pull(incoming)
        return (jax.tree.map(jnp.add, totals, grad_parameters), (result, grad_rows))
    totals, (results, grad_rows) = lax.scan(one, jax.tree.map(jnp.zeros_like, parameters), (sequences, returning))
    layout = (MICRO, SEQS, SEQ, D)
    outputs = results.reshape(layout).astype(jnp.bfloat16)
    return (outputs, grad_rows.reshape(layout), totals[0], totals[1], totals[2], totals[3].reshape(3, HEADS, HD), totals[4], totals[5], totals[6], totals[7], totals[8], totals[9].reshape(FF // 128, 128), totals[10], totals[11])
```

```python
import functools

import jax
import jax.numpy as jnp
from jax import lax
from jax.experimental import pallas as pl
from jax.experimental.pallas import tpu as pltpu
from jax.sharding import PartitionSpec as P

HD = 64
EPS = 1e-05
LOG2E = 1.4426950408889634
F32 = jnp.float32
BF16 = jnp.bfloat16
VMEM_LIMIT = 60 * 1024 * 1024
EXT = 64


def dot(a, b):
    return lax.dot_general(a, b, (((1,), (0,)), ((), ())), preferred_element_type=F32)


def dot_nt(a, b):
    return lax.dot_general(a, b, (((1,), (1,)), ((), ())), preferred_element_type=F32)


def norm_parts(rows):
    mean = jnp.mean(rows, axis=-1, keepdims=True)
    centered = rows - mean
    spread = jnp.mean(centered * centered, axis=-1, keepdims=True)
    scale = lax.rsqrt(spread + EPS)
    return (centered * scale, scale)


def norm_back(incoming, gain, n, scale):
    e = incoming * gain
    return (e - jnp.mean(e, axis=-1, keepdims=True) - n * jnp.mean(e * n, axis=-1, keepdims=True)) * scale


def params(steps=1):
    return pltpu.CompilerParams(
        dimension_semantics=("arbitrary",) * steps, vmem_limit_bytes=VMEM_LIMIT
    )


def cost(flops, moved, exps=0):
    return pl.CostEstimate(flops=int(flops), bytes_accessed=int(moved), transcendentals=int(exps))


def project_kernel(me_ref, own_ref, far_ref, w_ref, order_ref, out_ref, vec_ref, bias_ref):
    i = pl.program_id(0)
    width = out_ref.shape[2]

    @pl.when(i == 0)
    def _():
        turned = jnp.transpose(w_ref[:, 512:640].astype(F32))
        vec_ref[...] = turned[64:72]
        bias_ref[...] = dot(turned[64:72].astype(BF16), order_ref[...])

    far = ((i ^ me_ref[0]) & 1) == 1
    rows = jnp.where(far, far_ref[0], own_ref[0]).astype(F32)
    n, _ = norm_parts(rows)
    normed = (n * vec_ref[0:1] + vec_ref[1:2]).astype(BF16)
    full = dot(normed, w_ref[...])[:, : 3 * width] + bias_ref[2:3, :]
    full = full.astype(BF16)
    out_ref[0] = full[:, :width] * jnp.asarray(HD ** (-0.5), BF16)
    out_ref[1] = full[:, width : 2 * width]
    out_ref[2] = full[:, 2 * width :]


def project(me, own, far, w, order):
    half, rows, d = own.shape
    blocks = 2 * half
    width = order.shape[1] // 3
    return pl.pallas_call(
        project_kernel,
        out_shape=jax.ShapeDtypeStruct((3, blocks * rows, width), BF16),
        grid_spec=pltpu.PrefetchScalarGridSpec(
            num_scalar_prefetch=1,
            grid=(blocks,),
            in_specs=[
                pl.BlockSpec((1, rows, d), lambda i, me: ((i ^ me[0]) // 2, 0, 0)),
                pl.BlockSpec((1, rows, d), lambda i, me: ((i ^ me[0]) // 2, 0, 0)),
                pl.BlockSpec(w.shape, lambda i, me: (0, 0)),
                pl.BlockSpec(order.shape, lambda i, me: (0, 0)),
            ],
            out_specs=pl.BlockSpec((3, rows, width), lambda i, me: (0, i, 0)),
            scratch_shapes=[pltpu.VMEM((8, d), F32), pltpu.VMEM((8, 3 * width), F32)],
        ),
        compiler_params=params(),
        cost_estimate=cost(2 * blocks * rows * d * 3 * width, 8e6),
        name="project",
    )(me, own, far, w, order)


def head_mask(shape, h):
    lane = lax.broadcasted_iota(jnp.int32, shape, 1)
    return (lane >= h * HD) & (lane < (h + 1) * HD)


def attend_kernel(q_ref, k_ref, v_ref, o_ref, ot_ref, level_ref, vt_ref, qm_ref, m_ref, l_ref):
    i = pl.program_id(0)
    heads = q_ref.shape[2] // HD
    bq = q_ref.shape[1]
    half = bq // 2

    @pl.when(i == 0)
    def _():
        vt_ref[...] = jnp.transpose(v_ref[0].astype(F32)).astype(BF16)

    for h in range(heads):
        q = q_ref[0]
        qm_ref[h] = jnp.where(head_mask(q.shape, h), q, jnp.zeros_like(q))
    m_ref[...] = jnp.zeros_like(m_ref)
    l_ref[...] = jnp.zeros_like(l_ref)
    ot_ref[...] = jnp.zeros_like(ot_ref)

    def chunk(start, size, first, masked):
        cols = slice(first, bq)
        keys = k_ref[0, pl.ds(start, size), :]
        for h in range(heads):
            u = dot_nt(keys, qm_ref[h, first:bq, :]) * LOG2E
            if masked:
                key_pos = lax.broadcasted_iota(jnp.int32, u.shape, 0)
                row_pos = lax.broadcasted_iota(jnp.int32, u.shape, 1)
                allowed = key_pos <= row_pos
                u = jnp.where(allowed, u, 0.0)
            before = m_ref[h : h + 1, cols]
            peak = jnp.maximum(before, jnp.max(jnp.abs(u), axis=0, keepdims=True))
            fade = jnp.exp2(before - peak)
            upper = jnp.exp2(u - peak)
            lower = jnp.exp2(-peak - u)
            both = upper + lower
            if masked:
                both = jnp.where(allowed, both, 0.0)
            m_ref[h : h + 1, cols] = peak
            l_ref[h : h + 1, cols] = l_ref[h : h + 1, cols] * fade + jnp.sum(both, axis=0, keepdims=True)
            part = dot(vt_ref[h * HD : (h + 1) * HD, pl.ds(start, size)], (upper - lower).astype(BF16))
            ot_ref[h * HD : (h + 1) * HD, cols] = ot_ref[h * HD : (h + 1) * HD, cols] * fade + part

    def body(j, carry):
        chunk(pl.multiple_of(j * bq, bq), bq, 0, False)
        return carry

    lax.fori_loop(0, i, body, 0)
    base = pl.multiple_of(i * bq, bq)
    chunk(base, half, 0, True)
    chunk(pl.multiple_of(base + half, half), half, half, True)
    for h in range(heads):
        total = l_ref[h : h + 1, :]
        level_ref[h : h + 1, :] = m_ref[h : h + 1, :] + jnp.log2(total)
        ot_ref[h * HD : (h + 1) * HD, :] = ot_ref[h * HD : (h + 1) * HD, :] * (1.0 / total)
    o_ref[...] = jnp.transpose(ot_ref[...]).astype(BF16)


def attend(triple):
    _, span, width = triple.shape
    bq = min(512, span)
    heads = width // HD
    return pl.pallas_call(
        attend_kernel,
        out_shape=(
            jax.ShapeDtypeStruct((span, width), BF16),
            jax.ShapeDtypeStruct((width, span), F32),
            jax.ShapeDtypeStruct((8, span), F32),
        ),
        grid=(span // bq,),
        in_specs=[
            pl.BlockSpec((1, bq, width), lambda i: (0, i, 0)),
            pl.BlockSpec((1, span, width), lambda i: (1, 0, 0)),
            pl.BlockSpec((1, span, width), lambda i: (2, 0, 0)),
        ],
        out_specs=(
            pl.BlockSpec((bq, width), lambda i: (i, 0)),
            pl.BlockSpec((width, bq), lambda i: (0, i)),
            pl.BlockSpec((8, bq), lambda i: (0, i)),
        ),
        scratch_shapes=[
            pltpu.VMEM((width, span), BF16),
            pltpu.VMEM((heads, bq, width), BF16),
            pltpu.VMEM((8, bq), F32),
            pltpu.VMEM((8, bq), F32),
        ],
        compiler_params=params(),
        cost_estimate=cost(4 * span * span * width, 8e6, span * span * heads),
        name="attend",
    )(triple, triple, triple)


def attend_back_kernel(
    qkv_ref, grad_ref, ot_ref, level_ref, out_ref, qm_ref, gm_ref, kt_ref, dqt_ref, dot_ref, dk_ref, dv_ref
):
    j = pl.program_id(0)
    blocks = pl.num_programs(0)
    span, width = grad_ref.shape
    heads = width // HD
    count = qm_ref.shape[0]
    b = span // count
    half = b // 2

    @pl.when(j == 0)
    def _():
        turned = jnp.transpose(grad_ref[...].astype(F32))
        prod = turned * ot_ref[...]
        for h in range(heads):
            dot_ref[h : h + 1, :] = jnp.sum(prod[h * HD : (h + 1) * HD], axis=0, keepdims=True)
        kt_ref[...] = jnp.transpose(qkv_ref[1].astype(F32)).astype(BF16)
        dqt_ref[...] = jnp.zeros_like(dqt_ref)
        for n in range(count):
            q = qkv_ref[0, n * b : (n + 1) * b, :]
            g = grad_ref[n * b : (n + 1) * b, :]
            for h in range(heads):
                mask = head_mask(q.shape, h)
                qm_ref[n, h * b : (h + 1) * b, :] = jnp.where(mask, q, jnp.zeros_like(q))
                gm_ref[n, h * b : (h + 1) * b, :] = jnp.where(mask, g, jnp.zeros_like(g))

    dk_ref[...] = jnp.zeros_like(dk_ref)
    dv_ref[...] = jnp.zeros_like(dv_ref)

    def chunk(i, key_first, key_size, first, masked):
        start = pl.multiple_of(j * b + key_first, half)
        keys = qkv_ref[1, pl.ds(start, key_size), :]
        vals = qkv_ref[2, pl.ds(start, key_size), :]
        cols = b - first
        at = pl.multiple_of(i * b + first, half)
        for h in range(heads):
            lo = h * b + first
            qm = qm_ref[i, lo : lo + cols, :]
            gm = gm_ref[i, lo : lo + cols, :]
            level = level_ref[h : h + 1, pl.ds(at, cols)]
            inner = dot_ref[h : h + 1, pl.ds(at, cols)]
            u = dot_nt(keys, qm) * LOG2E
            upper = jnp.exp2(u - level)
            lower = jnp.exp2(-level - u)
            gw = dot_nt(vals, gm)
            weights = upper - lower
            gs = upper * (gw - inner) + lower * (gw + inner)
            if masked:
                key_pos = lax.broadcasted_iota(jnp.int32, u.shape, 0)
                row_pos = lax.broadcasted_iota(jnp.int32, u.shape, 1)
                allowed = key_pos <= row_pos
                weights = jnp.where(allowed, weights, 0.0)
                gs = jnp.where(allowed, gs, 0.0)
            weights = weights.astype(BF16)
            gs = gs.astype(BF16)
            rows = slice(key_first, key_first + key_size)
            dv_ref[rows, :] += dot(weights, gm)
            dk_ref[rows, :] += dot(gs, qm)
            dqt_ref[h * HD : (h + 1) * HD, pl.ds(at, cols)] += dot(
                kt_ref[h * HD : (h + 1) * HD, pl.ds(start, key_size)], gs
            )

    def body(i, carry):
        chunk(i, 0, b, 0, False)
        return carry

    chunk(j, 0, half, 0, True)
    chunk(j, half, half, half, True)
    lax.fori_loop(j + 1, blocks, body, 0)
    here = pl.ds(pl.multiple_of(j * b, b), b)
    out_ref[1, here, :] = dk_ref[...].astype(BF16)
    out_ref[2, here, :] = dv_ref[...].astype(BF16)

    @pl.when(j == blocks - 1)
    def _():
        out_ref[0] = jnp.transpose(dqt_ref[...] * (HD ** (-0.5))).astype(BF16)


def attend_back(triple, grad, ot, level):
    _, span, width = triple.shape
    b = min(512, span)
    count = span // b
    heads = width // HD
    whole = lambda *shape: pl.BlockSpec(shape, lambda j: (0,) * len(shape))
    return pl.pallas_call(
        attend_back_kernel,
        out_shape=jax.ShapeDtypeStruct(triple.shape, BF16),
        grid=(count,),
        in_specs=[
            whole(*triple.shape),
            whole(*grad.shape),
            whole(*ot.shape),
            whole(*level.shape),
        ],
        out_specs=whole(*triple.shape),
        scratch_shapes=[
            pltpu.VMEM((count, heads * b, width), BF16),
            pltpu.VMEM((count, heads * b, width), BF16),
            pltpu.VMEM((width, span), BF16),
            pltpu.VMEM((width, span), F32),
            pltpu.VMEM((8, span), F32),
            pltpu.VMEM((b, width), F32),
            pltpu.VMEM((b, width), F32),
        ],
        compiler_params=params(),
        cost_estimate=cost(10 * span * span * width, 1e7, span * span * heads),
        name="attend_back",
    )(triple, grad, ot, level)


def gelu_parts(u):
    c = 0.7978845608028654
    square = u * u
    th = jnp.tanh(c * u * (1.0 + 0.044715 * square))
    near = 0.5 * (1.0 + th)
    slope = near + (0.5 * c) * u * (1.0 - th * th) * (1.0 + (3.0 * 0.044715) * square)
    return (u * near, slope)


def middle_kernel(
    tok_ref,
    cot_ref,
    mix_ref,
    g_ref,
    gout_ref,
    order_ref,
    y_ref,
    gh_ref,
    dmix_ref,
    n2_ref,
    act_ref,
    gl_ref,
    gb_ref,
    vec_ref,
    gfb_ref,
    hid_ref,
    acc_ref,
    back_ref,
    ext_ref,
):
    t = pl.program_id(0)
    steps = pl.num_programs(0)
    half = mix_ref.shape[1]
    parts = gout_ref.shape[0]
    d = tok_ref.shape[1]
    width = mix_ref.shape[2]

    @pl.when(t == 0)
    def _():
        ext_ref[...] = jnp.transpose(gout_ref[0, :, 128:256].astype(F32))[64:72]
        total = tok_ref[...].astype(F32) + ext_ref[2:3]
        for s in range(parts):
            lhs = jnp.concatenate([mix_ref[s], mix_ref[parts + s]], axis=0)
            total = total + dot_nt(lhs, gout_ref[s, :, :width])
        hid_ref[...] = total
        n, _ = norm_parts(total)
        n2_ref[...] = (n * ext_ref[0:1] + ext_ref[1:2]).astype(BF16)
        acc_ref[...] = total + ext_ref[3:4]
        back_ref[...] = jnp.zeros_like(back_ref)

    ext = jnp.transpose(g_ref[0, :, 2 * d + 128 : 2 * d + 256].astype(F32))[64:72].astype(BF16)
    bias = dot(ext, order_ref[...])[4:5]
    fc = g_ref[0, :, :d]
    pj = g_ref[0, :, d : 2 * d]
    lifted = dot(n2_ref[...], fc) + bias
    act, slope = gelu_parts(lifted)
    act = act.astype(BF16)
    act_ref[0] = act
    gl32 = dot(cot_ref[...], pj) * slope
    gl = gl32.astype(BF16)
    gl_ref[0] = gl
    gfb_ref[0, 0:1, :] = jnp.sum(gl.astype(F32), axis=0, keepdims=True)
    acc_ref[...] += dot_nt(act, pj)
    back_ref[...] += dot_nt(gl, fc)

    @pl.when(t == steps - 1)
    def _():
        y_ref[...] = acc_ref[...].astype(BF16)
        n, scale = norm_parts(hid_ref[...])
        back = back_ref[...]
        cot = cot_ref[...].astype(F32)
        gh = cot + norm_back(back, ext_ref[0:1], n, scale)
        gh_ref[...] = gh
        gb = gh.astype(BF16)
        gb_ref[...] = gb
        vec_ref[0:1, :] = jnp.sum(back * n, axis=0, keepdims=True)
        vec_ref[1:2, :] = jnp.sum(back, axis=0, keepdims=True)
        vec_ref[2:3, :] = jnp.sum(gb.astype(F32), axis=0, keepdims=True)
        vec_ref[3:4, :] = jnp.sum(cot, axis=0, keepdims=True)
        vec_ref[4:8, :] = jnp.zeros((4, d), F32)
        for s in range(parts):
            dm = dot(gb, gout_ref[s, :, :width]).astype(BF16)
            dmix_ref[s] = dm[:half]
            dmix_ref[parts + s] = dm[half:]


def middle(tok, cot, mix, gathered, order):
    rows, d = tok.shape
    parts = gathered.shape[0]
    cols = gathered.shape[2]
    whole = lambda *shape: pl.BlockSpec(shape, lambda t: (0,) * len(shape))
    piece = lambda *shape: pl.BlockSpec(shape, lambda t: (t,) + (0,) * (len(shape) - 1))
    sds = jax.ShapeDtypeStruct
    return pl.pallas_call(
        middle_kernel,
        out_shape=(
            sds((rows, d), BF16),
            sds((rows, d), F32),
            sds(mix.shape, BF16),
            sds((rows, d), BF16),
            sds((parts, rows, d), BF16),
            sds((parts, rows, d), BF16),
            sds((rows, d), BF16),
            sds((8, d), F32),
            sds((parts, 8, d), F32),
        ),
        grid=(parts,),
        in_specs=[
            whole(rows, d),
            whole(rows, d),
            whole(*mix.shape),
            piece(1, d, cols),
            pl.BlockSpec((parts, d, 256), lambda t: (0, 0, cols // 256 - 1)),
            whole(*order.shape),
        ],
        out_specs=(
            whole(rows, d),
            whole(rows, d),
            whole(*mix.shape),
            whole(rows, d),
            piece(1, rows, d),
            piece(1, rows, d),
            whole(rows, d),
            whole(8, d),
            piece(1, 8, d),
        ),
        scratch_shapes=[
            pltpu.VMEM((rows, d), F32),
            pltpu.VMEM((rows, d), F32),
            pltpu.VMEM((rows, d), F32),
            pltpu.VMEM((8, d), F32),
        ],
        compiler_params=params(),
        cost_estimate=cost(2 * rows * d * d * 18, 3e7),
        name="middle",
    )(tok, cot, mix, gathered, gathered, order)


def weights_kernel(
    n2_ref, cot_ref, gb_ref, mix_ref, act_ref, gl_ref, vec_ref, gfb_ref, order_ref, out_ref, nt_ref, ct_ref, bt_ref
):
    t = pl.program_id(0)
    d = n2_ref.shape[1]
    width = mix_ref.shape[3]

    @pl.when(t == 0)
    def _():
        nt_ref[...] = jnp.transpose(n2_ref[...].astype(F32)).astype(BF16)
        ct_ref[...] = jnp.transpose(cot_ref[...].astype(F32)).astype(BF16)
        bt_ref[...] = jnp.transpose(gb_ref[...].astype(F32)).astype(BF16)

    out_ref[0, :, :d] = dot(nt_ref[...], gl_ref[0]).astype(BF16)
    out_ref[0, :, d : 2 * d] = dot(ct_ref[...], act_ref[0]).astype(BF16)
    mix = jnp.concatenate([mix_ref[0, 0], mix_ref[1, 0]], axis=0)
    out_ref[0, :, 2 * d : 2 * d + width] = dot(bt_ref[...], mix).astype(BF16)
    turned = dot_nt(gfb_ref[0].astype(BF16), order_ref[...])
    line = lax.broadcasted_iota(jnp.int32, turned.shape, 0)
    rows = jnp.where(line == 4, turned[0:1], vec_ref[...])
    tall = jnp.concatenate([rows, jnp.zeros((EXT - 8, d), F32)], axis=0)
    out_ref[0, :, 2 * d + width :] = jnp.transpose(tall).astype(BF16)


def weights(n2, cot, gb, mix, act, gl, vec, gfb, order):
    rows, d = n2.shape
    parts = act.shape[0]
    width = mix.shape[2]
    cols = 2 * d + width + EXT
    whole = lambda *shape: pl.BlockSpec(shape, lambda t: (0,) * len(shape))
    piece = lambda *shape: pl.BlockSpec(shape, lambda t: (t,) + (0,) * (len(shape) - 1))
    mix = mix.reshape(mix.shape[0] // parts, parts, mix.shape[1], width)
    return pl.pallas_call(
        weights_kernel,
        out_shape=jax.ShapeDtypeStruct((parts, d, cols), BF16),
        grid=(parts,),
        in_specs=[
            whole(rows, d),
            whole(rows, d),
            whole(rows, d),
            pl.BlockSpec((mix.shape[0], 1, mix.shape[2], width), lambda t: (0, t, 0, 0)),
            piece(1, rows, d),
            piece(1, rows, d),
            whole(8, d),
            piece(1, 8, d),
            whole(*order.shape),
        ],
        out_specs=piece(1, d, cols),
        scratch_shapes=[
            pltpu.VMEM((d, rows), BF16),
            pltpu.VMEM((d, rows), BF16),
            pltpu.VMEM((d, rows), BF16),
        ],
        compiler_params=params(),
        cost_estimate=cost(2 * rows * d * d * 9, 2.5e7),
        name="weights",
    )(n2, cot, gb, mix, act, gl, vec, gfb, order)


def project_back_kernel(
    me_ref, own_ref, far_ref, grad_ref, w_ref, keep_ref, send_ref, dw_ref, vec_ref, bias_ref, w3_ref, dw3_ref, gain_ref
):
    i = pl.program_id(0)
    steps = pl.num_programs(0)
    width = grad_ref.shape[2]

    @pl.when(i == 0)
    def _():
        gain_ref[...] = jnp.transpose(w_ref[:, 512:640].astype(F32))[64:72]
        for s in range(3):
            w3_ref[s] = w_ref[:, s * width : (s + 1) * width]
        dw3_ref[...] = jnp.zeros_like(dw3_ref)
        vec_ref[...] = jnp.zeros_like(vec_ref)
        bias_ref[...] = jnp.zeros_like(bias_ref)

    far = ((i ^ me_ref[0]) & 1) == 1
    rows = jnp.where(far, far_ref[0], own_ref[0]).astype(F32)
    n, _ = norm_parts(rows)
    normed = n * gain_ref[0:1] + gain_ref[1:2]
    turned = jnp.transpose(normed).astype(BF16)
    part = dot_nt(grad_ref[0], w3_ref[0])
    for s in range(1, 3):
        part = part + dot_nt(grad_ref[s], w3_ref[s])
    for s in range(3):
        dw3_ref[s] += dot(turned, grad_ref[s])
        bias_ref[s : s + 1, :] += jnp.sum(grad_ref[s].astype(F32), axis=0, keepdims=True)
    vec_ref[0:1, :] += jnp.sum(part * n, axis=0, keepdims=True)
    vec_ref[1:2, :] += jnp.sum(part, axis=0, keepdims=True)

    @pl.when(far)
    def _():
        send_ref[0] = part.astype(BF16)

    @pl.when(jnp.logical_not(far))
    def _():
        keep_ref[0] = part

    @pl.when(i == steps - 1)
    def _():
        dw_ref[...] = dw3_ref[...].astype(BF16)


def project_back(me, own, far, grad, w):
    half, rows, d = own.shape
    width = grad.shape[2]
    blocks = 2 * half
    sds = jax.ShapeDtypeStruct
    rel = lambda i, me: ((i ^ me[0]) // 2, 0, 0)
    return pl.pallas_call(
        project_back_kernel,
        out_shape=(
            sds((half, rows, d), F32),
            sds((half, rows, d), BF16),
            sds((3, d, width), BF16),
            sds((8, d), F32),
            sds((8, width), F32),
        ),
        grid_spec=pltpu.PrefetchScalarGridSpec(
            num_scalar_prefetch=1,
            grid=(blocks,),
            in_specs=[
                pl.BlockSpec((1, rows, d), rel),
                pl.BlockSpec((1, rows, d), rel),
                pl.BlockSpec((3, rows, width), lambda i, me: (0, i, 0)),
                pl.BlockSpec(w.shape, lambda i, me: (0, 0)),
            ],
            out_specs=(
                pl.BlockSpec((1, rows, d), rel),
                pl.BlockSpec((1, rows, d), rel),
                pl.BlockSpec((3, d, width), lambda i, me: (0, 0, 0)),
                pl.BlockSpec((8, d), lambda i, me: (0, 0)),
                pl.BlockSpec((8, width), lambda i, me: (0, 0)),
            ),
            scratch_shapes=[
                pltpu.VMEM((3, d, width), BF16),
                pltpu.VMEM((3, d, width), F32),
                pltpu.VMEM((8, d), F32),
            ],
        ),
        compiler_params=params(),
        cost_estimate=cost(4 * blocks * rows * d * 3 * width, 1.5e7),
        name="project_back",
    )(me, own, far, grad, w)


def one_hot_order(sources, targets, size, width):
    row = lax.broadcasted_iota(jnp.int32, (size, width), 0)
    return jnp.where(row == sources, 1.0, 0.0).astype(BF16)


def local(
    tokens,
    cotangent,
    ln1_gain,
    ln1_bias,
    qkv_weight,
    qkv_bias,
    out_weight,
    out_bias,
    ln2_gain,
    ln2_bias,
    fc_weight,
    fc_bias,
    proj_weight,
    proj_bias,
):
    sides = lax.axis_size("ctx")
    parts = lax.axis_size("tp")
    shards = lax.axis_size(("dp", "ctx"))
    group = sides * parts
    micro, _, rows, d = tokens.shape
    assert micro == sides == 2 and parts % 2 == 0
    side = lax.axis_index("ctx")
    me = side * parts + lax.axis_index("tp")
    me_array = jnp.full((1,), me, jnp.int32)
    tall = qkv_weight.shape[1]
    heads, piece = qkv_bias.shape[1], qkv_bias.shape[2]
    width = heads * HD
    lines, strip = fc_bias.shape

    def swap(array, mask):
        return lax.ppermute(array, ("ctx", "tp"), [(n, n ^ mask) for n in range(group)])

    tok = tokens[:, 0]
    cot = cotangent[:, 0]

    mine = lax.dynamic_index_in_dim(tok, side, 0, keepdims=False)
    other = lax.dynamic_index_in_dim(tok, 1 - side, 0, keepdims=False)
    blocks = []
    for mask in range(0, group, 2):
        block = other if mask >= parts else mine
        blocks.append(block if mask == 0 else swap(block, mask))
    own = jnp.stack(blocks)
    far = swap(own, 1)

    def column(values):
        return jnp.pad(values.reshape(-1, 1), ((0, tall - values.size), (0, 0)))

    narrow = jnp.concatenate(
        [
            qkv_weight.transpose(1, 0, 2).reshape(tall, 3 * width),
            column(ln1_gain),
            column(ln1_bias),
            column(qkv_bias),
            jnp.zeros((tall, EXT - 3), BF16),
        ],
        axis=1,
    )
    w_in = lax.all_to_all(
        jnp.broadcast_to(narrow[None], (shards,) + narrow.shape), ("dp", "ctx"), 0, 0, tiled=True
    ).reshape(d, 3 * width + EXT)

    wide = jnp.concatenate(
        [
            fc_weight,
            proj_weight.T,
            out_weight.T,
            column(ln2_gain),
            column(ln2_bias),
            column(out_bias),
            column(proj_bias),
            column(fc_bias),
            jnp.zeros((tall, EXT - 5), BF16),
        ],
        axis=1,
    )
    gathered = lax.all_gather(wide, ("tp", "dp", "ctx"), axis=0, tiled=True)
    gathered = gathered.reshape(parts, d, wide.shape[1])

    unit = lax.broadcasted_iota(jnp.int32, (1, 3 * width), 1)
    shard = unit % HD // piece
    order_in = one_hot_order(shard * tall + unit // HD * piece + unit % piece, None, d, 3 * width)
    unit = lax.broadcasted_iota(jnp.int32, (1, d), 1)
    shard = unit % 128 // strip
    order_fc = one_hot_order(shard * tall + unit // 128 * strip + unit % strip, None, d, d)

    triple = project(me_array, own, far, w_in, order_in)
    mixed, mixed_turned, level = attend(triple)
    mix = lax.all_to_all(mixed.reshape(group, rows, width), ("ctx", "tp"), 0, 0, tiled=True)

    tok_rows = tok.reshape(micro * rows, d)
    cot_rows = cot.reshape(micro * rows, d)
    y, grad_hidden, grad_mix, n2, act, gl, gb, vec, gfb = middle(
        tok_rows, cot_rows, mix, gathered, order_fc
    )
    grad_mix = lax.all_to_all(grad_mix, ("ctx", "tp"), 0, 0, tiled=True)
    grad_wide = weights(n2, cot_rows, gb, mix, act, gl, vec, gfb, order_fc)
    grad_wide = lax.psum_scatter(
        grad_wide.reshape(parts * d, wide.shape[1]), ("tp", "dp", "ctx"), scatter_dimension=0, tiled=True
    ).astype(F32)

    grad_triple = attend_back(triple, grad_mix.reshape(group * rows, width), mixed_turned, level)
    keep, send, grad_in, vec_in, bias_in = project_back(me_array, own, far, grad_triple, w_in)

    pair = keep + swap(send, 1).astype(F32)
    arrived = []
    for n, mask in enumerate(range(0, group, 2)):
        arrived.append(pair[n] if mask == 0 else swap(pair[n].astype(BF16), mask).astype(F32))
    near = sum(arrived[1 : parts // 2], arrived[0])
    away = sum(arrived[parts // 2 + 1 :], arrived[parts // 2])
    swapped = side == 1
    grad_normed = jnp.stack([jnp.where(swapped, away, near), jnp.where(swapped, near, away)])

    vec_in = vec_in[:2]
    mask = 1
    while mask < parts:
        vec_in = vec_in + swap(vec_in, mask)
        mask *= 2
    bias_cols = bias_in[:3].reshape(3, heads, shards, piece).transpose(2, 0, 1, 3).reshape(shards, 3 * heads * piece)
    bias_cols = jnp.pad(bias_cols, ((0, 0), (0, tall - 3 * heads * piece))).reshape(d, 1)
    narrow_grad = jnp.concatenate(
        [
            grad_in.transpose(1, 0, 2).reshape(d, 3 * width),
            vec_in.T.astype(BF16),
            bias_cols.astype(BF16),
            jnp.zeros((d, EXT - 3), BF16),
        ],
        axis=1,
    )
    narrow_grad = lax.all_to_all(
        narrow_grad.reshape(shards, tall, 3 * width + EXT), ("dp", "ctx"), 0, 0, tiled=True
    )
    narrow_grad = jnp.sum(narrow_grad.astype(F32), axis=0)

    n, scale = norm_parts(tok.astype(F32))
    gain = w_in[:, 3 * width].astype(F32)
    grad_tokens = grad_hidden.reshape(micro, rows, d) + norm_back(grad_normed, gain, n, scale)

    base = 3 * width
    grad_qkv_weight = narrow_grad[:, :base].reshape(tall, 3, width).transpose(1, 0, 2)
    grad_qkv_bias = narrow_grad[: 3 * heads * piece, base + 2].reshape(3, heads, piece)
    edge = 2 * d + width
    return (
        y.reshape(micro, 1, rows, d),
        grad_tokens[:, None],
        narrow_grad[:, base],
        narrow_grad[:, base + 1],
        grad_qkv_weight,
        grad_qkv_bias,
        grad_wide[:, 2 * d : edge].T,
        grad_wide[:, edge + 2],
        grad_wide[:, edge],
        grad_wide[:, edge + 1],
        grad_wide[:, :d],
        grad_wide[:, edge + 4].reshape(lines, strip),
        grad_wide[:, d : 2 * d].T,
        grad_wide[:, edge + 3],
    )


def solution(mesh):
    rows = P(None, "dp", ("ctx", "tp"), None)
    vector = P(("dp", "ctx"))
    joint = P(None, ("dp", "ctx"), "tp")
    joint_bias = P(None, "tp", ("dp", "ctx"))
    down = P("tp", ("dp", "ctx"))
    up = P(("dp", "ctx"), "tp")
    inner = (vector, vector, joint, joint_bias, down, vector, vector, vector, up, down, down, vector)
    return jax.shard_map(
        local,
        mesh=mesh,
        in_specs=(rows, rows) + inner,
        out_specs=(rows, rows) + inner,
        check_vma=False,
    )
```

```python
import functools

import jax
import jax.numpy as jnp
from jax import lax
from jax.experimental import pallas as pl
from jax.experimental.pallas import tpu as pltpu
from jax.sharding import PartitionSpec as P

HD = 64
EPS = 1e-05
LOG2E = 1.4426950408889634
F32 = jnp.float32
BF16 = jnp.bfloat16
VMEM_LIMIT = 60 * 1024 * 1024
EXT = 64


def dot(a, b):
    return lax.dot_general(a, b, (((1,), (0,)), ((), ())), preferred_element_type=F32)


def dot_nt(a, b):
    return lax.dot_general(a, b, (((1,), (1,)), ((), ())), preferred_element_type=F32)


def norm_parts(rows):
    mean = jnp.mean(rows, axis=-1, keepdims=True)
    centered = rows - mean
    spread = jnp.mean(centered * centered, axis=-1, keepdims=True)
    scale = lax.rsqrt(spread + EPS)
    return (centered * scale, scale)


def norm_back(incoming, gain, n, scale):
    e = incoming * gain
    return (e - jnp.mean(e, axis=-1, keepdims=True) - n * jnp.mean(e * n, axis=-1, keepdims=True)) * scale


def params(steps=1):
    return pltpu.CompilerParams(
        dimension_semantics=("arbitrary",) * steps, vmem_limit_bytes=VMEM_LIMIT
    )


def cost(flops, moved, exps=0):
    return pl.CostEstimate(flops=int(flops), bytes_accessed=int(moved), transcendentals=int(exps))


def pack_kernel(fc_ref, pj_ref, out_ref, qkv_ref, vec_ref, qb_ref, fb_ref, wide_ref, narrow_ref):
    tall, d = fc_ref.shape
    width = out_ref.shape[0]
    copies = narrow_ref.shape[0]
    columns = jnp.transpose(vec_ref[...].astype(F32)).astype(BF16)
    wide_ref[:, :d] = fc_ref[...]
    wide_ref[:, d : 2 * d] = jnp.transpose(pj_ref[...].astype(F32)).astype(BF16)
    wide_ref[:, 2 * d : 2 * d + width] = jnp.transpose(out_ref[...].astype(F32)).astype(BF16)
    edge = 2 * d + width
    wide_ref[:, edge:] = jnp.zeros((tall, EXT), BF16)
    wide_ref[:, edge : edge + 4] = columns[:, 2:6]
    rows, strip = fb_ref.shape
    wide_ref[:rows, edge + 8 : edge + 8 + strip] = fb_ref[...]
    for s in range(3):
        narrow_ref[0, :, s * width : (s + 1) * width] = qkv_ref[s]
    edge = 3 * width
    narrow_ref[0, :, edge:] = jnp.zeros((tall, EXT), BF16)
    narrow_ref[0, :, edge : edge + 2] = columns[:, :2]
    heads, piece = qb_ref.shape[1:]
    for s in range(3):
        narrow_ref[0, s * heads : (s + 1) * heads, edge + 8 : edge + 8 + piece] = qb_ref[s]
    whole = narrow_ref[0]
    for n in range(1, copies):
        narrow_ref[n] = whole


def pack(fc, pj, out, qkv, vec, qb, fb, copies):
    tall, d = fc.shape
    width = out.shape[0]
    return pl.pallas_call(
        pack_kernel,
        out_shape=(
            jax.ShapeDtypeStruct((tall, 2 * d + width + EXT), BF16),
            jax.ShapeDtypeStruct((copies, tall, 3 * width + EXT), BF16),
        ),
        compiler_params=pltpu.CompilerParams(vmem_limit_bytes=VMEM_LIMIT),
        cost_estimate=cost(0, 2e6),
        name="pack",
    )(fc, pj, out, qkv, vec, qb, fb)


def pick_rows(table, period):
    line = lax.broadcasted_iota(jnp.int32, table.shape, 0)
    lane = lax.broadcasted_iota(jnp.int32, table.shape, 1)
    return jnp.sum(jnp.where(line == (lane & (period - 1)), table, 0.0), axis=0, keepdims=True)


def spread_rows(row, lines, period):
    shape = (lines, row.shape[1])
    line = lax.broadcasted_iota(jnp.int32, shape, 0)
    lane = lax.broadcasted_iota(jnp.int32, shape, 1)
    return jnp.where(line == (lane & (period - 1)), jnp.broadcast_to(row, shape), 0.0).astype(BF16)


def project_kernel(piece, me_ref, own_ref, far_ref, w_ref, order_ref, out_ref, vec_ref, bias_ref):
    i = pl.program_id(0)
    width = out_ref.shape[2]

    @pl.when(i == 0)
    def _():
        turned = jnp.transpose(w_ref[:, 512:640].astype(F32))
        vec_ref[...] = turned[64:72]
        table = dot(turned[72:80].astype(BF16), order_ref[...])
        bias_ref[...] = jnp.broadcast_to(pick_rows(table, piece), bias_ref.shape)

    far = ((i ^ me_ref[0]) & 1) == 1
    rows = jnp.where(far, far_ref[0], own_ref[0]).astype(F32)
    n, _ = norm_parts(rows)
    normed = (n * vec_ref[0:1] + vec_ref[1:2]).astype(BF16)
    full = dot(normed, w_ref[...])[:, : 3 * width] + bias_ref[0:1, :]
    full = full.astype(BF16)
    out_ref[0] = full[:, :width] * jnp.asarray(HD ** (-0.5), BF16)
    out_ref[1] = full[:, width : 2 * width]
    out_ref[2] = full[:, 2 * width :]


def project(me, own, far, w, order, piece):
    half, rows, d = own.shape
    blocks = 2 * half
    width = order.shape[1] // 3
    return pl.pallas_call(
        functools.partial(project_kernel, piece),
        out_shape=jax.ShapeDtypeStruct((3, blocks * rows, width), BF16),
        grid_spec=pltpu.PrefetchScalarGridSpec(
            num_scalar_prefetch=1,
            grid=(blocks,),
            in_specs=[
                pl.BlockSpec((1, rows, d), lambda i, me: ((i ^ me[0]) // 2, 0, 0)),
                pl.BlockSpec((1, rows, d), lambda i, me: ((i ^ me[0]) // 2, 0, 0)),
                pl.BlockSpec(w.shape, lambda i, me: (0, 0)),
                pl.BlockSpec(order.shape, lambda i, me: (0, 0)),
            ],
            out_specs=pl.BlockSpec((3, rows, width), lambda i, me: (0, i, 0)),
            scratch_shapes=[pltpu.VMEM((8, d), F32), pltpu.VMEM((8, 3 * width), F32)],
        ),
        compiler_params=params(),
        cost_estimate=cost(2 * blocks * rows * d * 3 * width, 8e6),
        name="project",
    )(me, own, far, w, order)


def head_mask(shape, h):
    lane = lax.broadcasted_iota(jnp.int32, shape, 1)
    return (lane >= h * HD) & (lane < (h + 1) * HD)


def attend_kernel(q_ref, k_ref, v_ref, o_ref, ot_ref, level_ref, vt_ref, qm_ref, m_ref, l_ref):
    i = pl.program_id(0)
    heads = q_ref.shape[2] // HD
    bq = q_ref.shape[1]
    half = bq // 2

    @pl.when(i == 0)
    def _():
        vt_ref[...] = jnp.transpose(v_ref[0].astype(F32)).astype(BF16)

    for h in range(heads):
        q = q_ref[0]
        qm_ref[h] = jnp.where(head_mask(q.shape, h), q, jnp.zeros_like(q))
    m_ref[...] = jnp.zeros_like(m_ref)
    l_ref[...] = jnp.zeros_like(l_ref)
    ot_ref[...] = jnp.zeros_like(ot_ref)

    def chunk(start, size, first, masked):
        cols = slice(first, bq)
        keys = k_ref[0, pl.ds(start, size), :]
        for h in range(heads):
            u = dot_nt(keys, qm_ref[h, first:bq, :]) * LOG2E
            if masked:
                key_pos = lax.broadcasted_iota(jnp.int32, u.shape, 0)
                row_pos = lax.broadcasted_iota(jnp.int32, u.shape, 1)
                allowed = key_pos <= row_pos
                u = jnp.where(allowed, u, 0.0)
            before = m_ref[h : h + 1, cols]
            peak = jnp.maximum(before, jnp.max(jnp.abs(u), axis=0, keepdims=True))
            fade = jnp.exp2(before - peak)
            upper = jnp.exp2(u - peak)
            lower = jnp.exp2(-peak - u)
            both = upper + lower
            if masked:
                both = jnp.where(allowed, both, 0.0)
            m_ref[h : h + 1, cols] = peak
            l_ref[h : h + 1, cols] = l_ref[h : h + 1, cols] * fade + jnp.sum(both, axis=0, keepdims=True)
            part = dot(vt_ref[h * HD : (h + 1) * HD, pl.ds(start, size)], (upper - lower).astype(BF16))
            ot_ref[h * HD : (h + 1) * HD, cols] = ot_ref[h * HD : (h + 1) * HD, cols] * fade + part

    def body(j, carry):
        chunk(pl.multiple_of(j * bq, bq), bq, 0, False)
        return carry

    lax.fori_loop(0, i, body, 0)
    base = pl.multiple_of(i * bq, bq)
    chunk(base, half, 0, True)
    chunk(pl.multiple_of(base + half, half), half, half, True)
    for h in range(heads):
        total = l_ref[h : h + 1, :]
        level_ref[h : h + 1, :] = m_ref[h : h + 1, :] + jnp.log2(total)
        ot_ref[h * HD : (h + 1) * HD, :] = ot_ref[h * HD : (h + 1) * HD, :] * (1.0 / total)
    rows = o_ref.shape[2]
    for n in range(bq // rows):
        o_ref[n] = ot_ref[:, n * rows : (n + 1) * rows].astype(BF16)


def attend(triple, rows):
    _, span, width = triple.shape
    bq = min(512, span)
    heads = width // HD
    return pl.pallas_call(
        attend_kernel,
        out_shape=(
            jax.ShapeDtypeStruct((span // rows, width, rows), BF16),
            jax.ShapeDtypeStruct((width, span), F32),
            jax.ShapeDtypeStruct((8, span), F32),
        ),
        grid=(span // bq,),
        in_specs=[
            pl.BlockSpec((1, bq, width), lambda i: (0, i, 0)),
            pl.BlockSpec((1, span, width), lambda i: (1, 0, 0)),
            pl.BlockSpec((1, span, width), lambda i: (2, 0, 0)),
        ],
        out_specs=(
            pl.BlockSpec((bq // rows, width, rows), lambda i: (i, 0, 0)),
            pl.BlockSpec((width, bq), lambda i: (0, i)),
            pl.BlockSpec((8, bq), lambda i: (0, i)),
        ),
        scratch_shapes=[
            pltpu.VMEM((width, span), BF16),
            pltpu.VMEM((heads, bq, width), BF16),
            pltpu.VMEM((8, bq), F32),
            pltpu.VMEM((8, bq), F32),
        ],
        compiler_params=params(),
        cost_estimate=cost(4 * span * span * width, 8e6, span * span * heads),
        name="attend",
    )(triple, triple, triple)


def attend_back_kernel(
    qkv_ref, grad_ref, ot_ref, level_ref, out_ref, qm_ref, gm_ref, kt_ref, dqt_ref, dot_ref, dk_ref, dv_ref
):
    j = pl.program_id(0)
    blocks = pl.num_programs(0)
    span, width = qkv_ref.shape[1:]
    rows = grad_ref.shape[2]
    heads = width // HD
    count = qm_ref.shape[0]
    b = span // count
    half = b // 2

    @pl.when(j == 0)
    def _():
        for n in range(span // rows):
            cols = slice(n * rows, (n + 1) * rows)
            turned = grad_ref[n].astype(F32)
            prod = turned * ot_ref[:, cols]
            for h in range(heads):
                dot_ref[h : h + 1, cols] = jnp.sum(prod[h * HD : (h + 1) * HD], axis=0, keepdims=True)
            g = jnp.transpose(turned).astype(BF16)
            at = n * rows % b
            for h in range(heads):
                mask = head_mask(g.shape, h)
                gm_ref[n * rows // b, h * b + at : h * b + at + rows, :] = jnp.where(mask, g, jnp.zeros_like(g))
        kt_ref[...] = jnp.transpose(qkv_ref[1].astype(F32)).astype(BF16)
        dqt_ref[...] = jnp.zeros_like(dqt_ref)
        for n in range(count):
            q = qkv_ref[0, n * b : (n + 1) * b, :]
            for h in range(heads):
                mask = head_mask(q.shape, h)
                qm_ref[n, h * b : (h + 1) * b, :] = jnp.where(mask, q, jnp.zeros_like(q))

    dk_ref[...] = jnp.zeros_like(dk_ref)
    dv_ref[...] = jnp.zeros_like(dv_ref)

    def chunk(i, key_first, key_size, first, masked):
        start = pl.multiple_of(j * b + key_first, half)
        keys = qkv_ref[1, pl.ds(start, key_size), :]
        vals = qkv_ref[2, pl.ds(start, key_size), :]
        cols = b - first
        at = pl.multiple_of(i * b + first, half)
        for h in range(heads):
            lo = h * b + first
            qm = qm_ref[i, lo : lo + cols, :]
            gm = gm_ref[i, lo : lo + cols, :]
            level = level_ref[h : h + 1, pl.ds(at, cols)]
            inner = dot_ref[h : h + 1, pl.ds(at, cols)]
            u = dot_nt(keys, qm) * LOG2E
            upper = jnp.exp2(u - level)
            lower = jnp.exp2(-level - u)
            gw = dot_nt(vals, gm)
            weights = upper - lower
            gs = upper * (gw - inner) + lower * (gw + inner)
            if masked:
                key_pos = lax.broadcasted_iota(jnp.int32, u.shape, 0)
                row_pos = lax.broadcasted_iota(jnp.int32, u.shape, 1)
                allowed = key_pos <= row_pos
                weights = jnp.where(allowed, weights, 0.0)
                gs = jnp.where(allowed, gs, 0.0)
            weights = weights.astype(BF16)
            gs = gs.astype(BF16)
            rows = slice(key_first, key_first + key_size)
            dv_ref[rows, :] += dot(weights, gm)
            dk_ref[rows, :] += dot(gs, qm)
            dqt_ref[h * HD : (h + 1) * HD, pl.ds(at, cols)] += dot(
                kt_ref[h * HD : (h + 1) * HD, pl.ds(start, key_size)], gs
            )

    def body(i, carry):
        chunk(i, 0, b, 0, False)
        return carry

    chunk(j, 0, half, 0, True)
    chunk(j, half, half, half, True)
    lax.fori_loop(j + 1, blocks, body, 0)
    here = pl.ds(pl.multiple_of(j * b, b), b)
    out_ref[1, here, :] = dk_ref[...].astype(BF16)
    out_ref[2, here, :] = dv_ref[...].astype(BF16)

    @pl.when(j == blocks - 1)
    def _():
        out_ref[0] = jnp.transpose(dqt_ref[...] * (HD ** (-0.5))).astype(BF16)


def attend_back(triple, grad, ot, level):
    _, span, width = triple.shape
    b = min(512, span)
    count = span // b
    heads = width // HD
    whole = lambda *shape: pl.BlockSpec(shape, lambda j: (0,) * len(shape))
    return pl.pallas_call(
        attend_back_kernel,
        out_shape=jax.ShapeDtypeStruct(triple.shape, BF16),
        grid=(count,),
        in_specs=[
            whole(*triple.shape),
            whole(*grad.shape),
            whole(*ot.shape),
            whole(*level.shape),
        ],
        out_specs=whole(*triple.shape),
        scratch_shapes=[
            pltpu.VMEM((count, heads * b, width), BF16),
            pltpu.VMEM((count, heads * b, width), BF16),
            pltpu.VMEM((width, span), BF16),
            pltpu.VMEM((width, span), F32),
            pltpu.VMEM((8, span), F32),
            pltpu.VMEM((b, width), F32),
            pltpu.VMEM((b, width), F32),
        ],
        compiler_params=params(),
        cost_estimate=cost(10 * span * span * width, 1e7, span * span * heads),
        name="attend_back",
    )(triple, grad, ot, level)


def gelu_parts(u):
    c = 0.7978845608028654
    square = u * u
    th = jnp.tanh(c * u * (1.0 + 0.044715 * square))
    near = 0.5 * (1.0 + th)
    slope = near + (0.5 * c) * u * (1.0 - th * th) * (1.0 + (3.0 * 0.044715) * square)
    return (u * near, slope)


def middle_kernel(
    strip,
    tok_ref,
    cot_ref,
    mix_ref,
    g_ref,
    gout_ref,
    order_ref,
    y_ref,
    gh_ref,
    dmix_ref,
    n2_ref,
    act_ref,
    gl_ref,
    gb_ref,
    vec_ref,
    gfb_ref,
    hid_ref,
    acc_ref,
    back_ref,
    ext_ref,
):
    t = pl.program_id(0)
    steps = pl.num_programs(0)
    half = mix_ref.shape[2]
    parts = gout_ref.shape[0]
    d = tok_ref.shape[1]
    width = mix_ref.shape[1]

    @pl.when(t == 0)
    def _():
        ext_ref[...] = jnp.transpose(gout_ref[0, :, 128:256].astype(F32))[64:72]
        total = tok_ref[...].astype(F32) + ext_ref[2:3]
        for s in range(parts):
            lhs = jnp.concatenate([mix_ref[s], mix_ref[parts + s]], axis=1)
            lhs = jnp.transpose(lhs.astype(F32)).astype(BF16)
            total = total + dot_nt(lhs, gout_ref[s, :, :width])
        hid_ref[...] = total
        n, _ = norm_parts(total)
        n2_ref[...] = (n * ext_ref[0:1] + ext_ref[1:2]).astype(BF16)
        acc_ref[...] = total + ext_ref[3:4]
        back_ref[...] = jnp.zeros_like(back_ref)

    ext = jnp.transpose(g_ref[0, :, 2 * d + 128 : 2 * d + 256].astype(F32))[72:88].astype(BF16)
    bias = pick_rows(dot(ext, order_ref[...]), strip)
    fc = g_ref[0, :, :d]
    pj = g_ref[0, :, d : 2 * d]
    lifted = dot(n2_ref[...], fc) + bias
    act, slope = gelu_parts(lifted)
    act = act.astype(BF16)
    act_ref[0] = act
    gl32 = dot(cot_ref[...], pj) * slope
    gl = gl32.astype(BF16)
    gl_ref[0] = gl
    gfb_ref[0, 0:1, :] = jnp.sum(gl.astype(F32), axis=0, keepdims=True)
    acc_ref[...] += dot_nt(act, pj)
    back_ref[...] += dot_nt(gl, fc)

    @pl.when(t == steps - 1)
    def _():
        y_ref[...] = acc_ref[...].astype(BF16)
        n, scale = norm_parts(hid_ref[...])
        back = back_ref[...]
        cot = cot_ref[...].astype(F32)
        gh = cot + norm_back(back, ext_ref[0:1], n, scale)
        gh_ref[...] = gh
        gb = gh.astype(BF16)
        gb_ref[...] = gb
        vec_ref[0:1, :] = jnp.sum(back * n, axis=0, keepdims=True)
        vec_ref[1:2, :] = jnp.sum(back, axis=0, keepdims=True)
        vec_ref[2:3, :] = jnp.sum(gb.astype(F32), axis=0, keepdims=True)
        vec_ref[3:4, :] = jnp.sum(cot, axis=0, keepdims=True)
        vec_ref[4:8, :] = jnp.zeros((4, d), F32)
        for s in range(parts):
            dm = jnp.transpose(dot(gb, gout_ref[s, :, :width])).astype(BF16)
            dmix_ref[s] = dm[:, :half]
            dmix_ref[parts + s] = dm[:, half:]


def middle(tok, cot, mix, gathered, order, strip):
    rows, d = tok.shape
    parts = gathered.shape[0]
    cols = gathered.shape[2]
    whole = lambda *shape: pl.BlockSpec(shape, lambda t: (0,) * len(shape))
    piece = lambda *shape: pl.BlockSpec(shape, lambda t: (t,) + (0,) * (len(shape) - 1))
    sds = jax.ShapeDtypeStruct
    return pl.pallas_call(
        functools.partial(middle_kernel, strip),
        out_shape=(
            sds((rows, d), BF16),
            sds((rows, d), F32),
            sds(mix.shape, BF16),
            sds((rows, d), BF16),
            sds((parts, rows, d), BF16),
            sds((parts, rows, d), BF16),
            sds((rows, d), BF16),
            sds((8, d), F32),
            sds((parts, 8, d), F32),
        ),
        grid=(parts,),
        in_specs=[
            whole(rows, d),
            whole(rows, d),
            whole(*mix.shape),
            piece(1, d, cols),
            pl.BlockSpec((parts, d, 256), lambda t: (0, 0, cols // 256 - 1)),
            whole(*order.shape),
        ],
        out_specs=(
            whole(rows, d),
            whole(rows, d),
            whole(*mix.shape),
            whole(rows, d),
            piece(1, rows, d),
            piece(1, rows, d),
            whole(rows, d),
            whole(8, d),
            piece(1, 8, d),
        ),
        scratch_shapes=[
            pltpu.VMEM((rows, d), F32),
            pltpu.VMEM((rows, d), F32),
            pltpu.VMEM((rows, d), F32),
            pltpu.VMEM((8, d), F32),
        ],
        compiler_params=params(),
        cost_estimate=cost(2 * rows * d * d * 18, 3e7),
        name="middle",
    )(tok, cot, mix, gathered, gathered, order)


def weights_kernel(
    mode, strip, index_ref, n2_ref, cot_ref, gb_ref, mix_ref, act_ref, gl_ref, vec_ref, gfb_ref, order_ref, *rest
):
    s = pl.program_id(0)
    d = n2_ref.shape[1]
    width = mix_ref.shape[2]
    cols = 2 * d + width + EXT
    nt_ref, ct_ref, bt_ref = rest[-3:]

    @pl.when(s == 0)
    def _():
        nt_ref[...] = jnp.transpose(n2_ref[...].astype(F32)).astype(BF16)
        ct_ref[...] = jnp.transpose(cot_ref[...].astype(F32)).astype(BF16)
        bt_ref[...] = jnp.transpose(gb_ref[...].astype(F32)).astype(BF16)

    mix = jnp.concatenate([mix_ref[0, 0], mix_ref[1, 0]], axis=1)
    turned = dot_nt(spread_rows(gfb_ref[0, 0:1], 16, strip), order_ref[...])
    tall = jnp.concatenate([vec_ref[...], turned, jnp.zeros((EXT - 24, d), F32)], axis=0)
    if mode != "keep":
        out_ref = rest[0]
        out_ref[0, :, :d] = dot(nt_ref[...], gl_ref[0]).astype(BF16)
        out_ref[0, :, d : 2 * d] = dot(ct_ref[...], act_ref[0]).astype(BF16)
        out_ref[0, :, 2 * d : 2 * d + width] = dot_nt(bt_ref[...], mix).astype(BF16)
        out_ref[0, :, 2 * d + width :] = jnp.transpose(tall).astype(BF16)
        return
    came_ref, as_ref, ak_ref, bs_ref, bk_ref, sum_ref = rest[:6]
    sum_ref[:, 2 * d : 2 * d + width] = dot_nt(bt_ref[...], mix).astype(BF16)
    sum_ref[:, 2 * d + width :] = jnp.transpose(tall).astype(BF16)
    sum_ref[:, 2 * d :] = (sum_ref[:, 2 * d :].astype(F32) + came_ref[0, :, 2 * d :].astype(F32)).astype(BF16)
    sum_ref[:, :d] = (dot(nt_ref[...], gl_ref[0]) + came_ref[0, :, :d].astype(F32)).astype(BF16)
    sum_ref[:, d : 2 * d] = (dot(ct_ref[...], act_ref[0]) + came_ref[0, :, d : 2 * d].astype(F32)).astype(BF16)
    depth, step = as_ref.shape[1], as_ref.shape[2]
    order = halving_order(depth)
    cut = cols // 2

    def block(xr, zr):
        at = ((order[zr] ^ index_ref[2]) * 2 + (xr ^ index_ref[3])) * step
        return pl.ds(pl.multiple_of(at, 16), step)

    for zr in range(depth):
        bk_ref[0, zr] = sum_ref[block(0, zr), cut:]
        bs_ref[0, zr] = sum_ref[block(1, zr), cut:]

    @pl.when(s == 0)
    def _():
        for xr in range(2):
            for zr in range(depth):
                as_ref[xr, zr] = sum_ref[block(xr, zr), :cut]

    @pl.when(s == 1)
    def _():
        for xr in range(2):
            for zr in range(depth):
                ak_ref[xr, zr] = sum_ref[block(xr, zr), :cut]


def halving_order(count):
    bits = count.bit_length() - 1
    return [int(format(n, "b").zfill(bits)[::-1], 2) if bits else 0 for n in range(count)]


def weights(mode, index, n2, cot, gb, mix, act, gl, vec, gfb, order, strip, came=None, shards=None):
    rows, d = n2.shape
    parts = act.shape[0]
    width = mix.shape[1]
    cols = 2 * d + width + EXT
    steps = parts if mode == "all" else 2
    whole = lambda *shape: pl.BlockSpec(shape, lambda s, ix: (0,) * len(shape))
    piece = lambda *shape: pl.BlockSpec(shape, lambda s, ix: (ix[s],) + (0,) * (len(shape) - 1))
    mix = mix.reshape(mix.shape[0] // parts, parts, width, mix.shape[2])
    operands = [index, n2, cot, gb, mix, act, gl, vec, gfb, order]
    specs = [
        whole(rows, d),
        whole(rows, d),
        whole(rows, d),
        pl.BlockSpec((mix.shape[0], 1, width, mix.shape[3]), lambda s, ix: (0, ix[s], 0, 0)),
        piece(1, rows, d),
        piece(1, rows, d),
        whole(8, d),
        piece(1, 8, d),
        whole(*order.shape),
    ]
    scratch = [pltpu.VMEM((d, rows), BF16) for _ in range(3)]
    if mode == "keep":
        operands.append(came)
        specs.append(pl.BlockSpec((1, d, cols), lambda s, ix: (s, 0, 0)))
        block = (2, shards // 2, d // shards, cols // 2)
        sds = jax.ShapeDtypeStruct(block, BF16)
        out_shape = (sds,) * 4
        turn = pl.BlockSpec((1,) + block[1:], lambda s, ix: (1 - s, 0, 0, 0))
        out_specs = (whole(*block), whole(*block), turn, turn)
        scratch = [pltpu.VMEM((d, cols), BF16)] + scratch
    else:
        out_shape = jax.ShapeDtypeStruct((steps, d, cols), BF16)
        out_specs = pl.BlockSpec((1, d, cols), lambda s, ix: (s, 0, 0))
    return pl.pallas_call(
        functools.partial(weights_kernel, mode, strip),
        out_shape=out_shape,
        grid_spec=pltpu.PrefetchScalarGridSpec(
            num_scalar_prefetch=1,
            grid=(steps,),
            in_specs=specs,
            out_specs=out_specs,
            scratch_shapes=scratch,
        ),
        compiler_params=params(),
        cost_estimate=cost(2 * rows * d * cols * steps, 6e6 * steps),
        name="weights_" + mode,
    )(*operands)


def finish_wide_kernel(ak_ref, ar_ref, bk_ref, br_ref, fc_ref, pj_ref, out_ref, g_ref, b_ref, ob_ref, pb_ref, fb_ref):
    tall, d = fc_ref.shape
    width = out_ref.shape[0]
    cut = ak_ref.shape[1]
    a = ak_ref[...].astype(F32) + ar_ref[...].astype(F32)
    b = bk_ref[...].astype(F32) + br_ref[...].astype(F32)
    fc_ref[...] = a[:, :d]
    pj_ref[: cut - d, :] = jnp.transpose(a[:, d:])
    pj_ref[cut - d :, :] = jnp.transpose(b[:, : 2 * d - cut])
    rest = jnp.transpose(b[:, 2 * d - cut :])
    out_ref[...] = rest[:width]
    g_ref[...] = rest[width : width + 1]
    b_ref[...] = rest[width + 1 : width + 2]
    ob_ref[...] = rest[width + 2 : width + 3]
    pb_ref[...] = rest[width + 3 : width + 4]
    rows, strip = fb_ref.shape
    at = 2 * d - cut + width + 8
    fb_ref[...] = b[:rows, at : at + strip]


def finish_wide(ak, ar, bk, br, d, width, bias_shape):
    tall = ak.shape[0]
    sds = lambda *shape: jax.ShapeDtypeStruct(shape, F32)
    return pl.pallas_call(
        finish_wide_kernel,
        out_shape=(
            sds(tall, d),
            sds(d, tall),
            sds(width, tall),
            sds(1, tall),
            sds(1, tall),
            sds(1, tall),
            sds(1, tall),
            sds(*bias_shape),
        ),
        compiler_params=pltpu.CompilerParams(vmem_limit_bytes=VMEM_LIMIT),
        cost_estimate=cost(0, 2e6),
        name="finish_wide",
    )(ak, ar, bk, br)


def project_back_kernel(
    piece, me_ref, own_ref, far_ref, grad_ref, w_ref, order_ref, keep_ref, send_ref, dw_ref, w3_ref, dw3_ref, gain_ref, vec_ref, bias_ref
):
    i = pl.program_id(0)
    steps = pl.num_programs(0)
    width = grad_ref.shape[2]
    d = w_ref.shape[0]

    @pl.when(i == 0)
    def _():
        gain_ref[...] = jnp.transpose(w_ref[:, 512:640].astype(F32))[64:72]
        for s in range(3):
            w3_ref[s] = w_ref[:, s * width : (s + 1) * width]
        dw3_ref[...] = jnp.zeros_like(dw3_ref)
        vec_ref[...] = jnp.zeros_like(vec_ref)
        bias_ref[...] = jnp.zeros_like(bias_ref)

    far = ((i ^ me_ref[0]) & 1) == 1
    rows = jnp.where(far, far_ref[0], own_ref[0]).astype(F32)
    n, _ = norm_parts(rows)
    normed = n * gain_ref[0:1] + gain_ref[1:2]
    turned = jnp.transpose(normed).astype(BF16)
    part = dot_nt(grad_ref[0], w3_ref[0])
    for s in range(1, 3):
        part = part + dot_nt(grad_ref[s], w3_ref[s])
    for s in range(3):
        dw3_ref[s] += dot(turned, grad_ref[s])
        bias_ref[s : s + 1, :] += jnp.sum(grad_ref[s].astype(F32), axis=0, keepdims=True)
    vec_ref[0:1, :] += jnp.sum(part * n, axis=0, keepdims=True)
    vec_ref[1:2, :] += jnp.sum(part, axis=0, keepdims=True)

    @pl.when(far)
    def _():
        send_ref[0] = part.astype(BF16)

    @pl.when(jnp.logical_not(far))
    def _():
        keep_ref[0] = part

    @pl.when(i == steps - 1)
    def _():
        turned_bias = jnp.zeros((8, d), F32)
        for s in range(3):
            dw_ref[:, s * width : (s + 1) * width] = dw3_ref[s].astype(BF16)
            spread = spread_rows(bias_ref[s : s + 1, :], 8, piece)
            turned_bias = turned_bias + dot_nt(spread, order_ref[s])
        tall = jnp.concatenate([vec_ref[...], turned_bias, jnp.zeros((EXT - 16, d), F32)], axis=0)
        dw_ref[:, 3 * width :] = jnp.transpose(tall).astype(BF16)


def project_back(me, own, far, grad, w, order, piece):
    half, rows, d = own.shape
    width = grad.shape[2]
    blocks = 2 * half
    sds = jax.ShapeDtypeStruct
    rel = lambda i, me: ((i ^ me[0]) // 2, 0, 0)
    return pl.pallas_call(
        functools.partial(project_back_kernel, piece),
        out_shape=(
            sds((half, rows, d), F32),
            sds((half, rows, d), BF16),
            sds(w.shape, BF16),
        ),
        grid_spec=pltpu.PrefetchScalarGridSpec(
            num_scalar_prefetch=1,
            grid=(blocks,),
            in_specs=[
                pl.BlockSpec((1, rows, d), rel),
                pl.BlockSpec((1, rows, d), rel),
                pl.BlockSpec((3, rows, width), lambda i, me: (0, i, 0)),
                pl.BlockSpec(w.shape, lambda i, me: (0, 0)),
                pl.BlockSpec(order.shape, lambda i, me: (0, 0, 0)),
            ],
            out_specs=(
                pl.BlockSpec((1, rows, d), rel),
                pl.BlockSpec((1, rows, d), rel),
                pl.BlockSpec(w.shape, lambda i, me: (0, 0)),
            ),
            scratch_shapes=[
                pltpu.VMEM((3, d, width), BF16),
                pltpu.VMEM((3, d, width), F32),
                pltpu.VMEM((8, d), F32),
                pltpu.VMEM((8, d), F32),
                pltpu.VMEM((8, width), F32),
            ],
        ),
        compiler_params=params(),
        cost_estimate=cost(4 * blocks * rows * d * 3 * width, 1.5e7),
        name="project_back",
    )(me, own, far, grad, w, order)


def pair_kernel(keep_ref, came_ref, own_ref, *send_refs):
    n = pl.program_id(0)
    total = keep_ref[0] + came_ref[0].astype(F32)

    @pl.when(n == 0)
    def _():
        own_ref[...] = total

    for m, ref in enumerate(send_refs):

        @pl.when(n == m + 1)
        def _(ref=ref):
            ref[...] = total.astype(BF16)


def pair_sum(keep, came):
    half, rows, d = keep.shape
    piece = pl.BlockSpec((1, rows, d), lambda n: (n, 0, 0))
    flat = pl.BlockSpec((rows, d), lambda n: (0, 0))
    return pl.pallas_call(
        pair_kernel,
        out_shape=(jax.ShapeDtypeStruct((rows, d), F32),)
        + (jax.ShapeDtypeStruct((rows, d), BF16),) * (half - 1),
        grid=(half,),
        in_specs=[piece, piece],
        out_specs=(flat,) * half,
        compiler_params=params(),
        cost_estimate=cost(0, 7e6),
        name="pair_sum",
    )(keep, came)


def finish_narrow_kernel(g_ref, qkv_ref, qb_ref, vec_ref):
    total = g_ref[0].astype(F32)
    for n in range(1, g_ref.shape[0]):
        total = total + g_ref[n].astype(F32)
    width = qkv_ref.shape[2]
    for s in range(3):
        qkv_ref[s] = total[:, s * width : (s + 1) * width]
    heads, piece = qb_ref.shape[1:]
    edge = 3 * width + 8
    for s in range(3):
        qb_ref[s] = total[s * heads : (s + 1) * heads, edge : edge + piece]
    vec_ref[...] = jnp.transpose(total[:, 512:640])[64:72]


def finish_narrow(g, width, bias_shape):
    tall = g.shape[1]
    sds = lambda *shape: jax.ShapeDtypeStruct(shape, F32)
    return pl.pallas_call(
        finish_narrow_kernel,
        out_shape=(sds(3, tall, width), sds(*bias_shape), sds(8, tall)),
        compiler_params=pltpu.CompilerParams(vmem_limit_bytes=VMEM_LIMIT),
        cost_estimate=cost(0, 2e6),
        name="finish_narrow",
    )(g)


def finish_rows_kernel(side_ref, tok_ref, near_ref, near2_ref, away_ref, away2_ref, gh_ref, w_ref, out_ref, gain_ref):
    m = pl.program_id(0)

    @pl.when(m == 0)
    def _():
        gain_ref[...] = jnp.transpose(w_ref[:, 512:640].astype(F32))[64:72]

    n, scale = norm_parts(tok_ref[0].astype(F32))
    near = near_ref[...] + near2_ref[...].astype(F32)
    away = away_ref[...].astype(F32) + away2_ref[...].astype(F32)
    incoming = jnp.where(m == side_ref[0], near, away)
    out_ref[0] = gh_ref[0] + norm_back(incoming, gain_ref[0:1], n, scale)


def finish_rows(side, tok, near, near2, away, away2, gh, w):
    micro, rows, d = tok.shape
    piece = pl.BlockSpec((1, rows, d), lambda m, ix: (m, 0, 0))
    flat = pl.BlockSpec((rows, d), lambda m, ix: (0, 0))
    return pl.pallas_call(
        finish_rows_kernel,
        out_shape=jax.ShapeDtypeStruct((micro, rows, d), F32),
        grid_spec=pltpu.PrefetchScalarGridSpec(
            num_scalar_prefetch=1,
            grid=(micro,),
            in_specs=[piece, flat, flat, flat, flat, piece, pl.BlockSpec(w.shape, lambda m, ix: (0, 0))],
            out_specs=piece,
            scratch_shapes=[pltpu.VMEM((8, d), F32)],
        ),
        compiler_params=params(),
        cost_estimate=cost(0, 6e6),
        name="finish_rows",
    )(side, tok, near, near2, away, away2, gh, w)


def one_hot_order(sources, size):
    row = lax.broadcasted_iota(jnp.int32, (size, sources.shape[1]), 0)
    return jnp.where(row == sources, 1.0, 0.0).astype(BF16)


def plus(a, b):
    return (a.astype(F32) + b.astype(F32)).astype(BF16)


def local(
    tokens,
    cotangent,
    ln1_gain,
    ln1_bias,
    qkv_weight,
    qkv_bias,
    out_weight,
    out_bias,
    ln2_gain,
    ln2_bias,
    fc_weight,
    fc_bias,
    proj_weight,
    proj_bias,
):
    sides = lax.axis_size("ctx")
    parts = lax.axis_size("tp")
    shards = lax.axis_size(("dp", "ctx"))
    group = sides * parts
    micro, _, rows, d = tokens.shape
    assert micro == sides == 2 and parts == 4
    side = lax.axis_index("ctx")
    slot = lax.axis_index("tp")
    deep = lax.axis_index("dp")
    depth = lax.axis_size("dp")
    me = side * parts + slot
    me_array = jnp.full((1,), me, jnp.int32)
    side_array = jnp.full((1,), side, jnp.int32)
    tall = qkv_weight.shape[1]
    heads, piece = qkv_bias.shape[1], qkv_bias.shape[2]
    width = heads * HD
    lines, strip = fc_bias.shape

    def swap(array, mask):
        return lax.ppermute(array, ("ctx", "tp"), [(n, n ^ mask) for n in range(group)])

    def swap_deep(array, mask):
        return lax.ppermute(array, "dp", [(n, n ^ mask) for n in range(depth)])

    tok = tokens[:, 0]
    cot = cotangent[:, 0]

    vectors = jnp.stack([ln1_gain, ln1_bias, ln2_gain, ln2_bias, out_bias, proj_bias])
    wide, narrow = pack(fc_weight, proj_weight, out_weight, qkv_weight, vectors, qkv_bias, fc_bias, shards)

    gathered = lax.all_gather(wide, ("tp", "dp", "ctx"), axis=0, tiled=True)
    gathered = gathered.reshape(parts, d, wide.shape[1])

    mine = lax.dynamic_index_in_dim(tok, side, 0, keepdims=False)
    other = lax.dynamic_index_in_dim(tok, 1 - side, 0, keepdims=False)
    blocks = []
    for mask in range(0, group, 2):
        block = other if mask >= parts else mine
        blocks.append(block if mask == 0 else swap(block, mask))
    own = jnp.stack(blocks)
    far = swap(own, 1)

    w_in = lax.all_to_all(narrow, ("dp", "ctx"), 0, 0, tiled=True).reshape(d, narrow.shape[2])

    unit = lax.broadcasted_iota(jnp.int32, (1, 3 * width), 1)
    order_in = one_hot_order(unit % HD // piece * tall + unit // HD, d)
    unit = lax.broadcasted_iota(jnp.int32, (1, d), 1)
    order_fc = one_hot_order(unit % 128 // strip * tall + unit // 128, d)

    triple = project(me_array, own, far, w_in, order_in, piece)
    mixed, mixed_turned, level = attend(triple, rows)
    mix = lax.all_to_all(mixed, ("ctx", "tp"), 0, 0, tiled=True)

    tok_rows = tok.reshape(micro * rows, d)
    cot_rows = cot.reshape(micro * rows, d)
    y, grad_hidden, grad_mix, n2, act, gl, gb, vec, gfb = middle(
        tok_rows, cot_rows, mix, gathered, order_fc, strip
    )
    grad_mix = lax.all_to_all(grad_mix, ("ctx", "tp"), 0, 0, tiled=True)

    parcels = (n2, cot_rows, gb, mix, act, gl, vec, gfb, order_fc, strip)
    cut = wide.shape[1] // 2
    if tall % 16 == 0 and depth & (depth - 1) == 0:
        core, row = slot % 2, slot // 2
        index = lambda lane: jnp.stack([(1 - row) * 2 + lane, row * 2 + lane, deep, side]).astype(jnp.int32)
        came = swap(weights("send", index(1 - core), *parcels), 1)
        a_send, a_keep, b_send, b_keep = weights("keep", index(core), *parcels, came=came, shards=shards)
        a_came, b_came = swap(a_send, 2), swap(b_send, parts)
        a_send, a_keep = plus(a_keep[1], a_came[1]), plus(a_keep[0], a_came[0])
        b_send, b_keep = plus(b_keep[1], b_came[1]), plus(b_keep[0], b_came[0])
        a_came, b_came = swap(a_send, parts), swap(b_send, 2)
        left, mask = depth, 1
        while left > 1:
            left //= 2
            a_send, a_keep = plus(a_keep[left:], a_came[left:]), plus(a_keep[:left], a_came[:left])
            b_send, b_keep = plus(b_keep[left:], b_came[left:]), plus(b_keep[:left], b_came[:left])
            a_came, b_came = swap_deep(a_send, mask), swap_deep(b_send, mask)
            mask *= 2
        a_keep, a_came, b_keep, b_came = a_keep[0], a_came[0], b_keep[0], b_came[0]
    else:
        grad_wide = weights("all", jnp.arange(parts, dtype=jnp.int32), *parcels)
        grad_wide = lax.psum_scatter(
            grad_wide.reshape(parts * d, wide.shape[1]), ("tp", "dp", "ctx"), scatter_dimension=0, tiled=True
        )
        a_keep, b_keep = grad_wide[:, :cut], grad_wide[:, cut:]
        a_came, b_came = jnp.zeros_like(a_keep), jnp.zeros_like(b_keep)

    grad_triple = attend_back(triple, grad_mix, mixed_turned, level)
    order_back = order_in.reshape(d, 3, width).transpose(1, 0, 2)
    keep, send, grad_in = project_back(me_array, own, far, grad_triple, w_in, order_back, piece)

    near, *sends = pair_sum(keep, swap(send, 1))
    arrived = [swap(sends[n - 1], 2 * n) for n in range(1, group // 2)]

    grad_in = lax.all_to_all(grad_in.reshape(narrow.shape), ("dp", "ctx"), 0, 0, tiled=True)
    grad_qkv_weight, grad_qkv_bias, vec_in = finish_narrow(grad_in, width, qkv_bias.shape)
    mask = parts // 2
    while mask:
        vec_in = vec_in + swap(vec_in, mask)
        mask //= 2

    grad_tokens = finish_rows(
        side_array, tok, near, *arrived, grad_hidden.reshape(micro, rows, d), w_in
    )
    fc_grad, proj_grad, out_grad, gain2, shift2, out_b, proj_b, fc_b = finish_wide(
        a_keep, a_came, b_keep, b_came, d, width, fc_bias.shape
    )
    return (
        y.reshape(micro, 1, rows, d),
        grad_tokens[:, None],
        vec_in[0],
        vec_in[1],
        grad_qkv_weight,
        grad_qkv_bias,
        out_grad,
        out_b[0],
        gain2[0],
        shift2[0],
        fc_grad,
        fc_b,
        proj_grad,
        proj_b[0],
    )


def solution(mesh):
    rows = P(None, "dp", ("ctx", "tp"), None)
    vector = P(("dp", "ctx"))
    joint = P(None, ("dp", "ctx"), "tp")
    joint_bias = P(None, "tp", ("dp", "ctx"))
    down = P("tp", ("dp", "ctx"))
    up = P(("dp", "ctx"), "tp")
    inner = (vector, vector, joint, joint_bias, down, vector, vector, vector, up, down, down, vector)
    return jax.shard_map(
        local,
        mesh=mesh,
        in_specs=(rows, rows) + inner,
        out_specs=(rows, rows) + inner,
        check_vma=False,
    )
```

```python
import functools

import jax
import jax.numpy as jnp
from jax import lax
from jax.experimental import pallas as pl
from jax.experimental.pallas import tpu as pltpu
from jax.sharding import PartitionSpec as P

HD = 64
EPS = 1e-05
LOG2E = 1.4426950408889634
F32 = jnp.float32
BF16 = jnp.bfloat16
VMEM_LIMIT = 60 * 1024 * 1024
SMALL_LIMIT = 60 * 1024 * 1024
EXT = 64


def dot(a, b):
    return lax.dot_general(a, b, (((1,), (0,)), ((), ())), preferred_element_type=F32)


def dot_nt(a, b):
    return lax.dot_general(a, b, (((1,), (1,)), ((), ())), preferred_element_type=F32)


def norm_parts(rows):
    mean = jnp.mean(rows, axis=-1, keepdims=True)
    centered = rows - mean
    spread = jnp.mean(centered * centered, axis=-1, keepdims=True)
    scale = lax.rsqrt(spread + EPS)
    return (centered * scale, scale)


def norm_back(incoming, gain, n, scale):
    e = incoming * gain
    return (e - jnp.mean(e, axis=-1, keepdims=True) - n * jnp.mean(e * n, axis=-1, keepdims=True)) * scale


def params(limit=VMEM_LIMIT):
    return pltpu.CompilerParams(dimension_semantics=("arbitrary",), vmem_limit_bytes=limit)


def cost(flops, moved, exps=0):
    return pl.CostEstimate(flops=int(flops), bytes_accessed=int(moved), transcendentals=int(exps))


def pack_kernel(fc_ref, pj_ref, out_ref, qkv_ref, vec_ref, qb_ref, fb_ref, wide_ref, narrow_ref):
    tall, d = fc_ref.shape
    width = out_ref.shape[0]
    copies = narrow_ref.shape[0]
    columns = jnp.transpose(vec_ref[...].astype(F32)).astype(BF16)
    wide_ref[:, :d] = fc_ref[...]
    wide_ref[:, d : 2 * d] = jnp.transpose(pj_ref[...].astype(F32)).astype(BF16)
    wide_ref[:, 2 * d : 2 * d + width] = jnp.transpose(out_ref[...].astype(F32)).astype(BF16)
    edge = 2 * d + width
    wide_ref[:, edge:] = jnp.zeros((tall, EXT), BF16)
    wide_ref[:, edge : edge + 4] = columns[:, 2:6]
    rows, strip = fb_ref.shape
    wide_ref[:rows, edge + 8 : edge + 8 + strip] = fb_ref[...]
    for s in range(3):
        narrow_ref[0, :, s * width : (s + 1) * width] = qkv_ref[s]
    edge = 3 * width
    narrow_ref[0, :, edge:] = jnp.zeros((tall, EXT), BF16)
    narrow_ref[0, :, edge : edge + 2] = columns[:, :2]
    heads, piece = qb_ref.shape[1:]
    for s in range(3):
        narrow_ref[0, s * heads : (s + 1) * heads, edge + 8 : edge + 8 + piece] = qb_ref[s]
    whole = narrow_ref[0]
    for n in range(1, copies):
        narrow_ref[n] = whole


def pack(fc, pj, out, qkv, vec, qb, fb, copies):
    tall, d = fc.shape
    width = out.shape[0]
    return pl.pallas_call(
        pack_kernel,
        out_shape=(
            jax.ShapeDtypeStruct((tall, 2 * d + width + EXT), BF16),
            jax.ShapeDtypeStruct((copies, tall, 3 * width + EXT), BF16),
        ),
        compiler_params=pltpu.CompilerParams(vmem_limit_bytes=SMALL_LIMIT),
        cost_estimate=cost(0, 2e6),
        name="pack",
    )(fc, pj, out, qkv, vec, qb, fb)


def pick_rows(table, period):
    line = lax.broadcasted_iota(jnp.int32, table.shape, 0)
    lane = lax.broadcasted_iota(jnp.int32, table.shape, 1)
    return jnp.sum(jnp.where(line == (lane & (period - 1)), table, 0.0), axis=0, keepdims=True)


def spread_rows(row, lines, period):
    shape = (lines, row.shape[1])
    line = lax.broadcasted_iota(jnp.int32, shape, 0)
    lane = lax.broadcasted_iota(jnp.int32, shape, 1)
    return jnp.where(line == (lane & (period - 1)), jnp.broadcast_to(row, shape), 0.0).astype(BF16)


def project_kernel(piece, me_ref, own_ref, far_ref, w_ref, order_ref, out_ref, vec_ref, bias_ref):
    i = pl.program_id(0)
    width = out_ref.shape[2]

    @pl.when(i == 0)
    def _():
        turned = jnp.transpose(w_ref[:, 512:640].astype(F32))
        vec_ref[...] = turned[64:72]
        table = dot(turned[72:80].astype(BF16), order_ref[...])
        bias_ref[...] = jnp.broadcast_to(pick_rows(table, piece), bias_ref.shape)

    far = ((i ^ me_ref[0]) & 1) == 1
    rows = jnp.where(far, far_ref[0], own_ref[0]).astype(F32)
    n, _ = norm_parts(rows)
    normed = (n * vec_ref[0:1] + vec_ref[1:2]).astype(BF16)
    full = dot(normed, w_ref[...])[:, : 3 * width] + bias_ref[0:1, :]
    full = full.astype(BF16)
    out_ref[0] = full[:, :width] * jnp.asarray(HD ** (-0.5), BF16)
    out_ref[1] = full[:, width : 2 * width]
    out_ref[2] = full[:, 2 * width :]


def project(me, own, far, w, order, piece):
    half, rows, d = own.shape
    blocks = 2 * half
    width = order.shape[1] // 3
    return pl.pallas_call(
        functools.partial(project_kernel, piece),
        out_shape=jax.ShapeDtypeStruct((3, blocks * rows, width), BF16),
        grid_spec=pltpu.PrefetchScalarGridSpec(
            num_scalar_prefetch=1,
            grid=(blocks,),
            in_specs=[
                pl.BlockSpec((1, rows, d), lambda i, me: ((i ^ me[0]) // 2, 0, 0)),
                pl.BlockSpec((1, rows, d), lambda i, me: ((i ^ me[0]) // 2, 0, 0)),
                pl.BlockSpec(w.shape, lambda i, me: (0, 0)),
                pl.BlockSpec(order.shape, lambda i, me: (0, 0)),
            ],
            out_specs=pl.BlockSpec((3, rows, width), lambda i, me: (0, i, 0)),
            scratch_shapes=[pltpu.VMEM((8, d), F32), pltpu.VMEM((8, 3 * width), F32)],
        ),
        compiler_params=params(),
        cost_estimate=cost(2 * blocks * rows * d * 3 * width, 8e6),
        name="project",
    )(me, own, far, w, order)


def head_mask(shape, h):
    lane = lax.broadcasted_iota(jnp.int32, shape, 1)
    return (lane >= h * HD) & (lane < (h + 1) * HD)


def attend_kernel(q_ref, k_ref, v_ref, o_ref, ot_ref, level_ref, vt_ref, qm_ref, m_ref, l_ref):
    i = pl.program_id(0)
    heads = q_ref.shape[2] // HD
    bq = q_ref.shape[1]
    half = bq // 2

    @pl.when(i == 0)
    def _():
        vt_ref[...] = jnp.transpose(v_ref[0].astype(F32)).astype(BF16)

    for h in range(heads):
        q = q_ref[0]
        qm_ref[h] = jnp.where(head_mask(q.shape, h), q, jnp.zeros_like(q))
    m_ref[...] = jnp.zeros_like(m_ref)
    l_ref[...] = jnp.zeros_like(l_ref)
    ot_ref[...] = jnp.zeros_like(ot_ref)

    def chunk(start, size, first, masked):
        cols = slice(first, bq)
        keys = k_ref[0, pl.ds(start, size), :]
        for h in range(heads):
            u = dot_nt(keys, qm_ref[h, first:bq, :]) * LOG2E
            if masked:
                key_pos = lax.broadcasted_iota(jnp.int32, u.shape, 0)
                row_pos = lax.broadcasted_iota(jnp.int32, u.shape, 1)
                allowed = key_pos <= row_pos
                u = jnp.where(allowed, u, 0.0)
            before = m_ref[h : h + 1, cols]
            peak = jnp.maximum(before, jnp.max(jnp.abs(u), axis=0, keepdims=True))
            fade = jnp.exp2(before - peak)
            upper = jnp.exp2(u - peak)
            lower = jnp.exp2(-peak - u)
            both = upper + lower
            if masked:
                both = jnp.where(allowed, both, 0.0)
            m_ref[h : h + 1, cols] = peak
            l_ref[h : h + 1, cols] = l_ref[h : h + 1, cols] * fade + jnp.sum(both, axis=0, keepdims=True)
            part = dot(vt_ref[h * HD : (h + 1) * HD, pl.ds(start, size)], (upper - lower).astype(BF16))
            ot_ref[h * HD : (h + 1) * HD, cols] = ot_ref[h * HD : (h + 1) * HD, cols] * fade + part

    def body(j, carry):
        chunk(pl.multiple_of(j * bq, bq), bq, 0, False)
        return carry

    lax.fori_loop(0, i, body, 0)
    base = pl.multiple_of(i * bq, bq)
    chunk(base, half, 0, True)
    chunk(pl.multiple_of(base + half, half), half, half, True)
    for h in range(heads):
        total = l_ref[h : h + 1, :]
        level_ref[h : h + 1, :] = m_ref[h : h + 1, :] + jnp.log2(total)
        ot_ref[h * HD : (h + 1) * HD, :] = ot_ref[h * HD : (h + 1) * HD, :] * (1.0 / total)
    rows = o_ref.shape[2]
    for n in range(bq // rows):
        o_ref[n] = ot_ref[:, n * rows : (n + 1) * rows].astype(BF16)


def attend(triple, rows):
    _, span, width = triple.shape
    bq = min(512, span)
    heads = width // HD
    return pl.pallas_call(
        attend_kernel,
        out_shape=(
            jax.ShapeDtypeStruct((span // rows, width, rows), BF16),
            jax.ShapeDtypeStruct((width, span), F32),
            jax.ShapeDtypeStruct((8, span), F32),
        ),
        grid=(span // bq,),
        in_specs=[
            pl.BlockSpec((1, bq, width), lambda i: (0, i, 0)),
            pl.BlockSpec((1, span, width), lambda i: (1, 0, 0)),
            pl.BlockSpec((1, span, width), lambda i: (2, 0, 0)),
        ],
        out_specs=(
            pl.BlockSpec((bq // rows, width, rows), lambda i: (i, 0, 0)),
            pl.BlockSpec((width, bq), lambda i: (0, i)),
            pl.BlockSpec((8, bq), lambda i: (0, i)),
        ),
        scratch_shapes=[
            pltpu.VMEM((width, span), BF16),
            pltpu.VMEM((heads, bq, width), BF16),
            pltpu.VMEM((8, bq), F32),
            pltpu.VMEM((8, bq), F32),
        ],
        compiler_params=params(),
        cost_estimate=cost(4 * span * span * width, 8e6, span * span * heads),
        name="attend",
    )(triple, triple, triple)


def attend_back_kernel(
    qkv_ref, grad_ref, ot_ref, level_ref, out_ref, qm_ref, gm_ref, kt_ref, dqt_ref, dot_ref, dk_ref, dv_ref
):
    j = pl.program_id(0)
    blocks = pl.num_programs(0)
    span, width = qkv_ref.shape[1:]
    rows = grad_ref.shape[2]
    heads = width // HD
    count = qm_ref.shape[0]
    b = span // count
    half = b // 2

    @pl.when(j == 0)
    def _():
        for n in range(span // rows):
            cols = slice(n * rows, (n + 1) * rows)
            turned = grad_ref[n].astype(F32)
            prod = turned * ot_ref[:, cols]
            for h in range(heads):
                dot_ref[h : h + 1, cols] = jnp.sum(prod[h * HD : (h + 1) * HD], axis=0, keepdims=True)
            g = jnp.transpose(turned).astype(BF16)
            at = n * rows % b
            for h in range(heads):
                mask = head_mask(g.shape, h)
                gm_ref[n * rows // b, h * b + at : h * b + at + rows, :] = jnp.where(mask, g, jnp.zeros_like(g))
        kt_ref[...] = jnp.transpose(qkv_ref[1].astype(F32)).astype(BF16)
        dqt_ref[...] = jnp.zeros_like(dqt_ref)
        for n in range(count):
            q = qkv_ref[0, n * b : (n + 1) * b, :]
            for h in range(heads):
                mask = head_mask(q.shape, h)
                qm_ref[n, h * b : (h + 1) * b, :] = jnp.where(mask, q, jnp.zeros_like(q))

    dk_ref[...] = jnp.zeros_like(dk_ref)
    dv_ref[...] = jnp.zeros_like(dv_ref)

    def chunk(i, key_first, key_size, first, masked):
        start = pl.multiple_of(j * b + key_first, half)
        keys = qkv_ref[1, pl.ds(start, key_size), :]
        vals = qkv_ref[2, pl.ds(start, key_size), :]
        cols = b - first
        at = pl.multiple_of(i * b + first, half)
        for h in range(heads):
            lo = h * b + first
            qm = qm_ref[i, lo : lo + cols, :]
            gm = gm_ref[i, lo : lo + cols, :]
            level = level_ref[h : h + 1, pl.ds(at, cols)]
            inner = dot_ref[h : h + 1, pl.ds(at, cols)]
            u = dot_nt(keys, qm) * LOG2E
            upper = jnp.exp2(u - level)
            lower = jnp.exp2(-level - u)
            gw = dot_nt(vals, gm)
            weights = upper - lower
            gs = upper * (gw - inner) + lower * (gw + inner)
            if masked:
                key_pos = lax.broadcasted_iota(jnp.int32, u.shape, 0)
                row_pos = lax.broadcasted_iota(jnp.int32, u.shape, 1)
                allowed = key_pos <= row_pos
                weights = jnp.where(allowed, weights, 0.0)
                gs = jnp.where(allowed, gs, 0.0)
            weights = weights.astype(BF16)
            gs = gs.astype(BF16)
            rows = slice(key_first, key_first + key_size)
            dv_ref[rows, :] += dot(weights, gm)
            dk_ref[rows, :] += dot(gs, qm)
            dqt_ref[h * HD : (h + 1) * HD, pl.ds(at, cols)] += dot(
                kt_ref[h * HD : (h + 1) * HD, pl.ds(start, key_size)], gs
            )

    def body(i, carry):
        chunk(i, 0, b, 0, False)
        return carry

    chunk(j, 0, half, 0, True)
    chunk(j, half, half, half, True)
    lax.fori_loop(j + 1, blocks, body, 0)
    here = pl.ds(pl.multiple_of(j * b, b), b)
    out_ref[1, here, :] = dk_ref[...].astype(BF16)
    out_ref[2, here, :] = dv_ref[...].astype(BF16)

    @pl.when(j == blocks - 1)
    def _():
        out_ref[0] = jnp.transpose(dqt_ref[...] * (HD ** (-0.5))).astype(BF16)


def attend_back(triple, grad, ot, level):
    _, span, width = triple.shape
    b = min(512, span)
    count = span // b
    heads = width // HD
    whole = lambda *shape: pl.BlockSpec(shape, lambda j: (0,) * len(shape))
    return pl.pallas_call(
        attend_back_kernel,
        out_shape=jax.ShapeDtypeStruct(triple.shape, BF16),
        grid=(count,),
        in_specs=[
            whole(*triple.shape),
            whole(*grad.shape),
            whole(*ot.shape),
            whole(*level.shape),
        ],
        out_specs=whole(*triple.shape),
        scratch_shapes=[
            pltpu.VMEM((count, heads * b, width), BF16),
            pltpu.VMEM((count, heads * b, width), BF16),
            pltpu.VMEM((width, span), BF16),
            pltpu.VMEM((width, span), F32),
            pltpu.VMEM((8, span), F32),
            pltpu.VMEM((b, width), F32),
            pltpu.VMEM((b, width), F32),
        ],
        compiler_params=params(),
        cost_estimate=cost(10 * span * span * width, 1e7, span * span * heads),
        name="attend_back",
    )(triple, grad, ot, level)


def gelu_parts(u):
    c = 0.7978845608028654
    square = u * u
    th = jnp.tanh(c * u * (1.0 + 0.044715 * square))
    near = 0.5 * (1.0 + th)
    slope = near + (0.5 * c) * u * (1.0 - th * th) * (1.0 + (3.0 * 0.044715) * square)
    return (u * near, slope)


def middle_kernel(
    strip,
    tok_ref,
    cot_ref,
    mix_ref,
    g_ref,
    gout_ref,
    order_ref,
    y_ref,
    gh_ref,
    dmix_ref,
    n2_ref,
    act_ref,
    gl_ref,
    gb_ref,
    vec_ref,
    gfb_ref,
    hid_ref,
    acc_ref,
    back_ref,
    ext_ref,
):
    t = pl.program_id(0)
    steps = pl.num_programs(0)
    half = mix_ref.shape[2]
    parts = gout_ref.shape[0]
    d = tok_ref.shape[1]
    width = mix_ref.shape[1]

    @pl.when(t == 0)
    def _():
        ext_ref[...] = jnp.transpose(gout_ref[0, :, 128:256].astype(F32))[64:72]
        total = tok_ref[...].astype(F32) + ext_ref[2:3]
        for s in range(parts):
            lhs = jnp.concatenate([mix_ref[s], mix_ref[parts + s]], axis=1)
            lhs = jnp.transpose(lhs.astype(F32)).astype(BF16)
            total = total + dot_nt(lhs, gout_ref[s, :, :width])
        hid_ref[...] = total
        n, _ = norm_parts(total)
        n2_ref[...] = (n * ext_ref[0:1] + ext_ref[1:2]).astype(BF16)
        acc_ref[...] = total + ext_ref[3:4]
        back_ref[...] = jnp.zeros_like(back_ref)

    ext = jnp.transpose(g_ref[0, :, 2 * d + 128 : 2 * d + 256].astype(F32))[72:88].astype(BF16)
    bias = pick_rows(dot(ext, order_ref[...]), strip)
    fc = g_ref[0, :, :d]
    pj = g_ref[0, :, d : 2 * d]
    lifted = dot(n2_ref[...], fc) + bias
    act, slope = gelu_parts(lifted)
    act = act.astype(BF16)
    act_ref[0] = act
    gl32 = dot(cot_ref[...], pj) * slope
    gl = gl32.astype(BF16)
    gl_ref[0] = gl
    gfb_ref[0, 0:1, :] = jnp.sum(gl.astype(F32), axis=0, keepdims=True)
    acc_ref[...] += dot_nt(act, pj)
    back_ref[...] += dot_nt(gl, fc)

    @pl.when(t == steps - 1)
    def _():
        y_ref[...] = acc_ref[...].astype(BF16)
        n, scale = norm_parts(hid_ref[...])
        back = back_ref[...]
        cot = cot_ref[...].astype(F32)
        gh = cot + norm_back(back, ext_ref[0:1], n, scale)
        gh_ref[...] = gh
        gb = gh.astype(BF16)
        gb_ref[...] = gb
        vec_ref[0:1, :] = jnp.sum(back * n, axis=0, keepdims=True)
        vec_ref[1:2, :] = jnp.sum(back, axis=0, keepdims=True)
        vec_ref[2:3, :] = jnp.sum(gb.astype(F32), axis=0, keepdims=True)
        vec_ref[3:4, :] = jnp.sum(cot, axis=0, keepdims=True)
        vec_ref[4:8, :] = jnp.zeros((4, d), F32)
        for s in range(parts):
            dm = jnp.transpose(dot(gb, gout_ref[s, :, :width])).astype(BF16)
            dmix_ref[s] = dm[:, :half]
            dmix_ref[parts + s] = dm[:, half:]


def middle(tok, cot, mix, gathered, order, strip):
    rows, d = tok.shape
    parts = gathered.shape[0]
    cols = gathered.shape[2]
    whole = lambda *shape: pl.BlockSpec(shape, lambda t: (0,) * len(shape))
    piece = lambda *shape: pl.BlockSpec(shape, lambda t: (t,) + (0,) * (len(shape) - 1))
    sds = jax.ShapeDtypeStruct
    return pl.pallas_call(
        functools.partial(middle_kernel, strip),
        out_shape=(
            sds((rows, d), BF16),
            sds((rows, d), F32),
            sds(mix.shape, BF16),
            sds((rows, d), BF16),
            sds((parts, rows, d), BF16),
            sds((parts, rows, d), BF16),
            sds((rows, d), BF16),
            sds((8, d), F32),
            sds((parts, 8, d), F32),
        ),
        grid=(parts,),
        in_specs=[
            whole(rows, d),
            whole(rows, d),
            whole(*mix.shape),
            piece(1, d, cols),
            pl.BlockSpec((parts, d, 256), lambda t: (0, 0, cols // 256 - 1)),
            whole(*order.shape),
        ],
        out_specs=(
            whole(rows, d),
            whole(rows, d),
            whole(*mix.shape),
            whole(rows, d),
            piece(1, rows, d),
            piece(1, rows, d),
            whole(rows, d),
            whole(8, d),
            piece(1, 8, d),
        ),
        scratch_shapes=[
            pltpu.VMEM((rows, d), F32),
            pltpu.VMEM((rows, d), F32),
            pltpu.VMEM((rows, d), F32),
            pltpu.VMEM((8, d), F32),
        ],
        compiler_params=params(),
        cost_estimate=cost(2 * rows * d * d * 18, 3e7),
        name="middle",
    )(tok, cot, mix, gathered, gathered, order)


def weights_kernel(
    mode, strip, index_ref, n2_ref, cot_ref, gb_ref, mix_ref, act_ref, gl_ref, vec_ref, gfb_ref, order_ref, *rest
):
    s = pl.program_id(0)
    d = n2_ref.shape[1]
    width = mix_ref.shape[2]
    cols = 2 * d + width + EXT
    nt_ref, ct_ref, bt_ref = rest[-3:]

    @pl.when(s == 0)
    def _():
        nt_ref[...] = jnp.transpose(n2_ref[...].astype(F32)).astype(BF16)
        ct_ref[...] = jnp.transpose(cot_ref[...].astype(F32)).astype(BF16)
        bt_ref[...] = jnp.transpose(gb_ref[...].astype(F32)).astype(BF16)

    mix = jnp.concatenate([mix_ref[0, 0], mix_ref[1, 0]], axis=1)
    turned = dot_nt(spread_rows(gfb_ref[0, 0:1], 16, strip), order_ref[...])
    tall = jnp.concatenate([vec_ref[...], turned, jnp.zeros((EXT - 24, d), F32)], axis=0)
    if mode != "keep":
        out_ref = rest[0]
        out_ref[0, :, :d] = dot(nt_ref[...], gl_ref[0]).astype(BF16)
        out_ref[0, :, d : 2 * d] = dot(ct_ref[...], act_ref[0]).astype(BF16)
        out_ref[0, :, 2 * d : 2 * d + width] = dot_nt(bt_ref[...], mix).astype(BF16)
        out_ref[0, :, 2 * d + width :] = jnp.transpose(tall).astype(BF16)
        return
    came_ref, as_ref, ak_ref, bs_ref, bk_ref, sum_ref = rest[:6]
    sum_ref[:, 2 * d : 2 * d + width] = dot_nt(bt_ref[...], mix).astype(BF16)
    sum_ref[:, 2 * d + width :] = jnp.transpose(tall).astype(BF16)
    sum_ref[:, 2 * d :] = (sum_ref[:, 2 * d :].astype(F32) + came_ref[0, :, 2 * d :].astype(F32)).astype(BF16)
    sum_ref[:, :d] = (dot(nt_ref[...], gl_ref[0]) + came_ref[0, :, :d].astype(F32)).astype(BF16)
    sum_ref[:, d : 2 * d] = (dot(ct_ref[...], act_ref[0]) + came_ref[0, :, d : 2 * d].astype(F32)).astype(BF16)
    depth, step = as_ref.shape[1], as_ref.shape[2]
    cut = cols // 2

    def block(xr, zr):
        at = (zr * 2 + (xr ^ index_ref[2])) * step
        return pl.ds(pl.multiple_of(at, 16), step)

    for zr in range(depth):
        bk_ref[0, zr] = sum_ref[block(0, zr), cut:]
        bs_ref[0, zr] = sum_ref[block(1, zr), cut:]

    @pl.when(s == 0)
    def _():
        for xr in range(2):
            for zr in range(depth):
                as_ref[xr, zr] = sum_ref[block(xr, zr), :cut]

    @pl.when(s == 1)
    def _():
        for xr in range(2):
            for zr in range(depth):
                ak_ref[xr, zr] = sum_ref[block(xr, zr), :cut]


def weights(mode, index, n2, cot, gb, mix, act, gl, vec, gfb, order, strip, came=None, shards=None):
    rows, d = n2.shape
    parts = act.shape[0]
    width = mix.shape[1]
    cols = 2 * d + width + EXT
    steps = parts if mode == "all" else 2
    whole = lambda *shape: pl.BlockSpec(shape, lambda s, ix: (0,) * len(shape))
    piece = lambda *shape: pl.BlockSpec(shape, lambda s, ix: (ix[s],) + (0,) * (len(shape) - 1))
    mix = mix.reshape(mix.shape[0] // parts, parts, width, mix.shape[2])
    operands = [index, n2, cot, gb, mix, act, gl, vec, gfb, order]
    specs = [
        whole(rows, d),
        whole(rows, d),
        whole(rows, d),
        pl.BlockSpec((mix.shape[0], 1, width, mix.shape[3]), lambda s, ix: (0, ix[s], 0, 0)),
        piece(1, rows, d),
        piece(1, rows, d),
        whole(8, d),
        piece(1, 8, d),
        whole(*order.shape),
    ]
    scratch = [pltpu.VMEM((d, rows), BF16) for _ in range(3)]
    if mode == "keep":
        operands.append(came)
        specs.append(pl.BlockSpec((1, d, cols), lambda s, ix: (s, 0, 0)))
        block = (2, shards // 2, d // shards, cols // 2)
        sds = jax.ShapeDtypeStruct(block, BF16)
        out_shape = (sds,) * 4
        turn = pl.BlockSpec((1,) + block[1:], lambda s, ix: (1 - s, 0, 0, 0))
        out_specs = (whole(*block), whole(*block), turn, turn)
        scratch = [pltpu.VMEM((d, cols), BF16)] + scratch
    else:
        out_shape = jax.ShapeDtypeStruct((steps, d, cols), BF16)
        out_specs = pl.BlockSpec((1, d, cols), lambda s, ix: (s, 0, 0))
    return pl.pallas_call(
        functools.partial(weights_kernel, mode, strip),
        out_shape=out_shape,
        grid_spec=pltpu.PrefetchScalarGridSpec(
            num_scalar_prefetch=1,
            grid=(steps,),
            in_specs=specs,
            out_specs=out_specs,
            scratch_shapes=scratch,
        ),
        compiler_params=params(),
        cost_estimate=cost(2 * rows * d * cols * steps, 6e6 * steps),
        name="weights_" + mode,
    )(*operands)


def merge_kernel(side_ref, ak_ref, ac_ref, bk_ref, bc_ref, nk_ref, nc_ref, vec_ref, out_ref, turn_ref):
    depth, step, cut = ak_ref.shape
    at = 2 * cut + nk_ref.shape[2] - EXT
    turn_ref[...] = jnp.transpose(vec_ref[...])
    for z in range(depth):
        out_ref[z, :, :cut] = (ak_ref[z].astype(F32) + ac_ref[z].astype(F32)).astype(BF16)
        out_ref[z, :, cut : 2 * cut] = (bk_ref[z].astype(F32) + bc_ref[z].astype(F32)).astype(BF16)
        out_ref[z, :, 2 * cut :] = (nk_ref[z].astype(F32) + nc_ref[z].astype(F32)).astype(BF16)
        here = pl.ds(pl.multiple_of((2 * z + side_ref[0]) * step, 8), step)
        out_ref[z, :, at : at + 8] = turn_ref[here, :].astype(BF16)


def merge(side, *parts):
    depth, step, cut = parts[0].shape
    cols = 2 * cut + parts[4].shape[2]
    whole = lambda array: pl.BlockSpec(array.shape, lambda i, ix: (0,) * array.ndim)
    out = jax.ShapeDtypeStruct((depth, step, cols), BF16)
    return pl.pallas_call(
        merge_kernel,
        out_shape=out,
        grid_spec=pltpu.PrefetchScalarGridSpec(
            num_scalar_prefetch=1,
            grid=(1,),
            in_specs=[whole(p) for p in parts],
            out_specs=whole(out),
            scratch_shapes=[pltpu.VMEM(parts[6].shape[::-1], F32)],
        ),
        compiler_params=params(),
        cost_estimate=cost(0, 6e6),
        name="merge",
    )(side, *parts)


def finish_wide(t, fc_ref, pj_ref, out_ref, g_ref, b_ref, ob_ref, pb_ref, fb_ref):
    d = fc_ref.shape[1]
    width = out_ref.shape[0]
    fc_ref[...] = t[:, :d]
    pj_ref[...] = jnp.transpose(t[:, d : 2 * d])
    rest = jnp.transpose(t[:, 2 * d : 2 * d + width + EXT])
    out_ref[...] = rest[:width]
    g_ref[...] = rest[width : width + 1]
    b_ref[...] = rest[width + 1 : width + 2]
    ob_ref[...] = rest[width + 2 : width + 3]
    pb_ref[...] = rest[width + 3 : width + 4]
    rows, strip = fb_ref.shape
    at = 2 * d + width + 8
    fb_ref[...] = t[:rows, at : at + strip]


def finish_narrow(t, qkv_ref, qb_ref, vec_ref):
    width = qkv_ref.shape[2]
    for s in range(3):
        qkv_ref[s] = t[:, s * width : (s + 1) * width]
    heads, piece = qb_ref.shape[1:]
    edge = 3 * width + 8
    for s in range(3):
        qb_ref[s] = t[s * heads : (s + 1) * heads, edge : edge + piece]
    vec_ref[...] = jnp.transpose(t[:, 512:640])[64:72]


def total_of(ref):
    total = ref[0].astype(F32)
    for n in range(1, ref.shape[0]):
        total = total + ref[n].astype(F32)
    return total


def finish_kernel(*refs):
    total = total_of(refs[0])
    if len(refs) == 12:
        edge = total.shape[1] - 640
        finish_wide(total[:, :edge], *refs[1:9])
        finish_narrow(total[:, edge:], *refs[9:])
    else:
        finish_wide(total, *refs[2:10])
        finish_narrow(total_of(refs[1]), *refs[10:])


def finish(parts, d, width, fc_bias_shape, qkv_bias_shape):
    tall = parts[0].shape[1]
    sds = lambda *shape: jax.ShapeDtypeStruct(shape, F32)
    return pl.pallas_call(
        finish_kernel,
        out_shape=(
            sds(tall, d),
            sds(d, tall),
            sds(width, tall),
            sds(1, tall),
            sds(1, tall),
            sds(1, tall),
            sds(1, tall),
            sds(*fc_bias_shape),
            sds(3, tall, width),
            sds(*qkv_bias_shape),
            sds(8, tall),
        ),
        compiler_params=pltpu.CompilerParams(vmem_limit_bytes=SMALL_LIMIT),
        cost_estimate=cost(0, 4e6),
        name="finish",
    )(*parts)


def project_back_kernel(piece, me_ref, own_ref, far_ref, grad_ref, w_ref, order_ref, keep_ref, send_ref, sum_ref, *rest):
    parted = rest[:-6]
    dw_ref, w3_ref, dw3_ref, gain_ref, vec_ref, bias_ref = rest[-6:]
    i = pl.program_id(0)
    steps = pl.num_programs(0)
    width = grad_ref.shape[2]
    d = w_ref.shape[0]

    @pl.when(i == 0)
    def _():
        gain_ref[...] = jnp.transpose(w_ref[:, 512:640].astype(F32))[64:72]
        for s in range(3):
            w3_ref[s] = w_ref[:, s * width : (s + 1) * width]
        dw3_ref[...] = jnp.zeros_like(dw3_ref)
        vec_ref[...] = jnp.zeros_like(vec_ref)
        bias_ref[...] = jnp.zeros_like(bias_ref)

    far = ((i ^ me_ref[0]) & 1) == 1
    rows = jnp.where(far, far_ref[0], own_ref[0]).astype(F32)
    n, _ = norm_parts(rows)
    normed = n * gain_ref[0:1] + gain_ref[1:2]
    turned = jnp.transpose(normed).astype(BF16)
    part = dot_nt(grad_ref[0], w3_ref[0])
    for s in range(1, 3):
        part = part + dot_nt(grad_ref[s], w3_ref[s])
    for s in range(3):
        dw3_ref[s] += dot(turned, grad_ref[s])
        bias_ref[s : s + 1, :] += jnp.sum(grad_ref[s].astype(F32), axis=0, keepdims=True)
    vec_ref[0:1, :] += jnp.sum(part * n, axis=0, keepdims=True)
    vec_ref[1:2, :] += jnp.sum(part, axis=0, keepdims=True)

    @pl.when(far)
    def _():
        send_ref[0] = part.astype(BF16)

    @pl.when(jnp.logical_not(far))
    def _():
        keep_ref[0] = part

    @pl.when(i == steps - 1)
    def _():
        turned_bias = jnp.zeros((8, d), F32)
        for s in range(3):
            dw_ref[:, s * width : (s + 1) * width] = dw3_ref[s].astype(BF16)
            spread = spread_rows(bias_ref[s : s + 1, :], 8, piece)
            turned_bias = turned_bias + dot_nt(spread, order_ref[s])
        tall = jnp.concatenate([vec_ref[...], turned_bias, jnp.zeros((EXT - 16, d), F32)], axis=0)
        dw_ref[:, 3 * width :] = jnp.transpose(tall).astype(BF16)
        if not parted:
            sum_ref[...] = dw_ref[...]
            return
        sum_ref[...] = vec_ref[...]
        near_ref, away_ref = parted
        depth, step = near_ref.shape[:2]
        for z in range(depth):
            near_ref[z] = dw_ref[pl.ds(pl.multiple_of((2 * z + me_ref[1]) * step, 16), step), :]
            away_ref[z] = dw_ref[pl.ds(pl.multiple_of((2 * z + 1 - me_ref[1]) * step, 16), step), :]


def project_back(me, own, far, grad, w, order, piece, shards):
    half, rows, d = own.shape
    width = grad.shape[2]
    blocks = 2 * half
    sds = jax.ShapeDtypeStruct
    rel = lambda i, me: ((i ^ me[0]) // 2, 0, 0)
    whole = lambda *shape: pl.BlockSpec(shape, lambda i, me: (0,) * len(shape))
    last = [w.shape]
    if shards:
        last = [(8, d)] + [(shards // 2, d // shards, w.shape[1])] * 2
    return pl.pallas_call(
        functools.partial(project_back_kernel, piece),
        out_shape=(
            sds((half, rows, d), F32),
            sds((half, rows, d), BF16),
        )
        + tuple(sds(shape, BF16 if len(shape) == 3 or not shards else F32) for shape in last),
        grid_spec=pltpu.PrefetchScalarGridSpec(
            num_scalar_prefetch=1,
            grid=(blocks,),
            in_specs=[
                pl.BlockSpec((1, rows, d), rel),
                pl.BlockSpec((1, rows, d), rel),
                pl.BlockSpec((3, rows, width), lambda i, me: (0, i, 0)),
                pl.BlockSpec(w.shape, lambda i, me: (0, 0)),
                pl.BlockSpec(order.shape, lambda i, me: (0, 0, 0)),
            ],
            out_specs=(
                pl.BlockSpec((1, rows, d), rel),
                pl.BlockSpec((1, rows, d), rel),
            )
            + tuple(whole(*shape) for shape in last),
            scratch_shapes=[
                pltpu.VMEM(w.shape, BF16),
                pltpu.VMEM((3, d, width), BF16),
                pltpu.VMEM((3, d, width), F32),
                pltpu.VMEM((8, d), F32),
                pltpu.VMEM((8, d), F32),
                pltpu.VMEM((8, width), F32),
            ],
        ),
        compiler_params=params(),
        cost_estimate=cost(4 * blocks * rows * d * 3 * width, 1.5e7),
        name="project_back",
    )(me, own, far, grad, w, order)


def pair_kernel(keep_ref, came_ref, own_ref, *send_refs):
    n = pl.program_id(0)
    total = keep_ref[0] + came_ref[0].astype(F32)

    @pl.when(n == 0)
    def _():
        own_ref[...] = total

    for m, ref in enumerate(send_refs):

        @pl.when(n == m + 1)
        def _(ref=ref):
            ref[...] = total.astype(BF16)


def pair_sum(keep, came):
    half, rows, d = keep.shape
    piece = pl.BlockSpec((1, rows, d), lambda n: (n, 0, 0))
    flat = pl.BlockSpec((rows, d), lambda n: (0, 0))
    return pl.pallas_call(
        pair_kernel,
        out_shape=(jax.ShapeDtypeStruct((rows, d), F32),)
        + (jax.ShapeDtypeStruct((rows, d), BF16),) * (half - 1),
        grid=(half,),
        in_specs=[piece, piece],
        out_specs=(flat,) * half,
        compiler_params=params(SMALL_LIMIT),
        cost_estimate=cost(0, 7e6),
        name="pair_sum",
    )(keep, came)


def finish_rows_kernel(side_ref, tok_ref, near_ref, near2_ref, away_ref, away2_ref, gh_ref, w_ref, out_ref, gain_ref):
    m = pl.program_id(0)

    @pl.when(m == 0)
    def _():
        gain_ref[...] = jnp.transpose(w_ref[:, 512:640].astype(F32))[64:72]

    n, scale = norm_parts(tok_ref[0].astype(F32))
    near = near_ref[...] + near2_ref[...].astype(F32)
    away = away_ref[...].astype(F32) + away2_ref[...].astype(F32)
    incoming = jnp.where(m == side_ref[0], near, away)
    out_ref[0] = gh_ref[0] + norm_back(incoming, gain_ref[0:1], n, scale)


def finish_rows(side, tok, near, near2, away, away2, gh, w):
    micro, rows, d = tok.shape
    piece = pl.BlockSpec((1, rows, d), lambda m, ix: (m, 0, 0))
    flat = pl.BlockSpec((rows, d), lambda m, ix: (0, 0))
    return pl.pallas_call(
        finish_rows_kernel,
        out_shape=jax.ShapeDtypeStruct((micro, rows, d), F32),
        grid_spec=pltpu.PrefetchScalarGridSpec(
            num_scalar_prefetch=1,
            grid=(micro,),
            in_specs=[piece, flat, flat, flat, flat, piece, pl.BlockSpec(w.shape, lambda m, ix: (0, 0))],
            out_specs=piece,
            scratch_shapes=[pltpu.VMEM((8, d), F32)],
        ),
        compiler_params=params(SMALL_LIMIT),
        cost_estimate=cost(0, 6e6),
        name="finish_rows",
    )(side, tok, near, near2, away, away2, gh, w)


def one_hot_order(sources, size):
    row = lax.broadcasted_iota(jnp.int32, (size, sources.shape[1]), 0)
    return jnp.where(row == sources, 1.0, 0.0).astype(BF16)


barrier = lax.optimization_barrier


def plus(a, b):
    return (a.astype(F32) + b.astype(F32)).astype(BF16)


def local(
    tokens,
    cotangent,
    ln1_gain,
    ln1_bias,
    qkv_weight,
    qkv_bias,
    out_weight,
    out_bias,
    ln2_gain,
    ln2_bias,
    fc_weight,
    fc_bias,
    proj_weight,
    proj_bias,
):
    sides = lax.axis_size("ctx")
    parts = lax.axis_size("tp")
    shards = lax.axis_size(("dp", "ctx"))
    group = sides * parts
    micro, _, rows, d = tokens.shape
    assert micro == sides == 2 and parts == 4
    side = lax.axis_index("ctx")
    slot = lax.axis_index("tp")
    me = side * parts + slot
    me_array = jnp.stack([me, side]).astype(jnp.int32)
    side_array = jnp.full((1,), side, jnp.int32)
    tall = qkv_weight.shape[1]
    heads, piece = qkv_bias.shape[1], qkv_bias.shape[2]
    width = heads * HD
    lines, strip = fc_bias.shape

    def swap(array, mask):
        return lax.ppermute(array, ("ctx", "tp"), [(n, n ^ mask) for n in range(group)])

    tok = tokens[:, 0]
    cot = cotangent[:, 0]

    vectors = jnp.stack([ln1_gain, ln1_bias, ln2_gain, ln2_bias, out_bias, proj_bias])
    wide, narrow = pack(fc_weight, proj_weight, out_weight, qkv_weight, vectors, qkv_bias, fc_bias, shards)

    gathered = lax.all_gather(wide, ("tp", "dp", "ctx"), axis=0, tiled=True)
    gathered = gathered.reshape(parts, d, wide.shape[1])

    mine = lax.dynamic_index_in_dim(tok, side, 0, keepdims=False)
    other = lax.dynamic_index_in_dim(tok, 1 - side, 0, keepdims=False)
    blocks = []
    for mask in range(0, group, 2):
        block = other if mask >= parts else mine
        blocks.append(block if mask == 0 else swap(block, mask))
    own = jnp.stack(blocks)
    far = swap(own, 1)

    w_in = lax.all_to_all(narrow, ("dp", "ctx"), 0, 0, tiled=True).reshape(d, narrow.shape[2])

    unit = lax.broadcasted_iota(jnp.int32, (1, 3 * width), 1)
    order_in = one_hot_order(unit % HD // piece * tall + unit // HD, d)
    unit = lax.broadcasted_iota(jnp.int32, (1, d), 1)
    order_fc = one_hot_order(unit % 128 // strip * tall + unit // 128, d)

    triple = project(me_array, own, far, w_in, order_in, piece)
    mixed, mixed_turned, level = attend(triple, rows)
    mix = lax.all_to_all(mixed, ("ctx", "tp"), 0, 0, tiled=True)

    tok_rows = tok.reshape(micro * rows, d)
    cot_rows = cot.reshape(micro * rows, d)
    y, grad_hidden, grad_mix, n2, act, gl, gb, vec, gfb = middle(
        tok_rows, cot_rows, mix, gathered, order_fc, strip
    )
    grad_mix = lax.all_to_all(grad_mix, ("ctx", "tp"), 0, 0, tiled=True)

    parcels = (n2, cot_rows, gb, mix, act, gl, vec, gfb, order_fc, strip)
    exchange = tall % 16 == 0
    if exchange:
        core, row = slot % 2, slot // 2
        index = lambda lane: jnp.stack([(1 - row) * 2 + lane, row * 2 + lane, side]).astype(jnp.int32)
        came = swap(weights("send", index(1 - core), *parcels), 1)
        a_send, a_keep, b_send, b_keep = weights("keep", index(core), *parcels, came=came, shards=shards)
        a_came, b_came = swap(a_send, 2), swap(b_send, parts)
    else:
        grad_wide = weights("all", jnp.arange(parts, dtype=jnp.int32), *parcels)
        grad_wide = lax.psum_scatter(
            grad_wide.reshape(parts * d, wide.shape[1]), ("tp", "dp", "ctx"), scatter_dimension=0, tiled=True
        )

    grad_triple = attend_back(triple, grad_mix, mixed_turned, level)
    if exchange:
        a_came, b_came, grad_triple = barrier((a_came, b_came, grad_triple))
        a_send, b_send = plus(a_keep[1], a_came[1]), plus(b_keep[1], b_came[1])
        a_send, b_send, grad_triple = barrier((a_send, b_send, grad_triple))
        a_keep, b_keep = plus(a_keep[0], a_came[0]), plus(b_keep[0], b_came[0])
        a_came, b_came = swap(a_send, parts), swap(b_send, 2)
    order_back = order_in.reshape(d, 3, width).transpose(1, 0, 2)
    back = project_back(me_array, own, far, grad_triple, w_in, order_back, piece, shards if exchange else 0)
    if exchange:
        a_came, b_came, back = barrier((a_came, b_came, back))
    keep, send = back[:2]

    send_came = swap(send, 1)
    if exchange:
        vec_in, n_keep, n_send = back[2:]
        n_came = swap(n_send, parts)
        vec_in = vec_in + swap(vec_in, 1)
        vec_in, send_came = barrier((vec_in, send_came))
        vec_came = swap(vec_in, 2)
    near, *sends = pair_sum(keep, send_came)
    arrived = [swap(sends[n - 1], 2 * n) for n in range(1, group // 2)]

    if exchange:
        vec_came, near = barrier((vec_came, near))
        vec_in = vec_in + vec_came
        vec_in = vec_in + swap(vec_in, parts)
        total = merge(side_array, a_keep, a_came, b_keep, b_came, n_keep, n_came, vec_in)
        totals = (lax.all_to_all(total, "dp", 0, 0, tiled=True),)
    else:
        grad_in = back[2].reshape(narrow.shape)
        totals = (grad_wide[None], lax.all_to_all(grad_in, ("dp", "ctx"), 0, 0, tiled=True))

    grad_tokens = finish_rows(
        side_array, tok, near, *arrived, grad_hidden.reshape(micro, rows, d), w_in
    )
    done = finish(totals, d, width, fc_bias.shape, qkv_bias.shape)
    fc_grad, proj_grad, out_grad, gain2, shift2, out_b, proj_b, fc_b, grad_qkv_weight, grad_qkv_bias, vec_in = done
    if not exchange:
        mask = parts // 2
        while mask:
            vec_in = vec_in + swap(vec_in, mask)
            mask //= 2
    return (
        y.reshape(micro, 1, rows, d),
        grad_tokens[:, None],
        vec_in[0],
        vec_in[1],
        grad_qkv_weight,
        grad_qkv_bias,
        out_grad,
        out_b[0],
        gain2[0],
        shift2[0],
        fc_grad,
        fc_b,
        proj_grad,
        proj_b[0],
    )


def solution(mesh):
    rows = P(None, "dp", ("ctx", "tp"), None)
    vector = P(("dp", "ctx"))
    joint = P(None, ("dp", "ctx"), "tp")
    joint_bias = P(None, "tp", ("dp", "ctx"))
    down = P("tp", ("dp", "ctx"))
    up = P(("dp", "ctx"), "tp")
    inner = (vector, vector, joint, joint_bias, down, vector, vector, vector, up, down, down, vector)
    return jax.shard_map(
        local,
        mesh=mesh,
        in_specs=(rows, rows) + inner,
        out_specs=(rows, rows) + inner,
        check_vma=False,
    )
```

```python
import functools

import jax
import jax.numpy as jnp
from jax import lax
from jax.experimental import pallas as pl
from jax.experimental.pallas import tpu as pltpu
from jax.sharding import PartitionSpec as P

HD = 64
EPS = 1e-05
LOG2E = 1.4426950408889634
F32 = jnp.float32
BF16 = jnp.bfloat16
VMEM_LIMIT = 60 * 1024 * 1024
SMALL_LIMIT = 60 * 1024 * 1024
EXT = 64


def dot(a, b):
    return lax.dot_general(a, b, (((1,), (0,)), ((), ())), preferred_element_type=F32)


def dot_nt(a, b):
    return lax.dot_general(a, b, (((1,), (1,)), ((), ())), preferred_element_type=F32)


def norm_parts(rows):
    mean = jnp.mean(rows, axis=-1, keepdims=True)
    centered = rows - mean
    spread = jnp.mean(centered * centered, axis=-1, keepdims=True)
    scale = lax.rsqrt(spread + EPS)
    return (centered * scale, scale)


def norm_back(incoming, gain, n, scale):
    e = incoming * gain
    return (e - jnp.mean(e, axis=-1, keepdims=True) - n * jnp.mean(e * n, axis=-1, keepdims=True)) * scale


def params(limit=VMEM_LIMIT):
    return pltpu.CompilerParams(dimension_semantics=("arbitrary",), vmem_limit_bytes=limit)


def cost(flops, moved, exps=0):
    return pl.CostEstimate(flops=int(flops), bytes_accessed=int(moved), transcendentals=int(exps))


def pack_kernel(fc_ref, pj_ref, out_ref, qkv_ref, vec_ref, qb_ref, fb_ref, wide_ref, narrow_ref):
    tall, d = fc_ref.shape
    width = out_ref.shape[0]
    copies = narrow_ref.shape[0]
    columns = jnp.transpose(vec_ref[...].astype(F32)).astype(BF16)
    wide_ref[:, :d] = fc_ref[...]
    wide_ref[:, d : 2 * d] = pj_ref[...]
    wide_ref[:, 2 * d : 2 * d + width] = jnp.transpose(out_ref[...].astype(F32)).astype(BF16)
    edge = 2 * d + width
    wide_ref[:, edge:] = jnp.zeros((tall, EXT), BF16)
    wide_ref[:, edge : edge + 4] = columns[:, 2:6]
    rows, strip = fb_ref.shape
    wide_ref[:rows, edge + 8 : edge + 8 + strip] = fb_ref[...]
    for s in range(3):
        narrow_ref[0, :, s * width : (s + 1) * width] = qkv_ref[s]
    edge = 3 * width
    narrow_ref[0, :, edge:] = jnp.zeros((tall, EXT), BF16)
    narrow_ref[0, :, edge : edge + 2] = columns[:, :2]
    heads, piece = qb_ref.shape[1:]
    for s in range(3):
        narrow_ref[0, s * heads : (s + 1) * heads, edge + 8 : edge + 8 + piece] = qb_ref[s]
    whole = narrow_ref[0]
    for n in range(1, copies):
        narrow_ref[n] = whole


def pack(fc, pj, out, qkv, vec, qb, fb, copies):
    tall, d = fc.shape
    width = out.shape[0]
    return pl.pallas_call(
        pack_kernel,
        out_shape=(
            jax.ShapeDtypeStruct((tall, 2 * d + width + EXT), BF16),
            jax.ShapeDtypeStruct((copies, tall, 3 * width + EXT), BF16),
        ),
        compiler_params=pltpu.CompilerParams(vmem_limit_bytes=SMALL_LIMIT),
        cost_estimate=cost(0, 2e6),
        name="pack",
    )(fc, pj, out, qkv, vec, qb, fb)


def pick_rows(table, period):
    line = lax.broadcasted_iota(jnp.int32, table.shape, 0)
    lane = lax.broadcasted_iota(jnp.int32, table.shape, 1)
    return jnp.sum(jnp.where(line == (lane & (period - 1)), table, 0.0), axis=0, keepdims=True)


def spread_rows(row, lines, period):
    shape = (lines, row.shape[1])
    line = lax.broadcasted_iota(jnp.int32, shape, 0)
    lane = lax.broadcasted_iota(jnp.int32, shape, 1)
    return jnp.where(line == (lane & (period - 1)), jnp.broadcast_to(row, shape), 0.0).astype(BF16)


def project_kernel(piece, me_ref, own_ref, far_ref, w_ref, order_ref, out_ref, vec_ref, bias_ref):
    i = pl.program_id(0)
    width = out_ref.shape[2]

    @pl.when(i == 0)
    def _():
        turned = jnp.transpose(w_ref[:, 512:640].astype(F32))
        vec_ref[...] = turned[64:72]
        table = dot(turned[72:80].astype(BF16), order_ref[...])
        bias_ref[...] = jnp.broadcast_to(pick_rows(table, piece), bias_ref.shape)

    far = ((i ^ me_ref[0]) & 1) == 1
    rows = jnp.where(far, far_ref[0], own_ref[0]).astype(F32)
    n, _ = norm_parts(rows)
    normed = (n * vec_ref[0:1] + vec_ref[1:2]).astype(BF16)
    full = dot(normed, w_ref[...])[:, : 3 * width] + bias_ref[0:1, :]
    full = full.astype(BF16)
    out_ref[0] = full[:, :width] * jnp.asarray(HD ** (-0.5), BF16)
    out_ref[1] = full[:, width : 2 * width]
    out_ref[2] = full[:, 2 * width :]


def project(me, own, far, w, order, piece):
    half, rows, d = own.shape
    blocks = 2 * half
    width = order.shape[1] // 3
    return pl.pallas_call(
        functools.partial(project_kernel, piece),
        out_shape=jax.ShapeDtypeStruct((3, blocks * rows, width), BF16),
        grid_spec=pltpu.PrefetchScalarGridSpec(
            num_scalar_prefetch=1,
            grid=(blocks,),
            in_specs=[
                pl.BlockSpec((1, rows, d), lambda i, me: ((i ^ me[0]) // 2, 0, 0)),
                pl.BlockSpec((1, rows, d), lambda i, me: ((i ^ me[0]) // 2, 0, 0)),
                pl.BlockSpec(w.shape, lambda i, me: (0, 0)),
                pl.BlockSpec(order.shape, lambda i, me: (0, 0)),
            ],
            out_specs=pl.BlockSpec((3, rows, width), lambda i, me: (0, i, 0)),
            scratch_shapes=[pltpu.VMEM((8, d), F32), pltpu.VMEM((8, 3 * width), F32)],
        ),
        compiler_params=params(),
        cost_estimate=cost(2 * blocks * rows * d * 3 * width, 8e6),
        name="project",
    )(me, own, far, w, order)


def head_mask(shape, h):
    lane = lax.broadcasted_iota(jnp.int32, shape, 1)
    return (lane >= h * HD) & (lane < (h + 1) * HD)


def attend_kernel(q_ref, k_ref, v_ref, o_ref, ot_ref, level_ref, vt_ref, qm_ref, m_ref, l_ref):
    i = pl.program_id(0)
    heads = q_ref.shape[2] // HD
    bq = q_ref.shape[1]
    half = bq // 2

    @pl.when(i == 0)
    def _():
        vt_ref[...] = jnp.transpose(v_ref[0].astype(F32)).astype(BF16)

    for h in range(heads):
        q = q_ref[0]
        qm_ref[h] = jnp.where(head_mask(q.shape, h), q, jnp.zeros_like(q))
    m_ref[...] = jnp.zeros_like(m_ref)
    l_ref[...] = jnp.zeros_like(l_ref)
    ot_ref[...] = jnp.zeros_like(ot_ref)

    def chunk(start, size, first, masked):
        cols = slice(first, bq)
        keys = k_ref[0, pl.ds(start, size), :]
        for h in range(heads):
            u = dot_nt(keys, qm_ref[h, first:bq, :]) * LOG2E
            if masked:
                key_pos = lax.broadcasted_iota(jnp.int32, u.shape, 0)
                row_pos = lax.broadcasted_iota(jnp.int32, u.shape, 1)
                allowed = key_pos <= row_pos
                u = jnp.where(allowed, u, 0.0)
            before = m_ref[h : h + 1, cols]
            peak = jnp.maximum(before, jnp.max(jnp.abs(u), axis=0, keepdims=True))
            fade = jnp.exp2(before - peak)
            upper = jnp.exp2(u - peak)
            lower = jnp.exp2(-peak - u)
            both = upper + lower
            if masked:
                both = jnp.where(allowed, both, 0.0)
            m_ref[h : h + 1, cols] = peak
            l_ref[h : h + 1, cols] = l_ref[h : h + 1, cols] * fade + jnp.sum(both, axis=0, keepdims=True)
            part = dot(vt_ref[h * HD : (h + 1) * HD, pl.ds(start, size)], (upper - lower).astype(BF16))
            ot_ref[h * HD : (h + 1) * HD, cols] = ot_ref[h * HD : (h + 1) * HD, cols] * fade + part

    def body(j, carry):
        chunk(pl.multiple_of(j * bq, bq), bq, 0, False)
        return carry

    lax.fori_loop(0, i, body, 0)
    base = pl.multiple_of(i * bq, bq)
    chunk(base, half, 0, True)
    chunk(pl.multiple_of(base + half, half), half, half, True)
    for h in range(heads):
        total = l_ref[h : h + 1, :]
        level_ref[h : h + 1, :] = m_ref[h : h + 1, :] + jnp.log2(total)
        ot_ref[h * HD : (h + 1) * HD, :] = ot_ref[h * HD : (h + 1) * HD, :] * (1.0 / total)
    rows = o_ref.shape[2]
    for n in range(bq // rows):
        o_ref[n] = ot_ref[:, n * rows : (n + 1) * rows].astype(BF16)


def attend(triple, rows):
    _, span, width = triple.shape
    bq = min(512, span)
    heads = width // HD
    return pl.pallas_call(
        attend_kernel,
        out_shape=(
            jax.ShapeDtypeStruct((span // rows, width, rows), BF16),
            jax.ShapeDtypeStruct((width, span), F32),
            jax.ShapeDtypeStruct((8, span), F32),
        ),
        grid=(span // bq,),
        in_specs=[
            pl.BlockSpec((1, bq, width), lambda i: (0, i, 0)),
            pl.BlockSpec((1, span, width), lambda i: (1, 0, 0)),
            pl.BlockSpec((1, span, width), lambda i: (2, 0, 0)),
        ],
        out_specs=(
            pl.BlockSpec((bq // rows, width, rows), lambda i: (i, 0, 0)),
            pl.BlockSpec((width, bq), lambda i: (0, i)),
            pl.BlockSpec((8, bq), lambda i: (0, i)),
        ),
        scratch_shapes=[
            pltpu.VMEM((width, span), BF16),
            pltpu.VMEM((heads, bq, width), BF16),
            pltpu.VMEM((8, bq), F32),
            pltpu.VMEM((8, bq), F32),
        ],
        compiler_params=params(),
        cost_estimate=cost(4 * span * span * width, 8e6, span * span * heads),
        name="attend",
    )(triple, triple, triple)


def attend_back_kernel(
    qkv_ref, grad_ref, ot_ref, level_ref, out_ref, qm_ref, gm_ref, kt_ref, dqt_ref, dot_ref, dk_ref, dv_ref
):
    j = pl.program_id(0)
    blocks = pl.num_programs(0)
    span, width = qkv_ref.shape[1:]
    rows = grad_ref.shape[2]
    heads = width // HD
    count = qm_ref.shape[0]
    b = span // count
    half = b // 2

    @pl.when(j == 0)
    def _():
        for n in range(span // rows):
            cols = slice(n * rows, (n + 1) * rows)
            turned = grad_ref[n].astype(F32)
            prod = turned * ot_ref[:, cols]
            for h in range(heads):
                dot_ref[h : h + 1, cols] = jnp.sum(prod[h * HD : (h + 1) * HD], axis=0, keepdims=True)
            g = jnp.transpose(turned).astype(BF16)
            at = n * rows % b
            for h in range(heads):
                mask = head_mask(g.shape, h)
                gm_ref[n * rows // b, h * b + at : h * b + at + rows, :] = jnp.where(mask, g, jnp.zeros_like(g))
        kt_ref[...] = jnp.transpose(qkv_ref[1].astype(F32)).astype(BF16)
        dqt_ref[...] = jnp.zeros_like(dqt_ref)
        for n in range(count):
            q = qkv_ref[0, n * b : (n + 1) * b, :]
            for h in range(heads):
                mask = head_mask(q.shape, h)
                qm_ref[n, h * b : (h + 1) * b, :] = jnp.where(mask, q, jnp.zeros_like(q))

    dk_ref[...] = jnp.zeros_like(dk_ref)
    dv_ref[...] = jnp.zeros_like(dv_ref)

    def chunk(i, key_first, key_size, first, masked):
        start = pl.multiple_of(j * b + key_first, half)
        keys = qkv_ref[1, pl.ds(start, key_size), :]
        vals = qkv_ref[2, pl.ds(start, key_size), :]
        cols = b - first
        at = pl.multiple_of(i * b + first, half)
        for h in range(heads):
            lo = h * b + first
            qm = qm_ref[i, lo : lo + cols, :]
            gm = gm_ref[i, lo : lo + cols, :]
            level = level_ref[h : h + 1, pl.ds(at, cols)]
            inner = dot_ref[h : h + 1, pl.ds(at, cols)]
            u = dot_nt(keys, qm) * LOG2E
            upper = jnp.exp2(u - level)
            lower = jnp.exp2(-level - u)
            gw = dot_nt(vals, gm)
            weights = upper - lower
            gs = upper * (gw - inner) + lower * (gw + inner)
            if masked:
                key_pos = lax.broadcasted_iota(jnp.int32, u.shape, 0)
                row_pos = lax.broadcasted_iota(jnp.int32, u.shape, 1)
                allowed = key_pos <= row_pos
                weights = jnp.where(allowed, weights, 0.0)
                gs = jnp.where(allowed, gs, 0.0)
            weights = weights.astype(BF16)
            gs = gs.astype(BF16)
            rows = slice(key_first, key_first + key_size)
            dv_ref[rows, :] += dot(weights, gm)
            dk_ref[rows, :] += dot(gs, qm)
            dqt_ref[h * HD : (h + 1) * HD, pl.ds(at, cols)] += dot(
                kt_ref[h * HD : (h + 1) * HD, pl.ds(start, key_size)], gs
            )

    def body(i, carry):
        chunk(i, 0, b, 0, False)
        return carry

    chunk(j, 0, half, 0, True)
    chunk(j, half, half, half, True)
    lax.fori_loop(j + 1, blocks, body, 0)
    here = pl.ds(pl.multiple_of(j * b, b), b)
    out_ref[1, here, :] = dk_ref[...].astype(BF16)
    out_ref[2, here, :] = dv_ref[...].astype(BF16)

    @pl.when(j == blocks - 1)
    def _():
        out_ref[0] = jnp.transpose(dqt_ref[...] * (HD ** (-0.5))).astype(BF16)


def attend_back(triple, grad, ot, level):
    _, span, width = triple.shape
    b = min(512, span)
    count = span // b
    heads = width // HD
    whole = lambda *shape: pl.BlockSpec(shape, lambda j: (0,) * len(shape))
    return pl.pallas_call(
        attend_back_kernel,
        out_shape=jax.ShapeDtypeStruct(triple.shape, BF16),
        grid=(count,),
        in_specs=[
            whole(*triple.shape),
            whole(*grad.shape),
            whole(*ot.shape),
            whole(*level.shape),
        ],
        out_specs=whole(*triple.shape),
        scratch_shapes=[
            pltpu.VMEM((count, heads * b, width), BF16),
            pltpu.VMEM((count, heads * b, width), BF16),
            pltpu.VMEM((width, span), BF16),
            pltpu.VMEM((width, span), F32),
            pltpu.VMEM((8, span), F32),
            pltpu.VMEM((b, width), F32),
            pltpu.VMEM((b, width), F32),
        ],
        compiler_params=params(),
        cost_estimate=cost(10 * span * span * width, 1e7, span * span * heads),
        name="attend_back",
    )(triple, grad, ot, level)


def gelu_parts(u):
    c = 0.7978845608028654
    square = u * u
    th = jnp.tanh(c * u * (1.0 + 0.044715 * square))
    near = 0.5 * (1.0 + th)
    slope = near + (0.5 * c) * u * (1.0 - th * th) * (1.0 + (3.0 * 0.044715) * square)
    return (u * near, slope)


def middle_kernel(
    strip,
    tok_ref,
    cot_ref,
    mix_ref,
    g_ref,
    gout_ref,
    order_ref,
    y_ref,
    gh_ref,
    dmix_ref,
    n2_ref,
    act_ref,
    gl_ref,
    gb_ref,
    vec_ref,
    gfb_ref,
    hid_ref,
    acc_ref,
    back_ref,
    ext_ref,
):
    t = pl.program_id(0)
    steps = pl.num_programs(0)
    half = mix_ref.shape[2]
    parts = gout_ref.shape[0]
    d = tok_ref.shape[1]
    width = mix_ref.shape[1]

    @pl.when(t == 0)
    def _():
        ext_ref[...] = jnp.transpose(gout_ref[0, :, 128:256].astype(F32))[64:72]
        total = tok_ref[...].astype(F32) + ext_ref[2:3]
        for s in range(parts):
            lhs = jnp.concatenate([mix_ref[s], mix_ref[parts + s]], axis=1)
            lhs = jnp.transpose(lhs.astype(F32)).astype(BF16)
            total = total + dot_nt(lhs, gout_ref[s, :, :width])
        hid_ref[...] = total
        n, _ = norm_parts(total)
        n2_ref[...] = (n * ext_ref[0:1] + ext_ref[1:2]).astype(BF16)
        acc_ref[...] = total + ext_ref[3:4]
        back_ref[...] = jnp.zeros_like(back_ref)

    ext = jnp.transpose(g_ref[0, :, 2 * d + 128 : 2 * d + 256].astype(F32))[72:88].astype(BF16)
    bias = pick_rows(dot(ext, order_ref[...]), strip)
    fc = g_ref[0, :, :d]
    pj = g_ref[0, :, d : 2 * d]
    lifted = dot(n2_ref[...], fc) + bias
    act, slope = gelu_parts(lifted)
    act = act.astype(BF16)
    act_ref[0] = act
    gl32 = dot(cot_ref[...], pj) * slope
    gl = gl32.astype(BF16)
    gl_ref[0] = gl
    gfb_ref[0, 0:1, :] = jnp.sum(gl.astype(F32), axis=0, keepdims=True)
    acc_ref[...] += dot_nt(act, pj)
    back_ref[...] += dot_nt(gl, fc)

    @pl.when(t == steps - 1)
    def _():
        y_ref[...] = acc_ref[...].astype(BF16)
        n, scale = norm_parts(hid_ref[...])
        back = back_ref[...]
        cot = cot_ref[...].astype(F32)
        gh = cot + norm_back(back, ext_ref[0:1], n, scale)
        gh_ref[...] = gh
        gb = gh.astype(BF16)
        gb_ref[...] = gb
        vec_ref[0:1, :] = jnp.sum(back * n, axis=0, keepdims=True)
        vec_ref[1:2, :] = jnp.sum(back, axis=0, keepdims=True)
        vec_ref[2:3, :] = jnp.sum(gb.astype(F32), axis=0, keepdims=True)
        vec_ref[3:4, :] = jnp.sum(cot, axis=0, keepdims=True)
        vec_ref[4:8, :] = jnp.zeros((4, d), F32)
        for s in range(parts):
            dm = jnp.transpose(dot(gb, gout_ref[s, :, :width])).astype(BF16)
            dmix_ref[s] = dm[:, :half]
            dmix_ref[parts + s] = dm[:, half:]


def middle(tok, cot, mix, gathered, order, strip):
    rows, d = tok.shape
    parts = gathered.shape[0]
    cols = gathered.shape[2]
    whole = lambda *shape: pl.BlockSpec(shape, lambda t: (0,) * len(shape))
    piece = lambda *shape: pl.BlockSpec(shape, lambda t: (t,) + (0,) * (len(shape) - 1))
    sds = jax.ShapeDtypeStruct
    return pl.pallas_call(
        functools.partial(middle_kernel, strip),
        out_shape=(
            sds((rows, d), BF16),
            sds((rows, d), F32),
            sds(mix.shape, BF16),
            sds((rows, d), BF16),
            sds((parts, rows, d), BF16),
            sds((parts, rows, d), BF16),
            sds((rows, d), BF16),
            sds((8, d), F32),
            sds((parts, 8, d), F32),
        ),
        grid=(parts,),
        in_specs=[
            whole(rows, d),
            whole(rows, d),
            whole(*mix.shape),
            piece(1, d, cols),
            pl.BlockSpec((parts, d, 256), lambda t: (0, 0, cols // 256 - 1)),
            whole(*order.shape),
        ],
        out_specs=(
            whole(rows, d),
            whole(rows, d),
            whole(*mix.shape),
            whole(rows, d),
            piece(1, rows, d),
            piece(1, rows, d),
            whole(rows, d),
            whole(8, d),
            piece(1, 8, d),
        ),
        scratch_shapes=[
            pltpu.VMEM((rows, d), F32),
            pltpu.VMEM((rows, d), F32),
            pltpu.VMEM((rows, d), F32),
            pltpu.VMEM((8, d), F32),
        ],
        compiler_params=params(),
        cost_estimate=cost(2 * rows * d * d * 18, 3e7),
        name="middle",
    )(tok, cot, mix, gathered, gathered, order)


def weights_kernel(
    mode, strip, index_ref, n2_ref, cot_ref, gb_ref, mix_ref, act_ref, gl_ref, vec_ref, gfb_ref, order_ref, *rest
):
    s = pl.program_id(0)
    d = n2_ref.shape[1]
    width = mix_ref.shape[2]
    cols = 2 * d + width + EXT
    nt_ref, ct_ref, bt_ref = rest[-3:]

    @pl.when(s == 0)
    def _():
        nt_ref[...] = jnp.transpose(n2_ref[...].astype(F32)).astype(BF16)
        ct_ref[...] = jnp.transpose(cot_ref[...].astype(F32)).astype(BF16)
        bt_ref[...] = jnp.transpose(gb_ref[...].astype(F32)).astype(BF16)

    mix = jnp.concatenate([mix_ref[0, 0], mix_ref[1, 0]], axis=1)
    turned = dot_nt(spread_rows(gfb_ref[0, 0:1], 16, strip), order_ref[...])
    tall = jnp.concatenate([vec_ref[...], turned, jnp.zeros((EXT - 24, d), F32)], axis=0)
    if mode != "keep":
        out_ref = rest[0]
        out_ref[0, :, :d] = dot(nt_ref[...], gl_ref[0]).astype(BF16)
        out_ref[0, :, d : 2 * d] = dot(ct_ref[...], act_ref[0]).astype(BF16)
        out_ref[0, :, 2 * d : 2 * d + width] = dot_nt(bt_ref[...], mix).astype(BF16)
        out_ref[0, :, 2 * d + width :] = jnp.transpose(tall).astype(BF16)
        return
    came_ref, as_ref, ak_ref, bs_ref, bk_ref, sum_ref = rest[:6]
    sum_ref[:, 2 * d : 2 * d + width] = dot_nt(bt_ref[...], mix).astype(BF16)
    sum_ref[:, 2 * d + width :] = jnp.transpose(tall).astype(BF16)
    sum_ref[:, 2 * d :] = (sum_ref[:, 2 * d :].astype(F32) + came_ref[0, :, 2 * d :].astype(F32)).astype(BF16)
    sum_ref[:, :d] = (dot(nt_ref[...], gl_ref[0]) + came_ref[0, :, :d].astype(F32)).astype(BF16)
    sum_ref[:, d : 2 * d] = (dot(ct_ref[...], act_ref[0]) + came_ref[0, :, d : 2 * d].astype(F32)).astype(BF16)
    depth, step = as_ref.shape[1], as_ref.shape[2]
    cut = cols // 2

    def block(xr, zr):
        at = (zr * 2 + (xr ^ index_ref[2])) * step
        return pl.ds(pl.multiple_of(at, 16), step)

    for zr in range(depth):
        bk_ref[0, zr] = sum_ref[block(0, zr), cut:]
        bs_ref[0, zr] = sum_ref[block(1, zr), cut:]

    @pl.when(s == 0)
    def _():
        for xr in range(2):
            for zr in range(depth):
                as_ref[xr, zr] = sum_ref[block(xr, zr), :cut]

    @pl.when(s == 1)
    def _():
        for xr in range(2):
            for zr in range(depth):
                ak_ref[xr, zr] = sum_ref[block(xr, zr), :cut]


def weights(mode, index, n2, cot, gb, mix, act, gl, vec, gfb, order, strip, came=None, shards=None):
    rows, d = n2.shape
    parts = act.shape[0]
    width = mix.shape[1]
    cols = 2 * d + width + EXT
    steps = parts if mode == "all" else 2
    whole = lambda *shape: pl.BlockSpec(shape, lambda s, ix: (0,) * len(shape))
    piece = lambda *shape: pl.BlockSpec(shape, lambda s, ix: (ix[s],) + (0,) * (len(shape) - 1))
    mix = mix.reshape(mix.shape[0] // parts, parts, width, mix.shape[2])
    operands = [index, n2, cot, gb, mix, act, gl, vec, gfb, order]
    specs = [
        whole(rows, d),
        whole(rows, d),
        whole(rows, d),
        pl.BlockSpec((mix.shape[0], 1, width, mix.shape[3]), lambda s, ix: (0, ix[s], 0, 0)),
        piece(1, rows, d),
        piece(1, rows, d),
        whole(8, d),
        piece(1, 8, d),
        whole(*order.shape),
    ]
    scratch = [pltpu.VMEM((d, rows), BF16) for _ in range(3)]
    if mode == "keep":
        operands.append(came)
        specs.append(pl.BlockSpec((1, d, cols), lambda s, ix: (s, 0, 0)))
        block = (2, shards // 2, d // shards, cols // 2)
        sds = jax.ShapeDtypeStruct(block, BF16)
        out_shape = (sds,) * 4
        turn = pl.BlockSpec((1,) + block[1:], lambda s, ix: (1 - s, 0, 0, 0))
        out_specs = (whole(*block), whole(*block), turn, turn)
        scratch = [pltpu.VMEM((d, cols), BF16)] + scratch
    else:
        out_shape = jax.ShapeDtypeStruct((steps, d, cols), BF16)
        out_specs = pl.BlockSpec((1, d, cols), lambda s, ix: (s, 0, 0))
    return pl.pallas_call(
        functools.partial(weights_kernel, mode, strip),
        out_shape=out_shape,
        grid_spec=pltpu.PrefetchScalarGridSpec(
            num_scalar_prefetch=1,
            grid=(steps,),
            in_specs=specs,
            out_specs=out_specs,
            scratch_shapes=scratch,
        ),
        compiler_params=params(),
        cost_estimate=cost(2 * rows * d * cols * steps, 6e6 * steps),
        name="weights_" + mode,
    )(*operands)


def merge_kernel(place_ref, ak_ref, ac_ref, bk_ref, bc_ref, nk_ref, nc_ref, vec_ref, *rest):
    n = pl.program_id(0)
    turn_ref = rest[-1]
    step, cut = ak_ref.shape[1:]
    at = 2 * cut + nk_ref.shape[2] - EXT

    @pl.when(n == 0)
    def _():
        turn_ref[...] = jnp.transpose(vec_ref[...])

    here = pl.ds(pl.multiple_of((2 * (n ^ place_ref[1]) + place_ref[0]) * step, 8), step)
    for m, out_ref in enumerate(rest[:-1]):

        @pl.when(n == m)
        def _(out_ref=out_ref):
            out_ref[:, :cut] = (ak_ref[0].astype(F32) + ac_ref[0].astype(F32)).astype(BF16)
            out_ref[:, cut : 2 * cut] = (bk_ref[0].astype(F32) + bc_ref[0].astype(F32)).astype(BF16)
            out_ref[:, 2 * cut :] = (nk_ref[0].astype(F32) + nc_ref[0].astype(F32)).astype(BF16)
            out_ref[:, at : at + 8] = turn_ref[here, :].astype(BF16)


def merge(place, *parts):
    depth, step, cut = parts[0].shape
    cols = 2 * cut + parts[4].shape[2]
    piece = lambda array: pl.BlockSpec((1,) + array.shape[1:], lambda n, ix: (n ^ ix[1], 0, 0))
    whole = lambda array: pl.BlockSpec(array.shape, lambda n, ix: (0, 0))
    out = jax.ShapeDtypeStruct((step, cols), BF16)
    return pl.pallas_call(
        merge_kernel,
        out_shape=(out,) * depth,
        grid_spec=pltpu.PrefetchScalarGridSpec(
            num_scalar_prefetch=1,
            grid=(depth,),
            in_specs=[piece(p) for p in parts[:-1]] + [whole(parts[-1])],
            out_specs=(whole(out),) * depth,
            scratch_shapes=[pltpu.VMEM(parts[-1].shape[::-1], F32)],
        ),
        compiler_params=params(),
        cost_estimate=cost(0, 6e6),
        name="merge",
    )(place, *parts)


def finish_wide(t, fc_ref, pj_ref, out_ref, g_ref, b_ref, ob_ref, pb_ref, fb_ref):
    d = fc_ref.shape[1]
    width = out_ref.shape[0]
    fc_ref[...] = t[:, :d]
    pj_ref[...] = t[:, d : 2 * d]
    rest = jnp.transpose(t[:, 2 * d : 2 * d + width + EXT])
    out_ref[...] = rest[:width]
    g_ref[...] = rest[width : width + 1]
    b_ref[...] = rest[width + 1 : width + 2]
    ob_ref[...] = rest[width + 2 : width + 3]
    pb_ref[...] = rest[width + 3 : width + 4]
    rows, strip = fb_ref.shape
    at = 2 * d + width + 8
    fb_ref[...] = t[:rows, at : at + strip]


def finish_narrow(t, qkv_ref, qb_ref, gain_ref, shift_ref):
    width = qkv_ref.shape[2]
    for s in range(3):
        qkv_ref[s] = t[:, s * width : (s + 1) * width]
    heads, piece = qb_ref.shape[1:]
    edge = 3 * width + 8
    for s in range(3):
        qb_ref[s] = t[s * heads : (s + 1) * heads, edge : edge + piece]
    turned = jnp.transpose(t[:, 512:640])
    gain_ref[...] = turned[64:65]
    shift_ref[...] = turned[65:66]


def total_of(ref):
    total = ref[0].astype(F32)
    for n in range(1, ref.shape[0]):
        total = total + ref[n].astype(F32)
    return total


def finish_kernel(*refs):
    parts, outs = refs[:-12], refs[-12:]
    if len(parts) == 2:
        finish_wide(total_of(parts[0]), *outs[:8])
        finish_narrow(total_of(parts[1]), *outs[8:])
        return
    total = parts[0][...].astype(F32)
    for ref in parts[1:]:
        total = total + ref[...].astype(F32)
    edge = total.shape[1] - 640
    finish_wide(total[:, :edge], *outs[:8])
    finish_narrow(total[:, edge:], *outs[8:])


def finish(parts, d, width, fc_bias_shape, qkv_bias_shape):
    tall = parts[0].shape[-2]
    sds = lambda *shape: jax.ShapeDtypeStruct(shape, F32)
    return pl.pallas_call(
        finish_kernel,
        out_shape=(
            sds(tall, d),
            sds(tall, d),
            sds(width, tall),
            sds(1, tall),
            sds(1, tall),
            sds(1, tall),
            sds(1, tall),
            sds(*fc_bias_shape),
            sds(3, tall, width),
            sds(*qkv_bias_shape),
            sds(1, tall),
            sds(1, tall),
        ),
        compiler_params=pltpu.CompilerParams(vmem_limit_bytes=SMALL_LIMIT),
        cost_estimate=cost(0, 4e6),
        name="finish",
    )(*parts)


def project_back_kernel(piece, me_ref, own_ref, far_ref, grad_ref, w_ref, order_ref, keep_ref, send_ref, sum_ref, *rest):
    parted = rest[:-6]
    dw_ref, w3_ref, dw3_ref, gain_ref, vec_ref, bias_ref = rest[-6:]
    i = pl.program_id(0)
    steps = pl.num_programs(0)
    width = grad_ref.shape[2]
    d = w_ref.shape[0]

    @pl.when(i == 0)
    def _():
        gain_ref[...] = jnp.transpose(w_ref[:, 512:640].astype(F32))[64:72]
        for s in range(3):
            w3_ref[s] = w_ref[:, s * width : (s + 1) * width]
        dw3_ref[...] = jnp.zeros_like(dw3_ref)
        vec_ref[...] = jnp.zeros_like(vec_ref)
        bias_ref[...] = jnp.zeros_like(bias_ref)

    far = ((i ^ me_ref[0]) & 1) == 1
    rows = jnp.where(far, far_ref[0], own_ref[0]).astype(F32)
    n, _ = norm_parts(rows)
    normed = n * gain_ref[0:1] + gain_ref[1:2]
    turned = jnp.transpose(normed).astype(BF16)
    part = dot_nt(grad_ref[0], w3_ref[0])
    for s in range(1, 3):
        part = part + dot_nt(grad_ref[s], w3_ref[s])
    for s in range(3):
        dw3_ref[s] += dot(turned, grad_ref[s])
        bias_ref[s : s + 1, :] += jnp.sum(grad_ref[s].astype(F32), axis=0, keepdims=True)
    vec_ref[0:1, :] += jnp.sum(part * n, axis=0, keepdims=True)
    vec_ref[1:2, :] += jnp.sum(part, axis=0, keepdims=True)

    @pl.when(far)
    def _():
        send_ref[0] = part.astype(BF16)

    @pl.when(jnp.logical_not(far))
    def _():
        keep_ref[0] = part

    @pl.when(i == steps - 1)
    def _():
        turned_bias = jnp.zeros((8, d), F32)
        for s in range(3):
            dw_ref[:, s * width : (s + 1) * width] = dw3_ref[s].astype(BF16)
            spread = spread_rows(bias_ref[s : s + 1, :], 8, piece)
            turned_bias = turned_bias + dot_nt(spread, order_ref[s])
        tall = jnp.concatenate([vec_ref[...], turned_bias, jnp.zeros((EXT - 16, d), F32)], axis=0)
        dw_ref[:, 3 * width :] = jnp.transpose(tall).astype(BF16)
        if not parted:
            sum_ref[...] = dw_ref[...]
            return
        sum_ref[...] = vec_ref[...]
        near_ref, away_ref = parted
        depth, step = near_ref.shape[:2]
        for z in range(depth):
            near_ref[z] = dw_ref[pl.ds(pl.multiple_of((2 * z + me_ref[1]) * step, 16), step), :]
            away_ref[z] = dw_ref[pl.ds(pl.multiple_of((2 * z + 1 - me_ref[1]) * step, 16), step), :]


def project_back(me, own, far, grad, w, order, piece, shards):
    half, rows, d = own.shape
    width = grad.shape[2]
    blocks = 2 * half
    sds = jax.ShapeDtypeStruct
    rel = lambda i, me: ((i ^ me[0]) // 2, 0, 0)
    whole = lambda *shape: pl.BlockSpec(shape, lambda i, me: (0,) * len(shape))
    last = [w.shape]
    if shards:
        last = [(8, d)] + [(shards // 2, d // shards, w.shape[1])] * 2
    return pl.pallas_call(
        functools.partial(project_back_kernel, piece),
        out_shape=(
            sds((half, rows, d), F32),
            sds((half, rows, d), BF16),
        )
        + tuple(sds(shape, BF16 if len(shape) == 3 or not shards else F32) for shape in last),
        grid_spec=pltpu.PrefetchScalarGridSpec(
            num_scalar_prefetch=1,
            grid=(blocks,),
            in_specs=[
                pl.BlockSpec((1, rows, d), rel),
                pl.BlockSpec((1, rows, d), rel),
                pl.BlockSpec((3, rows, width), lambda i, me: (0, i, 0)),
                pl.BlockSpec(w.shape, lambda i, me: (0, 0)),
                pl.BlockSpec(order.shape, lambda i, me: (0, 0, 0)),
            ],
            out_specs=(
                pl.BlockSpec((1, rows, d), rel),
                pl.BlockSpec((1, rows, d), rel),
            )
            + tuple(whole(*shape) for shape in last),
            scratch_shapes=[
                pltpu.VMEM(w.shape, BF16),
                pltpu.VMEM((3, d, width), BF16),
                pltpu.VMEM((3, d, width), F32),
                pltpu.VMEM((8, d), F32),
                pltpu.VMEM((8, d), F32),
                pltpu.VMEM((8, width), F32),
            ],
        ),
        compiler_params=params(),
        cost_estimate=cost(4 * blocks * rows * d * 3 * width, 1.5e7),
        name="project_back",
    )(me, own, far, grad, w, order)


def pair_kernel(keep_ref, came_ref, own_ref, *send_refs):
    n = pl.program_id(0)
    total = keep_ref[0] + came_ref[0].astype(F32)

    @pl.when(n == 0)
    def _():
        own_ref[...] = total

    for m, ref in enumerate(send_refs):

        @pl.when(n == m + 1)
        def _(ref=ref):
            ref[...] = total.astype(BF16)


def pair_sum(keep, came):
    half, rows, d = keep.shape
    piece = pl.BlockSpec((1, rows, d), lambda n: (n, 0, 0))
    flat = pl.BlockSpec((rows, d), lambda n: (0, 0))
    return pl.pallas_call(
        pair_kernel,
        out_shape=(jax.ShapeDtypeStruct((rows, d), F32),)
        + (jax.ShapeDtypeStruct((rows, d), BF16),) * (half - 1),
        grid=(half,),
        in_specs=[piece, piece],
        out_specs=(flat,) * half,
        compiler_params=params(SMALL_LIMIT),
        cost_estimate=cost(0, 7e6),
        name="pair_sum",
    )(keep, came)


def finish_rows_kernel(side_ref, tok_ref, near_ref, near2_ref, away_ref, away2_ref, gh_ref, w_ref, out_ref, gain_ref):
    m = pl.program_id(0)

    @pl.when(m == 0)
    def _():
        gain_ref[...] = jnp.transpose(w_ref[:, 512:640].astype(F32))[64:72]

    n, scale = norm_parts(tok_ref[0].astype(F32))
    near = near_ref[...] + near2_ref[...].astype(F32)
    away = away_ref[...].astype(F32) + away2_ref[...].astype(F32)
    incoming = jnp.where(m == side_ref[0], near, away)
    out_ref[0] = gh_ref[0] + norm_back(incoming, gain_ref[0:1], n, scale)


def finish_rows(side, tok, near, near2, away, away2, gh, w):
    micro, rows, d = tok.shape
    piece = pl.BlockSpec((1, rows, d), lambda m, ix: (m, 0, 0))
    flat = pl.BlockSpec((rows, d), lambda m, ix: (0, 0))
    return pl.pallas_call(
        finish_rows_kernel,
        out_shape=jax.ShapeDtypeStruct((micro, rows, d), F32),
        grid_spec=pltpu.PrefetchScalarGridSpec(
            num_scalar_prefetch=1,
            grid=(micro,),
            in_specs=[piece, flat, flat, flat, flat, piece, pl.BlockSpec(w.shape, lambda m, ix: (0, 0))],
            out_specs=piece,
            scratch_shapes=[pltpu.VMEM((8, d), F32)],
        ),
        compiler_params=params(SMALL_LIMIT),
        cost_estimate=cost(0, 6e6),
        name="finish_rows",
    )(side, tok, near, near2, away, away2, gh, w)


def one_hot_order(sources, size):
    row = lax.broadcasted_iota(jnp.int32, (size, sources.shape[1]), 0)
    return jnp.where(row == sources, 1.0, 0.0).astype(BF16)


barrier = lax.optimization_barrier


def plus(a, b):
    return (a.astype(F32) + b.astype(F32)).astype(BF16)


def local(
    tokens,
    cotangent,
    ln1_gain,
    ln1_bias,
    qkv_weight,
    qkv_bias,
    out_weight,
    out_bias,
    ln2_gain,
    ln2_bias,
    fc_weight,
    fc_bias,
    proj_weight,
    proj_bias,
):
    sides = lax.axis_size("ctx")
    parts = lax.axis_size("tp")
    shards = lax.axis_size(("dp", "ctx"))
    group = sides * parts
    micro, _, rows, d = tokens.shape
    assert micro == sides == 2 and parts == 4
    side = lax.axis_index("ctx")
    slot = lax.axis_index("tp")
    me = side * parts + slot
    me_array = jnp.stack([me, side]).astype(jnp.int32)
    side_array = jnp.full((1,), side, jnp.int32)
    tall = qkv_weight.shape[1]
    heads, piece = qkv_bias.shape[1], qkv_bias.shape[2]
    width = heads * HD
    lines, strip = fc_bias.shape

    deep = lax.axis_index("dp")
    depth = lax.axis_size("dp")

    def swap_deep(array, mask):
        return lax.ppermute(array, "dp", [(n, n ^ mask) for n in range(depth)])

    def swap(array, mask):
        return lax.ppermute(array, ("ctx", "tp"), [(n, n ^ mask) for n in range(group)])

    tok = tokens[:, 0]
    cot = cotangent[:, 0]

    vectors = jnp.stack([ln1_gain, ln1_bias, ln2_gain, ln2_bias, out_bias, proj_bias])
    wide, narrow = pack(fc_weight, proj_weight.T, out_weight, qkv_weight, vectors, qkv_bias, fc_bias, shards)

    gathered = lax.all_gather(wide, ("tp", "dp", "ctx"), axis=0, tiled=True)
    gathered = gathered.reshape(parts, d, wide.shape[1])

    mine = lax.dynamic_index_in_dim(tok, side, 0, keepdims=False)
    other = lax.dynamic_index_in_dim(tok, 1 - side, 0, keepdims=False)
    blocks = []
    for mask in range(0, group, 2):
        block = other if mask >= parts else mine
        blocks.append(block if mask == 0 else swap(block, mask))
    own = jnp.stack(blocks)
    far = swap(own, 1)

    w_in = lax.all_to_all(narrow, ("dp", "ctx"), 0, 0, tiled=True).reshape(d, narrow.shape[2])

    unit = lax.broadcasted_iota(jnp.int32, (1, 3 * width), 1)
    order_in = one_hot_order(unit % HD // piece * tall + unit // HD, d)
    unit = lax.broadcasted_iota(jnp.int32, (1, d), 1)
    order_fc = one_hot_order(unit % 128 // strip * tall + unit // 128, d)

    order_back = order_in.reshape(d, 3, width).transpose(1, 0, 2)
    far, order_in, order_fc, order_back = barrier((far, order_in, order_fc, order_back))

    triple = project(me_array, own, far, w_in, order_in, piece)
    mixed, mixed_turned, level = attend(triple, rows)
    mix = lax.all_to_all(mixed, ("ctx", "tp"), 0, 0, tiled=True)

    tok_rows = tok.reshape(micro * rows, d)
    cot_rows = cot.reshape(micro * rows, d)
    y, grad_hidden, grad_mix, n2, act, gl, gb, vec, gfb = middle(
        tok_rows, cot_rows, mix, gathered, order_fc, strip
    )
    grad_mix = lax.all_to_all(grad_mix, ("ctx", "tp"), 0, 0, tiled=True)

    parcels = (n2, cot_rows, gb, mix, act, gl, vec, gfb, order_fc, strip)
    exchange = tall % 16 == 0 and depth & (depth - 1) == 0
    if exchange:
        core, row = slot % 2, slot // 2
        index = lambda lane: jnp.stack([(1 - row) * 2 + lane, row * 2 + lane, side]).astype(jnp.int32)
        came = swap(weights("send", index(1 - core), *parcels), 1)
        a_send, a_keep, b_send, b_keep = weights("keep", index(core), *parcels, came=came, shards=shards)
        a_came, b_came = swap(a_send, 2), swap(b_send, parts)
    else:
        grad_wide = weights("all", jnp.arange(parts, dtype=jnp.int32), *parcels)
        grad_wide = lax.psum_scatter(
            grad_wide.reshape(parts * d, wide.shape[1]), ("tp", "dp", "ctx"), scatter_dimension=0, tiled=True
        )

    grad_triple = attend_back(triple, grad_mix, mixed_turned, level)
    if exchange:
        a_came, b_came, grad_triple = barrier((a_came, b_came, grad_triple))
        a_send, b_send = plus(a_keep[1], a_came[1]), plus(b_keep[1], b_came[1])
        a_send, b_send, grad_triple = barrier((a_send, b_send, grad_triple))
        a_keep, b_keep = plus(a_keep[0], a_came[0]), plus(b_keep[0], b_came[0])
        a_came, b_came = swap(a_send, parts), swap(b_send, 2)
    back = project_back(me_array, own, far, grad_triple, w_in, order_back, piece, shards if exchange else 0)
    if exchange:
        a_came, b_came, back = barrier((a_came, b_came, back))
    keep, send = back[:2]

    send_came = swap(send, 1)
    if exchange:
        vec_in, n_keep, n_send = back[2:]
        n_came = swap(n_send, parts)
        vec_in = vec_in + swap(vec_in, 1)
        vec_in, send_came = barrier((vec_in, send_came))
        vec_came = swap(vec_in, 2)
    near, *sends = pair_sum(keep, send_came)
    arrived = [swap(sends[n - 1], 2 * n) for n in range(1, group // 2)]

    if exchange:
        vec_came, near = barrier((vec_came, near))
        vec_in = vec_in + vec_came
        vec_in = vec_in + swap(vec_in, parts)
        place = jnp.stack([side, deep]).astype(jnp.int32)
        totals = merge(place, a_keep, a_came, b_keep, b_came, n_keep, n_came, vec_in)
        totals = [totals[0]] + [swap_deep(totals[n], n) for n in range(1, depth)]
    else:
        grad_in = back[2].reshape(narrow.shape)
        totals = (grad_wide[None], lax.all_to_all(grad_in, ("dp", "ctx"), 0, 0, tiled=True))

    grad_tokens = finish_rows(
        side_array, tok, near, *arrived, grad_hidden.reshape(micro, rows, d), w_in
    )
    done = finish(totals, d, width, fc_bias.shape, qkv_bias.shape)
    fc_grad, proj_grad, out_grad, gain2, shift2, out_b, proj_b, fc_b, grad_qkv_weight, grad_qkv_bias, *pair = done
    if not exchange:
        mask = parts // 2
        while mask:
            pair = [v + swap(v, mask) for v in pair]
            mask //= 2
    return (
        y.reshape(micro, 1, rows, d),
        grad_tokens[:, None],
        pair[0][0],
        pair[1][0],
        grad_qkv_weight,
        grad_qkv_bias,
        out_grad,
        out_b[0],
        gain2[0],
        shift2[0],
        fc_grad,
        fc_b,
        proj_grad.T,
        proj_b[0],
    )


def solution(mesh):
    rows = P(None, "dp", ("ctx", "tp"), None)
    vector = P(("dp", "ctx"))
    joint = P(None, ("dp", "ctx"), "tp")
    joint_bias = P(None, "tp", ("dp", "ctx"))
    down = P("tp", ("dp", "ctx"))
    up = P(("dp", "ctx"), "tp")
    inner = (vector, vector, joint, joint_bias, down, vector, vector, vector, up, down, down, vector)
    return jax.shard_map(
        local,
        mesh=mesh,
        in_specs=(rows, rows) + inner,
        out_specs=(rows, rows) + inner,
        check_vma=False,
    )
```

```python
import functools

import jax
import jax.numpy as jnp
from jax import lax
from jax.experimental import pallas as pl
from jax.experimental.pallas import tpu as pltpu
from jax.sharding import PartitionSpec as P

HD = 64
EPS = 1e-05
LOG2E = 1.4426950408889634
F32 = jnp.float32
BF16 = jnp.bfloat16
VMEM_LIMIT = 60 * 1024 * 1024
SMALL_LIMIT = 60 * 1024 * 1024
EXT = 64


def dot(a, b):
    return lax.dot_general(a, b, (((1,), (0,)), ((), ())), preferred_element_type=F32)


def dot_nt(a, b):
    return lax.dot_general(a, b, (((1,), (1,)), ((), ())), preferred_element_type=F32)


def norm_parts(rows):
    mean = jnp.mean(rows, axis=-1, keepdims=True)
    centered = rows - mean
    spread = jnp.mean(centered * centered, axis=-1, keepdims=True)
    scale = lax.rsqrt(spread + EPS)
    return (centered * scale, scale)


def norm_back(incoming, gain, n, scale):
    e = incoming * gain
    return (e - jnp.mean(e, axis=-1, keepdims=True) - n * jnp.mean(e * n, axis=-1, keepdims=True)) * scale


def params(limit=VMEM_LIMIT):
    return pltpu.CompilerParams(dimension_semantics=("arbitrary",), vmem_limit_bytes=limit)


def cost(flops, moved, exps=0):
    return pl.CostEstimate(flops=int(flops), bytes_accessed=int(moved), transcendentals=int(exps))


def pack_kernel(fc_ref, pj_ref, out_ref, qkv_ref, vec_ref, qb_ref, fb_ref, wide_ref, narrow_ref):
    tall, d = fc_ref.shape
    width = out_ref.shape[0]
    copies = narrow_ref.shape[0]
    columns = jnp.transpose(vec_ref[...].astype(F32)).astype(BF16)
    wide_ref[:, :d] = fc_ref[...]
    wide_ref[:, d : 2 * d] = pj_ref[...]
    wide_ref[:, 2 * d : 2 * d + width] = jnp.transpose(out_ref[...].astype(F32)).astype(BF16)
    edge = 2 * d + width
    wide_ref[:, edge:] = jnp.zeros((tall, EXT), BF16)
    wide_ref[:, edge : edge + 4] = columns[:, 2:6]
    rows, strip = fb_ref.shape
    wide_ref[:rows, edge + 8 : edge + 8 + strip] = fb_ref[...]
    for s in range(3):
        narrow_ref[0, :, s * width : (s + 1) * width] = qkv_ref[s]
    edge = 3 * width
    narrow_ref[0, :, edge:] = jnp.zeros((tall, EXT), BF16)
    narrow_ref[0, :, edge : edge + 2] = columns[:, :2]
    heads, piece = qb_ref.shape[1:]
    for s in range(3):
        narrow_ref[0, s * heads : (s + 1) * heads, edge + 8 : edge + 8 + piece] = qb_ref[s]
    whole = narrow_ref[0]
    for n in range(1, copies):
        narrow_ref[n] = whole


def pack(fc, pj, out, qkv, vec, qb, fb, copies):
    tall, d = fc.shape
    width = out.shape[0]
    return pl.pallas_call(
        pack_kernel,
        out_shape=(
            jax.ShapeDtypeStruct((tall, 2 * d + width + EXT), BF16),
            jax.ShapeDtypeStruct((copies, tall, 3 * width + EXT), BF16),
        ),
        compiler_params=pltpu.CompilerParams(vmem_limit_bytes=SMALL_LIMIT),
        cost_estimate=cost(0, 2e6),
        name="pack",
    )(fc, pj, out, qkv, vec, qb, fb)


def pick_rows(table, period):
    line = lax.broadcasted_iota(jnp.int32, table.shape, 0)
    lane = lax.broadcasted_iota(jnp.int32, table.shape, 1)
    return jnp.sum(jnp.where(line == (lane & (period - 1)), table, 0.0), axis=0, keepdims=True)


def spread_rows(row, lines, period):
    shape = (lines, row.shape[1])
    line = lax.broadcasted_iota(jnp.int32, shape, 0)
    lane = lax.broadcasted_iota(jnp.int32, shape, 1)
    return jnp.where(line == (lane & (period - 1)), jnp.broadcast_to(row, shape), 0.0).astype(BF16)


def project_kernel(piece, me_ref, own_ref, far_ref, w_ref, order_ref, out_ref, vec_ref, bias_ref):
    i = pl.program_id(0)
    width = out_ref.shape[2]

    @pl.when(i == 0)
    def _():
        turned = jnp.transpose(w_ref[:, 512:640].astype(F32))
        vec_ref[...] = turned[64:72]
        table = dot(turned[72:80].astype(BF16), order_ref[...])
        bias_ref[...] = jnp.broadcast_to(pick_rows(table, piece), bias_ref.shape)

    far = ((i ^ me_ref[0]) & 1) == 1
    rows = jnp.where(far, far_ref[0], own_ref[0]).astype(F32)
    n, _ = norm_parts(rows)
    normed = (n * vec_ref[0:1] + vec_ref[1:2]).astype(BF16)
    full = dot(normed, w_ref[...])[:, : 3 * width] + bias_ref[0:1, :]
    full = full.astype(BF16)
    out_ref[0] = full[:, :width] * jnp.asarray(HD ** (-0.5), BF16)
    out_ref[1] = full[:, width : 2 * width]
    out_ref[2] = full[:, 2 * width :]


def project(me, own, far, w, order, piece):
    half, rows, d = own.shape
    blocks = 2 * half
    width = order.shape[1] // 3
    return pl.pallas_call(
        functools.partial(project_kernel, piece),
        out_shape=jax.ShapeDtypeStruct((3, blocks * rows, width), BF16),
        grid_spec=pltpu.PrefetchScalarGridSpec(
            num_scalar_prefetch=1,
            grid=(blocks,),
            in_specs=[
                pl.BlockSpec((1, rows, d), lambda i, me: ((i ^ me[0]) // 2, 0, 0)),
                pl.BlockSpec((1, rows, d), lambda i, me: ((i ^ me[0]) // 2, 0, 0)),
                pl.BlockSpec(w.shape, lambda i, me: (0, 0)),
                pl.BlockSpec(order.shape, lambda i, me: (0, 0)),
            ],
            out_specs=pl.BlockSpec((3, rows, width), lambda i, me: (0, i, 0)),
            scratch_shapes=[pltpu.VMEM((8, d), F32), pltpu.VMEM((8, 3 * width), F32)],
        ),
        compiler_params=params(),
        cost_estimate=cost(2 * blocks * rows * d * 3 * width, 8e6),
        name="project",
    )(me, own, far, w, order)


def head_mask(shape, h):
    lane = lax.broadcasted_iota(jnp.int32, shape, 1)
    return (lane >= h * HD) & (lane < (h + 1) * HD)


def attend_kernel(q_ref, k_ref, v_ref, o_ref, ot_ref, level_ref, vt_ref, qm_ref, m_ref, l_ref):
    i = pl.program_id(0)
    heads = q_ref.shape[2] // HD
    bq = q_ref.shape[1]
    half = bq // 2

    @pl.when(i == 0)
    def _():
        vt_ref[...] = jnp.transpose(v_ref[0].astype(F32)).astype(BF16)

    for h in range(heads):
        q = q_ref[0]
        qm_ref[h] = jnp.where(head_mask(q.shape, h), q, jnp.zeros_like(q))
    m_ref[...] = jnp.zeros_like(m_ref)
    l_ref[...] = jnp.zeros_like(l_ref)
    ot_ref[...] = jnp.zeros_like(ot_ref)

    def chunk(start, size, first, masked):
        cols = slice(first, bq)
        keys = k_ref[0, pl.ds(start, size), :]
        for h in range(heads):
            u = dot_nt(keys, qm_ref[h, first:bq, :]) * LOG2E
            if masked:
                key_pos = lax.broadcasted_iota(jnp.int32, u.shape, 0)
                row_pos = lax.broadcasted_iota(jnp.int32, u.shape, 1)
                allowed = key_pos <= row_pos
                u = jnp.where(allowed, u, 0.0)
            before = m_ref[h : h + 1, cols]
            peak = jnp.maximum(before, jnp.max(jnp.abs(u), axis=0, keepdims=True))
            fade = jnp.exp2(before - peak)
            upper = jnp.exp2(u - peak)
            lower = jnp.exp2(-peak - u)
            both = upper + lower
            if masked:
                both = jnp.where(allowed, both, 0.0)
            m_ref[h : h + 1, cols] = peak
            l_ref[h : h + 1, cols] = l_ref[h : h + 1, cols] * fade + jnp.sum(both, axis=0, keepdims=True)
            part = dot(vt_ref[h * HD : (h + 1) * HD, pl.ds(start, size)], (upper - lower).astype(BF16))
            ot_ref[h * HD : (h + 1) * HD, cols] = ot_ref[h * HD : (h + 1) * HD, cols] * fade + part

    def body(j, carry):
        chunk(pl.multiple_of(j * bq, bq), bq, 0, False)
        return carry

    lax.fori_loop(0, i, body, 0)
    base = pl.multiple_of(i * bq, bq)
    chunk(base, half, 0, True)
    chunk(pl.multiple_of(base + half, half), half, half, True)
    for h in range(heads):
        total = l_ref[h : h + 1, :]
        level_ref[h : h + 1, :] = m_ref[h : h + 1, :] + jnp.log2(total)
        ot_ref[h * HD : (h + 1) * HD, :] = ot_ref[h * HD : (h + 1) * HD, :] * (1.0 / total)
    rows = o_ref.shape[2]
    for n in range(bq // rows):
        o_ref[n] = ot_ref[:, n * rows : (n + 1) * rows].astype(BF16)


def attend(triple, rows):
    _, span, width = triple.shape
    bq = min(512, span)
    heads = width // HD
    return pl.pallas_call(
        attend_kernel,
        out_shape=(
            jax.ShapeDtypeStruct((span // rows, width, rows), BF16),
            jax.ShapeDtypeStruct((width, span), F32),
            jax.ShapeDtypeStruct((8, span), F32),
        ),
        grid=(span // bq,),
        in_specs=[
            pl.BlockSpec((1, bq, width), lambda i: (0, i, 0)),
            pl.BlockSpec((1, span, width), lambda i: (1, 0, 0)),
            pl.BlockSpec((1, span, width), lambda i: (2, 0, 0)),
        ],
        out_specs=(
            pl.BlockSpec((bq // rows, width, rows), lambda i: (i, 0, 0)),
            pl.BlockSpec((width, bq), lambda i: (0, i)),
            pl.BlockSpec((8, bq), lambda i: (0, i)),
        ),
        scratch_shapes=[
            pltpu.VMEM((width, span), BF16),
            pltpu.VMEM((heads, bq, width), BF16),
            pltpu.VMEM((8, bq), F32),
            pltpu.VMEM((8, bq), F32),
        ],
        compiler_params=params(),
        cost_estimate=cost(4 * span * span * width, 8e6, span * span * heads),
        name="attend",
    )(triple, triple, triple)


def attend_back_kernel(
    qkv_ref, grad_ref, ot_ref, level_ref, out_ref, qm_ref, gm_ref, kt_ref, dqt_ref, dot_ref, dk_ref, dv_ref
):
    j = pl.program_id(0)
    blocks = pl.num_programs(0)
    span, width = qkv_ref.shape[1:]
    rows = grad_ref.shape[2]
    heads = width // HD
    count = qm_ref.shape[0]
    b = span // count
    half = b // 2

    @pl.when(j == 0)
    def _():
        for n in range(span // rows):
            cols = slice(n * rows, (n + 1) * rows)
            turned = grad_ref[n].astype(F32)
            prod = turned * ot_ref[:, cols]
            for h in range(heads):
                dot_ref[h : h + 1, cols] = jnp.sum(prod[h * HD : (h + 1) * HD], axis=0, keepdims=True)
            g = jnp.transpose(turned).astype(BF16)
            at = n * rows % b
            for h in range(heads):
                mask = head_mask(g.shape, h)
                gm_ref[n * rows // b, h * b + at : h * b + at + rows, :] = jnp.where(mask, g, jnp.zeros_like(g))
        kt_ref[...] = jnp.transpose(qkv_ref[1].astype(F32)).astype(BF16)
        dqt_ref[...] = jnp.zeros_like(dqt_ref)
        for n in range(count):
            q = qkv_ref[0, n * b : (n + 1) * b, :]
            for h in range(heads):
                mask = head_mask(q.shape, h)
                qm_ref[n, h * b : (h + 1) * b, :] = jnp.where(mask, q, jnp.zeros_like(q))

    dk_ref[...] = jnp.zeros_like(dk_ref)
    dv_ref[...] = jnp.zeros_like(dv_ref)

    def chunk(i, key_first, key_size, first, masked):
        start = pl.multiple_of(j * b + key_first, half)
        keys = qkv_ref[1, pl.ds(start, key_size), :]
        vals = qkv_ref[2, pl.ds(start, key_size), :]
        cols = b - first
        at = pl.multiple_of(i * b + first, half)
        for h in range(heads):
            lo = h * b + first
            qm = qm_ref[i, lo : lo + cols, :]
            gm = gm_ref[i, lo : lo + cols, :]
            level = level_ref[h : h + 1, pl.ds(at, cols)]
            inner = dot_ref[h : h + 1, pl.ds(at, cols)]
            u = dot_nt(keys, qm) * LOG2E
            upper = jnp.exp2(u - level)
            lower = jnp.exp2(-level - u)
            gw = dot_nt(vals, gm)
            weights = upper - lower
            gs = upper * (gw - inner) + lower * (gw + inner)
            if masked:
                key_pos = lax.broadcasted_iota(jnp.int32, u.shape, 0)
                row_pos = lax.broadcasted_iota(jnp.int32, u.shape, 1)
                allowed = key_pos <= row_pos
                weights = jnp.where(allowed, weights, 0.0)
                gs = jnp.where(allowed, gs, 0.0)
            weights = weights.astype(BF16)
            gs = gs.astype(BF16)
            rows = slice(key_first, key_first + key_size)
            dv_ref[rows, :] += dot(weights, gm)
            dk_ref[rows, :] += dot(gs, qm)
            dqt_ref[h * HD : (h + 1) * HD, pl.ds(at, cols)] += dot(
                kt_ref[h * HD : (h + 1) * HD, pl.ds(start, key_size)], gs
            )

    def body(i, carry):
        chunk(i, 0, b, 0, False)
        return carry

    chunk(j, 0, half, 0, True)
    chunk(j, half, half, half, True)
    lax.fori_loop(j + 1, blocks, body, 0)
    here = pl.ds(pl.multiple_of(j * b, b), b)
    out_ref[1, here, :] = dk_ref[...].astype(BF16)
    out_ref[2, here, :] = dv_ref[...].astype(BF16)

    @pl.when(j == blocks - 1)
    def _():
        out_ref[0] = jnp.transpose(dqt_ref[...] * (HD ** (-0.5))).astype(BF16)


def attend_back(triple, grad, ot, level):
    _, span, width = triple.shape
    b = min(512, span)
    count = span // b
    heads = width // HD
    whole = lambda *shape: pl.BlockSpec(shape, lambda j: (0,) * len(shape))
    return pl.pallas_call(
        attend_back_kernel,
        out_shape=jax.ShapeDtypeStruct(triple.shape, BF16),
        grid=(count,),
        in_specs=[
            whole(*triple.shape),
            whole(*grad.shape),
            whole(*ot.shape),
            whole(*level.shape),
        ],
        out_specs=whole(*triple.shape),
        scratch_shapes=[
            pltpu.VMEM((count, heads * b, width), BF16),
            pltpu.VMEM((count, heads * b, width), BF16),
            pltpu.VMEM((width, span), BF16),
            pltpu.VMEM((width, span), F32),
            pltpu.VMEM((8, span), F32),
            pltpu.VMEM((b, width), F32),
            pltpu.VMEM((b, width), F32),
        ],
        compiler_params=params(),
        cost_estimate=cost(10 * span * span * width, 1e7, span * span * heads),
        name="attend_back",
    )(triple, grad, ot, level)


def gelu_parts(u):
    c = 0.7978845608028654
    square = u * u
    th = jnp.tanh(c * u * (1.0 + 0.044715 * square))
    near = 0.5 * (1.0 + th)
    slope = near + (0.5 * c) * u * (1.0 - th * th) * (1.0 + (3.0 * 0.044715) * square)
    return (u * near, slope)


def middle_kernel(
    strip,
    tok_ref,
    cot_ref,
    mix_ref,
    g_ref,
    gout_ref,
    order_ref,
    y_ref,
    gh_ref,
    dmix_ref,
    n2_ref,
    act_ref,
    gl_ref,
    gb_ref,
    vec_ref,
    gfb_ref,
    hid_ref,
    acc_ref,
    back_ref,
    ext_ref,
):
    t = pl.program_id(0)
    steps = pl.num_programs(0)
    half = mix_ref.shape[2]
    parts = gout_ref.shape[0]
    d = tok_ref.shape[1]
    width = mix_ref.shape[1]

    @pl.when(t == 0)
    def _():
        ext_ref[...] = jnp.transpose(gout_ref[0, :, 128:256].astype(F32))[64:72]
        total = tok_ref[...].astype(F32) + ext_ref[2:3]
        for s in range(parts):
            lhs = jnp.concatenate([mix_ref[s], mix_ref[parts + s]], axis=1)
            lhs = jnp.transpose(lhs.astype(F32)).astype(BF16)
            total = total + dot_nt(lhs, gout_ref[s, :, :width])
        hid_ref[...] = total
        n, _ = norm_parts(total)
        n2_ref[...] = (n * ext_ref[0:1] + ext_ref[1:2]).astype(BF16)
        acc_ref[...] = total + ext_ref[3:4]
        back_ref[...] = jnp.zeros_like(back_ref)

    ext = jnp.transpose(g_ref[0, :, 2 * d + 128 : 2 * d + 256].astype(F32))[72:88].astype(BF16)
    bias = pick_rows(dot(ext, order_ref[...]), strip)
    fc = g_ref[0, :, :d]
    pj = g_ref[0, :, d : 2 * d]
    lifted = dot(n2_ref[...], fc) + bias
    act, slope = gelu_parts(lifted)
    act = act.astype(BF16)
    act_ref[0] = act
    gl32 = dot(cot_ref[...], pj) * slope
    gl = gl32.astype(BF16)
    gl_ref[0] = gl
    gfb_ref[0, 0:1, :] = jnp.sum(gl.astype(F32), axis=0, keepdims=True)
    acc_ref[...] += dot_nt(act, pj)
    back_ref[...] += dot_nt(gl, fc)

    @pl.when(t == steps - 1)
    def _():
        y_ref[...] = acc_ref[...].astype(BF16)
        n, scale = norm_parts(hid_ref[...])
        back = back_ref[...]
        cot = cot_ref[...].astype(F32)
        gh = cot + norm_back(back, ext_ref[0:1], n, scale)
        gh_ref[...] = gh
        gb = gh.astype(BF16)
        gb_ref[...] = gb
        vec_ref[0:1, :] = jnp.sum(back * n, axis=0, keepdims=True)
        vec_ref[1:2, :] = jnp.sum(back, axis=0, keepdims=True)
        vec_ref[2:3, :] = jnp.sum(gb.astype(F32), axis=0, keepdims=True)
        vec_ref[3:4, :] = jnp.sum(cot, axis=0, keepdims=True)
        vec_ref[4:8, :] = jnp.zeros((4, d), F32)
        for s in range(parts):
            dm = jnp.transpose(dot(gb, gout_ref[s, :, :width])).astype(BF16)
            dmix_ref[s] = dm[:, :half]
            dmix_ref[parts + s] = dm[:, half:]


def middle(tok, cot, mix, gathered, order, strip):
    rows, d = tok.shape
    parts = gathered.shape[0]
    cols = gathered.shape[2]
    whole = lambda *shape: pl.BlockSpec(shape, lambda t: (0,) * len(shape))
    piece = lambda *shape: pl.BlockSpec(shape, lambda t: (t,) + (0,) * (len(shape) - 1))
    sds = jax.ShapeDtypeStruct
    return pl.pallas_call(
        functools.partial(middle_kernel, strip),
        out_shape=(
            sds((rows, d), BF16),
            sds((rows, d), F32),
            sds(mix.shape, BF16),
            sds((rows, d), BF16),
            sds((parts, rows, d), BF16),
            sds((parts, rows, d), BF16),
            sds((rows, d), BF16),
            sds((8, d), F32),
            sds((parts, 8, d), F32),
        ),
        grid=(parts,),
        in_specs=[
            whole(rows, d),
            whole(rows, d),
            whole(*mix.shape),
            piece(1, d, cols),
            pl.BlockSpec((parts, d, 256), lambda t: (0, 0, cols // 256 - 1)),
            whole(*order.shape),
        ],
        out_specs=(
            whole(rows, d),
            whole(rows, d),
            whole(*mix.shape),
            whole(rows, d),
            piece(1, rows, d),
            piece(1, rows, d),
            whole(rows, d),
            whole(8, d),
            piece(1, 8, d),
        ),
        scratch_shapes=[
            pltpu.VMEM((rows, d), F32),
            pltpu.VMEM((rows, d), F32),
            pltpu.VMEM((rows, d), F32),
            pltpu.VMEM((8, d), F32),
        ],
        compiler_params=params(),
        cost_estimate=cost(2 * rows * d * d * 18, 3e7),
        name="middle",
    )(tok, cot, mix, gathered, gathered, order)


def weights_kernel(
    mode, strip, index_ref, n2_ref, cot_ref, gb_ref, mix_ref, act_ref, gl_ref, vec_ref, gfb_ref, order_ref, *rest
):
    s = pl.program_id(0)
    d = n2_ref.shape[1]
    width = mix_ref.shape[2]
    cols = 2 * d + width + EXT
    nt_ref, ct_ref, bt_ref = rest[-3:]

    @pl.when(s == 0)
    def _():
        nt_ref[...] = jnp.transpose(n2_ref[...].astype(F32)).astype(BF16)
        ct_ref[...] = jnp.transpose(cot_ref[...].astype(F32)).astype(BF16)
        bt_ref[...] = jnp.transpose(gb_ref[...].astype(F32)).astype(BF16)

    mix = jnp.concatenate([mix_ref[0, 0], mix_ref[1, 0]], axis=1)
    turned = dot_nt(spread_rows(gfb_ref[0, 0:1], 16, strip), order_ref[...])
    tall = jnp.concatenate([vec_ref[...], turned, jnp.zeros((EXT - 24, d), F32)], axis=0)
    if mode != "keep":
        out_ref = rest[0]
        out_ref[0, :, :d] = dot(nt_ref[...], gl_ref[0]).astype(BF16)
        out_ref[0, :, d : 2 * d] = dot(ct_ref[...], act_ref[0]).astype(BF16)
        out_ref[0, :, 2 * d : 2 * d + width] = dot_nt(bt_ref[...], mix).astype(BF16)
        out_ref[0, :, 2 * d + width :] = jnp.transpose(tall).astype(BF16)
        return
    came_ref, as_ref, ak_ref, bs_ref, bk_ref, sum_ref = rest[:6]
    sum_ref[:, 2 * d : 2 * d + width] = dot_nt(bt_ref[...], mix).astype(BF16)
    sum_ref[:, 2 * d + width :] = jnp.transpose(tall).astype(BF16)
    sum_ref[:, 2 * d :] = (sum_ref[:, 2 * d :].astype(F32) + came_ref[0, :, 2 * d :].astype(F32)).astype(BF16)
    sum_ref[:, :d] = (dot(nt_ref[...], gl_ref[0]) + came_ref[0, :, :d].astype(F32)).astype(BF16)
    sum_ref[:, d : 2 * d] = (dot(ct_ref[...], act_ref[0]) + came_ref[0, :, d : 2 * d].astype(F32)).astype(BF16)
    depth, step = as_ref.shape[1], as_ref.shape[2]
    cut = cols // 2

    def block(xr, zr):
        at = (zr * 2 + (xr ^ index_ref[2])) * step
        return pl.ds(pl.multiple_of(at, 16), step)

    for zr in range(depth):
        bk_ref[0, zr] = sum_ref[block(0, zr), cut:]
        bs_ref[0, zr] = sum_ref[block(1, zr), cut:]

    @pl.when(s == 0)
    def _():
        for xr in range(2):
            for zr in range(depth):
                as_ref[xr, zr] = sum_ref[block(xr, zr), :cut]

    @pl.when(s == 1)
    def _():
        for xr in range(2):
            for zr in range(depth):
                ak_ref[xr, zr] = sum_ref[block(xr, zr), :cut]


def weights(mode, index, n2, cot, gb, mix, act, gl, vec, gfb, order, strip, came=None, shards=None):
    rows, d = n2.shape
    parts = act.shape[0]
    width = mix.shape[1]
    cols = 2 * d + width + EXT
    steps = parts if mode == "all" else 2
    whole = lambda *shape: pl.BlockSpec(shape, lambda s, ix: (0,) * len(shape))
    piece = lambda *shape: pl.BlockSpec(shape, lambda s, ix: (ix[s],) + (0,) * (len(shape) - 1))
    mix = mix.reshape(mix.shape[0] // parts, parts, width, mix.shape[2])
    operands = [index, n2, cot, gb, mix, act, gl, vec, gfb, order]
    specs = [
        whole(rows, d),
        whole(rows, d),
        whole(rows, d),
        pl.BlockSpec((mix.shape[0], 1, width, mix.shape[3]), lambda s, ix: (0, ix[s], 0, 0)),
        piece(1, rows, d),
        piece(1, rows, d),
        whole(8, d),
        piece(1, 8, d),
        whole(*order.shape),
    ]
    scratch = [pltpu.VMEM((d, rows), BF16) for _ in range(3)]
    if mode == "keep":
        operands.append(came)
        specs.append(pl.BlockSpec((1, d, cols), lambda s, ix: (s, 0, 0)))
        block = (2, shards // 2, d // shards, cols // 2)
        sds = jax.ShapeDtypeStruct(block, BF16)
        out_shape = (sds,) * 4
        turn = pl.BlockSpec((1,) + block[1:], lambda s, ix: (1 - s, 0, 0, 0))
        out_specs = (whole(*block), whole(*block), turn, turn)
        scratch = [pltpu.VMEM((d, cols), BF16)] + scratch
    else:
        out_shape = jax.ShapeDtypeStruct((steps, d, cols), BF16)
        out_specs = pl.BlockSpec((1, d, cols), lambda s, ix: (s, 0, 0))
    return pl.pallas_call(
        functools.partial(weights_kernel, mode, strip),
        out_shape=out_shape,
        grid_spec=pltpu.PrefetchScalarGridSpec(
            num_scalar_prefetch=1,
            grid=(steps,),
            in_specs=specs,
            out_specs=out_specs,
            scratch_shapes=scratch,
        ),
        compiler_params=params(),
        cost_estimate=cost(2 * rows * d * cols * steps, 6e6 * steps),
        name="weights_" + mode,
    )(*operands)


def wide_sum_kernel(place_ref, ak_ref, ac_ref, bk_ref, bc_ref, keep_ref, send_ref):
    cut = ak_ref.shape[2]
    for ref, members in ((send_ref, (1, 2)), (keep_ref, (0, 3))):
        for n, m in enumerate(members):
            z = pl.ds(place_ref[0] ^ m, 1)
            ref[n : n + 1, :, :cut] = (ak_ref[z].astype(F32) + ac_ref[z].astype(F32)).astype(BF16)
            ref[n : n + 1, :, cut:] = (bk_ref[z].astype(F32) + bc_ref[z].astype(F32)).astype(BF16)


def wide_sum(place, *parts):
    depth, step, cut = parts[0].shape
    whole = lambda array: pl.BlockSpec(array.shape, lambda i, ix: (0, 0, 0))
    out = jax.ShapeDtypeStruct((depth // 2, step, 2 * cut), BF16)
    return pl.pallas_call(
        wide_sum_kernel,
        out_shape=(out, out),
        grid_spec=pltpu.PrefetchScalarGridSpec(
            num_scalar_prefetch=1,
            grid=(1,),
            in_specs=[whole(p) for p in parts],
            out_specs=(whole(out), whole(out)),
        ),
        compiler_params=params(),
        cost_estimate=cost(0, 4e6),
        name="wide_sum",
    )(place, *parts)


def finish_wide_kernel(*refs):
    fc_ref, pj_ref, out_ref, g_ref, b_ref, ob_ref, pb_ref, fb_ref = refs[-8:]
    d = fc_ref.shape[1]
    width = out_ref.shape[0]
    t = refs[0][0].astype(F32)
    for ref in refs[1:-8]:
        t = t + ref[0].astype(F32)
    fc_ref[...] = t[:, :d]
    pj_ref[...] = t[:, d : 2 * d]
    rest = jnp.transpose(t[:, 2 * d : 2 * d + width + EXT])
    out_ref[...] = rest[:width]
    g_ref[...] = rest[width : width + 1]
    b_ref[...] = rest[width + 1 : width + 2]
    ob_ref[...] = rest[width + 2 : width + 3]
    pb_ref[...] = rest[width + 3 : width + 4]
    rows, strip = fb_ref.shape
    at = 2 * d + width + 8
    fb_ref[...] = t[:rows, at : at + strip]


def finish_wide(parts, d, width, bias_shape):
    tall = parts[0].shape[1]
    sds = lambda *shape: jax.ShapeDtypeStruct(shape, F32)
    return pl.pallas_call(
        finish_wide_kernel,
        out_shape=(
            sds(tall, d),
            sds(tall, d),
            sds(width, tall),
            sds(1, tall),
            sds(1, tall),
            sds(1, tall),
            sds(1, tall),
            sds(*bias_shape),
        ),
        compiler_params=pltpu.CompilerParams(vmem_limit_bytes=SMALL_LIMIT),
        cost_estimate=cost(0, 2e6),
        name="finish_wide",
    )(*parts)


def finish_narrow_kernel(g_ref, qkv_ref, qb_ref, vec_ref):
    t = g_ref[0].astype(F32)
    for n in range(1, g_ref.shape[0]):
        t = t + g_ref[n].astype(F32)
    width = qkv_ref.shape[2]
    for s in range(3):
        qkv_ref[s] = t[:, s * width : (s + 1) * width]
    heads, piece = qb_ref.shape[1:]
    edge = 3 * width + 8
    for s in range(3):
        qb_ref[s] = t[s * heads : (s + 1) * heads, edge : edge + piece]
    vec_ref[...] = jnp.transpose(t[:, 512:640])[64:72]


def finish_narrow(g, width, bias_shape):
    tall = g.shape[1]
    sds = lambda *shape: jax.ShapeDtypeStruct(shape, F32)
    return pl.pallas_call(
        finish_narrow_kernel,
        out_shape=(sds(3, tall, width), sds(*bias_shape), sds(8, tall)),
        compiler_params=pltpu.CompilerParams(vmem_limit_bytes=SMALL_LIMIT),
        cost_estimate=cost(0, 2e6),
        name="finish_narrow",
    )(g)


def project_back_kernel(
    piece, me_ref, own_ref, far_ref, grad_ref, w_ref, order_ref, keep_ref, send_ref, dw_ref, w3_ref, dw3_ref, gain_ref, vec_ref, bias_ref
):
    i = pl.program_id(0)
    steps = pl.num_programs(0)
    width = grad_ref.shape[2]
    d = w_ref.shape[0]

    @pl.when(i == 0)
    def _():
        gain_ref[...] = jnp.transpose(w_ref[:, 512:640].astype(F32))[64:72]
        for s in range(3):
            w3_ref[s] = w_ref[:, s * width : (s + 1) * width]
        dw3_ref[...] = jnp.zeros_like(dw3_ref)
        vec_ref[...] = jnp.zeros_like(vec_ref)
        bias_ref[...] = jnp.zeros_like(bias_ref)

    far = ((i ^ me_ref[0]) & 1) == 1
    rows = jnp.where(far, far_ref[0], own_ref[0]).astype(F32)
    n, _ = norm_parts(rows)
    normed = n * gain_ref[0:1] + gain_ref[1:2]
    turned = jnp.transpose(normed).astype(BF16)
    part = dot_nt(grad_ref[0], w3_ref[0])
    for s in range(1, 3):
        part = part + dot_nt(grad_ref[s], w3_ref[s])
    for s in range(3):
        dw3_ref[s] += dot(turned, grad_ref[s])
        bias_ref[s : s + 1, :] += jnp.sum(grad_ref[s].astype(F32), axis=0, keepdims=True)
    vec_ref[0:1, :] += jnp.sum(part * n, axis=0, keepdims=True)
    vec_ref[1:2, :] += jnp.sum(part, axis=0, keepdims=True)

    @pl.when(far)
    def _():
        send_ref[0] = part.astype(BF16)

    @pl.when(jnp.logical_not(far))
    def _():
        keep_ref[0] = part

    @pl.when(i == steps - 1)
    def _():
        turned_bias = jnp.zeros((8, d), F32)
        for s in range(3):
            dw_ref[:, s * width : (s + 1) * width] = dw3_ref[s].astype(BF16)
            spread = spread_rows(bias_ref[s : s + 1, :], 8, piece)
            turned_bias = turned_bias + dot_nt(spread, order_ref[s])
        tall = jnp.concatenate([vec_ref[...], turned_bias, jnp.zeros((EXT - 16, d), F32)], axis=0)
        dw_ref[:, 3 * width :] = jnp.transpose(tall).astype(BF16)


def project_back(me, own, far, grad, w, order, piece):
    half, rows, d = own.shape
    width = grad.shape[2]
    blocks = 2 * half
    sds = jax.ShapeDtypeStruct
    rel = lambda i, me: ((i ^ me[0]) // 2, 0, 0)
    return pl.pallas_call(
        functools.partial(project_back_kernel, piece),
        out_shape=(
            sds((half, rows, d), F32),
            sds((half, rows, d), BF16),
            sds(w.shape, BF16),
        ),
        grid_spec=pltpu.PrefetchScalarGridSpec(
            num_scalar_prefetch=1,
            grid=(blocks,),
            in_specs=[
                pl.BlockSpec((1, rows, d), rel),
                pl.BlockSpec((1, rows, d), rel),
                pl.BlockSpec((3, rows, width), lambda i, me: (0, i, 0)),
                pl.BlockSpec(w.shape, lambda i, me: (0, 0)),
                pl.BlockSpec(order.shape, lambda i, me: (0, 0, 0)),
            ],
            out_specs=(
                pl.BlockSpec((1, rows, d), rel),
                pl.BlockSpec((1, rows, d), rel),
                pl.BlockSpec(w.shape, lambda i, me: (0, 0)),
            ),
            scratch_shapes=[
                pltpu.VMEM((3, d, width), BF16),
                pltpu.VMEM((3, d, width), F32),
                pltpu.VMEM((8, d), F32),
                pltpu.VMEM((8, d), F32),
                pltpu.VMEM((8, width), F32),
            ],
        ),
        compiler_params=params(),
        cost_estimate=cost(4 * blocks * rows * d * 3 * width, 1.5e7),
        name="project_back",
    )(me, own, far, grad, w, order)


def pair_kernel(keep_ref, came_ref, own_ref, *send_refs):
    n = pl.program_id(0)
    total = keep_ref[0] + came_ref[0].astype(F32)

    @pl.when(n == 0)
    def _():
        own_ref[...] = total

    for m, ref in enumerate(send_refs):

        @pl.when(n == m + 1)
        def _(ref=ref):
            ref[...] = total.astype(BF16)


def pair_sum(keep, came):
    half, rows, d = keep.shape
    piece = pl.BlockSpec((1, rows, d), lambda n: (n, 0, 0))
    flat = pl.BlockSpec((rows, d), lambda n: (0, 0))
    return pl.pallas_call(
        pair_kernel,
        out_shape=(jax.ShapeDtypeStruct((rows, d), F32),)
        + (jax.ShapeDtypeStruct((rows, d), BF16),) * (half - 1),
        grid=(half,),
        in_specs=[piece, piece],
        out_specs=(flat,) * half,
        compiler_params=params(SMALL_LIMIT),
        cost_estimate=cost(0, 7e6),
        name="pair_sum",
    )(keep, came)


def finish_rows_kernel(side_ref, tok_ref, near_ref, near2_ref, away_ref, away2_ref, gh_ref, w_ref, out_ref, gain_ref):
    m = pl.program_id(0)

    @pl.when(m == 0)
    def _():
        gain_ref[...] = jnp.transpose(w_ref[:, 512:640].astype(F32))[64:72]

    n, scale = norm_parts(tok_ref[0].astype(F32))
    near = near_ref[...] + near2_ref[...].astype(F32)
    away = away_ref[...].astype(F32) + away2_ref[...].astype(F32)
    incoming = jnp.where(m == side_ref[0], near, away)
    out_ref[0] = gh_ref[0] + norm_back(incoming, gain_ref[0:1], n, scale)


def finish_rows(side, tok, near, near2, away, away2, gh, w):
    micro, rows, d = tok.shape
    piece = pl.BlockSpec((1, rows, d), lambda m, ix: (m, 0, 0))
    flat = pl.BlockSpec((rows, d), lambda m, ix: (0, 0))
    return pl.pallas_call(
        finish_rows_kernel,
        out_shape=jax.ShapeDtypeStruct((micro, rows, d), F32),
        grid_spec=pltpu.PrefetchScalarGridSpec(
            num_scalar_prefetch=1,
            grid=(micro,),
            in_specs=[piece, flat, flat, flat, flat, piece, pl.BlockSpec(w.shape, lambda m, ix: (0, 0))],
            out_specs=piece,
            scratch_shapes=[pltpu.VMEM((8, d), F32)],
        ),
        compiler_params=params(SMALL_LIMIT),
        cost_estimate=cost(0, 6e6),
        name="finish_rows",
    )(side, tok, near, near2, away, away2, gh, w)


def one_hot_order(sources, size):
    row = lax.broadcasted_iota(jnp.int32, (size, sources.shape[1]), 0)
    return jnp.where(row == sources, 1.0, 0.0).astype(BF16)


barrier = lax.optimization_barrier


def plus(a, b):
    return (a.astype(F32) + b.astype(F32)).astype(BF16)


def local(
    tokens,
    cotangent,
    ln1_gain,
    ln1_bias,
    qkv_weight,
    qkv_bias,
    out_weight,
    out_bias,
    ln2_gain,
    ln2_bias,
    fc_weight,
    fc_bias,
    proj_weight,
    proj_bias,
):
    sides = lax.axis_size("ctx")
    parts = lax.axis_size("tp")
    shards = lax.axis_size(("dp", "ctx"))
    group = sides * parts
    micro, _, rows, d = tokens.shape
    assert micro == sides == 2 and parts == 4
    side = lax.axis_index("ctx")
    slot = lax.axis_index("tp")
    me = side * parts + slot
    me_array = jnp.stack([me, side]).astype(jnp.int32)
    side_array = jnp.full((1,), side, jnp.int32)
    tall = qkv_weight.shape[1]
    heads, piece = qkv_bias.shape[1], qkv_bias.shape[2]
    width = heads * HD
    lines, strip = fc_bias.shape

    deep = lax.axis_index("dp")
    depth = lax.axis_size("dp")

    def swap_deep(array, mask):
        return lax.ppermute(array, "dp", [(n, n ^ mask) for n in range(depth)])

    def swap(array, mask):
        return lax.ppermute(array, ("ctx", "tp"), [(n, n ^ mask) for n in range(group)])

    tok = tokens[:, 0]
    cot = cotangent[:, 0]

    vectors = jnp.stack([ln1_gain, ln1_bias, ln2_gain, ln2_bias, out_bias, proj_bias])
    wide, narrow = pack(fc_weight, proj_weight.T, out_weight, qkv_weight, vectors, qkv_bias, fc_bias, shards)

    gathered = lax.all_gather(wide, ("tp", "dp", "ctx"), axis=0, tiled=True)
    gathered = gathered.reshape(parts, d, wide.shape[1])

    mine = lax.dynamic_index_in_dim(tok, side, 0, keepdims=False)
    other = lax.dynamic_index_in_dim(tok, 1 - side, 0, keepdims=False)
    blocks = []
    for mask in range(0, group, 2):
        block = other if mask >= parts else mine
        blocks.append(block if mask == 0 else swap(block, mask))
    own = jnp.stack(blocks)
    far = swap(own, 1)

    w_in = lax.all_to_all(narrow, ("dp", "ctx"), 0, 0, tiled=True).reshape(d, narrow.shape[2])

    unit = lax.broadcasted_iota(jnp.int32, (1, 3 * width), 1)
    order_in = one_hot_order(unit % HD // piece * tall + unit // HD, d)
    unit = lax.broadcasted_iota(jnp.int32, (1, d), 1)
    order_fc = one_hot_order(unit % 128 // strip * tall + unit // 128, d)

    order_back = order_in.reshape(d, 3, width).transpose(1, 0, 2)
    far, order_in, order_fc, order_back = barrier((far, order_in, order_fc, order_back))

    triple = project(me_array, own, far, w_in, order_in, piece)
    mixed, mixed_turned, level = attend(triple, rows)
    mix = lax.all_to_all(mixed, ("ctx", "tp"), 0, 0, tiled=True)

    tok_rows = tok.reshape(micro * rows, d)
    cot_rows = cot.reshape(micro * rows, d)
    y, grad_hidden, grad_mix, n2, act, gl, gb, vec, gfb = middle(
        tok_rows, cot_rows, mix, gathered, order_fc, strip
    )
    grad_mix = lax.all_to_all(grad_mix, ("ctx", "tp"), 0, 0, tiled=True)

    parcels = (n2, cot_rows, gb, mix, act, gl, vec, gfb, order_fc, strip)
    exchange = tall % 16 == 0 and depth == 4
    if exchange:
        core, row = slot % 2, slot // 2
        index = lambda lane: jnp.stack([(1 - row) * 2 + lane, row * 2 + lane, side]).astype(jnp.int32)
        came = swap(weights("send", index(1 - core), *parcels), 1)
        a_send, a_keep, b_send, b_keep = weights("keep", index(core), *parcels, came=came, shards=shards)
        a_came, b_came = swap(a_send, 2), swap(b_send, parts)
    else:
        grad_wide = weights("all", jnp.arange(parts, dtype=jnp.int32), *parcels)
        grad_wide = lax.psum_scatter(
            grad_wide.reshape(parts * d, wide.shape[1]), ("tp", "dp", "ctx"), scatter_dimension=0, tiled=True
        )

    grad_triple = attend_back(triple, grad_mix, mixed_turned, level)
    if exchange:
        a_came, b_came, grad_triple = barrier((a_came, b_came, grad_triple))
        a_send, b_send = plus(a_keep[1], a_came[1]), plus(b_keep[1], b_came[1])
        a_send, b_send, grad_triple = barrier((a_send, b_send, grad_triple))
        a_keep, b_keep = plus(a_keep[0], a_came[0]), plus(b_keep[0], b_came[0])
        a_came, b_came = swap(a_send, parts), swap(b_send, 2)
    keep, send, grad_in = project_back(me_array, own, far, grad_triple, w_in, order_back, piece)
    if exchange:
        a_came, b_came, keep, send, grad_in = barrier((a_came, b_came, keep, send, grad_in))

    send_came = swap(send, 1)
    grad_in = lax.all_to_all(grad_in.reshape(narrow.shape), ("dp", "ctx"), 0, 0, tiled=True)
    if exchange:
        place = jnp.full((1,), deep, jnp.int32)
        z_keep, z_send = wide_sum(place, a_keep, a_came, b_keep, b_came)
        z_send, send_came = barrier((z_send, send_came))
        z_came = swap_deep(z_send, 1)
    near, *sends = pair_sum(keep, send_came)
    arrived = [swap(sends[n - 1], 2 * n) for n in range(1, group // 2)]

    grad_qkv_weight, grad_qkv_bias, vec_in = finish_narrow(grad_in, width, qkv_bias.shape)
    mask = parts // 2
    while mask:
        vec_in = vec_in + swap(vec_in, mask)
        mask //= 2

    if exchange:
        z_send = plus(z_keep[1:], z_came[1:])
        wide_parts = [z_keep, z_came, swap_deep(z_send, 3)]
    else:
        wide_parts = [grad_wide[None]]
    grad_tokens = finish_rows(
        side_array, tok, near, *arrived, grad_hidden.reshape(micro, rows, d), w_in
    )
    fc_grad, proj_grad, out_grad, gain2, shift2, out_b, proj_b, fc_b = finish_wide(
        wide_parts, d, width, fc_bias.shape
    )
    return (
        y.reshape(micro, 1, rows, d),
        grad_tokens[:, None],
        vec_in[0],
        vec_in[1],
        grad_qkv_weight,
        grad_qkv_bias,
        out_grad,
        out_b[0],
        gain2[0],
        shift2[0],
        fc_grad,
        fc_b,
        proj_grad.T,
        proj_b[0],
    )


def solution(mesh):
    rows = P(None, "dp", ("ctx", "tp"), None)
    vector = P(("dp", "ctx"))
    joint = P(None, ("dp", "ctx"), "tp")
    joint_bias = P(None, "tp", ("dp", "ctx"))
    down = P("tp", ("dp", "ctx"))
    up = P(("dp", "ctx"), "tp")
    inner = (vector, vector, joint, joint_bias, down, vector, vector, vector, up, down, down, vector)
    return jax.shard_map(
        local,
        mesh=mesh,
        in_specs=(rows, rows) + inner,
        out_specs=(rows, rows) + inner,
        check_vma=False,
    )
```

```python
import functools

import jax
import jax.numpy as jnp
from jax import lax
from jax.experimental import pallas as pl
from jax.experimental.pallas import tpu as pltpu
from jax.sharding import PartitionSpec as P

HD = 64
EPS = 1e-05
LOG2E = 1.4426950408889634
F32 = jnp.float32
BF16 = jnp.bfloat16
VMEM_LIMIT = 60 * 1024 * 1024
SMALL_LIMIT = 60 * 1024 * 1024
EXT = 64


def dot(a, b):
    return lax.dot_general(a, b, (((1,), (0,)), ((), ())), preferred_element_type=F32)


def dot_nt(a, b):
    return lax.dot_general(a, b, (((1,), (1,)), ((), ())), preferred_element_type=F32)


def norm_parts(rows):
    mean = jnp.mean(rows, axis=-1, keepdims=True)
    centered = rows - mean
    spread = jnp.mean(centered * centered, axis=-1, keepdims=True)
    scale = lax.rsqrt(spread + EPS)
    return (centered * scale, scale)


def norm_back(incoming, gain, n, scale):
    e = incoming * gain
    return (e - jnp.mean(e, axis=-1, keepdims=True) - n * jnp.mean(e * n, axis=-1, keepdims=True)) * scale


def params(limit=VMEM_LIMIT):
    return pltpu.CompilerParams(dimension_semantics=("arbitrary",), vmem_limit_bytes=limit)


def cost(flops, moved, exps=0):
    return pl.CostEstimate(flops=int(flops), bytes_accessed=int(moved), transcendentals=int(exps))


def pack_kernel(fc_ref, pj_ref, out_ref, qkv_ref, qb_ref, fb_ref, *rest):
    vec_refs, wide_ref, narrow_ref = rest[:-2], rest[-2], rest[-1]
    tall, d = fc_ref.shape
    width = out_ref.shape[0]
    copies = narrow_ref.shape[0]
    vectors = jnp.concatenate([ref[...].astype(F32) for ref in vec_refs] + [jnp.zeros((2, tall), F32)], axis=0)
    columns = jnp.transpose(vectors).astype(BF16)
    wide_ref[:, :d] = fc_ref[...]
    wide_ref[:, d : 2 * d] = pj_ref[...]
    wide_ref[:, 2 * d : 2 * d + width] = jnp.transpose(out_ref[...].astype(F32)).astype(BF16)
    edge = 2 * d + width
    wide_ref[:, edge:] = jnp.zeros((tall, EXT), BF16)
    wide_ref[:, edge : edge + 4] = columns[:, 2:6]
    rows, strip = fb_ref.shape
    wide_ref[:rows, edge + 8 : edge + 8 + strip] = fb_ref[...]
    for s in range(3):
        narrow_ref[0, :, s * width : (s + 1) * width] = qkv_ref[s]
    edge = 3 * width
    narrow_ref[0, :, edge:] = jnp.zeros((tall, EXT), BF16)
    narrow_ref[0, :, edge : edge + 2] = columns[:, :2]
    heads, piece = qb_ref.shape[1:]
    for s in range(3):
        narrow_ref[0, s * heads : (s + 1) * heads, edge + 8 : edge + 8 + piece] = qb_ref[s]
    whole = narrow_ref[0]
    for n in range(1, copies):
        narrow_ref[n] = whole


def pack(fc, pj, out, qkv, vec, qb, fb, copies):
    tall, d = fc.shape
    width = out.shape[0]
    return pl.pallas_call(
        pack_kernel,
        out_shape=(
            jax.ShapeDtypeStruct((tall, 2 * d + width + EXT), BF16),
            jax.ShapeDtypeStruct((copies, tall, 3 * width + EXT), BF16),
        ),
        compiler_params=pltpu.CompilerParams(vmem_limit_bytes=SMALL_LIMIT),
        cost_estimate=cost(0, 2e6),
        name="pack",
    )(fc, pj, out, qkv, qb, fb, *vec)


def pick_rows(table, period):
    line = lax.broadcasted_iota(jnp.int32, table.shape, 0)
    lane = lax.broadcasted_iota(jnp.int32, table.shape, 1)
    return jnp.sum(jnp.where(line == (lane & (period - 1)), table, 0.0), axis=0, keepdims=True)


def spread_rows(row, lines, period):
    shape = (lines, row.shape[1])
    line = lax.broadcasted_iota(jnp.int32, shape, 0)
    lane = lax.broadcasted_iota(jnp.int32, shape, 1)
    return jnp.where(line == (lane & (period - 1)), jnp.broadcast_to(row, shape), 0.0).astype(BF16)


def project_kernel(piece, me_ref, own_ref, far_ref, w_ref, order_ref, out_ref, vec_ref, bias_ref):
    i = pl.program_id(0)
    width = out_ref.shape[2]

    @pl.when(i == 0)
    def _():
        turned = jnp.transpose(w_ref[:, 512:640].astype(F32))
        vec_ref[...] = turned[64:72]
        table = dot(turned[72:80].astype(BF16), order_ref[...])
        bias_ref[...] = jnp.broadcast_to(pick_rows(table, piece), bias_ref.shape)

    far = ((i ^ me_ref[0]) & 1) == 1
    rows = jnp.where(far, far_ref[0], own_ref[0]).astype(F32)
    n, _ = norm_parts(rows)
    normed = (n * vec_ref[0:1] + vec_ref[1:2]).astype(BF16)
    full = dot(normed, w_ref[...])[:, : 3 * width] + bias_ref[0:1, :]
    full = full.astype(BF16)
    out_ref[0] = full[:, :width] * jnp.asarray(HD ** (-0.5), BF16)
    out_ref[1] = full[:, width : 2 * width]
    out_ref[2] = full[:, 2 * width :]


def project(me, own, far, w, order, piece):
    half, rows, d = own.shape
    blocks = 2 * half
    width = order.shape[1] // 3
    return pl.pallas_call(
        functools.partial(project_kernel, piece),
        out_shape=jax.ShapeDtypeStruct((3, blocks * rows, width), BF16),
        grid_spec=pltpu.PrefetchScalarGridSpec(
            num_scalar_prefetch=1,
            grid=(blocks,),
            in_specs=[
                pl.BlockSpec((1, rows, d), lambda i, me: ((i ^ me[0]) // 2, 0, 0)),
                pl.BlockSpec((1, rows, d), lambda i, me: ((i ^ me[0]) // 2, 0, 0)),
                pl.BlockSpec(w.shape, lambda i, me: (0, 0)),
                pl.BlockSpec(order.shape, lambda i, me: (0, 0)),
            ],
            out_specs=pl.BlockSpec((3, rows, width), lambda i, me: (0, i, 0)),
            scratch_shapes=[pltpu.VMEM((8, d), F32), pltpu.VMEM((8, 3 * width), F32)],
        ),
        compiler_params=params(),
        cost_estimate=cost(2 * blocks * rows * d * 3 * width, 8e6),
        name="project",
    )(me, own, far, w, order)


def head_mask(shape, h):
    lane = lax.broadcasted_iota(jnp.int32, shape, 1)
    return (lane >= h * HD) & (lane < (h + 1) * HD)


def attend_kernel(q_ref, k_ref, v_ref, o_ref, ot_ref, level_ref, vt_ref, qm_ref, m_ref, l_ref):
    i = pl.program_id(0)
    heads = q_ref.shape[2] // HD
    bq = q_ref.shape[1]
    half = bq // 2

    @pl.when(i == 0)
    def _():
        vt_ref[...] = jnp.transpose(v_ref[0].astype(F32)).astype(BF16)

    for h in range(heads):
        q = q_ref[0]
        qm_ref[h] = jnp.where(head_mask(q.shape, h), q, jnp.zeros_like(q))
    m_ref[...] = jnp.zeros_like(m_ref)
    l_ref[...] = jnp.zeros_like(l_ref)
    ot_ref[...] = jnp.zeros_like(ot_ref)

    def chunk(start, size, first, masked):
        cols = slice(first, bq)
        keys = k_ref[0, pl.ds(start, size), :]
        for h in range(heads):
            u = dot_nt(keys, qm_ref[h, first:bq, :]) * LOG2E
            if masked:
                key_pos = lax.broadcasted_iota(jnp.int32, u.shape, 0)
                row_pos = lax.broadcasted_iota(jnp.int32, u.shape, 1)
                allowed = key_pos <= row_pos
                u = jnp.where(allowed, u, 0.0)
            before = m_ref[h : h + 1, cols]
            peak = jnp.maximum(before, jnp.max(jnp.abs(u), axis=0, keepdims=True))
            fade = jnp.exp2(before - peak)
            upper = jnp.exp2(u - peak)
            lower = jnp.exp2(-peak - u)
            both = upper + lower
            if masked:
                both = jnp.where(allowed, both, 0.0)
            m_ref[h : h + 1, cols] = peak
            l_ref[h : h + 1, cols] = l_ref[h : h + 1, cols] * fade + jnp.sum(both, axis=0, keepdims=True)
            part = dot(vt_ref[h * HD : (h + 1) * HD, pl.ds(start, size)], (upper - lower).astype(BF16))
            ot_ref[h * HD : (h + 1) * HD, cols] = ot_ref[h * HD : (h + 1) * HD, cols] * fade + part

    def body(j, carry):
        chunk(pl.multiple_of(j * bq, bq), bq, 0, False)
        return carry

    lax.fori_loop(0, i, body, 0)
    base = pl.multiple_of(i * bq, bq)
    chunk(base, half, 0, True)
    chunk(pl.multiple_of(base + half, half), half, half, True)
    for h in range(heads):
        total = l_ref[h : h + 1, :]
        level_ref[h : h + 1, :] = m_ref[h : h + 1, :] + jnp.log2(total)
        ot_ref[h * HD : (h + 1) * HD, :] = ot_ref[h * HD : (h + 1) * HD, :] * (1.0 / total)
    rows = o_ref.shape[2]
    for n in range(bq // rows):
        o_ref[n] = ot_ref[:, n * rows : (n + 1) * rows].astype(BF16)


def attend(triple, rows):
    _, span, width = triple.shape
    bq = min(512, span)
    heads = width // HD
    return pl.pallas_call(
        attend_kernel,
        out_shape=(
            jax.ShapeDtypeStruct((span // rows, width, rows), BF16),
            jax.ShapeDtypeStruct((width, span), F32),
            jax.ShapeDtypeStruct((8, span), F32),
        ),
        grid=(span // bq,),
        in_specs=[
            pl.BlockSpec((1, bq, width), lambda i: (0, i, 0)),
            pl.BlockSpec((1, span, width), lambda i: (1, 0, 0)),
            pl.BlockSpec((1, span, width), lambda i: (2, 0, 0)),
        ],
        out_specs=(
            pl.BlockSpec((bq // rows, width, rows), lambda i: (i, 0, 0)),
            pl.BlockSpec((width, bq), lambda i: (0, i)),
            pl.BlockSpec((8, bq), lambda i: (0, i)),
        ),
        scratch_shapes=[
            pltpu.VMEM((width, span), BF16),
            pltpu.VMEM((heads, bq, width), BF16),
            pltpu.VMEM((8, bq), F32),
            pltpu.VMEM((8, bq), F32),
        ],
        compiler_params=params(),
        cost_estimate=cost(4 * span * span * width, 8e6, span * span * heads),
        name="attend",
    )(triple, triple, triple)


def attend_back_kernel(
    qkv_ref, grad_ref, ot_ref, level_ref, out_ref, qm_ref, gm_ref, kt_ref, dqt_ref, dot_ref, dk_ref, dv_ref
):
    j = pl.program_id(0)
    blocks = pl.num_programs(0)
    span, width = qkv_ref.shape[1:]
    rows = grad_ref.shape[2]
    heads = width // HD
    count = qm_ref.shape[0]
    b = span // count
    half = b // 2

    @pl.when(j == 0)
    def _():
        for n in range(span // rows):
            cols = slice(n * rows, (n + 1) * rows)
            turned = grad_ref[n].astype(F32)
            prod = turned * ot_ref[:, cols]
            for h in range(heads):
                dot_ref[h : h + 1, cols] = jnp.sum(prod[h * HD : (h + 1) * HD], axis=0, keepdims=True)
            g = jnp.transpose(turned).astype(BF16)
            at = n * rows % b
            for h in range(heads):
                mask = head_mask(g.shape, h)
                gm_ref[n * rows // b, h * b + at : h * b + at + rows, :] = jnp.where(mask, g, jnp.zeros_like(g))
        kt_ref[...] = jnp.transpose(qkv_ref[1].astype(F32)).astype(BF16)
        dqt_ref[...] = jnp.zeros_like(dqt_ref)
        for n in range(count):
            q = qkv_ref[0, n * b : (n + 1) * b, :]
            for h in range(heads):
                mask = head_mask(q.shape, h)
                qm_ref[n, h * b : (h + 1) * b, :] = jnp.where(mask, q, jnp.zeros_like(q))

    dk_ref[...] = jnp.zeros_like(dk_ref)
    dv_ref[...] = jnp.zeros_like(dv_ref)

    def chunk(i, key_first, key_size, first, masked):
        start = pl.multiple_of(j * b + key_first, half)
        keys = qkv_ref[1, pl.ds(start, key_size), :]
        vals = qkv_ref[2, pl.ds(start, key_size), :]
        cols = b - first
        at = pl.multiple_of(i * b + first, half)
        for h in range(heads):
            lo = h * b + first
            qm = qm_ref[i, lo : lo + cols, :]
            gm = gm_ref[i, lo : lo + cols, :]
            level = level_ref[h : h + 1, pl.ds(at, cols)]
            inner = dot_ref[h : h + 1, pl.ds(at, cols)]
            u = dot_nt(keys, qm) * LOG2E
            upper = jnp.exp2(u - level)
            lower = jnp.exp2(-level - u)
            gw = dot_nt(vals, gm)
            weights = upper - lower
            gs = upper * (gw - inner) + lower * (gw + inner)
            if masked:
                key_pos = lax.broadcasted_iota(jnp.int32, u.shape, 0)
                row_pos = lax.broadcasted_iota(jnp.int32, u.shape, 1)
                allowed = key_pos <= row_pos
                weights = jnp.where(allowed, weights, 0.0)
                gs = jnp.where(allowed, gs, 0.0)
            weights = weights.astype(BF16)
            gs = gs.astype(BF16)
            rows = slice(key_first, key_first + key_size)
            dv_ref[rows, :] += dot(weights, gm)
            dk_ref[rows, :] += dot(gs, qm)
            dqt_ref[h * HD : (h + 1) * HD, pl.ds(at, cols)] += dot(
                kt_ref[h * HD : (h + 1) * HD, pl.ds(start, key_size)], gs
            )

    def body(i, carry):
        chunk(i, 0, b, 0, False)
        return carry

    chunk(j, 0, half, 0, True)
    chunk(j, half, half, half, True)
    lax.fori_loop(j + 1, blocks, body, 0)
    here = pl.ds(pl.multiple_of(j * b, b), b)
    out_ref[1, here, :] = dk_ref[...].astype(BF16)
    out_ref[2, here, :] = dv_ref[...].astype(BF16)

    @pl.when(j == blocks - 1)
    def _():
        out_ref[0] = jnp.transpose(dqt_ref[...] * (HD ** (-0.5))).astype(BF16)


def attend_back(triple, grad, ot, level):
    _, span, width = triple.shape
    b = min(512, span)
    count = span // b
    heads = width // HD
    whole = lambda *shape: pl.BlockSpec(shape, lambda j: (0,) * len(shape))
    return pl.pallas_call(
        attend_back_kernel,
        out_shape=jax.ShapeDtypeStruct(triple.shape, BF16),
        grid=(count,),
        in_specs=[
            whole(*triple.shape),
            whole(*grad.shape),
            whole(*ot.shape),
            whole(*level.shape),
        ],
        out_specs=whole(*triple.shape),
        scratch_shapes=[
            pltpu.VMEM((count, heads * b, width), BF16),
            pltpu.VMEM((count, heads * b, width), BF16),
            pltpu.VMEM((width, span), BF16),
            pltpu.VMEM((width, span), F32),
            pltpu.VMEM((8, span), F32),
            pltpu.VMEM((b, width), F32),
            pltpu.VMEM((b, width), F32),
        ],
        compiler_params=params(),
        cost_estimate=cost(10 * span * span * width, 1e7, span * span * heads),
        name="attend_back",
    )(triple, grad, ot, level)


def gelu_parts(u):
    c = 0.7978845608028654
    square = u * u
    th = jnp.tanh(c * u * (1.0 + 0.044715 * square))
    near = 0.5 * (1.0 + th)
    slope = near + (0.5 * c) * u * (1.0 - th * th) * (1.0 + (3.0 * 0.044715) * square)
    return (u * near, slope)


def middle_kernel(
    strip,
    tok_ref,
    cot_ref,
    mix_ref,
    g_ref,
    gout_ref,
    order_ref,
    y_ref,
    gh_ref,
    dmix_ref,
    n2_ref,
    act_ref,
    gl_ref,
    gb_ref,
    vec_ref,
    gfb_ref,
    hid_ref,
    acc_ref,
    back_ref,
    ext_ref,
):
    t = pl.program_id(0)
    steps = pl.num_programs(0)
    half = mix_ref.shape[2]
    parts = gout_ref.shape[0]
    d = tok_ref.shape[1]
    width = mix_ref.shape[1]

    @pl.when(t == 0)
    def _():
        ext_ref[...] = jnp.transpose(gout_ref[0, :, 128:256].astype(F32))[64:72]
        total = tok_ref[...].astype(F32) + ext_ref[2:3]
        for s in range(parts):
            lhs = jnp.concatenate([mix_ref[s], mix_ref[parts + s]], axis=1)
            lhs = jnp.transpose(lhs.astype(F32)).astype(BF16)
            total = total + dot_nt(lhs, gout_ref[s, :, :width])
        hid_ref[...] = total
        n, _ = norm_parts(total)
        n2_ref[...] = (n * ext_ref[0:1] + ext_ref[1:2]).astype(BF16)
        acc_ref[...] = total + ext_ref[3:4]
        back_ref[...] = jnp.zeros_like(back_ref)

    ext = jnp.transpose(g_ref[0, :, 2 * d + 128 : 2 * d + 256].astype(F32))[72:88].astype(BF16)
    bias = pick_rows(dot(ext, order_ref[...]), strip)
    fc = g_ref[0, :, :d]
    pj = g_ref[0, :, d : 2 * d]
    lifted = dot(n2_ref[...], fc) + bias
    act, slope = gelu_parts(lifted)
    act = act.astype(BF16)
    act_ref[0] = act
    gl32 = dot(cot_ref[...], pj) * slope
    gl = gl32.astype(BF16)
    gl_ref[0] = gl
    gfb_ref[0, 0:1, :] = jnp.sum(gl.astype(F32), axis=0, keepdims=True)
    acc_ref[...] += dot_nt(act, pj)
    back_ref[...] += dot_nt(gl, fc)

    @pl.when(t == steps - 1)
    def _():
        y_ref[...] = acc_ref[...].astype(BF16)
        n, scale = norm_parts(hid_ref[...])
        back = back_ref[...]
        cot = cot_ref[...].astype(F32)
        gh = cot + norm_back(back, ext_ref[0:1], n, scale)
        gh_ref[...] = gh
        gb = gh.astype(BF16)
        gb_ref[...] = gb
        vec_ref[0:1, :] = jnp.sum(back * n, axis=0, keepdims=True)
        vec_ref[1:2, :] = jnp.sum(back, axis=0, keepdims=True)
        vec_ref[2:3, :] = jnp.sum(gb.astype(F32), axis=0, keepdims=True)
        vec_ref[3:4, :] = jnp.sum(cot, axis=0, keepdims=True)
        vec_ref[4:8, :] = jnp.zeros((4, d), F32)
        for s in range(parts):
            dm = jnp.transpose(dot(gb, gout_ref[s, :, :width])).astype(BF16)
            dmix_ref[s] = dm[:, :half]
            dmix_ref[parts + s] = dm[:, half:]


def middle(tok, cot, mix, gathered, order, strip):
    rows, d = tok.shape
    parts = gathered.shape[0]
    cols = gathered.shape[2]
    whole = lambda *shape: pl.BlockSpec(shape, lambda t: (0,) * len(shape))
    piece = lambda *shape: pl.BlockSpec(shape, lambda t: (t,) + (0,) * (len(shape) - 1))
    sds = jax.ShapeDtypeStruct
    return pl.pallas_call(
        functools.partial(middle_kernel, strip),
        out_shape=(
            sds((rows, d), BF16),
            sds((rows, d), F32),
            sds(mix.shape, BF16),
            sds((rows, d), BF16),
            sds((parts, rows, d), BF16),
            sds((parts, rows, d), BF16),
            sds((rows, d), BF16),
            sds((8, d), F32),
            sds((parts, 8, d), F32),
        ),
        grid=(parts,),
        in_specs=[
            whole(rows, d),
            whole(rows, d),
            whole(*mix.shape),
            piece(1, d, cols),
            pl.BlockSpec((parts, d, 256), lambda t: (0, 0, cols // 256 - 1)),
            whole(*order.shape),
        ],
        out_specs=(
            whole(rows, d),
            whole(rows, d),
            whole(*mix.shape),
            whole(rows, d),
            piece(1, rows, d),
            piece(1, rows, d),
            whole(rows, d),
            whole(8, d),
            piece(1, 8, d),
        ),
        scratch_shapes=[
            pltpu.VMEM((rows, d), F32),
            pltpu.VMEM((rows, d), F32),
            pltpu.VMEM((rows, d), F32),
            pltpu.VMEM((8, d), F32),
        ],
        compiler_params=params(),
        cost_estimate=cost(2 * rows * d * d * 18, 3e7),
        name="middle",
    )(tok, cot, mix, gathered, gathered, order)


def weights_kernel(
    mode, strip, index_ref, n2_ref, cot_ref, gb_ref, mix_ref, act_ref, gl_ref, vec_ref, gfb_ref, order_ref, *rest
):
    s = pl.program_id(0)
    d = n2_ref.shape[1]
    width = mix_ref.shape[2]
    cols = 2 * d + width + EXT
    nt_ref, ct_ref, bt_ref = rest[-3:]

    @pl.when(s == 0)
    def _():
        nt_ref[...] = jnp.transpose(n2_ref[...].astype(F32)).astype(BF16)
        ct_ref[...] = jnp.transpose(cot_ref[...].astype(F32)).astype(BF16)
        bt_ref[...] = jnp.transpose(gb_ref[...].astype(F32)).astype(BF16)

    mix = jnp.concatenate([mix_ref[0, 0], mix_ref[1, 0]], axis=1)
    turned = dot_nt(spread_rows(gfb_ref[0, 0:1], 16, strip), order_ref[...])
    tall = jnp.concatenate([vec_ref[...], turned, jnp.zeros((EXT - 24, d), F32)], axis=0)
    if mode != "keep":
        out_ref = rest[0]
        out_ref[0, :, :d] = dot(nt_ref[...], gl_ref[0]).astype(BF16)
        out_ref[0, :, d : 2 * d] = dot(ct_ref[...], act_ref[0]).astype(BF16)
        out_ref[0, :, 2 * d : 2 * d + width] = dot_nt(bt_ref[...], mix).astype(BF16)
        out_ref[0, :, 2 * d + width :] = jnp.transpose(tall).astype(BF16)
        return
    came_ref, as_ref, ak_ref, bs_ref, bk_ref, sum_ref = rest[:6]
    sum_ref[:, 2 * d : 2 * d + width] = dot_nt(bt_ref[...], mix).astype(BF16)
    sum_ref[:, 2 * d + width :] = jnp.transpose(tall).astype(BF16)
    sum_ref[:, 2 * d :] = (sum_ref[:, 2 * d :].astype(F32) + came_ref[0, :, 2 * d :].astype(F32)).astype(BF16)
    sum_ref[:, :d] = (dot(nt_ref[...], gl_ref[0]) + came_ref[0, :, :d].astype(F32)).astype(BF16)
    sum_ref[:, d : 2 * d] = (dot(ct_ref[...], act_ref[0]) + came_ref[0, :, d : 2 * d].astype(F32)).astype(BF16)
    depth, step = as_ref.shape[1], as_ref.shape[2]
    cut = cols // 2

    def block(xr, zr):
        at = (zr * 2 + (xr ^ index_ref[2])) * step
        return pl.ds(pl.multiple_of(at, 16), step)

    for zr in range(depth):
        bk_ref[0, zr] = sum_ref[block(0, zr), cut:]
        bs_ref[0, zr] = sum_ref[block(1, zr), cut:]

    @pl.when(s == 0)
    def _():
        for xr in range(2):
            for zr in range(depth):
                as_ref[xr, zr] = sum_ref[block(xr, zr), :cut]

    @pl.when(s == 1)
    def _():
        for xr in range(2):
            for zr in range(depth):
                ak_ref[xr, zr] = sum_ref[block(xr, zr), :cut]


def weights(mode, index, n2, cot, gb, mix, act, gl, vec, gfb, order, strip, came=None, shards=None):
    rows, d = n2.shape
    parts = act.shape[0]
    width = mix.shape[1]
    cols = 2 * d + width + EXT
    steps = parts if mode == "all" else 2
    whole = lambda *shape: pl.BlockSpec(shape, lambda s, ix: (0,) * len(shape))
    piece = lambda *shape: pl.BlockSpec(shape, lambda s, ix: (ix[s],) + (0,) * (len(shape) - 1))
    mix = mix.reshape(mix.shape[0] // parts, parts, width, mix.shape[2])
    operands = [index, n2, cot, gb, mix, act, gl, vec, gfb, order]
    specs = [
        whole(rows, d),
        whole(rows, d),
        whole(rows, d),
        pl.BlockSpec((mix.shape[0], 1, width, mix.shape[3]), lambda s, ix: (0, ix[s], 0, 0)),
        piece(1, rows, d),
        piece(1, rows, d),
        whole(8, d),
        piece(1, 8, d),
        whole(*order.shape),
    ]
    scratch = [pltpu.VMEM((d, rows), BF16) for _ in range(3)]
    if mode == "keep":
        operands.append(came)
        specs.append(pl.BlockSpec((1, d, cols), lambda s, ix: (s, 0, 0)))
        block = (2, shards // 2, d // shards, cols // 2)
        sds = jax.ShapeDtypeStruct(block, BF16)
        out_shape = (sds,) * 4
        turn = pl.BlockSpec((1,) + block[1:], lambda s, ix: (1 - s, 0, 0, 0))
        out_specs = (whole(*block), whole(*block), turn, turn)
        scratch = [pltpu.VMEM((d, cols), BF16)] + scratch
    else:
        out_shape = jax.ShapeDtypeStruct((steps, d, cols), BF16)
        out_specs = pl.BlockSpec((1, d, cols), lambda s, ix: (s, 0, 0))
    return pl.pallas_call(
        functools.partial(weights_kernel, mode, strip),
        out_shape=out_shape,
        grid_spec=pltpu.PrefetchScalarGridSpec(
            num_scalar_prefetch=1,
            grid=(steps,),
            in_specs=specs,
            out_specs=out_specs,
            scratch_shapes=scratch,
        ),
        compiler_params=params(),
        cost_estimate=cost(2 * rows * d * cols * steps, 6e6 * steps),
        name="weights_" + mode,
    )(*operands)


def wide_sum_kernel(place_ref, *refs):
    for i, masks in enumerate(((1, 3), (3, 1))):
        mine_ref, first_ref, second_ref = refs[3 * i : 3 * i + 3]
        keep_ref, send_ref = refs[6 + 2 * i : 8 + 2 * i]
        for ref, base in ((send_ref, masks[0]), (keep_ref, 0)):
            for n, m in enumerate((base, base ^ masks[1])):
                z = pl.ds(place_ref[0] ^ m, 1)
                total = mine_ref[0, z].astype(F32) + first_ref[0, z].astype(F32)
                ref[n : n + 1] = (total + second_ref[z].astype(F32)).astype(BF16)


def wide_sum(place, *parts):
    depth, step, cut = parts[2].shape
    first = pl.BlockSpec((1, depth, step, cut), lambda i, ix: (0, 0, 0, 0))
    last = pl.BlockSpec((depth, step, cut), lambda i, ix: (0, 0, 0))
    out = jax.ShapeDtypeStruct((depth // 2, step, cut), BF16)
    return pl.pallas_call(
        wide_sum_kernel,
        out_shape=(out,) * 4,
        grid_spec=pltpu.PrefetchScalarGridSpec(
            num_scalar_prefetch=1,
            grid=(1,),
            in_specs=[first, first, last] * 2,
            out_specs=(pl.BlockSpec(out.shape, lambda i, ix: (0, 0, 0)),) * 4,
        ),
        compiler_params=params(),
        cost_estimate=cost(0, 4e6),
        name="wide_sum",
    )(place, *parts)


def finish_wide_kernel(*refs):
    fc_ref, pj_ref, out_ref, g_ref, b_ref, ob_ref, pb_ref, fb_ref = refs[-8:]
    d = fc_ref.shape[1]
    width = out_ref.shape[0]
    halves = []
    count = (len(refs) - 8) // 2
    for parts in (refs[:count], refs[count : 2 * count]):
        t = parts[0][0].astype(F32)
        for ref in parts[1:]:
            t = t + ref[0].astype(F32)
        halves.append(t)
    t = jnp.concatenate(halves, axis=1)
    fc_ref[...] = t[:, :d]
    pj_ref[...] = t[:, d : 2 * d]
    rest = jnp.transpose(t[:, 2 * d : 2 * d + width + EXT])
    out_ref[...] = rest[:width]
    g_ref[...] = rest[width : width + 1]
    b_ref[...] = rest[width + 1 : width + 2]
    ob_ref[...] = rest[width + 2 : width + 3]
    pb_ref[...] = rest[width + 3 : width + 4]
    rows, strip = fb_ref.shape
    at = 2 * d + width + 8
    fb_ref[...] = t[:rows, at : at + strip]


def finish_wide(parts, d, width, bias_shape):
    tall = parts[0].shape[1]
    sds = lambda *shape: jax.ShapeDtypeStruct(shape, F32)
    return pl.pallas_call(
        finish_wide_kernel,
        out_shape=(
            sds(tall, d),
            sds(tall, d),
            sds(width, tall),
            sds(1, tall),
            sds(1, tall),
            sds(1, tall),
            sds(1, tall),
            sds(*bias_shape),
        ),
        compiler_params=pltpu.CompilerParams(vmem_limit_bytes=SMALL_LIMIT),
        cost_estimate=cost(0, 2e6),
        name="finish_wide",
    )(*parts)


def finish_narrow_kernel(g_ref, qkv_ref, qb_ref, vec_ref):
    t = g_ref[0].astype(F32)
    for n in range(1, g_ref.shape[0]):
        t = t + g_ref[n].astype(F32)
    width = qkv_ref.shape[2]
    for s in range(3):
        qkv_ref[s] = t[:, s * width : (s + 1) * width]
    heads, piece = qb_ref.shape[1:]
    edge = 3 * width + 8
    for s in range(3):
        qb_ref[s] = t[s * heads : (s + 1) * heads, edge : edge + piece]
    vec_ref[...] = jnp.transpose(t[:, 512:640])[64:72]


def finish_narrow(g, width, bias_shape):
    tall = g.shape[1]
    sds = lambda *shape: jax.ShapeDtypeStruct(shape, F32)
    return pl.pallas_call(
        finish_narrow_kernel,
        out_shape=(sds(3, tall, width), sds(*bias_shape), sds(8, tall)),
        compiler_params=pltpu.CompilerParams(vmem_limit_bytes=SMALL_LIMIT),
        cost_estimate=cost(0, 2e6),
        name="finish_narrow",
    )(g)


def project_back_kernel(
    piece, me_ref, own_ref, far_ref, grad_ref, w_ref, order_ref, keep_ref, send_ref, dw_ref, w3_ref, dw3_ref, gain_ref, vec_ref, bias_ref
):
    i = pl.program_id(0)
    steps = pl.num_programs(0)
    width = grad_ref.shape[2]
    d = w_ref.shape[0]

    @pl.when(i == 0)
    def _():
        gain_ref[...] = jnp.transpose(w_ref[:, 512:640].astype(F32))[64:72]
        for s in range(3):
            w3_ref[s] = w_ref[:, s * width : (s + 1) * width]
        dw3_ref[...] = jnp.zeros_like(dw3_ref)
        vec_ref[...] = jnp.zeros_like(vec_ref)
        bias_ref[...] = jnp.zeros_like(bias_ref)

    far = ((i ^ me_ref[0]) & 1) == 1
    rows = jnp.where(far, far_ref[0], own_ref[0]).astype(F32)
    n, _ = norm_parts(rows)
    normed = n * gain_ref[0:1] + gain_ref[1:2]
    turned = jnp.transpose(normed).astype(BF16)
    part = dot_nt(grad_ref[0], w3_ref[0])
    for s in range(1, 3):
        part = part + dot_nt(grad_ref[s], w3_ref[s])
    for s in range(3):
        dw3_ref[s] += dot(turned, grad_ref[s])
        bias_ref[s : s + 1, :] += jnp.sum(grad_ref[s].astype(F32), axis=0, keepdims=True)
    vec_ref[0:1, :] += jnp.sum(part * n, axis=0, keepdims=True)
    vec_ref[1:2, :] += jnp.sum(part, axis=0, keepdims=True)

    @pl.when(far)
    def _():
        send_ref[0] = part.astype(BF16)

    @pl.when(jnp.logical_not(far))
    def _():
        keep_ref[0] = part

    @pl.when(i == steps - 1)
    def _():
        turned_bias = jnp.zeros((8, d), F32)
        for s in range(3):
            dw_ref[:, s * width : (s + 1) * width] = dw3_ref[s].astype(BF16)
            spread = spread_rows(bias_ref[s : s + 1, :], 8, piece)
            turned_bias = turned_bias + dot_nt(spread, order_ref[s])
        tall = jnp.concatenate([vec_ref[...], turned_bias, jnp.zeros((EXT - 16, d), F32)], axis=0)
        dw_ref[:, 3 * width :] = jnp.transpose(tall).astype(BF16)


def project_back(me, own, far, grad, w, order, piece):
    half, rows, d = own.shape
    width = grad.shape[2]
    blocks = 2 * half
    sds = jax.ShapeDtypeStruct
    rel = lambda i, me: ((i ^ me[0]) // 2, 0, 0)
    return pl.pallas_call(
        functools.partial(project_back_kernel, piece),
        out_shape=(
            sds((half, rows, d), F32),
            sds((half, rows, d), BF16),
            sds(w.shape, BF16),
        ),
        grid_spec=pltpu.PrefetchScalarGridSpec(
            num_scalar_prefetch=1,
            grid=(blocks,),
            in_specs=[
                pl.BlockSpec((1, rows, d), rel),
                pl.BlockSpec((1, rows, d), rel),
                pl.BlockSpec((3, rows, width), lambda i, me: (0, i, 0)),
                pl.BlockSpec(w.shape, lambda i, me: (0, 0)),
                pl.BlockSpec(order.shape, lambda i, me: (0, 0, 0)),
            ],
            out_specs=(
                pl.BlockSpec((1, rows, d), rel),
                pl.BlockSpec((1, rows, d), rel),
                pl.BlockSpec(w.shape, lambda i, me: (0, 0)),
            ),
            scratch_shapes=[
                pltpu.VMEM((3, d, width), BF16),
                pltpu.VMEM((3, d, width), F32),
                pltpu.VMEM((8, d), F32),
                pltpu.VMEM((8, d), F32),
                pltpu.VMEM((8, width), F32),
            ],
        ),
        compiler_params=params(),
        cost_estimate=cost(4 * blocks * rows * d * 3 * width, 1.5e7),
        name="project_back",
    )(me, own, far, grad, w, order)


def pair_kernel(keep_ref, came_ref, own_ref, *send_refs):
    n = pl.program_id(0)
    total = keep_ref[0] + came_ref[0].astype(F32)

    @pl.when(n == 0)
    def _():
        own_ref[...] = total

    for m, ref in enumerate(send_refs):

        @pl.when(n == m + 1)
        def _(ref=ref):
            ref[...] = total.astype(BF16)


def pair_sum(keep, came):
    half, rows, d = keep.shape
    piece = pl.BlockSpec((1, rows, d), lambda n: (n, 0, 0))
    flat = pl.BlockSpec((rows, d), lambda n: (0, 0))
    return pl.pallas_call(
        pair_kernel,
        out_shape=(jax.ShapeDtypeStruct((rows, d), F32),)
        + (jax.ShapeDtypeStruct((rows, d), BF16),) * (half - 1),
        grid=(half,),
        in_specs=[piece, piece],
        out_specs=(flat,) * half,
        compiler_params=params(SMALL_LIMIT),
        cost_estimate=cost(0, 7e6),
        name="pair_sum",
    )(keep, came)


def finish_rows_kernel(side_ref, tok_ref, near_ref, near2_ref, away_ref, away2_ref, gh_ref, w_ref, out_ref, gain_ref):
    m = pl.program_id(0)

    @pl.when(m == 0)
    def _():
        gain_ref[...] = jnp.transpose(w_ref[:, 512:640].astype(F32))[64:72]

    n, scale = norm_parts(tok_ref[0].astype(F32))
    near = near_ref[...] + near2_ref[...].astype(F32)
    away = away_ref[...].astype(F32) + away2_ref[...].astype(F32)
    incoming = jnp.where(m == side_ref[0], near, away)
    out_ref[0] = gh_ref[0] + norm_back(incoming, gain_ref[0:1], n, scale)


def finish_rows(side, tok, near, near2, away, away2, gh, w):
    micro, rows, d = tok.shape
    piece = pl.BlockSpec((1, rows, d), lambda m, ix: (m, 0, 0))
    flat = pl.BlockSpec((rows, d), lambda m, ix: (0, 0))
    return pl.pallas_call(
        finish_rows_kernel,
        out_shape=jax.ShapeDtypeStruct((micro, rows, d), F32),
        grid_spec=pltpu.PrefetchScalarGridSpec(
            num_scalar_prefetch=1,
            grid=(micro,),
            in_specs=[piece, flat, flat, flat, flat, piece, pl.BlockSpec(w.shape, lambda m, ix: (0, 0))],
            out_specs=piece,
            scratch_shapes=[pltpu.VMEM((8, d), F32)],
        ),
        compiler_params=params(SMALL_LIMIT),
        cost_estimate=cost(0, 6e6),
        name="finish_rows",
    )(side, tok, near, near2, away, away2, gh, w)


def one_hot_order(sources, size):
    row = lax.broadcasted_iota(jnp.int32, (size, sources.shape[1]), 0)
    return jnp.where(row == sources, 1.0, 0.0).astype(BF16)


barrier = lax.optimization_barrier


def plus(a, b):
    return (a.astype(F32) + b.astype(F32)).astype(BF16)


def local(
    tokens,
    cotangent,
    ln1_gain,
    ln1_bias,
    qkv_weight,
    qkv_bias,
    out_weight,
    out_bias,
    ln2_gain,
    ln2_bias,
    fc_weight,
    fc_bias,
    proj_weight,
    proj_bias,
):
    sides = lax.axis_size("ctx")
    parts = lax.axis_size("tp")
    shards = lax.axis_size(("dp", "ctx"))
    group = sides * parts
    micro, _, rows, d = tokens.shape
    assert micro == sides == 2 and parts == 4
    side = lax.axis_index("ctx")
    slot = lax.axis_index("tp")
    me = side * parts + slot
    me_array = jnp.stack([me, side]).astype(jnp.int32)
    side_array = jnp.full((1,), side, jnp.int32)
    tall = qkv_weight.shape[1]
    heads, piece = qkv_bias.shape[1], qkv_bias.shape[2]
    width = heads * HD
    lines, strip = fc_bias.shape

    deep = lax.axis_index("dp")
    depth = lax.axis_size("dp")

    def swap_deep(array, mask):
        return lax.ppermute(array, "dp", [(n, n ^ mask) for n in range(depth)])

    def swap(array, mask):
        return lax.ppermute(array, ("ctx", "tp"), [(n, n ^ mask) for n in range(group)])

    tok = tokens[:, 0]
    cot = cotangent[:, 0]

    vectors = [v[None] for v in (ln1_gain, ln1_bias, ln2_gain, ln2_bias, out_bias, proj_bias)]
    wide, narrow = pack(fc_weight, proj_weight.T, out_weight, qkv_weight, vectors, qkv_bias, fc_bias, shards)

    gathered = lax.all_gather(wide, ("tp", "dp", "ctx"), axis=0, tiled=True)
    gathered = gathered.reshape(parts, d, wide.shape[1])

    mine = lax.dynamic_index_in_dim(tok, side, 0, keepdims=False)
    other = lax.dynamic_index_in_dim(tok, 1 - side, 0, keepdims=False)
    blocks = []
    for mask in range(0, group, 2):
        block = other if mask >= parts else mine
        blocks.append(block if mask == 0 else swap(block, mask))
    own = jnp.stack(blocks)
    far = swap(own, 1)

    w_in = lax.all_to_all(narrow, ("dp", "ctx"), 0, 0, tiled=True).reshape(d, narrow.shape[2])

    unit = lax.broadcasted_iota(jnp.int32, (1, 3 * width), 1)
    order_in = one_hot_order(unit % HD // piece * tall + unit // HD, d)
    unit = lax.broadcasted_iota(jnp.int32, (1, d), 1)
    order_fc = one_hot_order(unit % 128 // strip * tall + unit // 128, d)

    order_back = order_in.reshape(d, 3, width).transpose(1, 0, 2)
    far, order_in, order_fc, order_back = barrier((far, order_in, order_fc, order_back))

    triple = project(me_array, own, far, w_in, order_in, piece)
    mixed, mixed_turned, level = attend(triple, rows)
    mix = lax.all_to_all(mixed, ("ctx", "tp"), 0, 0, tiled=True)

    tok_rows = tok.reshape(micro * rows, d)
    cot_rows = cot.reshape(micro * rows, d)
    y, grad_hidden, grad_mix, n2, act, gl, gb, vec, gfb = middle(
        tok_rows, cot_rows, mix, gathered, order_fc, strip
    )
    grad_mix = lax.all_to_all(grad_mix, ("ctx", "tp"), 0, 0, tiled=True)

    parcels = (n2, cot_rows, gb, mix, act, gl, vec, gfb, order_fc, strip)
    exchange = tall % 16 == 0 and depth == 4
    if exchange:
        core, row = slot % 2, slot // 2
        index = lambda lane: jnp.stack([(1 - row) * 2 + lane, row * 2 + lane, side]).astype(jnp.int32)
        came = swap(weights("send", index(1 - core), *parcels), 1)
        a_send, a_keep, b_send, b_keep = weights("keep", index(core), *parcels, came=came, shards=shards)
        a_came, b_came = swap(a_send, 2), swap(b_send, parts)
    else:
        grad_wide = weights("all", jnp.arange(parts, dtype=jnp.int32), *parcels)
        grad_wide = lax.psum_scatter(
            grad_wide.reshape(parts * d, wide.shape[1]), ("tp", "dp", "ctx"), scatter_dimension=0, tiled=True
        )

    grad_triple = attend_back(triple, grad_mix, mixed_turned, level)
    if exchange:
        a_came, b_came, grad_triple = barrier((a_came, b_came, grad_triple))
        a_send, b_send = plus(a_keep[1], a_came[1]), plus(b_keep[1], b_came[1])
        a_send, b_send, grad_triple = barrier((a_send, b_send, grad_triple))
        a_last, b_last = swap(a_send, parts), swap(b_send, 2)
    keep, send, grad_in = project_back(me_array, own, far, grad_triple, w_in, order_back, piece)
    if exchange:
        a_last, b_last, keep, send, grad_in = barrier((a_last, b_last, keep, send, grad_in))

    send_came = swap(send, 1)
    grad_in = lax.all_to_all(grad_in.reshape(narrow.shape), ("dp", "ctx"), 0, 0, tiled=True)
    if exchange:
        place = jnp.full((1,), deep, jnp.int32)
        a_kept, a_send, b_kept, b_send = wide_sum(place, a_keep, a_came, a_last, b_keep, b_came, b_last)
        a_send, send_came = barrier((a_send, send_came))
        a_came, b_came = swap_deep(a_send, 1), swap_deep(b_send, 3)
    near, *sends = pair_sum(keep, send_came)
    arrived = [swap(sends[n - 1], 2 * n) for n in range(1, group // 2)]

    if exchange:
        grad_in, a_came, b_came, near = barrier((grad_in, a_came, b_came, near))
    grad_qkv_weight, grad_qkv_bias, vec_in = finish_narrow(grad_in, width, qkv_bias.shape)
    mask = parts // 2
    while mask:
        vec_in = vec_in + swap(vec_in, mask)
        mask //= 2

    if exchange:
        a_last = swap_deep(plus(a_kept[1:], a_came[1:]), 3)
        b_last = swap_deep(plus(b_kept[1:], b_came[1:]), 1)
        wide_parts = [a_kept, a_came, a_last, b_kept, b_came, b_last]
    else:
        cut = wide.shape[1] // 2
        wide_parts = [grad_wide[None, :, :cut], grad_wide[None, :, cut:]]
    grad_tokens = finish_rows(
        side_array, tok, near, *arrived, grad_hidden.reshape(micro, rows, d), w_in
    )
    fc_grad, proj_grad, out_grad, gain2, shift2, out_b, proj_b, fc_b = finish_wide(
        wide_parts, d, width, fc_bias.shape
    )
    return (
        y.reshape(micro, 1, rows, d),
        grad_tokens[:, None],
        vec_in[0],
        vec_in[1],
        grad_qkv_weight,
        grad_qkv_bias,
        out_grad,
        out_b[0],
        gain2[0],
        shift2[0],
        fc_grad,
        fc_b,
        proj_grad.T,
        proj_b[0],
    )


def solution(mesh):
    rows = P(None, "dp", ("ctx", "tp"), None)
    vector = P(("dp", "ctx"))
    joint = P(None, ("dp", "ctx"), "tp")
    joint_bias = P(None, "tp", ("dp", "ctx"))
    down = P("tp", ("dp", "ctx"))
    up = P(("dp", "ctx"), "tp")
    inner = (vector, vector, joint, joint_bias, down, vector, vector, vector, up, down, down, vector)
    return jax.shard_map(
        local,
        mesh=mesh,
        in_specs=(rows, rows) + inner,
        out_specs=(rows, rows) + inner,
        check_vma=False,
    )
```

```python
import functools

import jax
import jax.numpy as jnp
from jax import lax
from jax.experimental import pallas as pl
from jax.experimental.pallas import tpu as pltpu
from jax.sharding import PartitionSpec as P

HD = 64
EPS = 1e-05
LOG2E = 1.4426950408889634
F32 = jnp.float32
BF16 = jnp.bfloat16
VMEM_LIMIT = 60 * 1024 * 1024
SMALL_LIMIT = 60 * 1024 * 1024
EXT = 64


def dot(a, b):
    return lax.dot_general(a, b, (((1,), (0,)), ((), ())), preferred_element_type=F32)


def dot_nt(a, b):
    return lax.dot_general(a, b, (((1,), (1,)), ((), ())), preferred_element_type=F32)


def norm_parts(rows):
    mean = jnp.mean(rows, axis=-1, keepdims=True)
    centered = rows - mean
    spread = jnp.mean(centered * centered, axis=-1, keepdims=True)
    scale = lax.rsqrt(spread + EPS)
    return (centered * scale, scale)


def norm_back(incoming, gain, n, scale):
    e = incoming * gain
    return (e - jnp.mean(e, axis=-1, keepdims=True) - n * jnp.mean(e * n, axis=-1, keepdims=True)) * scale


def params(limit=VMEM_LIMIT):
    return pltpu.CompilerParams(dimension_semantics=("arbitrary",), vmem_limit_bytes=limit)


def cost(flops, moved, exps=0):
    return pl.CostEstimate(flops=int(flops), bytes_accessed=int(moved), transcendentals=int(exps))


def pack_kernel(fc_ref, pj_ref, out_ref, qkv_ref, qb_ref, fb_ref, *rest):
    vec_refs, wide_ref, narrow_ref = rest[:-2], rest[-2], rest[-1]
    tall, d = fc_ref.shape
    width = out_ref.shape[0]
    copies = narrow_ref.shape[0]
    vectors = jnp.concatenate([ref[...].astype(F32) for ref in vec_refs] + [jnp.zeros((2, tall), F32)], axis=0)
    columns = jnp.transpose(vectors).astype(BF16)
    wide_ref[:, :d] = fc_ref[...]
    wide_ref[:, d : 2 * d] = pj_ref[...]
    wide_ref[:, 2 * d : 2 * d + width] = jnp.transpose(out_ref[...].astype(F32)).astype(BF16)
    edge = 2 * d + width
    wide_ref[:, edge:] = jnp.zeros((tall, EXT), BF16)
    wide_ref[:, edge : edge + 4] = columns[:, 2:6]
    rows, strip = fb_ref.shape
    wide_ref[:rows, edge + 8 : edge + 8 + strip] = fb_ref[...]
    for s in range(3):
        narrow_ref[0, :, s * width : (s + 1) * width] = qkv_ref[s]
    edge = 3 * width
    narrow_ref[0, :, edge:] = jnp.zeros((tall, EXT), BF16)
    narrow_ref[0, :, edge : edge + 2] = columns[:, :2]
    heads, piece = qb_ref.shape[1:]
    for s in range(3):
        narrow_ref[0, s * heads : (s + 1) * heads, edge + 8 : edge + 8 + piece] = qb_ref[s]
    whole = narrow_ref[0]
    for n in range(1, copies):
        narrow_ref[n] = whole


def pack(fc, pj, out, qkv, vec, qb, fb, copies):
    tall, d = fc.shape
    width = out.shape[0]
    return pl.pallas_call(
        pack_kernel,
        out_shape=(
            jax.ShapeDtypeStruct((tall, 2 * d + width + EXT), BF16),
            jax.ShapeDtypeStruct((copies, tall, 3 * width + EXT), BF16),
        ),
        compiler_params=pltpu.CompilerParams(vmem_limit_bytes=SMALL_LIMIT),
        cost_estimate=cost(0, 2e6),
        name="pack",
    )(fc, pj, out, qkv, qb, fb, *vec)


def pick_rows(table, period):
    line = lax.broadcasted_iota(jnp.int32, table.shape, 0)
    lane = lax.broadcasted_iota(jnp.int32, table.shape, 1)
    return jnp.sum(jnp.where(line == (lane & (period - 1)), table, 0.0), axis=0, keepdims=True)


def spread_rows(row, lines, period):
    shape = (lines, row.shape[1])
    line = lax.broadcasted_iota(jnp.int32, shape, 0)
    lane = lax.broadcasted_iota(jnp.int32, shape, 1)
    return jnp.where(line == (lane & (period - 1)), jnp.broadcast_to(row, shape), 0.0).astype(BF16)


def project_kernel(piece, me_ref, own_ref, far_ref, w_ref, order_ref, out_ref, vec_ref, bias_ref):
    i = pl.program_id(0)
    width = out_ref.shape[2]

    @pl.when(i == 0)
    def _():
        turned = jnp.transpose(w_ref[:, 512:640].astype(F32))
        vec_ref[...] = turned[64:72]
        table = dot(turned[72:80].astype(BF16), order_ref[...])
        bias_ref[...] = jnp.broadcast_to(pick_rows(table, piece), bias_ref.shape)

    far = ((i ^ me_ref[0]) & 1) == 1
    rows = jnp.where(far, far_ref[0], own_ref[0]).astype(F32)
    n, _ = norm_parts(rows)
    normed = (n * vec_ref[0:1] + vec_ref[1:2]).astype(BF16)
    full = dot(normed, w_ref[...])[:, : 3 * width] + bias_ref[0:1, :]
    full = full.astype(BF16)
    out_ref[0] = full[:, :width] * jnp.asarray(HD ** (-0.5), BF16)
    out_ref[1] = full[:, width : 2 * width]
    out_ref[2] = full[:, 2 * width :]


def project(me, own, far, w, order, piece):
    half, rows, d = own.shape
    blocks = 2 * half
    width = order.shape[1] // 3
    return pl.pallas_call(
        functools.partial(project_kernel, piece),
        out_shape=jax.ShapeDtypeStruct((3, blocks * rows, width), BF16),
        grid_spec=pltpu.PrefetchScalarGridSpec(
            num_scalar_prefetch=1,
            grid=(blocks,),
            in_specs=[
                pl.BlockSpec((1, rows, d), lambda i, me: ((i ^ me[0]) // 2, 0, 0)),
                pl.BlockSpec((1, rows, d), lambda i, me: ((i ^ me[0]) // 2, 0, 0)),
                pl.BlockSpec(w.shape, lambda i, me: (0, 0)),
                pl.BlockSpec(order.shape, lambda i, me: (0, 0)),
            ],
            out_specs=pl.BlockSpec((3, rows, width), lambda i, me: (0, i, 0)),
            scratch_shapes=[pltpu.VMEM((8, d), F32), pltpu.VMEM((8, 3 * width), F32)],
        ),
        compiler_params=params(),
        cost_estimate=cost(2 * blocks * rows * d * 3 * width, 8e6),
        name="project",
    )(me, own, far, w, order)


def head_mask(shape, h):
    lane = lax.broadcasted_iota(jnp.int32, shape, 1)
    return (lane >= h * HD) & (lane < (h + 1) * HD)


def attend_kernel(q_ref, k_ref, v_ref, o_ref, ot_ref, level_ref, vt_ref, qm_ref, m_ref, l_ref):
    i = pl.program_id(0)
    heads = q_ref.shape[2] // HD
    bq = q_ref.shape[1]
    half = bq // 2

    @pl.when(i == 0)
    def _():
        vt_ref[...] = jnp.transpose(v_ref[0].astype(F32)).astype(BF16)

    for h in range(heads):
        q = q_ref[0]
        qm_ref[h] = jnp.where(head_mask(q.shape, h), q, jnp.zeros_like(q))
    m_ref[...] = jnp.zeros_like(m_ref)
    l_ref[...] = jnp.zeros_like(l_ref)
    ot_ref[...] = jnp.zeros_like(ot_ref)

    def chunk(start, size, first, masked):
        cols = slice(first, bq)
        keys = k_ref[0, pl.ds(start, size), :]
        for h in range(heads):
            u = dot_nt(keys, qm_ref[h, first:bq, :]) * LOG2E
            if masked:
                key_pos = lax.broadcasted_iota(jnp.int32, u.shape, 0)
                row_pos = lax.broadcasted_iota(jnp.int32, u.shape, 1)
                allowed = key_pos <= row_pos
                u = jnp.where(allowed, u, 0.0)
            before = m_ref[h : h + 1, cols]
            peak = jnp.maximum(before, jnp.max(jnp.abs(u), axis=0, keepdims=True))
            fade = jnp.exp2(before - peak)
            upper = jnp.exp2(u - peak)
            lower = jnp.exp2(-peak - u)
            both = upper + lower
            if masked:
                both = jnp.where(allowed, both, 0.0)
            m_ref[h : h + 1, cols] = peak
            l_ref[h : h + 1, cols] = l_ref[h : h + 1, cols] * fade + jnp.sum(both, axis=0, keepdims=True)
            part = dot(vt_ref[h * HD : (h + 1) * HD, pl.ds(start, size)], (upper - lower).astype(BF16))
            ot_ref[h * HD : (h + 1) * HD, cols] = ot_ref[h * HD : (h + 1) * HD, cols] * fade + part

    def body(j, carry):
        chunk(pl.multiple_of(j * bq, bq), bq, 0, False)
        return carry

    lax.fori_loop(0, i, body, 0)
    base = pl.multiple_of(i * bq, bq)
    chunk(base, half, 0, True)
    chunk(pl.multiple_of(base + half, half), half, half, True)
    for h in range(heads):
        total = l_ref[h : h + 1, :]
        level_ref[h : h + 1, :] = m_ref[h : h + 1, :] + jnp.log2(total)
        ot_ref[h * HD : (h + 1) * HD, :] = ot_ref[h * HD : (h + 1) * HD, :] * (1.0 / total)
    rows = o_ref.shape[2]
    for n in range(bq // rows):
        o_ref[n] = ot_ref[:, n * rows : (n + 1) * rows].astype(BF16)


def attend(triple, rows):
    _, span, width = triple.shape
    bq = min(512, span)
    heads = width // HD
    return pl.pallas_call(
        attend_kernel,
        out_shape=(
            jax.ShapeDtypeStruct((span // rows, width, rows), BF16),
            jax.ShapeDtypeStruct((width, span), F32),
            jax.ShapeDtypeStruct((8, span), F32),
        ),
        grid=(span // bq,),
        in_specs=[
            pl.BlockSpec((1, bq, width), lambda i: (0, i, 0)),
            pl.BlockSpec((1, span, width), lambda i: (1, 0, 0)),
            pl.BlockSpec((1, span, width), lambda i: (2, 0, 0)),
        ],
        out_specs=(
            pl.BlockSpec((bq // rows, width, rows), lambda i: (i, 0, 0)),
            pl.BlockSpec((width, bq), lambda i: (0, i)),
            pl.BlockSpec((8, bq), lambda i: (0, i)),
        ),
        scratch_shapes=[
            pltpu.VMEM((width, span), BF16),
            pltpu.VMEM((heads, bq, width), BF16),
            pltpu.VMEM((8, bq), F32),
            pltpu.VMEM((8, bq), F32),
        ],
        compiler_params=params(),
        cost_estimate=cost(4 * span * span * width, 8e6, span * span * heads),
        name="attend",
    )(triple, triple, triple)


def attend_back_kernel(
    qkv_ref, grad_ref, ot_ref, level_ref, out_ref, qm_ref, gm_ref, kt_ref, dqt_ref, dot_ref, dk_ref, dv_ref
):
    j = pl.program_id(0)
    blocks = pl.num_programs(0)
    span, width = qkv_ref.shape[1:]
    rows = grad_ref.shape[2]
    heads = width // HD
    count = qm_ref.shape[0]
    b = span // count
    half = b // 2

    @pl.when(j == 0)
    def _():
        for n in range(span // rows):
            cols = slice(n * rows, (n + 1) * rows)
            turned = grad_ref[n].astype(F32)
            prod = turned * ot_ref[:, cols]
            for h in range(heads):
                dot_ref[h : h + 1, cols] = jnp.sum(prod[h * HD : (h + 1) * HD], axis=0, keepdims=True)
            g = jnp.transpose(turned).astype(BF16)
            at = n * rows % b
            for h in range(heads):
                mask = head_mask(g.shape, h)
                gm_ref[n * rows // b, h * b + at : h * b + at + rows, :] = jnp.where(mask, g, jnp.zeros_like(g))
        kt_ref[...] = jnp.transpose(qkv_ref[1].astype(F32)).astype(BF16)
        dqt_ref[...] = jnp.zeros_like(dqt_ref)
        for n in range(count):
            q = qkv_ref[0, n * b : (n + 1) * b, :]
            for h in range(heads):
                mask = head_mask(q.shape, h)
                qm_ref[n, h * b : (h + 1) * b, :] = jnp.where(mask, q, jnp.zeros_like(q))

    dk_ref[...] = jnp.zeros_like(dk_ref)
    dv_ref[...] = jnp.zeros_like(dv_ref)

    def chunk(i, key_first, key_size, first, masked):
        start = pl.multiple_of(j * b + key_first, half)
        keys = qkv_ref[1, pl.ds(start, key_size), :]
        vals = qkv_ref[2, pl.ds(start, key_size), :]
        cols = b - first
        at = pl.multiple_of(i * b + first, half)
        for h in range(heads):
            lo = h * b + first
            qm = qm_ref[i, lo : lo + cols, :]
            gm = gm_ref[i, lo : lo + cols, :]
            level = level_ref[h : h + 1, pl.ds(at, cols)]
            inner = dot_ref[h : h + 1, pl.ds(at, cols)]
            u = dot_nt(keys, qm) * LOG2E
            upper = jnp.exp2(u - level)
            lower = jnp.exp2(-level - u)
            gw = dot_nt(vals, gm)
            weights = upper - lower
            gs = upper * (gw - inner) + lower * (gw + inner)
            if masked:
                key_pos = lax.broadcasted_iota(jnp.int32, u.shape, 0)
                row_pos = lax.broadcasted_iota(jnp.int32, u.shape, 1)
                allowed = key_pos <= row_pos
                weights = jnp.where(allowed, weights, 0.0)
                gs = jnp.where(allowed, gs, 0.0)
            weights = weights.astype(BF16)
            gs = gs.astype(BF16)
            rows = slice(key_first, key_first + key_size)
            dv_ref[rows, :] += dot(weights, gm)
            dk_ref[rows, :] += dot(gs, qm)
            dqt_ref[h * HD : (h + 1) * HD, pl.ds(at, cols)] += dot(
                kt_ref[h * HD : (h + 1) * HD, pl.ds(start, key_size)], gs
            )

    def body(i, carry):
        chunk(i, 0, b, 0, False)
        return carry

    chunk(j, 0, half, 0, True)
    chunk(j, half, half, half, True)
    lax.fori_loop(j + 1, blocks, body, 0)
    here = pl.ds(pl.multiple_of(j * b, b), b)
    out_ref[1, here, :] = dk_ref[...].astype(BF16)
    out_ref[2, here, :] = dv_ref[...].astype(BF16)

    @pl.when(j == blocks - 1)
    def _():
        out_ref[0] = jnp.transpose(dqt_ref[...] * (HD ** (-0.5))).astype(BF16)


def attend_back(triple, grad, ot, level):
    _, span, width = triple.shape
    b = min(512, span)
    count = span // b
    heads = width // HD
    whole = lambda *shape: pl.BlockSpec(shape, lambda j: (0,) * len(shape))
    return pl.pallas_call(
        attend_back_kernel,
        out_shape=jax.ShapeDtypeStruct(triple.shape, BF16),
        grid=(count,),
        in_specs=[
            whole(*triple.shape),
            whole(*grad.shape),
            whole(*ot.shape),
            whole(*level.shape),
        ],
        out_specs=whole(*triple.shape),
        scratch_shapes=[
            pltpu.VMEM((count, heads * b, width), BF16),
            pltpu.VMEM((count, heads * b, width), BF16),
            pltpu.VMEM((width, span), BF16),
            pltpu.VMEM((width, span), F32),
            pltpu.VMEM((8, span), F32),
            pltpu.VMEM((b, width), F32),
            pltpu.VMEM((b, width), F32),
        ],
        compiler_params=params(),
        cost_estimate=cost(10 * span * span * width, 1e7, span * span * heads),
        name="attend_back",
    )(triple, grad, ot, level)


def gelu_parts(u):
    c = 0.7978845608028654
    square = u * u
    th = jnp.tanh(c * u * (1.0 + 0.044715 * square))
    near = 0.5 * (1.0 + th)
    slope = near + (0.5 * c) * u * (1.0 - th * th) * (1.0 + (3.0 * 0.044715) * square)
    return (u * near, slope)


def middle_kernel(
    strip,
    tok_ref,
    cot_ref,
    mix_ref,
    g_ref,
    gout_ref,
    order_ref,
    y_ref,
    gh_ref,
    dmix_ref,
    n2_ref,
    act_ref,
    gl_ref,
    gb_ref,
    vec_ref,
    gfb_ref,
    hid_ref,
    acc_ref,
    back_ref,
    ext_ref,
):
    t = pl.program_id(0)
    steps = pl.num_programs(0)
    half = mix_ref.shape[2]
    parts = gout_ref.shape[0]
    d = tok_ref.shape[1]
    width = mix_ref.shape[1]

    @pl.when(t == 0)
    def _():
        ext_ref[...] = jnp.transpose(gout_ref[0, :, 128:256].astype(F32))[64:72]
        total = tok_ref[...].astype(F32) + ext_ref[2:3]
        for s in range(parts):
            lhs = jnp.concatenate([mix_ref[s], mix_ref[parts + s]], axis=1)
            lhs = jnp.transpose(lhs.astype(F32)).astype(BF16)
            total = total + dot_nt(lhs, gout_ref[s, :, :width])
        hid_ref[...] = total
        n, _ = norm_parts(total)
        n2_ref[...] = (n * ext_ref[0:1] + ext_ref[1:2]).astype(BF16)
        acc_ref[...] = total + ext_ref[3:4]
        back_ref[...] = jnp.zeros_like(back_ref)

    ext = jnp.transpose(g_ref[0, :, 2 * d + 128 : 2 * d + 256].astype(F32))[72:88].astype(BF16)
    bias = pick_rows(dot(ext, order_ref[...]), strip)
    fc = g_ref[0, :, :d]
    pj = g_ref[0, :, d : 2 * d]
    lifted = dot(n2_ref[...], fc) + bias
    act, slope = gelu_parts(lifted)
    act = act.astype(BF16)
    act_ref[0] = act
    gl32 = dot(cot_ref[...], pj) * slope
    gl = gl32.astype(BF16)
    gl_ref[0] = gl
    gfb_ref[0, 0:1, :] = jnp.sum(gl.astype(F32), axis=0, keepdims=True)
    acc_ref[...] += dot_nt(act, pj)
    back_ref[...] += dot_nt(gl, fc)

    @pl.when(t == steps - 1)
    def _():
        y_ref[...] = acc_ref[...].astype(BF16)
        n, scale = norm_parts(hid_ref[...])
        back = back_ref[...]
        cot = cot_ref[...].astype(F32)
        gh = cot + norm_back(back, ext_ref[0:1], n, scale)
        gh_ref[...] = gh
        gb = gh.astype(BF16)
        gb_ref[...] = gb
        vec_ref[0:1, :] = jnp.sum(back * n, axis=0, keepdims=True)
        vec_ref[1:2, :] = jnp.sum(back, axis=0, keepdims=True)
        vec_ref[2:3, :] = jnp.sum(gb.astype(F32), axis=0, keepdims=True)
        vec_ref[3:4, :] = jnp.sum(cot, axis=0, keepdims=True)
        vec_ref[4:8, :] = jnp.zeros((4, d), F32)
        for s in range(parts):
            dm = jnp.transpose(dot(gb, gout_ref[s, :, :width])).astype(BF16)
            dmix_ref[s] = dm[:, :half]
            dmix_ref[parts + s] = dm[:, half:]


def middle(tok, cot, mix, gathered, order, strip):
    rows, d = tok.shape
    parts = gathered.shape[0]
    cols = gathered.shape[2]
    whole = lambda *shape: pl.BlockSpec(shape, lambda t: (0,) * len(shape))
    piece = lambda *shape: pl.BlockSpec(shape, lambda t: (t,) + (0,) * (len(shape) - 1))
    sds = jax.ShapeDtypeStruct
    return pl.pallas_call(
        functools.partial(middle_kernel, strip),
        out_shape=(
            sds((rows, d), BF16),
            sds((rows, d), F32),
            sds(mix.shape, BF16),
            sds((rows, d), BF16),
            sds((parts, rows, d), BF16),
            sds((parts, rows, d), BF16),
            sds((rows, d), BF16),
            sds((8, d), F32),
            sds((parts, 8, d), F32),
        ),
        grid=(parts,),
        in_specs=[
            whole(rows, d),
            whole(rows, d),
            whole(*mix.shape),
            piece(1, d, cols),
            pl.BlockSpec((parts, d, 256), lambda t: (0, 0, cols // 256 - 1)),
            whole(*order.shape),
        ],
        out_specs=(
            whole(rows, d),
            whole(rows, d),
            whole(*mix.shape),
            whole(rows, d),
            piece(1, rows, d),
            piece(1, rows, d),
            whole(rows, d),
            whole(8, d),
            piece(1, 8, d),
        ),
        scratch_shapes=[
            pltpu.VMEM((rows, d), F32),
            pltpu.VMEM((rows, d), F32),
            pltpu.VMEM((rows, d), F32),
            pltpu.VMEM((8, d), F32),
        ],
        compiler_params=params(),
        cost_estimate=cost(2 * rows * d * d * 18, 3e7),
        name="middle",
    )(tok, cot, mix, gathered, gathered, order)


def weights_kernel(
    mode, strip, index_ref, n2_ref, cot_ref, gb_ref, mix_ref, act_ref, gl_ref, vec_ref, gfb_ref, order_ref, *rest
):
    s = pl.program_id(0)
    d = n2_ref.shape[1]
    width = mix_ref.shape[2]
    cols = 2 * d + width + EXT
    nt_ref, ct_ref, bt_ref = rest[-3:]

    @pl.when(s == 0)
    def _():
        nt_ref[...] = jnp.transpose(n2_ref[...].astype(F32)).astype(BF16)
        ct_ref[...] = jnp.transpose(cot_ref[...].astype(F32)).astype(BF16)
        bt_ref[...] = jnp.transpose(gb_ref[...].astype(F32)).astype(BF16)

    mix = jnp.concatenate([mix_ref[0, 0], mix_ref[1, 0]], axis=1)
    turned = dot_nt(spread_rows(gfb_ref[0, 0:1], 16, strip), order_ref[...])
    tall = jnp.concatenate([vec_ref[...], turned, jnp.zeros((EXT - 24, d), F32)], axis=0)
    if mode != "keep":
        out_ref = rest[0]
        out_ref[0, :, :d] = dot(nt_ref[...], gl_ref[0]).astype(BF16)
        out_ref[0, :, d : 2 * d] = dot(ct_ref[...], act_ref[0]).astype(BF16)
        out_ref[0, :, 2 * d : 2 * d + width] = dot_nt(bt_ref[...], mix).astype(BF16)
        out_ref[0, :, 2 * d + width :] = jnp.transpose(tall).astype(BF16)
        return
    came_ref, as_ref, ak_ref, bs_ref, bk_ref, sum_ref = rest[:6]
    sum_ref[:, 2 * d : 2 * d + width] = dot_nt(bt_ref[...], mix).astype(BF16)
    sum_ref[:, 2 * d + width :] = jnp.transpose(tall).astype(BF16)
    sum_ref[:, 2 * d :] = (sum_ref[:, 2 * d :].astype(F32) + came_ref[0, :, 2 * d :].astype(F32)).astype(BF16)
    sum_ref[:, :d] = (dot(nt_ref[...], gl_ref[0]) + came_ref[0, :, :d].astype(F32)).astype(BF16)
    sum_ref[:, d : 2 * d] = (dot(ct_ref[...], act_ref[0]) + came_ref[0, :, d : 2 * d].astype(F32)).astype(BF16)
    depth, step = as_ref.shape[1], as_ref.shape[2]
    cut = cols // 2

    def block(xr, zr):
        at = (zr * 2 + (xr ^ index_ref[2])) * step
        return pl.ds(pl.multiple_of(at, 16), step)

    for zr in range(depth):
        bk_ref[0, zr] = sum_ref[block(0, zr), cut:]
        bs_ref[0, zr] = sum_ref[block(1, zr), cut:]

    @pl.when(s == 0)
    def _():
        for xr in range(2):
            for zr in range(depth):
                as_ref[xr, zr] = sum_ref[block(xr, zr), :cut]

    @pl.when(s == 1)
    def _():
        for xr in range(2):
            for zr in range(depth):
                ak_ref[xr, zr] = sum_ref[block(xr, zr), :cut]


def weights(mode, index, n2, cot, gb, mix, act, gl, vec, gfb, order, strip, came=None, shards=None):
    rows, d = n2.shape
    parts = act.shape[0]
    width = mix.shape[1]
    cols = 2 * d + width + EXT
    steps = parts if mode == "all" else 2
    whole = lambda *shape: pl.BlockSpec(shape, lambda s, ix: (0,) * len(shape))
    piece = lambda *shape: pl.BlockSpec(shape, lambda s, ix: (ix[s],) + (0,) * (len(shape) - 1))
    mix = mix.reshape(mix.shape[0] // parts, parts, width, mix.shape[2])
    operands = [index, n2, cot, gb, mix, act, gl, vec, gfb, order]
    specs = [
        whole(rows, d),
        whole(rows, d),
        whole(rows, d),
        pl.BlockSpec((mix.shape[0], 1, width, mix.shape[3]), lambda s, ix: (0, ix[s], 0, 0)),
        piece(1, rows, d),
        piece(1, rows, d),
        whole(8, d),
        piece(1, 8, d),
        whole(*order.shape),
    ]
    scratch = [pltpu.VMEM((d, rows), BF16) for _ in range(3)]
    if mode == "keep":
        operands.append(came)
        specs.append(pl.BlockSpec((1, d, cols), lambda s, ix: (s, 0, 0)))
        block = (2, shards // 2, d // shards, cols // 2)
        sds = jax.ShapeDtypeStruct(block, BF16)
        out_shape = (sds,) * 4
        turn = pl.BlockSpec((1,) + block[1:], lambda s, ix: (1 - s, 0, 0, 0))
        out_specs = (whole(*block), whole(*block), turn, turn)
        scratch = [pltpu.VMEM((d, cols), BF16)] + scratch
    else:
        out_shape = jax.ShapeDtypeStruct((steps, d, cols), BF16)
        out_specs = pl.BlockSpec((1, d, cols), lambda s, ix: (s, 0, 0))
    return pl.pallas_call(
        functools.partial(weights_kernel, mode, strip),
        out_shape=out_shape,
        grid_spec=pltpu.PrefetchScalarGridSpec(
            num_scalar_prefetch=1,
            grid=(steps,),
            in_specs=specs,
            out_specs=out_specs,
            scratch_shapes=scratch,
        ),
        compiler_params=params(),
        cost_estimate=cost(2 * rows * d * cols * steps, 6e6 * steps),
        name="weights_" + mode,
    )(*operands)


def wide_sum_kernel(place_ref, *refs):
    for i, masks in enumerate(((1, 3), (3, 1))):
        mine_ref, first_ref, second_ref = refs[3 * i : 3 * i + 3]
        keep_ref, send_ref = refs[6 + 2 * i : 8 + 2 * i]
        for ref, base in ((send_ref, masks[0]), (keep_ref, 0)):
            for n, m in enumerate((base, base ^ masks[1])):
                z = pl.ds(place_ref[0] ^ m, 1)
                total = mine_ref[0, z].astype(F32) + first_ref[0, z].astype(F32)
                ref[n : n + 1] = (total + second_ref[z].astype(F32)).astype(BF16)


def wide_sum(place, *parts):
    depth, step, cut = parts[2].shape
    first = pl.BlockSpec((1, depth, step, cut), lambda i, ix: (0, 0, 0, 0))
    last = pl.BlockSpec((depth, step, cut), lambda i, ix: (0, 0, 0))
    out = jax.ShapeDtypeStruct((depth // 2, step, cut), BF16)
    return pl.pallas_call(
        wide_sum_kernel,
        out_shape=(out,) * 4,
        grid_spec=pltpu.PrefetchScalarGridSpec(
            num_scalar_prefetch=1,
            grid=(1,),
            in_specs=[first, first, last] * 2,
            out_specs=(pl.BlockSpec(out.shape, lambda i, ix: (0, 0, 0)),) * 4,
        ),
        compiler_params=params(),
        cost_estimate=cost(0, 4e6),
        name="wide_sum",
    )(place, *parts)


def finish_wide_kernel(*refs):
    fc_ref, pj_ref, out_ref, g_ref, b_ref, ob_ref, pb_ref, fb_ref = refs[-8:]
    d = fc_ref.shape[1]
    width = out_ref.shape[0]
    halves = []
    count = (len(refs) - 8) // 2
    for parts in (refs[:count], refs[count : 2 * count]):
        t = parts[0][0].astype(F32)
        for ref in parts[1:]:
            t = t + ref[0].astype(F32)
        halves.append(t)
    t = jnp.concatenate(halves, axis=1)
    fc_ref[...] = t[:, :d]
    pj_ref[...] = t[:, d : 2 * d]
    rest = jnp.transpose(t[:, 2 * d : 2 * d + width + EXT])
    out_ref[...] = rest[:width]
    g_ref[...] = rest[width : width + 1]
    b_ref[...] = rest[width + 1 : width + 2]
    ob_ref[...] = rest[width + 2 : width + 3]
    pb_ref[...] = rest[width + 3 : width + 4]
    rows, strip = fb_ref.shape
    at = 2 * d + width + 8
    fb_ref[...] = t[:rows, at : at + strip]


def finish_wide(parts, d, width, bias_shape):
    tall = parts[0].shape[1]
    sds = lambda *shape: jax.ShapeDtypeStruct(shape, F32)
    return pl.pallas_call(
        finish_wide_kernel,
        out_shape=(
            sds(tall, d),
            sds(tall, d),
            sds(width, tall),
            sds(1, tall),
            sds(1, tall),
            sds(1, tall),
            sds(1, tall),
            sds(*bias_shape),
        ),
        compiler_params=pltpu.CompilerParams(vmem_limit_bytes=SMALL_LIMIT),
        cost_estimate=cost(0, 2e6),
        name="finish_wide",
    )(*parts)


def finish_narrow_kernel(g_ref, qkv_ref, qb_ref, vec_ref):
    t = g_ref[0].astype(F32)
    for n in range(1, g_ref.shape[0]):
        t = t + g_ref[n].astype(F32)
    width = qkv_ref.shape[2]
    for s in range(3):
        qkv_ref[s] = t[:, s * width : (s + 1) * width]
    heads, piece = qb_ref.shape[1:]
    edge = 3 * width + 8
    for s in range(3):
        qb_ref[s] = t[s * heads : (s + 1) * heads, edge : edge + piece]
    vec_ref[...] = jnp.transpose(t[:, 512:640])[64:72]


def finish_narrow(g, width, bias_shape):
    tall = g.shape[1]
    sds = lambda *shape: jax.ShapeDtypeStruct(shape, F32)
    return pl.pallas_call(
        finish_narrow_kernel,
        out_shape=(sds(3, tall, width), sds(*bias_shape), sds(8, tall)),
        compiler_params=pltpu.CompilerParams(vmem_limit_bytes=SMALL_LIMIT),
        cost_estimate=cost(0, 2e6),
        name="finish_narrow",
    )(g)


def project_back_kernel(
    piece, me_ref, own_ref, far_ref, grad_ref, w_ref, order_ref, keep_ref, send_ref, dw_ref, w3_ref, dw3_ref, gain_ref, vec_ref, bias_ref
):
    i = pl.program_id(0)
    steps = pl.num_programs(0)
    width = grad_ref.shape[2]
    d = w_ref.shape[0]

    @pl.when(i == 0)
    def _():
        gain_ref[...] = jnp.transpose(w_ref[:, 512:640].astype(F32))[64:72]
        for s in range(3):
            w3_ref[s] = w_ref[:, s * width : (s + 1) * width]
        dw3_ref[...] = jnp.zeros_like(dw3_ref)
        vec_ref[...] = jnp.zeros_like(vec_ref)
        bias_ref[...] = jnp.zeros_like(bias_ref)

    far = ((i ^ me_ref[0]) & 1) == 1
    rows = jnp.where(far, far_ref[0], own_ref[0]).astype(F32)
    n, _ = norm_parts(rows)
    normed = n * gain_ref[0:1] + gain_ref[1:2]
    turned = jnp.transpose(normed).astype(BF16)
    part = dot_nt(grad_ref[0], w3_ref[0])
    for s in range(1, 3):
        part = part + dot_nt(grad_ref[s], w3_ref[s])
    for s in range(3):
        dw3_ref[s] += dot(turned, grad_ref[s])
        bias_ref[s : s + 1, :] += jnp.sum(grad_ref[s].astype(F32), axis=0, keepdims=True)
    vec_ref[0:1, :] += jnp.sum(part * n, axis=0, keepdims=True)
    vec_ref[1:2, :] += jnp.sum(part, axis=0, keepdims=True)

    @pl.when(far)
    def _():
        send_ref[0] = part.astype(BF16)

    @pl.when(jnp.logical_not(far))
    def _():
        keep_ref[0] = part

    @pl.when(i == steps - 1)
    def _():
        turned_bias = jnp.zeros((8, d), F32)
        for s in range(3):
            dw_ref[:, s * width : (s + 1) * width] = dw3_ref[s].astype(BF16)
            spread = spread_rows(bias_ref[s : s + 1, :], 8, piece)
            turned_bias = turned_bias + dot_nt(spread, order_ref[s])
        tall = jnp.concatenate([vec_ref[...], turned_bias, jnp.zeros((EXT - 16, d), F32)], axis=0)
        dw_ref[:, 3 * width :] = jnp.transpose(tall).astype(BF16)


def project_back(me, own, far, grad, w, order, piece):
    half, rows, d = own.shape
    width = grad.shape[2]
    blocks = 2 * half
    sds = jax.ShapeDtypeStruct
    rel = lambda i, me: ((i ^ me[0]) // 2, 0, 0)
    return pl.pallas_call(
        functools.partial(project_back_kernel, piece),
        out_shape=(
            sds((half, rows, d), F32),
            sds((half, rows, d), BF16),
            sds(w.shape, BF16),
        ),
        grid_spec=pltpu.PrefetchScalarGridSpec(
            num_scalar_prefetch=1,
            grid=(blocks,),
            in_specs=[
                pl.BlockSpec((1, rows, d), rel),
                pl.BlockSpec((1, rows, d), rel),
                pl.BlockSpec((3, rows, width), lambda i, me: (0, i, 0)),
                pl.BlockSpec(w.shape, lambda i, me: (0, 0)),
                pl.BlockSpec(order.shape, lambda i, me: (0, 0, 0)),
            ],
            out_specs=(
                pl.BlockSpec((1, rows, d), rel),
                pl.BlockSpec((1, rows, d), rel),
                pl.BlockSpec(w.shape, lambda i, me: (0, 0)),
            ),
            scratch_shapes=[
                pltpu.VMEM((3, d, width), BF16),
                pltpu.VMEM((3, d, width), F32),
                pltpu.VMEM((8, d), F32),
                pltpu.VMEM((8, d), F32),
                pltpu.VMEM((8, width), F32),
            ],
        ),
        compiler_params=params(),
        cost_estimate=cost(4 * blocks * rows * d * 3 * width, 1.5e7),
        name="project_back",
    )(me, own, far, grad, w, order)


def pair_kernel(keep_ref, came_ref, own_ref, *send_refs):
    n = pl.program_id(0)
    total = keep_ref[0] + came_ref[0].astype(F32)

    @pl.when(n == 0)
    def _():
        own_ref[...] = total

    for m, ref in enumerate(send_refs):

        @pl.when(n == m + 1)
        def _(ref=ref):
            ref[...] = total.astype(BF16)


def pair_sum(keep, came):
    half, rows, d = keep.shape
    piece = pl.BlockSpec((1, rows, d), lambda n: (n, 0, 0))
    flat = pl.BlockSpec((rows, d), lambda n: (0, 0))
    return pl.pallas_call(
        pair_kernel,
        out_shape=(jax.ShapeDtypeStruct((rows, d), F32),)
        + (jax.ShapeDtypeStruct((rows, d), BF16),) * (half - 1),
        grid=(half,),
        in_specs=[piece, piece],
        out_specs=(flat,) * half,
        compiler_params=params(SMALL_LIMIT),
        cost_estimate=cost(0, 7e6),
        name="pair_sum",
    )(keep, came)


def finish_rows_kernel(side_ref, tok_ref, near_ref, near2_ref, away_ref, away2_ref, gh_ref, w_ref, out_ref, gain_ref):
    m = pl.program_id(0)

    @pl.when(m == 0)
    def _():
        gain_ref[...] = jnp.transpose(w_ref[:, 512:640].astype(F32))[64:72]

    n, scale = norm_parts(tok_ref[0].astype(F32))
    near = near_ref[...] + near2_ref[...].astype(F32)
    away = away_ref[...].astype(F32) + away2_ref[...].astype(F32)
    incoming = jnp.where(m == side_ref[0], near, away)
    out_ref[0] = gh_ref[0] + norm_back(incoming, gain_ref[0:1], n, scale)


def finish_rows(side, tok, near, near2, away, away2, gh, w):
    micro, rows, d = tok.shape
    piece = pl.BlockSpec((1, rows, d), lambda m, ix: (m, 0, 0))
    flat = pl.BlockSpec((rows, d), lambda m, ix: (0, 0))
    return pl.pallas_call(
        finish_rows_kernel,
        out_shape=jax.ShapeDtypeStruct((micro, rows, d), F32),
        grid_spec=pltpu.PrefetchScalarGridSpec(
            num_scalar_prefetch=1,
            grid=(micro,),
            in_specs=[piece, flat, flat, flat, flat, piece, pl.BlockSpec(w.shape, lambda m, ix: (0, 0))],
            out_specs=piece,
            scratch_shapes=[pltpu.VMEM((8, d), F32)],
        ),
        compiler_params=params(SMALL_LIMIT),
        cost_estimate=cost(0, 6e6),
        name="finish_rows",
    )(side, tok, near, near2, away, away2, gh, w)


def one_hot_order(sources, size):
    row = lax.broadcasted_iota(jnp.int32, (size, sources.shape[1]), 0)
    return jnp.where(row == sources, 1.0, 0.0).astype(BF16)


barrier = lax.optimization_barrier


def plus(a, b):
    return (a.astype(F32) + b.astype(F32)).astype(BF16)


def local(
    tokens,
    cotangent,
    ln1_gain,
    ln1_bias,
    qkv_weight,
    qkv_bias,
    out_weight,
    out_bias,
    ln2_gain,
    ln2_bias,
    fc_weight,
    fc_bias,
    proj_weight,
    proj_bias,
):
    sides = lax.axis_size("ctx")
    parts = lax.axis_size("tp")
    shards = lax.axis_size(("dp", "ctx"))
    group = sides * parts
    micro, _, rows, d = tokens.shape
    assert micro == sides == 2 and parts == 4
    side = lax.axis_index("ctx")
    slot = lax.axis_index("tp")
    me = side * parts + slot
    me_array = jnp.stack([me, side]).astype(jnp.int32)
    side_array = jnp.full((1,), side, jnp.int32)
    tall = qkv_weight.shape[1]
    heads, piece = qkv_bias.shape[1], qkv_bias.shape[2]
    width = heads * HD
    lines, strip = fc_bias.shape

    deep = lax.axis_index("dp")
    depth = lax.axis_size("dp")

    def swap_deep(array, mask):
        return lax.ppermute(array, "dp", [(n, n ^ mask) for n in range(depth)])

    def swap(array, mask):
        return lax.ppermute(array, ("ctx", "tp"), [(n, n ^ mask) for n in range(group)])

    tok = tokens[:, 0]
    cot = cotangent[:, 0]

    vectors = [v[None] for v in (ln1_gain, ln1_bias, ln2_gain, ln2_bias, out_bias, proj_bias)]
    wide, narrow = pack(fc_weight, proj_weight.T, out_weight, qkv_weight, vectors, qkv_bias, fc_bias, shards)

    gathered = lax.all_gather(wide, ("tp", "dp", "ctx"), axis=0, tiled=True)
    gathered = gathered.reshape(parts, d, wide.shape[1])

    mine = lax.dynamic_index_in_dim(tok, side, 0, keepdims=False)
    other = lax.dynamic_index_in_dim(tok, 1 - side, 0, keepdims=False)
    blocks = []
    for mask in range(0, group, 2):
        block = other if mask >= parts else mine
        blocks.append(block if mask == 0 else swap(block, mask))
    own = jnp.stack(blocks)
    far = swap(own, 1)

    w_in = lax.all_to_all(narrow, ("dp", "ctx"), 0, 0, tiled=True).reshape(d, narrow.shape[2])

    unit = lax.broadcasted_iota(jnp.int32, (1, 3 * width), 1)
    order_in = one_hot_order(unit % HD // piece * tall + unit // HD, d)
    unit = lax.broadcasted_iota(jnp.int32, (1, d), 1)
    order_fc = one_hot_order(unit % 128 // strip * tall + unit // 128, d)

    order_back = order_in.reshape(d, 3, width).transpose(1, 0, 2)
    far, order_in, order_fc, order_back = barrier((far, order_in, order_fc, order_back))

    triple = project(me_array, own, far, w_in, order_in, piece)
    mixed, mixed_turned, level = attend(triple, rows)
    mix = lax.all_to_all(mixed, ("ctx", "tp"), 0, 0, tiled=True)

    tok_rows = tok.reshape(micro * rows, d)
    cot_rows = cot.reshape(micro * rows, d)
    y, grad_hidden, grad_mix, n2, act, gl, gb, vec, gfb = middle(
        tok_rows, cot_rows, mix, gathered, order_fc, strip
    )
    grad_mix = lax.all_to_all(grad_mix, ("ctx", "tp"), 0, 0, tiled=True)

    parcels = (n2, cot_rows, gb, mix, act, gl, vec, gfb, order_fc, strip)
    exchange = tall % 16 == 0 and depth == 4
    if exchange:
        core, row = slot % 2, slot // 2
        index = lambda lane: jnp.stack([(1 - row) * 2 + lane, row * 2 + lane, side]).astype(jnp.int32)
        came = swap(weights("send", index(1 - core), *parcels), 1)
        a_send, a_keep, b_send, b_keep = weights("keep", index(core), *parcels, came=came, shards=shards)
        a_came, b_came = swap(a_send, 2), swap(b_send, parts)
    else:
        grad_wide = weights("all", jnp.arange(parts, dtype=jnp.int32), *parcels)
        grad_wide = lax.psum_scatter(
            grad_wide.reshape(parts * d, wide.shape[1]), ("tp", "dp", "ctx"), scatter_dimension=0, tiled=True
        )

    grad_triple = attend_back(triple, grad_mix, mixed_turned, level)
    if exchange:
        a_came, b_came, grad_triple = barrier((a_came, b_came, grad_triple))
        a_send, b_send = plus(a_keep[1], a_came[1]), plus(b_keep[1], b_came[1])
        a_send, b_send, grad_triple = barrier((a_send, b_send, grad_triple))
        a_last, b_last = swap(a_send, parts), swap(b_send, 2)
    keep, send, grad_in = project_back(me_array, own, far, grad_triple, w_in, order_back, piece)
    if exchange:
        a_last, b_last, keep, send, grad_in = barrier((a_last, b_last, keep, send, grad_in))

    send_came = swap(send, 1)
    grad_in = lax.all_to_all(grad_in.reshape(narrow.shape), ("dp", "ctx"), 0, 0, tiled=True)
    if exchange:
        place = jnp.full((1,), deep, jnp.int32)
        a_kept, a_send, b_kept, b_send = wide_sum(place, a_keep, a_came, a_last, b_keep, b_came, b_last)
        a_send, send_came = barrier((a_send, send_came))
        a_came, b_came = swap_deep(a_send, 1), swap_deep(b_send, 3)
    near, *sends = pair_sum(keep, send_came)
    arrived = [swap(sends[n - 1], 2 * n) for n in range(1, group // 2)]

    if exchange:
        a_came, b_came, near = barrier((a_came, b_came, near))
        a_send, b_send = plus(a_kept[1:], a_came[1:]), plus(b_kept[1:], b_came[1:])
        a_send, b_send, grad_in = barrier((a_send, b_send, grad_in))
        a_last, b_last = swap_deep(a_send, 3), swap_deep(b_send, 1)
        wide_parts = [a_kept, a_came, a_last, b_kept, b_came, b_last]
    else:
        cut = wide.shape[1] // 2
        wide_parts = [grad_wide[None, :, :cut], grad_wide[None, :, cut:]]
    grad_qkv_weight, grad_qkv_bias, vec_in = finish_narrow(grad_in, width, qkv_bias.shape)
    vec_came = swap(vec_in, 2)
    grad_tokens = finish_rows(
        side_array, tok, near, *arrived, grad_hidden.reshape(micro, rows, d), w_in
    )
    vec_came, grad_tokens = barrier((vec_came, grad_tokens))
    vec_in = vec_in + vec_came
    vec_came = swap(vec_in, 1)
    fc_grad, proj_grad, out_grad, gain2, shift2, out_b, proj_b, fc_b = finish_wide(
        wide_parts, d, width, fc_bias.shape
    )
    vec_came, fc_grad = barrier((vec_came, fc_grad))
    vec_in = vec_in + vec_came
    return (
        y.reshape(micro, 1, rows, d),
        grad_tokens[:, None],
        vec_in[0],
        vec_in[1],
        grad_qkv_weight,
        grad_qkv_bias,
        out_grad,
        out_b[0],
        gain2[0],
        shift2[0],
        fc_grad,
        fc_b,
        proj_grad.T,
        proj_b[0],
    )


def solution(mesh):
    rows = P(None, "dp", ("ctx", "tp"), None)
    vector = P(("dp", "ctx"))
    joint = P(None, ("dp", "ctx"), "tp")
    joint_bias = P(None, "tp", ("dp", "ctx"))
    down = P("tp", ("dp", "ctx"))
    up = P(("dp", "ctx"), "tp")
    inner = (vector, vector, joint, joint_bias, down, vector, vector, vector, up, down, down, vector)
    return jax.shard_map(
        local,
        mesh=mesh,
        in_specs=(rows, rows) + inner,
        out_specs=(rows, rows) + inner,
        check_vma=False,
    )
```

```python
import functools

import jax
import jax.numpy as jnp
from jax import lax
from jax.experimental import pallas as pl
from jax.experimental.pallas import tpu as pltpu
from jax.sharding import PartitionSpec as P

HD = 64
EPS = 1e-05
LOG2E = 1.4426950408889634
F32 = jnp.float32
BF16 = jnp.bfloat16
VMEM_LIMIT = 60 * 1024 * 1024
SMALL_LIMIT = 60 * 1024 * 1024
EXT = 64


def dot(a, b):
    return lax.dot_general(a, b, (((1,), (0,)), ((), ())), preferred_element_type=F32)


def dot_nt(a, b):
    return lax.dot_general(a, b, (((1,), (1,)), ((), ())), preferred_element_type=F32)


def norm_parts(rows):
    mean = jnp.mean(rows, axis=-1, keepdims=True)
    centered = rows - mean
    spread = jnp.mean(centered * centered, axis=-1, keepdims=True)
    scale = lax.rsqrt(spread + EPS)
    return (centered * scale, scale)


def norm_back(incoming, gain, n, scale):
    e = incoming * gain
    return (e - jnp.mean(e, axis=-1, keepdims=True) - n * jnp.mean(e * n, axis=-1, keepdims=True)) * scale


def params(limit=VMEM_LIMIT):
    return pltpu.CompilerParams(dimension_semantics=("arbitrary",), vmem_limit_bytes=limit)


def cost(flops, moved, exps=0):
    return pl.CostEstimate(flops=int(flops), bytes_accessed=int(moved), transcendentals=int(exps))


def pack_kernel(fc_ref, pj_ref, out_ref, qkv_ref, qb_ref, fb_ref, *rest):
    vec_refs, wide_ref, narrow_ref = rest[:-2], rest[-2], rest[-1]
    tall, d = fc_ref.shape
    width = out_ref.shape[0]
    copies = narrow_ref.shape[0]
    vectors = jnp.concatenate([ref[...].astype(F32) for ref in vec_refs] + [jnp.zeros((2, tall), F32)], axis=0)
    columns = jnp.transpose(vectors).astype(BF16)
    wide_ref[:, :d] = fc_ref[...]
    wide_ref[:, d : 2 * d] = pj_ref[...]
    wide_ref[:, 2 * d : 2 * d + width] = jnp.transpose(out_ref[...].astype(F32)).astype(BF16)
    edge = 2 * d + width
    wide_ref[:, edge:] = jnp.zeros((tall, EXT), BF16)
    wide_ref[:, edge : edge + 4] = columns[:, 2:6]
    rows, strip = fb_ref.shape
    wide_ref[:rows, edge + 8 : edge + 8 + strip] = fb_ref[...]
    for s in range(3):
        narrow_ref[0, :, s * width : (s + 1) * width] = qkv_ref[s]
    edge = 3 * width
    narrow_ref[0, :, edge:] = jnp.zeros((tall, EXT), BF16)
    narrow_ref[0, :, edge : edge + 2] = columns[:, :2]
    heads, piece = qb_ref.shape[1:]
    for s in range(3):
        narrow_ref[0, s * heads : (s + 1) * heads, edge + 8 : edge + 8 + piece] = qb_ref[s]
    whole = narrow_ref[0]
    for n in range(1, copies):
        narrow_ref[n] = whole


def pack(fc, pj, out, qkv, vec, qb, fb, copies):
    tall, d = fc.shape
    width = out.shape[0]
    return pl.pallas_call(
        pack_kernel,
        out_shape=(
            jax.ShapeDtypeStruct((tall, 2 * d + width + EXT), BF16),
            jax.ShapeDtypeStruct((copies, tall, 3 * width + EXT), BF16),
        ),
        compiler_params=pltpu.CompilerParams(vmem_limit_bytes=SMALL_LIMIT),
        cost_estimate=cost(0, 2e6),
        name="pack",
    )(fc, pj, out, qkv, qb, fb, *vec)


def pick_rows(table, period):
    line = lax.broadcasted_iota(jnp.int32, table.shape, 0)
    lane = lax.broadcasted_iota(jnp.int32, table.shape, 1)
    return jnp.sum(jnp.where(line == (lane & (period - 1)), table, 0.0), axis=0, keepdims=True)


def spread_rows(row, lines, period):
    shape = (lines, row.shape[1])
    line = lax.broadcasted_iota(jnp.int32, shape, 0)
    lane = lax.broadcasted_iota(jnp.int32, shape, 1)
    return jnp.where(line == (lane & (period - 1)), jnp.broadcast_to(row, shape), 0.0).astype(BF16)


def project_kernel(piece, me_ref, own_ref, far_ref, w_ref, order_ref, out_ref, vec_ref, bias_ref):
    i = pl.program_id(0)
    width = out_ref.shape[2]

    @pl.when(i == 0)
    def _():
        turned = jnp.transpose(w_ref[:, 512:640].astype(F32))
        vec_ref[...] = turned[64:72]
        table = dot(turned[72:80].astype(BF16), order_ref[...])
        bias_ref[...] = jnp.broadcast_to(pick_rows(table, piece), bias_ref.shape)

    far = ((i ^ me_ref[0]) & 1) == 1
    rows = jnp.where(far, far_ref[0], own_ref[0]).astype(F32)
    n, _ = norm_parts(rows)
    normed = (n * vec_ref[0:1] + vec_ref[1:2]).astype(BF16)
    full = dot(normed, w_ref[...])[:, : 3 * width] + bias_ref[0:1, :]
    full = full.astype(BF16)
    out_ref[0] = full[:, :width] * jnp.asarray(HD ** (-0.5), BF16)
    out_ref[1] = full[:, width : 2 * width]
    out_ref[2] = full[:, 2 * width :]


def project(me, own, far, w, order, piece):
    half, rows, d = own.shape
    blocks = 2 * half
    width = order.shape[1] // 3
    return pl.pallas_call(
        functools.partial(project_kernel, piece),
        out_shape=jax.ShapeDtypeStruct((3, blocks * rows, width), BF16),
        grid_spec=pltpu.PrefetchScalarGridSpec(
            num_scalar_prefetch=1,
            grid=(blocks,),
            in_specs=[
                pl.BlockSpec((1, rows, d), lambda i, me: ((i ^ me[0]) // 2, 0, 0)),
                pl.BlockSpec((1, rows, d), lambda i, me: ((i ^ me[0]) // 2, 0, 0)),
                pl.BlockSpec(w.shape, lambda i, me: (0, 0)),
                pl.BlockSpec(order.shape, lambda i, me: (0, 0)),
            ],
            out_specs=pl.BlockSpec((3, rows, width), lambda i, me: (0, i, 0)),
            scratch_shapes=[pltpu.VMEM((8, d), F32), pltpu.VMEM((8, 3 * width), F32)],
        ),
        compiler_params=params(),
        cost_estimate=cost(2 * blocks * rows * d * 3 * width, 8e6),
        name="project",
    )(me, own, far, w, order)


def head_mask(shape, h):
    lane = lax.broadcasted_iota(jnp.int32, shape, 1)
    return (lane >= h * HD) & (lane < (h + 1) * HD)


def attend_kernel(q_ref, k_ref, v_ref, o_ref, ot_ref, level_ref, vt_ref, qm_ref, m_ref, l_ref):
    i = pl.program_id(0)
    heads = q_ref.shape[2] // HD
    bq = q_ref.shape[1]
    half = bq // 2

    @pl.when(i == 0)
    def _():
        vt_ref[...] = jnp.transpose(v_ref[0].astype(F32)).astype(BF16)

    for h in range(heads):
        q = q_ref[0]
        qm_ref[h] = jnp.where(head_mask(q.shape, h), q, jnp.zeros_like(q))
    m_ref[...] = jnp.zeros_like(m_ref)
    l_ref[...] = jnp.zeros_like(l_ref)
    ot_ref[...] = jnp.zeros_like(ot_ref)

    def chunk(start, size, first, masked):
        cols = slice(first, bq)
        keys = k_ref[0, pl.ds(start, size), :]
        for h in range(heads):
            u = dot_nt(keys, qm_ref[h, first:bq, :]) * LOG2E
            if masked:
                key_pos = lax.broadcasted_iota(jnp.int32, u.shape, 0)
                row_pos = lax.broadcasted_iota(jnp.int32, u.shape, 1)
                allowed = key_pos <= row_pos
                u = jnp.where(allowed, u, 0.0)
            before = m_ref[h : h + 1, cols]
            peak = jnp.maximum(before, jnp.max(jnp.abs(u), axis=0, keepdims=True))
            fade = jnp.exp2(before - peak)
            upper = jnp.exp2(u - peak)
            lower = jnp.exp2(-peak - u)
            both = upper + lower
            if masked:
                both = jnp.where(allowed, both, 0.0)
            m_ref[h : h + 1, cols] = peak
            l_ref[h : h + 1, cols] = l_ref[h : h + 1, cols] * fade + jnp.sum(both, axis=0, keepdims=True)
            part = dot(vt_ref[h * HD : (h + 1) * HD, pl.ds(start, size)], (upper - lower).astype(BF16))
            ot_ref[h * HD : (h + 1) * HD, cols] = ot_ref[h * HD : (h + 1) * HD, cols] * fade + part

    def body(j, carry):
        chunk(pl.multiple_of(j * bq, bq), bq, 0, False)
        return carry

    lax.fori_loop(0, i, body, 0)
    base = pl.multiple_of(i * bq, bq)
    chunk(base, half, 0, True)
    chunk(pl.multiple_of(base + half, half), half, half, True)
    for h in range(heads):
        total = l_ref[h : h + 1, :]
        level_ref[h : h + 1, :] = m_ref[h : h + 1, :] + jnp.log2(total)
        ot_ref[h * HD : (h + 1) * HD, :] = ot_ref[h * HD : (h + 1) * HD, :] * (1.0 / total)
    rows = o_ref.shape[2]
    for n in range(bq // rows):
        o_ref[n] = ot_ref[:, n * rows : (n + 1) * rows].astype(BF16)


def attend(triple, rows):
    _, span, width = triple.shape
    bq = min(512, span)
    heads = width // HD
    return pl.pallas_call(
        attend_kernel,
        out_shape=(
            jax.ShapeDtypeStruct((span // rows, width, rows), BF16),
            jax.ShapeDtypeStruct((width, span), F32),
            jax.ShapeDtypeStruct((8, span), F32),
        ),
        grid=(span // bq,),
        in_specs=[
            pl.BlockSpec((1, bq, width), lambda i: (0, i, 0)),
            pl.BlockSpec((1, span, width), lambda i: (1, 0, 0)),
            pl.BlockSpec((1, span, width), lambda i: (2, 0, 0)),
        ],
        out_specs=(
            pl.BlockSpec((bq // rows, width, rows), lambda i: (i, 0, 0)),
            pl.BlockSpec((width, bq), lambda i: (0, i)),
            pl.BlockSpec((8, bq), lambda i: (0, i)),
        ),
        scratch_shapes=[
            pltpu.VMEM((width, span), BF16),
            pltpu.VMEM((heads, bq, width), BF16),
            pltpu.VMEM((8, bq), F32),
            pltpu.VMEM((8, bq), F32),
        ],
        compiler_params=params(),
        cost_estimate=cost(4 * span * span * width, 8e6, span * span * heads),
        name="attend",
    )(triple, triple, triple)


def attend_back_kernel(
    qkv_ref, grad_ref, ot_ref, level_ref, out_ref, qm_ref, gm_ref, kt_ref, dqt_ref, dot_ref, dk_ref, dv_ref
):
    j = pl.program_id(0)
    blocks = pl.num_programs(0)
    span, width = qkv_ref.shape[1:]
    rows = grad_ref.shape[2]
    heads = width // HD
    count = qm_ref.shape[0]
    b = span // count
    half = b // 2

    @pl.when(j == 0)
    def _():
        for n in range(span // rows):
            cols = slice(n * rows, (n + 1) * rows)
            turned = grad_ref[n].astype(F32)
            prod = turned * ot_ref[:, cols]
            for h in range(heads):
                dot_ref[h : h + 1, cols] = jnp.sum(prod[h * HD : (h + 1) * HD], axis=0, keepdims=True)
            g = jnp.transpose(turned).astype(BF16)
            at = n * rows % b
            for h in range(heads):
                mask = head_mask(g.shape, h)
                gm_ref[n * rows // b, h * b + at : h * b + at + rows, :] = jnp.where(mask, g, jnp.zeros_like(g))
        kt_ref[...] = jnp.transpose(qkv_ref[1].astype(F32)).astype(BF16)
        dqt_ref[...] = jnp.zeros_like(dqt_ref)
        for n in range(count):
            q = qkv_ref[0, n * b : (n + 1) * b, :]
            for h in range(heads):
                mask = head_mask(q.shape, h)
                qm_ref[n, h * b : (h + 1) * b, :] = jnp.where(mask, q, jnp.zeros_like(q))

    dk_ref[...] = jnp.zeros_like(dk_ref)
    dv_ref[...] = jnp.zeros_like(dv_ref)

    def chunk(i, key_first, key_size, first, masked):
        start = pl.multiple_of(j * b + key_first, half)
        keys = qkv_ref[1, pl.ds(start, key_size), :]
        vals = qkv_ref[2, pl.ds(start, key_size), :]
        cols = b - first
        at = pl.multiple_of(i * b + first, half)
        for h in range(heads):
            lo = h * b + first
            qm = qm_ref[i, lo : lo + cols, :]
            gm = gm_ref[i, lo : lo + cols, :]
            level = level_ref[h : h + 1, pl.ds(at, cols)]
            inner = dot_ref[h : h + 1, pl.ds(at, cols)]
            u = dot_nt(keys, qm) * LOG2E
            upper = jnp.exp2(u - level)
            lower = jnp.exp2(-level - u)
            gw = dot_nt(vals, gm)
            weights = upper - lower
            gs = upper * (gw - inner) + lower * (gw + inner)
            if masked:
                key_pos = lax.broadcasted_iota(jnp.int32, u.shape, 0)
                row_pos = lax.broadcasted_iota(jnp.int32, u.shape, 1)
                allowed = key_pos <= row_pos
                weights = jnp.where(allowed, weights, 0.0)
                gs = jnp.where(allowed, gs, 0.0)
            weights = weights.astype(BF16)
            gs = gs.astype(BF16)
            rows = slice(key_first, key_first + key_size)
            dv_ref[rows, :] += dot(weights, gm)
            dk_ref[rows, :] += dot(gs, qm)
            dqt_ref[h * HD : (h + 1) * HD, pl.ds(at, cols)] += dot(
                kt_ref[h * HD : (h + 1) * HD, pl.ds(start, key_size)], gs
            )

    def body(i, carry):
        chunk(i, 0, b, 0, False)
        return carry

    chunk(j, 0, half, 0, True)
    chunk(j, half, half, half, True)
    lax.fori_loop(j + 1, blocks, body, 0)
    here = pl.ds(pl.multiple_of(j * b, b), b)
    out_ref[1, here, :] = dk_ref[...].astype(BF16)
    out_ref[2, here, :] = dv_ref[...].astype(BF16)

    @pl.when(j == blocks - 1)
    def _():
        out_ref[0] = jnp.transpose(dqt_ref[...] * (HD ** (-0.5))).astype(BF16)


def attend_back(triple, grad, ot, level):
    _, span, width = triple.shape
    b = min(512, span)
    count = span // b
    heads = width // HD
    whole = lambda *shape: pl.BlockSpec(shape, lambda j: (0,) * len(shape))
    return pl.pallas_call(
        attend_back_kernel,
        out_shape=jax.ShapeDtypeStruct(triple.shape, BF16),
        grid=(count,),
        in_specs=[
            whole(*triple.shape),
            whole(*grad.shape),
            whole(*ot.shape),
            whole(*level.shape),
        ],
        out_specs=whole(*triple.shape),
        scratch_shapes=[
            pltpu.VMEM((count, heads * b, width), BF16),
            pltpu.VMEM((count, heads * b, width), BF16),
            pltpu.VMEM((width, span), BF16),
            pltpu.VMEM((width, span), F32),
            pltpu.VMEM((8, span), F32),
            pltpu.VMEM((b, width), F32),
            pltpu.VMEM((b, width), F32),
        ],
        compiler_params=params(),
        cost_estimate=cost(10 * span * span * width, 1e7, span * span * heads),
        name="attend_back",
    )(triple, grad, ot, level)


def gelu_parts(u):
    c = 0.7978845608028654
    square = u * u
    th = jnp.tanh(c * u * (1.0 + 0.044715 * square))
    near = 0.5 * (1.0 + th)
    slope = near + (0.5 * c) * u * (1.0 - th * th) * (1.0 + (3.0 * 0.044715) * square)
    return (u * near, slope)


def middle_kernel(
    strip,
    tok_ref,
    cot_ref,
    mix_ref,
    g_ref,
    gout_ref,
    order_ref,
    y_ref,
    gh_ref,
    dmix_ref,
    n2_ref,
    act_ref,
    gl_ref,
    gb_ref,
    vec_ref,
    gfb_ref,
    hid_ref,
    acc_ref,
    back_ref,
    ext_ref,
):
    t = pl.program_id(0)
    steps = pl.num_programs(0)
    half = mix_ref.shape[2]
    parts = gout_ref.shape[0]
    d = tok_ref.shape[1]
    width = mix_ref.shape[1]

    @pl.when(t == 0)
    def _():
        ext_ref[...] = jnp.transpose(gout_ref[0, :, 128:256].astype(F32))[64:72]
        total = tok_ref[...].astype(F32) + ext_ref[2:3]
        for s in range(parts):
            lhs = jnp.concatenate([mix_ref[s], mix_ref[parts + s]], axis=1)
            lhs = jnp.transpose(lhs.astype(F32)).astype(BF16)
            total = total + dot_nt(lhs, gout_ref[s, :, :width])
        hid_ref[...] = total
        n, _ = norm_parts(total)
        n2_ref[...] = (n * ext_ref[0:1] + ext_ref[1:2]).astype(BF16)
        acc_ref[...] = total + ext_ref[3:4]
        back_ref[...] = jnp.zeros_like(back_ref)

    ext = jnp.transpose(g_ref[0, :, 2 * d + 128 : 2 * d + 256].astype(F32))[72:88].astype(BF16)
    bias = pick_rows(dot(ext, order_ref[...]), strip)
    fc = g_ref[0, :, :d]
    pj = g_ref[0, :, d : 2 * d]
    lifted = dot(n2_ref[...], fc) + bias
    act, slope = gelu_parts(lifted)
    act = act.astype(BF16)
    act_ref[0] = act
    gl32 = dot(cot_ref[...], pj) * slope
    gl = gl32.astype(BF16)
    gl_ref[0] = gl
    gfb_ref[0, 0:1, :] = jnp.sum(gl.astype(F32), axis=0, keepdims=True)
    acc_ref[...] += dot_nt(act, pj)
    back_ref[...] += dot_nt(gl, fc)

    @pl.when(t == steps - 1)
    def _():
        y_ref[...] = acc_ref[...].astype(BF16)
        n, scale = norm_parts(hid_ref[...])
        back = back_ref[...]
        cot = cot_ref[...].astype(F32)
        gh = cot + norm_back(back, ext_ref[0:1], n, scale)
        gh_ref[...] = gh
        gb = gh.astype(BF16)
        gb_ref[...] = gb
        vec_ref[0:1, :] = jnp.sum(back * n, axis=0, keepdims=True)
        vec_ref[1:2, :] = jnp.sum(back, axis=0, keepdims=True)
        vec_ref[2:3, :] = jnp.sum(gb.astype(F32), axis=0, keepdims=True)
        vec_ref[3:4, :] = jnp.sum(cot, axis=0, keepdims=True)
        vec_ref[4:8, :] = jnp.zeros((4, d), F32)
        for s in range(parts):
            dm = jnp.transpose(dot(gb, gout_ref[s, :, :width])).astype(BF16)
            dmix_ref[s] = dm[:, :half]
            dmix_ref[parts + s] = dm[:, half:]


def middle(tok, cot, mix, gathered, order, strip):
    rows, d = tok.shape
    parts = gathered.shape[0]
    cols = gathered.shape[2]
    whole = lambda *shape: pl.BlockSpec(shape, lambda t: (0,) * len(shape))
    piece = lambda *shape: pl.BlockSpec(shape, lambda t: (t,) + (0,) * (len(shape) - 1))
    sds = jax.ShapeDtypeStruct
    return pl.pallas_call(
        functools.partial(middle_kernel, strip),
        out_shape=(
            sds((rows, d), BF16),
            sds((rows, d), F32),
            sds(mix.shape, BF16),
            sds((rows, d), BF16),
            sds((parts, rows, d), BF16),
            sds((parts, rows, d), BF16),
            sds((rows, d), BF16),
            sds((8, d), F32),
            sds((parts, 8, d), F32),
        ),
        grid=(parts,),
        in_specs=[
            whole(rows, d),
            whole(rows, d),
            whole(*mix.shape),
            piece(1, d, cols),
            pl.BlockSpec((parts, d, 256), lambda t: (0, 0, cols // 256 - 1)),
            whole(*order.shape),
        ],
        out_specs=(
            whole(rows, d),
            whole(rows, d),
            whole(*mix.shape),
            whole(rows, d),
            piece(1, rows, d),
            piece(1, rows, d),
            whole(rows, d),
            whole(8, d),
            piece(1, 8, d),
        ),
        scratch_shapes=[
            pltpu.VMEM((rows, d), F32),
            pltpu.VMEM((rows, d), F32),
            pltpu.VMEM((rows, d), F32),
            pltpu.VMEM((8, d), F32),
        ],
        compiler_params=params(),
        cost_estimate=cost(2 * rows * d * d * 18, 3e7),
        name="middle",
    )(tok, cot, mix, gathered, gathered, order)


def weights_kernel(
    mode, strip, index_ref, n2_ref, cot_ref, gb_ref, mix_ref, act_ref, gl_ref, vec_ref, gfb_ref, order_ref, *rest
):
    s = pl.program_id(0)
    d = n2_ref.shape[1]
    width = mix_ref.shape[2]
    cols = 2 * d + width + EXT
    nt_ref, ct_ref, bt_ref = rest[-3:]

    @pl.when(s == 0)
    def _():
        nt_ref[...] = jnp.transpose(n2_ref[...].astype(F32)).astype(BF16)
        ct_ref[...] = jnp.transpose(cot_ref[...].astype(F32)).astype(BF16)
        bt_ref[...] = jnp.transpose(gb_ref[...].astype(F32)).astype(BF16)

    mix = jnp.concatenate([mix_ref[0, 0], mix_ref[1, 0]], axis=1)
    turned = dot_nt(spread_rows(gfb_ref[0, 0:1], 16, strip), order_ref[...])
    tall = jnp.concatenate([vec_ref[...], turned, jnp.zeros((EXT - 24, d), F32)], axis=0)
    if mode != "keep":
        out_ref = rest[0]
        out_ref[0, :, :d] = dot(nt_ref[...], gl_ref[0]).astype(BF16)
        out_ref[0, :, d : 2 * d] = dot(ct_ref[...], act_ref[0]).astype(BF16)
        out_ref[0, :, 2 * d : 2 * d + width] = dot_nt(bt_ref[...], mix).astype(BF16)
        out_ref[0, :, 2 * d + width :] = jnp.transpose(tall).astype(BF16)
        return
    came_ref, as_ref, ak_ref, bs_ref, bk_ref, sum_ref = rest[:6]
    sum_ref[:, 2 * d : 2 * d + width] = dot_nt(bt_ref[...], mix).astype(BF16)
    sum_ref[:, 2 * d + width :] = jnp.transpose(tall).astype(BF16)
    sum_ref[:, 2 * d :] = (sum_ref[:, 2 * d :].astype(F32) + came_ref[0, :, 2 * d :].astype(F32)).astype(BF16)
    sum_ref[:, :d] = (dot(nt_ref[...], gl_ref[0]) + came_ref[0, :, :d].astype(F32)).astype(BF16)
    sum_ref[:, d : 2 * d] = (dot(ct_ref[...], act_ref[0]) + came_ref[0, :, d : 2 * d].astype(F32)).astype(BF16)
    depth, step = as_ref.shape[1], as_ref.shape[2]
    cut = cols // 2

    def block(xr, zr):
        at = (zr * 2 + (xr ^ index_ref[2])) * step
        return pl.ds(pl.multiple_of(at, 16), step)

    for zr in range(depth):
        bk_ref[0, zr] = sum_ref[block(0, zr), cut:]
        bs_ref[0, zr] = sum_ref[block(1, zr), cut:]

    @pl.when(s == 0)
    def _():
        for xr in range(2):
            for zr in range(depth):
                as_ref[xr, zr] = sum_ref[block(xr, zr), :cut]

    @pl.when(s == 1)
    def _():
        for xr in range(2):
            for zr in range(depth):
                ak_ref[xr, zr] = sum_ref[block(xr, zr), :cut]


def weights(mode, index, n2, cot, gb, mix, act, gl, vec, gfb, order, strip, came=None, shards=None):
    rows, d = n2.shape
    parts = act.shape[0]
    width = mix.shape[1]
    cols = 2 * d + width + EXT
    steps = parts if mode == "all" else 2
    whole = lambda *shape: pl.BlockSpec(shape, lambda s, ix: (0,) * len(shape))
    piece = lambda *shape: pl.BlockSpec(shape, lambda s, ix: (ix[s],) + (0,) * (len(shape) - 1))
    mix = mix.reshape(mix.shape[0] // parts, parts, width, mix.shape[2])
    operands = [index, n2, cot, gb, mix, act, gl, vec, gfb, order]
    specs = [
        whole(rows, d),
        whole(rows, d),
        whole(rows, d),
        pl.BlockSpec((mix.shape[0], 1, width, mix.shape[3]), lambda s, ix: (0, ix[s], 0, 0)),
        piece(1, rows, d),
        piece(1, rows, d),
        whole(8, d),
        piece(1, 8, d),
        whole(*order.shape),
    ]
    scratch = [pltpu.VMEM((d, rows), BF16) for _ in range(3)]
    if mode == "keep":
        operands.append(came)
        specs.append(pl.BlockSpec((1, d, cols), lambda s, ix: (s, 0, 0)))
        block = (2, shards // 2, d // shards, cols // 2)
        sds = jax.ShapeDtypeStruct(block, BF16)
        out_shape = (sds,) * 4
        turn = pl.BlockSpec((1,) + block[1:], lambda s, ix: (1 - s, 0, 0, 0))
        out_specs = (whole(*block), whole(*block), turn, turn)
        scratch = [pltpu.VMEM((d, cols), BF16)] + scratch
    else:
        out_shape = jax.ShapeDtypeStruct((steps, d, cols), BF16)
        out_specs = pl.BlockSpec((1, d, cols), lambda s, ix: (s, 0, 0))
    return pl.pallas_call(
        functools.partial(weights_kernel, mode, strip),
        out_shape=out_shape,
        grid_spec=pltpu.PrefetchScalarGridSpec(
            num_scalar_prefetch=1,
            grid=(steps,),
            in_specs=specs,
            out_specs=out_specs,
            scratch_shapes=scratch,
        ),
        compiler_params=params(),
        cost_estimate=cost(2 * rows * d * cols * steps, 6e6 * steps),
        name="weights_" + mode,
    )(*operands)


def wide_sum_kernel(place_ref, *refs):
    keep_ref, send_ref = refs[6:]
    cut = keep_ref.shape[2] // 2
    for i in range(2):
        mine_ref, first_ref, second_ref = refs[3 * i : 3 * i + 3]
        for ref, members in ((send_ref, (1, 2)), (keep_ref, (0, 3))):
            for n, m in enumerate(members):
                z = pl.ds(place_ref[0] ^ m, 1)
                total = mine_ref[0, z].astype(F32) + first_ref[0, z].astype(F32)
                ref[n : n + 1, :, i * cut : (i + 1) * cut] = (total + second_ref[z].astype(F32)).astype(BF16)


def wide_sum(place, *parts):
    depth, step, cut = parts[2].shape
    first = pl.BlockSpec((1, depth, step, cut), lambda i, ix: (0, 0, 0, 0))
    last = pl.BlockSpec((depth, step, cut), lambda i, ix: (0, 0, 0))
    out = jax.ShapeDtypeStruct((depth // 2, step, 2 * cut), BF16)
    return pl.pallas_call(
        wide_sum_kernel,
        out_shape=(out, out),
        grid_spec=pltpu.PrefetchScalarGridSpec(
            num_scalar_prefetch=1,
            grid=(1,),
            in_specs=[first, first, last] * 2,
            out_specs=(pl.BlockSpec(out.shape, lambda i, ix: (0, 0, 0)),) * 2,
        ),
        compiler_params=params(),
        cost_estimate=cost(0, 4e6),
        name="wide_sum",
    )(place, *parts)


def finish_wide_kernel(*refs):
    fc_ref, pj_ref, out_ref, g_ref, b_ref, ob_ref, pb_ref, fb_ref = refs[-8:]
    d = fc_ref.shape[1]
    width = out_ref.shape[0]
    t = refs[0][0].astype(F32)
    for ref in refs[1:-8]:
        t = t + ref[0].astype(F32)
    fc_ref[...] = t[:, :d]
    pj_ref[...] = t[:, d : 2 * d]
    rest = jnp.transpose(t[:, 2 * d : 2 * d + width + EXT])
    out_ref[...] = rest[:width]
    g_ref[...] = rest[width : width + 1]
    b_ref[...] = rest[width + 1 : width + 2]
    ob_ref[...] = rest[width + 2 : width + 3]
    pb_ref[...] = rest[width + 3 : width + 4]
    rows, strip = fb_ref.shape
    at = 2 * d + width + 8
    fb_ref[...] = t[:rows, at : at + strip]


def finish_wide(parts, d, width, bias_shape):
    tall = parts[0].shape[1]
    sds = lambda *shape: jax.ShapeDtypeStruct(shape, F32)
    return pl.pallas_call(
        finish_wide_kernel,
        out_shape=(
            sds(tall, d),
            sds(tall, d),
            sds(width, tall),
            sds(1, tall),
            sds(1, tall),
            sds(1, tall),
            sds(1, tall),
            sds(*bias_shape),
        ),
        compiler_params=pltpu.CompilerParams(vmem_limit_bytes=SMALL_LIMIT),
        cost_estimate=cost(0, 2e6),
        name="finish_wide",
    )(*parts)


def finish_narrow_kernel(g_ref, qkv_ref, qb_ref, vec_ref):
    t = g_ref[0].astype(F32)
    for n in range(1, g_ref.shape[0]):
        t = t + g_ref[n].astype(F32)
    width = qkv_ref.shape[2]
    for s in range(3):
        qkv_ref[s] = t[:, s * width : (s + 1) * width]
    heads, piece = qb_ref.shape[1:]
    edge = 3 * width + 8
    for s in range(3):
        qb_ref[s] = t[s * heads : (s + 1) * heads, edge : edge + piece]
    vec_ref[...] = jnp.transpose(t[:, 512:640])[64:72]


def finish_narrow(g, width, bias_shape):
    tall = g.shape[1]
    sds = lambda *shape: jax.ShapeDtypeStruct(shape, F32)
    return pl.pallas_call(
        finish_narrow_kernel,
        out_shape=(sds(3, tall, width), sds(*bias_shape), sds(8, tall)),
        compiler_params=pltpu.CompilerParams(vmem_limit_bytes=SMALL_LIMIT),
        cost_estimate=cost(0, 2e6),
        name="finish_narrow",
    )(g)


def project_back_kernel(
    piece, me_ref, own_ref, far_ref, grad_ref, w_ref, order_ref, keep_ref, send_ref, dw_ref, w3_ref, dw3_ref, gain_ref, vec_ref, bias_ref
):
    i = pl.program_id(0)
    steps = pl.num_programs(0)
    width = grad_ref.shape[2]
    d = w_ref.shape[0]

    @pl.when(i == 0)
    def _():
        gain_ref[...] = jnp.transpose(w_ref[:, 512:640].astype(F32))[64:72]
        for s in range(3):
            w3_ref[s] = w_ref[:, s * width : (s + 1) * width]
        dw3_ref[...] = jnp.zeros_like(dw3_ref)
        vec_ref[...] = jnp.zeros_like(vec_ref)
        bias_ref[...] = jnp.zeros_like(bias_ref)

    far = ((i ^ me_ref[0]) & 1) == 1
    rows = jnp.where(far, far_ref[0], own_ref[0]).astype(F32)
    n, _ = norm_parts(rows)
    normed = n * gain_ref[0:1] + gain_ref[1:2]
    turned = jnp.transpose(normed).astype(BF16)
    part = dot_nt(grad_ref[0], w3_ref[0])
    for s in range(1, 3):
        part = part + dot_nt(grad_ref[s], w3_ref[s])
    for s in range(3):
        dw3_ref[s] += dot(turned, grad_ref[s])
        bias_ref[s : s + 1, :] += jnp.sum(grad_ref[s].astype(F32), axis=0, keepdims=True)
    vec_ref[0:1, :] += jnp.sum(part * n, axis=0, keepdims=True)
    vec_ref[1:2, :] += jnp.sum(part, axis=0, keepdims=True)

    @pl.when(far)
    def _():
        send_ref[0] = part.astype(BF16)

    @pl.when(jnp.logical_not(far))
    def _():
        keep_ref[0] = part

    @pl.when(i == steps - 1)
    def _():
        turned_bias = jnp.zeros((8, d), F32)
        for s in range(3):
            dw_ref[:, s * width : (s + 1) * width] = dw3_ref[s].astype(BF16)
            spread = spread_rows(bias_ref[s : s + 1, :], 8, piece)
            turned_bias = turned_bias + dot_nt(spread, order_ref[s])
        tall = jnp.concatenate([vec_ref[...], turned_bias, jnp.zeros((EXT - 16, d), F32)], axis=0)
        dw_ref[:, 3 * width :] = jnp.transpose(tall).astype(BF16)


def project_back(me, own, far, grad, w, order, piece):
    half, rows, d = own.shape
    width = grad.shape[2]
    blocks = 2 * half
    sds = jax.ShapeDtypeStruct
    rel = lambda i, me: ((i ^ me[0]) // 2, 0, 0)
    return pl.pallas_call(
        functools.partial(project_back_kernel, piece),
        out_shape=(
            sds((half, rows, d), F32),
            sds((half, rows, d), BF16),
            sds(w.shape, BF16),
        ),
        grid_spec=pltpu.PrefetchScalarGridSpec(
            num_scalar_prefetch=1,
            grid=(blocks,),
            in_specs=[
                pl.BlockSpec((1, rows, d), rel),
                pl.BlockSpec((1, rows, d), rel),
                pl.BlockSpec((3, rows, width), lambda i, me: (0, i, 0)),
                pl.BlockSpec(w.shape, lambda i, me: (0, 0)),
                pl.BlockSpec(order.shape, lambda i, me: (0, 0, 0)),
            ],
            out_specs=(
                pl.BlockSpec((1, rows, d), rel),
                pl.BlockSpec((1, rows, d), rel),
                pl.BlockSpec(w.shape, lambda i, me: (0, 0)),
            ),
            scratch_shapes=[
                pltpu.VMEM((3, d, width), BF16),
                pltpu.VMEM((3, d, width), F32),
                pltpu.VMEM((8, d), F32),
                pltpu.VMEM((8, d), F32),
                pltpu.VMEM((8, width), F32),
            ],
        ),
        compiler_params=params(),
        cost_estimate=cost(4 * blocks * rows * d * 3 * width, 1.5e7),
        name="project_back",
    )(me, own, far, grad, w, order)


def pair_kernel(keep_ref, came_ref, own_ref, *send_refs):
    n = pl.program_id(0)
    total = keep_ref[0] + came_ref[0].astype(F32)

    @pl.when(n == 0)
    def _():
        own_ref[...] = total

    for m, ref in enumerate(send_refs):

        @pl.when(n == m + 1)
        def _(ref=ref):
            ref[...] = total.astype(BF16)


def pair_sum(keep, came):
    half, rows, d = keep.shape
    piece = pl.BlockSpec((1, rows, d), lambda n: (n, 0, 0))
    flat = pl.BlockSpec((rows, d), lambda n: (0, 0))
    return pl.pallas_call(
        pair_kernel,
        out_shape=(jax.ShapeDtypeStruct((rows, d), F32),)
        + (jax.ShapeDtypeStruct((rows, d), BF16),) * (half - 1),
        grid=(half,),
        in_specs=[piece, piece],
        out_specs=(flat,) * half,
        compiler_params=params(SMALL_LIMIT),
        cost_estimate=cost(0, 7e6),
        name="pair_sum",
    )(keep, came)


def finish_rows_kernel(side_ref, tok_ref, near_ref, near2_ref, away_ref, away2_ref, gh_ref, w_ref, out_ref, gain_ref):
    m = pl.program_id(0)

    @pl.when(m == 0)
    def _():
        gain_ref[...] = jnp.transpose(w_ref[:, 512:640].astype(F32))[64:72]

    n, scale = norm_parts(tok_ref[0].astype(F32))
    near = near_ref[...] + near2_ref[...].astype(F32)
    away = away_ref[...].astype(F32) + away2_ref[...].astype(F32)
    incoming = jnp.where(m == side_ref[0], near, away)
    out_ref[0] = gh_ref[0] + norm_back(incoming, gain_ref[0:1], n, scale)


def finish_rows(side, tok, near, near2, away, away2, gh, w):
    micro, rows, d = tok.shape
    piece = pl.BlockSpec((1, rows, d), lambda m, ix: (m, 0, 0))
    flat = pl.BlockSpec((rows, d), lambda m, ix: (0, 0))
    return pl.pallas_call(
        finish_rows_kernel,
        out_shape=jax.ShapeDtypeStruct((micro, rows, d), F32),
        grid_spec=pltpu.PrefetchScalarGridSpec(
            num_scalar_prefetch=1,
            grid=(micro,),
            in_specs=[piece, flat, flat, flat, flat, piece, pl.BlockSpec(w.shape, lambda m, ix: (0, 0))],
            out_specs=piece,
            scratch_shapes=[pltpu.VMEM((8, d), F32)],
        ),
        compiler_params=params(SMALL_LIMIT),
        cost_estimate=cost(0, 6e6),
        name="finish_rows",
    )(side, tok, near, near2, away, away2, gh, w)


def one_hot_order(sources, size):
    row = lax.broadcasted_iota(jnp.int32, (size, sources.shape[1]), 0)
    return jnp.where(row == sources, 1.0, 0.0).astype(BF16)


barrier = lax.optimization_barrier


def plus(a, b):
    return (a.astype(F32) + b.astype(F32)).astype(BF16)


def local(
    tokens,
    cotangent,
    ln1_gain,
    ln1_bias,
    qkv_weight,
    qkv_bias,
    out_weight,
    out_bias,
    ln2_gain,
    ln2_bias,
    fc_weight,
    fc_bias,
    proj_weight,
    proj_bias,
):
    sides = lax.axis_size("ctx")
    parts = lax.axis_size("tp")
    shards = lax.axis_size(("dp", "ctx"))
    group = sides * parts
    micro, _, rows, d = tokens.shape
    assert micro == sides == 2 and parts == 4
    side = lax.axis_index("ctx")
    slot = lax.axis_index("tp")
    me = side * parts + slot
    me_array = jnp.stack([me, side]).astype(jnp.int32)
    side_array = jnp.full((1,), side, jnp.int32)
    tall = qkv_weight.shape[1]
    heads, piece = qkv_bias.shape[1], qkv_bias.shape[2]
    width = heads * HD
    lines, strip = fc_bias.shape

    deep = lax.axis_index("dp")
    depth = lax.axis_size("dp")

    def swap_deep(array, mask):
        return lax.ppermute(array, "dp", [(n, n ^ mask) for n in range(depth)])

    def swap(array, mask):
        return lax.ppermute(array, ("ctx", "tp"), [(n, n ^ mask) for n in range(group)])

    tok = tokens[:, 0]
    cot = cotangent[:, 0]

    vectors = [v[None] for v in (ln1_gain, ln1_bias, ln2_gain, ln2_bias, out_bias, proj_bias)]
    wide, narrow = pack(fc_weight, proj_weight.T, out_weight, qkv_weight, vectors, qkv_bias, fc_bias, shards)

    gathered = lax.all_gather(wide, ("tp", "dp", "ctx"), axis=0, tiled=True)
    gathered = gathered.reshape(parts, d, wide.shape[1])

    mine = lax.dynamic_index_in_dim(tok, side, 0, keepdims=False)
    other = lax.dynamic_index_in_dim(tok, 1 - side, 0, keepdims=False)
    blocks = []
    for mask in range(0, group, 2):
        block = other if mask >= parts else mine
        blocks.append(block if mask == 0 else swap(block, mask))
    own = jnp.stack(blocks)
    far = swap(own, 1)

    w_in = lax.all_to_all(narrow, ("dp", "ctx"), 0, 0, tiled=True).reshape(d, narrow.shape[2])

    unit = lax.broadcasted_iota(jnp.int32, (1, 3 * width), 1)
    order_in = one_hot_order(unit % HD // piece * tall + unit // HD, d)
    unit = lax.broadcasted_iota(jnp.int32, (1, d), 1)
    order_fc = one_hot_order(unit % 128 // strip * tall + unit // 128, d)

    order_back = order_in.reshape(d, 3, width).transpose(1, 0, 2)
    far, order_in, order_fc, order_back = barrier((far, order_in, order_fc, order_back))

    triple = project(me_array, own, far, w_in, order_in, piece)
    mixed, mixed_turned, level = attend(triple, rows)
    mix = lax.all_to_all(mixed, ("ctx", "tp"), 0, 0, tiled=True)

    tok_rows = tok.reshape(micro * rows, d)
    cot_rows = cot.reshape(micro * rows, d)
    y, grad_hidden, grad_mix, n2, act, gl, gb, vec, gfb = middle(
        tok_rows, cot_rows, mix, gathered, order_fc, strip
    )
    grad_mix = lax.all_to_all(grad_mix, ("ctx", "tp"), 0, 0, tiled=True)

    parcels = (n2, cot_rows, gb, mix, act, gl, vec, gfb, order_fc, strip)
    exchange = tall % 16 == 0 and depth == 4
    if exchange:
        core, row = slot % 2, slot // 2
        index = lambda lane: jnp.stack([(1 - row) * 2 + lane, row * 2 + lane, side]).astype(jnp.int32)
        came = swap(weights("send", index(1 - core), *parcels), 1)
        a_send, a_keep, b_send, b_keep = weights("keep", index(core), *parcels, came=came, shards=shards)
        a_came, b_came = swap(a_send, 2), swap(b_send, parts)
    else:
        grad_wide = weights("all", jnp.arange(parts, dtype=jnp.int32), *parcels)
        grad_wide = lax.psum_scatter(
            grad_wide.reshape(parts * d, wide.shape[1]), ("tp", "dp", "ctx"), scatter_dimension=0, tiled=True
        )

    grad_triple = attend_back(triple, grad_mix, mixed_turned, level)
    if exchange:
        a_came, b_came, grad_triple = barrier((a_came, b_came, grad_triple))
        a_send, b_send = plus(a_keep[1], a_came[1]), plus(b_keep[1], b_came[1])
        a_send, b_send, grad_triple = barrier((a_send, b_send, grad_triple))
        a_last, b_last = swap(a_send, parts), swap(b_send, 2)
    keep, send, grad_in = project_back(me_array, own, far, grad_triple, w_in, order_back, piece)
    if exchange:
        a_last, b_last, keep, send, grad_in = barrier((a_last, b_last, keep, send, grad_in))

    send_came = swap(send, 1)
    grad_in = lax.all_to_all(grad_in.reshape(narrow.shape), ("dp", "ctx"), 0, 0, tiled=True)
    if exchange:
        place = jnp.full((1,), deep, jnp.int32)
        z_kept, z_send = wide_sum(place, a_keep, a_came, a_last, b_keep, b_came, b_last)
        z_send, send_came = barrier((z_send, send_came))
        z_came = swap_deep(z_send, 1)
    near, *sends = pair_sum(keep, send_came)
    arrived = [swap(sends[n - 1], 2 * n) for n in range(1, group // 2)]

    if exchange:
        z_came, near = barrier((z_came, near))
        z_send = plus(z_kept[1:], z_came[1:])
        z_send, grad_in = barrier((z_send, grad_in))
        wide_parts = [z_kept, z_came, swap_deep(z_send, 3)]
    else:
        wide_parts = [grad_wide[None]]
    grad_qkv_weight, grad_qkv_bias, vec_in = finish_narrow(grad_in, width, qkv_bias.shape)
    vec_came = swap(vec_in, 2)
    grad_tokens = finish_rows(
        side_array, tok, near, *arrived, grad_hidden.reshape(micro, rows, d), w_in
    )
    vec_came, grad_tokens = barrier((vec_came, grad_tokens))
    vec_in = vec_in + vec_came
    vec_came = swap(vec_in, 1)
    fc_grad, proj_grad, out_grad, gain2, shift2, out_b, proj_b, fc_b = finish_wide(
        wide_parts, d, width, fc_bias.shape
    )
    vec_came, fc_grad = barrier((vec_came, fc_grad))
    vec_in = vec_in + vec_came
    return (
        y.reshape(micro, 1, rows, d),
        grad_tokens[:, None],
        vec_in[0],
        vec_in[1],
        grad_qkv_weight,
        grad_qkv_bias,
        out_grad,
        out_b[0],
        gain2[0],
        shift2[0],
        fc_grad,
        fc_b,
        proj_grad.T,
        proj_b[0],
    )


def solution(mesh):
    rows = P(None, "dp", ("ctx", "tp"), None)
    vector = P(("dp", "ctx"))
    joint = P(None, ("dp", "ctx"), "tp")
    joint_bias = P(None, "tp", ("dp", "ctx"))
    down = P("tp", ("dp", "ctx"))
    up = P(("dp", "ctx"), "tp")
    inner = (vector, vector, joint, joint_bias, down, vector, vector, vector, up, down, down, vector)
    return jax.shard_map(
        local,
        mesh=mesh,
        in_specs=(rows, rows) + inner,
        out_specs=(rows, rows) + inner,
        check_vma=False,
    )
```

```python
import functools

import jax
import jax.numpy as jnp
from jax import lax
from jax.experimental import pallas as pl
from jax.experimental.pallas import tpu as pltpu
from jax.sharding import PartitionSpec as P

HD = 64
EPS = 1e-05
LOG2E = 1.4426950408889634
F32 = jnp.float32
BF16 = jnp.bfloat16
VMEM_LIMIT = 60 * 1024 * 1024
SMALL_LIMIT = 60 * 1024 * 1024
EXT = 64


def dot(a, b):
    return lax.dot_general(a, b, (((1,), (0,)), ((), ())), preferred_element_type=F32)


def dot_nt(a, b):
    return lax.dot_general(a, b, (((1,), (1,)), ((), ())), preferred_element_type=F32)


def norm_parts(rows):
    mean = jnp.mean(rows, axis=-1, keepdims=True)
    centered = rows - mean
    spread = jnp.mean(centered * centered, axis=-1, keepdims=True)
    scale = lax.rsqrt(spread + EPS)
    return (centered * scale, scale)


def norm_back(incoming, gain, n, scale):
    e = incoming * gain
    return (e - jnp.mean(e, axis=-1, keepdims=True) - n * jnp.mean(e * n, axis=-1, keepdims=True)) * scale


def params(limit=VMEM_LIMIT):
    return pltpu.CompilerParams(dimension_semantics=("arbitrary",), vmem_limit_bytes=limit)


def cost(flops, moved, exps=0):
    return pl.CostEstimate(flops=int(flops), bytes_accessed=int(moved), transcendentals=int(exps))


def pack_kernel(fc_ref, pj_ref, out_ref, qkv_ref, qb_ref, fb_ref, *rest):
    vec_refs, wide_ref, narrow_ref = rest[:-2], rest[-2], rest[-1]
    tall, d = fc_ref.shape
    width = out_ref.shape[0]
    copies = narrow_ref.shape[0]
    vectors = jnp.concatenate([ref[...].astype(F32) for ref in vec_refs] + [jnp.zeros((2, tall), F32)], axis=0)
    columns = jnp.transpose(vectors).astype(BF16)
    wide_ref[:, :d] = fc_ref[...]
    wide_ref[:, d : 2 * d] = pj_ref[...]
    wide_ref[:, 2 * d : 2 * d + width] = jnp.transpose(out_ref[...].astype(F32)).astype(BF16)
    edge = 2 * d + width
    wide_ref[:, edge:] = jnp.zeros((tall, EXT), BF16)
    wide_ref[:, edge : edge + 4] = columns[:, 2:6]
    rows, strip = fb_ref.shape
    wide_ref[:rows, edge + 8 : edge + 8 + strip] = fb_ref[...]
    for s in range(3):
        narrow_ref[0, :, s * width : (s + 1) * width] = qkv_ref[s]
    edge = 3 * width
    narrow_ref[0, :, edge:] = jnp.zeros((tall, EXT), BF16)
    narrow_ref[0, :, edge : edge + 2] = columns[:, :2]
    heads, piece = qb_ref.shape[1:]
    for s in range(3):
        narrow_ref[0, s * heads : (s + 1) * heads, edge + 8 : edge + 8 + piece] = qb_ref[s]
    whole = narrow_ref[0]
    for n in range(1, copies):
        narrow_ref[n] = whole


def pack(fc, pj, out, qkv, vec, qb, fb, copies):
    tall, d = fc.shape
    width = out.shape[0]
    return pl.pallas_call(
        pack_kernel,
        out_shape=(
            jax.ShapeDtypeStruct((tall, 2 * d + width + EXT), BF16),
            jax.ShapeDtypeStruct((copies, tall, 3 * width + EXT), BF16),
        ),
        compiler_params=pltpu.CompilerParams(vmem_limit_bytes=SMALL_LIMIT),
        cost_estimate=cost(0, 2e6),
        name="pack",
    )(fc, pj, out, qkv, qb, fb, *vec)


def pick_rows(table, period):
    line = lax.broadcasted_iota(jnp.int32, table.shape, 0)
    lane = lax.broadcasted_iota(jnp.int32, table.shape, 1)
    return jnp.sum(jnp.where(line == (lane & (period - 1)), table, 0.0), axis=0, keepdims=True)


def spread_rows(row, lines, period):
    shape = (lines, row.shape[1])
    line = lax.broadcasted_iota(jnp.int32, shape, 0)
    lane = lax.broadcasted_iota(jnp.int32, shape, 1)
    return jnp.where(line == (lane & (period - 1)), jnp.broadcast_to(row, shape), 0.0).astype(BF16)


def project_kernel(piece, me_ref, own_ref, far_ref, w_ref, order_ref, out_ref, vec_ref, bias_ref):
    i = pl.program_id(0)
    width = out_ref.shape[2]

    @pl.when(i == 0)
    def _():
        turned = jnp.transpose(w_ref[:, 512:640].astype(F32))
        vec_ref[...] = turned[64:72]
        table = dot(turned[72:80].astype(BF16), order_ref[...])
        bias_ref[...] = jnp.broadcast_to(pick_rows(table, piece), bias_ref.shape)

    far = ((i ^ me_ref[0]) & 1) == 1
    rows = jnp.where(far, far_ref[0], own_ref[0]).astype(F32)
    n, _ = norm_parts(rows)
    normed = (n * vec_ref[0:1] + vec_ref[1:2]).astype(BF16)
    full = dot(normed, w_ref[...])[:, : 3 * width] + bias_ref[0:1, :]
    full = full.astype(BF16)
    out_ref[0] = full[:, :width] * jnp.asarray(HD ** (-0.5), BF16)
    out_ref[1] = full[:, width : 2 * width]
    out_ref[2] = full[:, 2 * width :]


def project(me, own, far, w, order, piece):
    half, rows, d = own.shape
    blocks = 2 * half
    width = order.shape[1] // 3
    return pl.pallas_call(
        functools.partial(project_kernel, piece),
        out_shape=jax.ShapeDtypeStruct((3, blocks * rows, width), BF16),
        grid_spec=pltpu.PrefetchScalarGridSpec(
            num_scalar_prefetch=1,
            grid=(blocks,),
            in_specs=[
                pl.BlockSpec((1, rows, d), lambda i, me: ((i ^ me[0]) // 2, 0, 0)),
                pl.BlockSpec((1, rows, d), lambda i, me: ((i ^ me[0]) // 2, 0, 0)),
                pl.BlockSpec(w.shape, lambda i, me: (0, 0)),
                pl.BlockSpec(order.shape, lambda i, me: (0, 0)),
            ],
            out_specs=pl.BlockSpec((3, rows, width), lambda i, me: (0, i, 0)),
            scratch_shapes=[pltpu.VMEM((8, d), F32), pltpu.VMEM((8, 3 * width), F32)],
        ),
        compiler_params=params(),
        cost_estimate=cost(2 * blocks * rows * d * 3 * width, 8e6),
        name="project",
    )(me, own, far, w, order)


def head_mask(shape, h):
    lane = lax.broadcasted_iota(jnp.int32, shape, 1)
    return (lane >= h * HD) & (lane < (h + 1) * HD)


def attend_kernel(q_ref, k_ref, v_ref, o_ref, ot_ref, level_ref, vt_ref, qm_ref, m_ref, l_ref):
    i = pl.program_id(0)
    heads = q_ref.shape[2] // HD
    bq = q_ref.shape[1]
    half = bq // 2

    @pl.when(i == 0)
    def _():
        vt_ref[...] = jnp.transpose(v_ref[0].astype(F32)).astype(BF16)

    for h in range(heads):
        q = q_ref[0]
        qm_ref[h] = jnp.where(head_mask(q.shape, h), q, jnp.zeros_like(q))
    m_ref[...] = jnp.zeros_like(m_ref)
    l_ref[...] = jnp.zeros_like(l_ref)
    ot_ref[...] = jnp.zeros_like(ot_ref)

    def chunk(start, size, first, masked):
        cols = slice(first, bq)
        keys = k_ref[0, pl.ds(start, size), :]
        for h in range(heads):
            u = dot_nt(keys, qm_ref[h, first:bq, :]) * LOG2E
            if masked:
                key_pos = lax.broadcasted_iota(jnp.int32, u.shape, 0)
                row_pos = lax.broadcasted_iota(jnp.int32, u.shape, 1)
                allowed = key_pos <= row_pos
                u = jnp.where(allowed, u, 0.0)
            before = m_ref[h : h + 1, cols]
            peak = jnp.maximum(before, jnp.max(jnp.abs(u), axis=0, keepdims=True))
            fade = jnp.exp2(before - peak)
            upper = jnp.exp2(u - peak)
            lower = jnp.exp2(-peak - u)
            both = upper + lower
            if masked:
                both = jnp.where(allowed, both, 0.0)
            m_ref[h : h + 1, cols] = peak
            l_ref[h : h + 1, cols] = l_ref[h : h + 1, cols] * fade + jnp.sum(both, axis=0, keepdims=True)
            part = dot(vt_ref[h * HD : (h + 1) * HD, pl.ds(start, size)], (upper - lower).astype(BF16))
            ot_ref[h * HD : (h + 1) * HD, cols] = ot_ref[h * HD : (h + 1) * HD, cols] * fade + part

    def body(j, carry):
        chunk(pl.multiple_of(j * bq, bq), bq, 0, False)
        return carry

    lax.fori_loop(0, i, body, 0)
    base = pl.multiple_of(i * bq, bq)
    chunk(base, half, 0, True)
    chunk(pl.multiple_of(base + half, half), half, half, True)
    for h in range(heads):
        total = l_ref[h : h + 1, :]
        level_ref[h : h + 1, :] = m_ref[h : h + 1, :] + jnp.log2(total)
        ot_ref[h * HD : (h + 1) * HD, :] = ot_ref[h * HD : (h + 1) * HD, :] * (1.0 / total)
    rows = o_ref.shape[2]
    for n in range(bq // rows):
        o_ref[n] = ot_ref[:, n * rows : (n + 1) * rows].astype(BF16)


def attend(triple, rows):
    _, span, width = triple.shape
    bq = min(512, span)
    heads = width // HD
    return pl.pallas_call(
        attend_kernel,
        out_shape=(
            jax.ShapeDtypeStruct((span // rows, width, rows), BF16),
            jax.ShapeDtypeStruct((width, span), F32),
            jax.ShapeDtypeStruct((8, span), F32),
        ),
        grid=(span // bq,),
        in_specs=[
            pl.BlockSpec((1, bq, width), lambda i: (0, i, 0)),
            pl.BlockSpec((1, span, width), lambda i: (1, 0, 0)),
            pl.BlockSpec((1, span, width), lambda i: (2, 0, 0)),
        ],
        out_specs=(
            pl.BlockSpec((bq // rows, width, rows), lambda i: (i, 0, 0)),
            pl.BlockSpec((width, bq), lambda i: (0, i)),
            pl.BlockSpec((8, bq), lambda i: (0, i)),
        ),
        scratch_shapes=[
            pltpu.VMEM((width, span), BF16),
            pltpu.VMEM((heads, bq, width), BF16),
            pltpu.VMEM((8, bq), F32),
            pltpu.VMEM((8, bq), F32),
        ],
        compiler_params=params(),
        cost_estimate=cost(4 * span * span * width, 8e6, span * span * heads),
        name="attend",
    )(triple, triple, triple)


def attend_back_kernel(
    qkv_ref, grad_ref, ot_ref, level_ref, out_ref, qm_ref, gm_ref, kt_ref, dqt_ref, dot_ref, dk_ref, dv_ref
):
    j = pl.program_id(0)
    blocks = pl.num_programs(0)
    span, width = qkv_ref.shape[1:]
    rows = grad_ref.shape[2]
    heads = width // HD
    count = qm_ref.shape[0]
    b = span // count
    half = b // 2

    @pl.when(j == 0)
    def _():
        for n in range(span // rows):
            cols = slice(n * rows, (n + 1) * rows)
            turned = grad_ref[n].astype(F32)
            prod = turned * ot_ref[:, cols]
            for h in range(heads):
                dot_ref[h : h + 1, cols] = jnp.sum(prod[h * HD : (h + 1) * HD], axis=0, keepdims=True)
            g = jnp.transpose(turned).astype(BF16)
            at = n * rows % b
            for h in range(heads):
                mask = head_mask(g.shape, h)
                gm_ref[n * rows // b, h * b + at : h * b + at + rows, :] = jnp.where(mask, g, jnp.zeros_like(g))
        kt_ref[...] = jnp.transpose(qkv_ref[1].astype(F32)).astype(BF16)
        dqt_ref[...] = jnp.zeros_like(dqt_ref)
        for n in range(count):
            q = qkv_ref[0, n * b : (n + 1) * b, :]
            for h in range(heads):
                mask = head_mask(q.shape, h)
                qm_ref[n, h * b : (h + 1) * b, :] = jnp.where(mask, q, jnp.zeros_like(q))

    dk_ref[...] = jnp.zeros_like(dk_ref)
    dv_ref[...] = jnp.zeros_like(dv_ref)

    def chunk(i, key_first, key_size, first, masked):
        start = pl.multiple_of(j * b + key_first, half)
        keys = qkv_ref[1, pl.ds(start, key_size), :]
        vals = qkv_ref[2, pl.ds(start, key_size), :]
        cols = b - first
        at = pl.multiple_of(i * b + first, half)
        for h in range(heads):
            lo = h * b + first
            qm = qm_ref[i, lo : lo + cols, :]
            gm = gm_ref[i, lo : lo + cols, :]
            level = level_ref[h : h + 1, pl.ds(at, cols)]
            inner = dot_ref[h : h + 1, pl.ds(at, cols)]
            u = dot_nt(keys, qm) * LOG2E
            upper = jnp.exp2(u - level)
            lower = jnp.exp2(-level - u)
            gw = dot_nt(vals, gm)
            weights = upper - lower
            gs = upper * (gw - inner) + lower * (gw + inner)
            if masked:
                key_pos = lax.broadcasted_iota(jnp.int32, u.shape, 0)
                row_pos = lax.broadcasted_iota(jnp.int32, u.shape, 1)
                allowed = key_pos <= row_pos
                weights = jnp.where(allowed, weights, 0.0)
                gs = jnp.where(allowed, gs, 0.0)
            weights = weights.astype(BF16)
            gs = gs.astype(BF16)
            rows = slice(key_first, key_first + key_size)
            dv_ref[rows, :] += dot(weights, gm)
            dk_ref[rows, :] += dot(gs, qm)
            dqt_ref[h * HD : (h + 1) * HD, pl.ds(at, cols)] += dot(
                kt_ref[h * HD : (h + 1) * HD, pl.ds(start, key_size)], gs
            )

    def body(i, carry):
        chunk(i, 0, b, 0, False)
        return carry

    chunk(j, 0, half, 0, True)
    chunk(j, half, half, half, True)
    lax.fori_loop(j + 1, blocks, body, 0)
    here = pl.ds(pl.multiple_of(j * b, b), b)
    out_ref[1, here, :] = dk_ref[...].astype(BF16)
    out_ref[2, here, :] = dv_ref[...].astype(BF16)

    @pl.when(j == blocks - 1)
    def _():
        out_ref[0] = jnp.transpose(dqt_ref[...] * (HD ** (-0.5))).astype(BF16)


def attend_back(triple, grad, ot, level):
    _, span, width = triple.shape
    b = min(512, span)
    count = span // b
    heads = width // HD
    whole = lambda *shape: pl.BlockSpec(shape, lambda j: (0,) * len(shape))
    return pl.pallas_call(
        attend_back_kernel,
        out_shape=jax.ShapeDtypeStruct(triple.shape, BF16),
        grid=(count,),
        in_specs=[
            whole(*triple.shape),
            whole(*grad.shape),
            whole(*ot.shape),
            whole(*level.shape),
        ],
        out_specs=whole(*triple.shape),
        scratch_shapes=[
            pltpu.VMEM((count, heads * b, width), BF16),
            pltpu.VMEM((count, heads * b, width), BF16),
            pltpu.VMEM((width, span), BF16),
            pltpu.VMEM((width, span), F32),
            pltpu.VMEM((8, span), F32),
            pltpu.VMEM((b, width), F32),
            pltpu.VMEM((b, width), F32),
        ],
        compiler_params=params(),
        cost_estimate=cost(10 * span * span * width, 1e7, span * span * heads),
        name="attend_back",
    )(triple, grad, ot, level)


def gelu_parts(u):
    c = 0.7978845608028654
    square = u * u
    th = jnp.tanh(c * u * (1.0 + 0.044715 * square))
    near = 0.5 * (1.0 + th)
    slope = near + (0.5 * c) * u * (1.0 - th * th) * (1.0 + (3.0 * 0.044715) * square)
    return (u * near, slope)


def middle_kernel(
    strip,
    tok_ref,
    cot_ref,
    mix_ref,
    g_ref,
    gout_ref,
    order_ref,
    y_ref,
    gh_ref,
    dmix_ref,
    n2_ref,
    act_ref,
    gl_ref,
    gb_ref,
    vec_ref,
    gfb_ref,
    hid_ref,
    acc_ref,
    back_ref,
    ext_ref,
):
    t = pl.program_id(0)
    steps = pl.num_programs(0)
    half = mix_ref.shape[2]
    parts = gout_ref.shape[0]
    d = tok_ref.shape[1]
    width = mix_ref.shape[1]

    @pl.when(t == 0)
    def _():
        ext_ref[...] = jnp.transpose(gout_ref[0, :, 128:256].astype(F32))[64:72]
        total = tok_ref[...].astype(F32) + ext_ref[2:3]
        for s in range(parts):
            lhs = jnp.concatenate([mix_ref[s], mix_ref[parts + s]], axis=1)
            lhs = jnp.transpose(lhs.astype(F32)).astype(BF16)
            total = total + dot_nt(lhs, gout_ref[s, :, :width])
        hid_ref[...] = total
        n, _ = norm_parts(total)
        n2_ref[...] = (n * ext_ref[0:1] + ext_ref[1:2]).astype(BF16)
        acc_ref[...] = total + ext_ref[3:4]
        back_ref[...] = jnp.zeros_like(back_ref)

    ext = jnp.transpose(g_ref[0, :, 2 * d + 128 : 2 * d + 256].astype(F32))[72:88].astype(BF16)
    bias = pick_rows(dot(ext, order_ref[...]), strip)
    fc = g_ref[0, :, :d]
    pj = g_ref[0, :, d : 2 * d]
    lifted = dot(n2_ref[...], fc) + bias
    act, slope = gelu_parts(lifted)
    act = act.astype(BF16)
    act_ref[0] = act
    gl32 = dot(cot_ref[...], pj) * slope
    gl = gl32.astype(BF16)
    gl_ref[0] = gl
    gfb_ref[0, 0:1, :] = jnp.sum(gl.astype(F32), axis=0, keepdims=True)
    acc_ref[...] += dot_nt(act, pj)
    back_ref[...] += dot_nt(gl, fc)

    @pl.when(t == steps - 1)
    def _():
        y_ref[...] = acc_ref[...].astype(BF16)
        n, scale = norm_parts(hid_ref[...])
        back = back_ref[...]
        cot = cot_ref[...].astype(F32)
        gh = cot + norm_back(back, ext_ref[0:1], n, scale)
        gh_ref[...] = gh
        gb = gh.astype(BF16)
        gb_ref[...] = gb
        vec_ref[0:1, :] = jnp.sum(back * n, axis=0, keepdims=True)
        vec_ref[1:2, :] = jnp.sum(back, axis=0, keepdims=True)
        vec_ref[2:3, :] = jnp.sum(gb.astype(F32), axis=0, keepdims=True)
        vec_ref[3:4, :] = jnp.sum(cot, axis=0, keepdims=True)
        vec_ref[4:8, :] = jnp.zeros((4, d), F32)
        for s in range(parts):
            dm = jnp.transpose(dot(gb, gout_ref[s, :, :width])).astype(BF16)
            dmix_ref[s] = dm[:, :half]
            dmix_ref[parts + s] = dm[:, half:]


def middle(tok, cot, mix, gathered, order, strip):
    rows, d = tok.shape
    parts = gathered.shape[0]
    cols = gathered.shape[2]
    whole = lambda *shape: pl.BlockSpec(shape, lambda t: (0,) * len(shape))
    piece = lambda *shape: pl.BlockSpec(shape, lambda t: (t,) + (0,) * (len(shape) - 1))
    sds = jax.ShapeDtypeStruct
    return pl.pallas_call(
        functools.partial(middle_kernel, strip),
        out_shape=(
            sds((rows, d), BF16),
            sds((rows, d), F32),
            sds(mix.shape, BF16),
            sds((rows, d), BF16),
            sds((parts, rows, d), BF16),
            sds((parts, rows, d), BF16),
            sds((rows, d), BF16),
            sds((8, d), F32),
            sds((parts, 8, d), F32),
        ),
        grid=(parts,),
        in_specs=[
            whole(rows, d),
            whole(rows, d),
            whole(*mix.shape),
            piece(1, d, cols),
            pl.BlockSpec((parts, d, 256), lambda t: (0, 0, cols // 256 - 1)),
            whole(*order.shape),
        ],
        out_specs=(
            whole(rows, d),
            whole(rows, d),
            whole(*mix.shape),
            whole(rows, d),
            piece(1, rows, d),
            piece(1, rows, d),
            whole(rows, d),
            whole(8, d),
            piece(1, 8, d),
        ),
        scratch_shapes=[
            pltpu.VMEM((rows, d), F32),
            pltpu.VMEM((rows, d), F32),
            pltpu.VMEM((rows, d), F32),
            pltpu.VMEM((8, d), F32),
        ],
        compiler_params=params(),
        cost_estimate=cost(2 * rows * d * d * 18, 3e7),
        name="middle",
    )(tok, cot, mix, gathered, gathered, order)


def weights_kernel(
    mode, strip, index_ref, n2_ref, cot_ref, gb_ref, mix_ref, act_ref, gl_ref, vec_ref, gfb_ref, order_ref, *rest
):
    s = pl.program_id(0)
    d = n2_ref.shape[1]
    width = mix_ref.shape[2]
    cols = 2 * d + width + EXT
    nt_ref, ct_ref, bt_ref = rest[-3:]

    @pl.when(s == 0)
    def _():
        nt_ref[...] = jnp.transpose(n2_ref[...].astype(F32)).astype(BF16)
        ct_ref[...] = jnp.transpose(cot_ref[...].astype(F32)).astype(BF16)
        bt_ref[...] = jnp.transpose(gb_ref[...].astype(F32)).astype(BF16)

    mix = jnp.concatenate([mix_ref[0, 0], mix_ref[1, 0]], axis=1)
    turned = dot_nt(spread_rows(gfb_ref[0, 0:1], 16, strip), order_ref[...])
    tall = jnp.concatenate([vec_ref[...], turned, jnp.zeros((EXT - 24, d), F32)], axis=0)
    if mode != "keep":
        out_ref = rest[0]
        out_ref[0, :, :d] = dot(nt_ref[...], gl_ref[0]).astype(BF16)
        out_ref[0, :, d : 2 * d] = dot(ct_ref[...], act_ref[0]).astype(BF16)
        out_ref[0, :, 2 * d : 2 * d + width] = dot_nt(bt_ref[...], mix).astype(BF16)
        out_ref[0, :, 2 * d + width :] = jnp.transpose(tall).astype(BF16)
        return
    came_ref, as_ref, ak_ref, bs_ref, bk_ref, sum_ref = rest[:6]
    sum_ref[:, 2 * d : 2 * d + width] = dot_nt(bt_ref[...], mix).astype(BF16)
    sum_ref[:, 2 * d + width :] = jnp.transpose(tall).astype(BF16)
    sum_ref[:, 2 * d :] = (sum_ref[:, 2 * d :].astype(F32) + came_ref[0, :, 2 * d :].astype(F32)).astype(BF16)
    sum_ref[:, :d] = (dot(nt_ref[...], gl_ref[0]) + came_ref[0, :, :d].astype(F32)).astype(BF16)
    sum_ref[:, d : 2 * d] = (dot(ct_ref[...], act_ref[0]) + came_ref[0, :, d : 2 * d].astype(F32)).astype(BF16)
    depth, step = as_ref.shape[1], as_ref.shape[2]
    cut = cols // 2

    def block(xr, zr):
        at = (zr * 2 + (xr ^ index_ref[2])) * step
        return pl.ds(pl.multiple_of(at, 16), step)

    for zr in range(depth):
        bk_ref[0, zr] = sum_ref[block(0, zr), cut:]
        bs_ref[0, zr] = sum_ref[block(1, zr), cut:]

    @pl.when(s == 0)
    def _():
        for xr in range(2):
            for zr in range(depth):
                as_ref[xr, zr] = sum_ref[block(xr, zr), :cut]

    @pl.when(s == 1)
    def _():
        for xr in range(2):
            for zr in range(depth):
                ak_ref[xr, zr] = sum_ref[block(xr, zr), :cut]


def weights(mode, index, n2, cot, gb, mix, act, gl, vec, gfb, order, strip, came=None, shards=None):
    rows, d = n2.shape
    parts = act.shape[0]
    width = mix.shape[1]
    cols = 2 * d + width + EXT
    steps = parts if mode == "all" else 2
    whole = lambda *shape: pl.BlockSpec(shape, lambda s, ix: (0,) * len(shape))
    piece = lambda *shape: pl.BlockSpec(shape, lambda s, ix: (ix[s],) + (0,) * (len(shape) - 1))
    mix = mix.reshape(mix.shape[0] // parts, parts, width, mix.shape[2])
    operands = [index, n2, cot, gb, mix, act, gl, vec, gfb, order]
    specs = [
        whole(rows, d),
        whole(rows, d),
        whole(rows, d),
        pl.BlockSpec((mix.shape[0], 1, width, mix.shape[3]), lambda s, ix: (0, ix[s], 0, 0)),
        piece(1, rows, d),
        piece(1, rows, d),
        whole(8, d),
        piece(1, 8, d),
        whole(*order.shape),
    ]
    scratch = [pltpu.VMEM((d, rows), BF16) for _ in range(3)]
    if mode == "keep":
        operands.append(came)
        specs.append(pl.BlockSpec((1, d, cols), lambda s, ix: (s, 0, 0)))
        block = (2, shards // 2, d // shards, cols // 2)
        sds = jax.ShapeDtypeStruct(block, BF16)
        out_shape = (sds,) * 4
        turn = pl.BlockSpec((1,) + block[1:], lambda s, ix: (1 - s, 0, 0, 0))
        out_specs = (whole(*block), whole(*block), turn, turn)
        scratch = [pltpu.VMEM((d, cols), BF16)] + scratch
    else:
        out_shape = jax.ShapeDtypeStruct((steps, d, cols), BF16)
        out_specs = pl.BlockSpec((1, d, cols), lambda s, ix: (s, 0, 0))
    return pl.pallas_call(
        functools.partial(weights_kernel, mode, strip),
        out_shape=out_shape,
        grid_spec=pltpu.PrefetchScalarGridSpec(
            num_scalar_prefetch=1,
            grid=(steps,),
            in_specs=specs,
            out_specs=out_specs,
            scratch_shapes=scratch,
        ),
        compiler_params=params(),
        cost_estimate=cost(2 * rows * d * cols * steps, 6e6 * steps),
        name="weights_" + mode,
    )(*operands)


def wide_sum_kernel(place_ref, *refs):
    keep_ref, send_ref = refs[6:]
    cut = keep_ref.shape[2] // 2
    for i in range(2):
        mine_ref, first_ref, second_ref = refs[3 * i : 3 * i + 3]
        for ref, members in ((send_ref, (1, 2)), (keep_ref, (0, 3))):
            for n, m in enumerate(members):
                z = pl.ds(place_ref[0] ^ m, 1)
                total = mine_ref[0, z].astype(F32) + first_ref[0, z].astype(F32)
                ref[n : n + 1, :, i * cut : (i + 1) * cut] = (total + second_ref[z].astype(F32)).astype(BF16)


def wide_sum(place, *parts):
    depth, step, cut = parts[2].shape
    first = pl.BlockSpec((1, depth, step, cut), lambda i, ix: (0, 0, 0, 0))
    last = pl.BlockSpec((depth, step, cut), lambda i, ix: (0, 0, 0))
    out = jax.ShapeDtypeStruct((depth // 2, step, 2 * cut), BF16)
    return pl.pallas_call(
        wide_sum_kernel,
        out_shape=(out, out),
        grid_spec=pltpu.PrefetchScalarGridSpec(
            num_scalar_prefetch=1,
            grid=(1,),
            in_specs=[first, first, last] * 2,
            out_specs=(pl.BlockSpec(out.shape, lambda i, ix: (0, 0, 0)),) * 2,
        ),
        compiler_params=params(),
        cost_estimate=cost(0, 4e6),
        name="wide_sum",
    )(place, *parts)


def finish_wide_kernel(*refs):
    fc_ref, pj_ref, out_ref, g_ref, b_ref, ob_ref, pb_ref, fb_ref = refs[-8:]
    d = fc_ref.shape[1]
    width = out_ref.shape[0]
    t = refs[0][0].astype(F32)
    for ref in refs[1:-8]:
        t = t + ref[0].astype(F32)
    fc_ref[...] = t[:, :d]
    pj_ref[...] = t[:, d : 2 * d]
    rest = jnp.transpose(t[:, 2 * d : 2 * d + width + EXT])
    out_ref[...] = rest[:width]
    g_ref[...] = rest[width : width + 1]
    b_ref[...] = rest[width + 1 : width + 2]
    ob_ref[...] = rest[width + 2 : width + 3]
    pb_ref[...] = rest[width + 3 : width + 4]
    rows, strip = fb_ref.shape
    at = 2 * d + width + 8
    fb_ref[...] = t[:rows, at : at + strip]


def finish_wide(parts, d, width, bias_shape):
    tall = parts[0].shape[1]
    sds = lambda *shape: jax.ShapeDtypeStruct(shape, F32)
    return pl.pallas_call(
        finish_wide_kernel,
        out_shape=(
            sds(tall, d),
            sds(tall, d),
            sds(width, tall),
            sds(1, tall),
            sds(1, tall),
            sds(1, tall),
            sds(1, tall),
            sds(*bias_shape),
        ),
        compiler_params=pltpu.CompilerParams(vmem_limit_bytes=SMALL_LIMIT),
        cost_estimate=cost(0, 2e6),
        name="finish_wide",
    )(*parts)


def finish_narrow_kernel(g_ref, qkv_ref, qb_ref, vec_ref):
    t = g_ref[0].astype(F32)
    for n in range(1, g_ref.shape[0]):
        t = t + g_ref[n].astype(F32)
    width = qkv_ref.shape[2]
    for s in range(3):
        qkv_ref[s] = t[:, s * width : (s + 1) * width]
    heads, piece = qb_ref.shape[1:]
    edge = 3 * width + 8
    for s in range(3):
        qb_ref[s] = t[s * heads : (s + 1) * heads, edge : edge + piece]
    vec_ref[...] = jnp.transpose(t[:, 512:640])[64:72]


def finish_narrow(g, width, bias_shape):
    tall = g.shape[1]
    sds = lambda *shape: jax.ShapeDtypeStruct(shape, F32)
    return pl.pallas_call(
        finish_narrow_kernel,
        out_shape=(sds(3, tall, width), sds(*bias_shape), sds(8, tall)),
        compiler_params=pltpu.CompilerParams(vmem_limit_bytes=SMALL_LIMIT),
        cost_estimate=cost(0, 2e6),
        name="finish_narrow",
    )(g)


def project_back_kernel(
    piece, me_ref, own_ref, far_ref, grad_ref, w_ref, order_ref, keep_ref, send_ref, dw_ref, w3_ref, dw3_ref, gain_ref, vec_ref, bias_ref
):
    i = pl.program_id(0)
    steps = pl.num_programs(0)
    width = grad_ref.shape[2]
    d = w_ref.shape[0]

    @pl.when(i == 0)
    def _():
        gain_ref[...] = jnp.transpose(w_ref[:, 512:640].astype(F32))[64:72]
        for s in range(3):
            w3_ref[s] = w_ref[:, s * width : (s + 1) * width]
        dw3_ref[...] = jnp.zeros_like(dw3_ref)
        vec_ref[...] = jnp.zeros_like(vec_ref)
        bias_ref[...] = jnp.zeros_like(bias_ref)

    far = ((i ^ me_ref[0]) & 1) == 1
    rows = jnp.where(far, far_ref[0], own_ref[0]).astype(F32)
    n, _ = norm_parts(rows)
    normed = n * gain_ref[0:1] + gain_ref[1:2]
    turned = jnp.transpose(normed).astype(BF16)
    part = dot_nt(grad_ref[0], w3_ref[0])
    for s in range(1, 3):
        part = part + dot_nt(grad_ref[s], w3_ref[s])
    for s in range(3):
        dw3_ref[s] += dot(turned, grad_ref[s])
        bias_ref[s : s + 1, :] += jnp.sum(grad_ref[s].astype(F32), axis=0, keepdims=True)
    vec_ref[0:1, :] += jnp.sum(part * n, axis=0, keepdims=True)
    vec_ref[1:2, :] += jnp.sum(part, axis=0, keepdims=True)

    @pl.when(far)
    def _():
        send_ref[0] = part.astype(BF16)

    @pl.when(jnp.logical_not(far))
    def _():
        keep_ref[0] = part.astype(BF16)

    @pl.when(i == steps - 1)
    def _():
        turned_bias = jnp.zeros((8, d), F32)
        for s in range(3):
            dw_ref[:, s * width : (s + 1) * width] = dw3_ref[s].astype(BF16)
            spread = spread_rows(bias_ref[s : s + 1, :], 8, piece)
            turned_bias = turned_bias + dot_nt(spread, order_ref[s])
        tall = jnp.concatenate([vec_ref[...], turned_bias, jnp.zeros((EXT - 16, d), F32)], axis=0)
        dw_ref[:, 3 * width :] = jnp.transpose(tall).astype(BF16)


def project_back(me, own, far, grad, w, order, piece):
    half, rows, d = own.shape
    width = grad.shape[2]
    blocks = 2 * half
    sds = jax.ShapeDtypeStruct
    rel = lambda i, me: ((i ^ me[0]) // 2, 0, 0)
    return pl.pallas_call(
        functools.partial(project_back_kernel, piece),
        out_shape=(
            sds((half, rows, d), BF16),
            sds((half, rows, d), BF16),
            sds(w.shape, BF16),
        ),
        grid_spec=pltpu.PrefetchScalarGridSpec(
            num_scalar_prefetch=1,
            grid=(blocks,),
            in_specs=[
                pl.BlockSpec((1, rows, d), rel),
                pl.BlockSpec((1, rows, d), rel),
                pl.BlockSpec((3, rows, width), lambda i, me: (0, i, 0)),
                pl.BlockSpec(w.shape, lambda i, me: (0, 0)),
                pl.BlockSpec(order.shape, lambda i, me: (0, 0, 0)),
            ],
            out_specs=(
                pl.BlockSpec((1, rows, d), rel),
                pl.BlockSpec((1, rows, d), rel),
                pl.BlockSpec(w.shape, lambda i, me: (0, 0)),
            ),
            scratch_shapes=[
                pltpu.VMEM((3, d, width), BF16),
                pltpu.VMEM((3, d, width), F32),
                pltpu.VMEM((8, d), F32),
                pltpu.VMEM((8, d), F32),
                pltpu.VMEM((8, width), F32),
            ],
        ),
        compiler_params=params(),
        cost_estimate=cost(4 * blocks * rows * d * 3 * width, 1.5e7),
        name="project_back",
    )(me, own, far, grad, w, order)


def pair_kernel(keep_ref, came_ref, own_ref, *send_refs):
    n = pl.program_id(0)
    total = keep_ref[0].astype(F32) + came_ref[0].astype(F32)

    @pl.when(n == 0)
    def _():
        own_ref[...] = total

    for m, ref in enumerate(send_refs):

        @pl.when(n == m + 1)
        def _(ref=ref):
            ref[...] = total.astype(BF16)


def pair_sum(keep, came):
    half, rows, d = keep.shape
    piece = pl.BlockSpec((1, rows, d), lambda n: (n, 0, 0))
    flat = pl.BlockSpec((rows, d), lambda n: (0, 0))
    return pl.pallas_call(
        pair_kernel,
        out_shape=(jax.ShapeDtypeStruct((rows, d), F32),)
        + (jax.ShapeDtypeStruct((rows, d), BF16),) * (half - 1),
        grid=(half,),
        in_specs=[piece, piece],
        out_specs=(flat,) * half,
        compiler_params=params(SMALL_LIMIT),
        cost_estimate=cost(0, 7e6),
        name="pair_sum",
    )(keep, came)


def finish_rows_kernel(side_ref, tok_ref, near_ref, near2_ref, away_ref, away2_ref, gh_ref, w_ref, out_ref, gain_ref):
    m = pl.program_id(0)

    @pl.when(m == 0)
    def _():
        gain_ref[...] = jnp.transpose(w_ref[:, 512:640].astype(F32))[64:72]

    n, scale = norm_parts(tok_ref[0].astype(F32))
    near = near_ref[...] + near2_ref[...].astype(F32)
    away = away_ref[...].astype(F32) + away2_ref[...].astype(F32)
    incoming = jnp.where(m == side_ref[0], near, away)
    out_ref[0] = gh_ref[0] + norm_back(incoming, gain_ref[0:1], n, scale)


def finish_rows(side, tok, near, near2, away, away2, gh, w):
    micro, rows, d = tok.shape
    piece = pl.BlockSpec((1, rows, d), lambda m, ix: (m, 0, 0))
    flat = pl.BlockSpec((rows, d), lambda m, ix: (0, 0))
    return pl.pallas_call(
        finish_rows_kernel,
        out_shape=jax.ShapeDtypeStruct((micro, rows, d), F32),
        grid_spec=pltpu.PrefetchScalarGridSpec(
            num_scalar_prefetch=1,
            grid=(micro,),
            in_specs=[piece, flat, flat, flat, flat, piece, pl.BlockSpec(w.shape, lambda m, ix: (0, 0))],
            out_specs=piece,
            scratch_shapes=[pltpu.VMEM((8, d), F32)],
        ),
        compiler_params=params(SMALL_LIMIT),
        cost_estimate=cost(0, 6e6),
        name="finish_rows",
    )(side, tok, near, near2, away, away2, gh, w)


def one_hot_order(sources, size):
    row = lax.broadcasted_iota(jnp.int32, (size, sources.shape[1]), 0)
    return jnp.where(row == sources, 1.0, 0.0).astype(BF16)


barrier = lax.optimization_barrier


def plus(a, b):
    return (a.astype(F32) + b.astype(F32)).astype(BF16)


def local(
    tokens,
    cotangent,
    ln1_gain,
    ln1_bias,
    qkv_weight,
    qkv_bias,
    out_weight,
    out_bias,
    ln2_gain,
    ln2_bias,
    fc_weight,
    fc_bias,
    proj_weight,
    proj_bias,
):
    sides = lax.axis_size("ctx")
    parts = lax.axis_size("tp")
    shards = lax.axis_size(("dp", "ctx"))
    group = sides * parts
    micro, _, rows, d = tokens.shape
    assert micro == sides == 2 and parts == 4
    side = lax.axis_index("ctx")
    slot = lax.axis_index("tp")
    me = side * parts + slot
    me_array = jnp.stack([me, side]).astype(jnp.int32)
    side_array = jnp.full((1,), side, jnp.int32)
    tall = qkv_weight.shape[1]
    heads, piece = qkv_bias.shape[1], qkv_bias.shape[2]
    width = heads * HD
    lines, strip = fc_bias.shape

    deep = lax.axis_index("dp")
    depth = lax.axis_size("dp")

    def swap_deep(array, mask):
        return lax.ppermute(array, "dp", [(n, n ^ mask) for n in range(depth)])

    def swap(array, mask):
        return lax.ppermute(array, ("ctx", "tp"), [(n, n ^ mask) for n in range(group)])

    tok = tokens[:, 0]
    cot = cotangent[:, 0]

    vectors = [v[None] for v in (ln1_gain, ln1_bias, ln2_gain, ln2_bias, out_bias, proj_bias)]
    wide, narrow = pack(fc_weight, proj_weight.T, out_weight, qkv_weight, vectors, qkv_bias, fc_bias, shards)

    gathered = lax.all_gather(wide, ("tp", "dp", "ctx"), axis=0, tiled=True)
    gathered = gathered.reshape(parts, d, wide.shape[1])

    mine = lax.dynamic_index_in_dim(tok, side, 0, keepdims=False)
    other = lax.dynamic_index_in_dim(tok, 1 - side, 0, keepdims=False)
    blocks = []
    for mask in range(0, group, 2):
        block = other if mask >= parts else mine
        blocks.append(block if mask == 0 else swap(block, mask))
    own = jnp.stack(blocks)
    far = swap(own, 1)

    w_in = lax.all_to_all(narrow, ("dp", "ctx"), 0, 0, tiled=True).reshape(d, narrow.shape[2])

    unit = lax.broadcasted_iota(jnp.int32, (1, 3 * width), 1)
    order_in = one_hot_order(unit % HD // piece * tall + unit // HD, d)
    unit = lax.broadcasted_iota(jnp.int32, (1, d), 1)
    order_fc = one_hot_order(unit % 128 // strip * tall + unit // 128, d)

    order_back = order_in.reshape(d, 3, width).transpose(1, 0, 2)
    far, order_in, order_fc, order_back = barrier((far, order_in, order_fc, order_back))

    triple = project(me_array, own, far, w_in, order_in, piece)
    mixed, mixed_turned, level = attend(triple, rows)
    mix = lax.all_to_all(mixed, ("ctx", "tp"), 0, 0, tiled=True)

    tok_rows = tok.reshape(micro * rows, d)
    cot_rows = cot.reshape(micro * rows, d)
    y, grad_hidden, grad_mix, n2, act, gl, gb, vec, gfb = middle(
        tok_rows, cot_rows, mix, gathered, order_fc, strip
    )
    grad_mix = lax.all_to_all(grad_mix, ("ctx", "tp"), 0, 0, tiled=True)

    parcels = (n2, cot_rows, gb, mix, act, gl, vec, gfb, order_fc, strip)
    exchange = tall % 16 == 0 and depth == 4
    if exchange:
        core, row = slot % 2, slot // 2
        index = lambda lane: jnp.stack([(1 - row) * 2 + lane, row * 2 + lane, side]).astype(jnp.int32)
        came = swap(weights("send", index(1 - core), *parcels), 1)
        a_send, a_keep, b_send, b_keep = weights("keep", index(core), *parcels, came=came, shards=shards)
        a_came, b_came = swap(a_send, 2), swap(b_send, parts)
    else:
        grad_wide = weights("all", jnp.arange(parts, dtype=jnp.int32), *parcels)
        grad_wide = lax.psum_scatter(
            grad_wide.reshape(parts * d, wide.shape[1]), ("tp", "dp", "ctx"), scatter_dimension=0, tiled=True
        )

    grad_triple = attend_back(triple, grad_mix, mixed_turned, level)
    if exchange:
        a_came, b_came, grad_triple = barrier((a_came, b_came, grad_triple))
        a_send, b_send = plus(a_keep[1], a_came[1]), plus(b_keep[1], b_came[1])
        a_send, b_send, grad_triple = barrier((a_send, b_send, grad_triple))
        a_last, b_last = swap(a_send, parts), swap(b_send, 2)
    keep, send, grad_in = project_back(me_array, own, far, grad_triple, w_in, order_back, piece)
    if exchange:
        a_last, b_last, keep, send, grad_in = barrier((a_last, b_last, keep, send, grad_in))

    send_came = swap(send, 1)
    grad_in = lax.all_to_all(grad_in.reshape(narrow.shape), ("dp", "ctx"), 0, 0, tiled=True)
    if exchange:
        place = jnp.full((1,), deep, jnp.int32)
        z_kept, z_send = wide_sum(place, a_keep, a_came, a_last, b_keep, b_came, b_last)
        z_send, send_came = barrier((z_send, send_came))
        z_came = swap_deep(z_send, 1)
    near, *sends = pair_sum(keep, send_came)
    arrived = [swap(sends[n - 1], 2 * n) for n in range(1, group // 2)]

    if exchange:
        z_came, near = barrier((z_came, near))
        z_send = plus(z_kept[1:], z_came[1:])
        z_send, grad_in = barrier((z_send, grad_in))
        wide_parts = [z_kept, z_came, swap_deep(z_send, 3)]
    else:
        wide_parts = [grad_wide[None]]
    grad_qkv_weight, grad_qkv_bias, vec_in = finish_narrow(grad_in, width, qkv_bias.shape)
    vec_came = swap(vec_in, 2)
    grad_tokens = finish_rows(
        side_array, tok, near, *arrived, grad_hidden.reshape(micro, rows, d), w_in
    )
    vec_came, grad_tokens = barrier((vec_came, grad_tokens))
    vec_in = vec_in + vec_came
    vec_came = swap(vec_in, 1)
    fc_grad, proj_grad, out_grad, gain2, shift2, out_b, proj_b, fc_b = finish_wide(
        wide_parts, d, width, fc_bias.shape
    )
    vec_came, fc_grad = barrier((vec_came, fc_grad))
    vec_in = vec_in + vec_came
    return (
        y.reshape(micro, 1, rows, d),
        grad_tokens[:, None],
        vec_in[0],
        vec_in[1],
        grad_qkv_weight,
        grad_qkv_bias,
        out_grad,
        out_b[0],
        gain2[0],
        shift2[0],
        fc_grad,
        fc_b,
        proj_grad.T,
        proj_b[0],
    )


def solution(mesh):
    rows = P(None, "dp", ("ctx", "tp"), None)
    vector = P(("dp", "ctx"))
    joint = P(None, ("dp", "ctx"), "tp")
    joint_bias = P(None, "tp", ("dp", "ctx"))
    down = P("tp", ("dp", "ctx"))
    up = P(("dp", "ctx"), "tp")
    inner = (vector, vector, joint, joint_bias, down, vector, vector, vector, up, down, down, vector)
    return jax.shard_map(
        local,
        mesh=mesh,
        in_specs=(rows, rows) + inner,
        out_specs=(rows, rows) + inner,
        check_vma=False,
    )
```
